128 devices in a mesh: data: 64 (over z, y, x), stage: 2 (over core).
Axes of the slice: x: 4, y: 4, z: 4, core: 2. Of those that a mesh axis runs over, the one named last changes fastest.
Arguments:
- act_in: bfloat16 [32, 64, 8, 512], P(None, 'data')
- cot_out: bfloat16 [32, 64, 8, 512], P(None, 'data')
- w_gate: bfloat16 [2, 2, 512, 2048], P(None, 'stage', 'data')
- w_in: bfloat16 [2, 2, 512, 2048], P(None, 'stage', 'data')
- w_out: bfloat16 [2, 2, 2048, 512], P(None, 'stage', 'data')
Outputs:
- output 1: bfloat16 [32, 64, 8, 512], P(None, 'data')
- output 2: float32 [2, 2, 512, 2048], P(None, 'stage', 'data')
- output 3: float32 [2, 2, 512, 2048], P(None, 'stage', 'data')
- output 4: float32 [2, 2, 2048, 512], P(None, 'stage', 'data')
All inputs are finite; a program needn't handle non-finite values.
Results may differ from the reference program's by a relative error of at most 0.0108.
Values are sent between devices in bfloat16 or wider.
A program may use at most 1 GiB of HBM per device.

```python
import jax
import jax.numpy as jnp
from jax import lax

DMODEL = 512
FFN_DIM = 2048
STAGES = 2
NUM_MICRO = 32
BATCH_ROWS = 64
SEQLEN = 8
NORM_EPS = 1e-6


def setup_inputs(seed: int = 0) -> dict:
    sub_keys = jax.random.split(jax.random.key(seed), 5)
    act_shape = (NUM_MICRO, BATCH_ROWS, SEQLEN, DMODEL)
    up_shape = (2, STAGES, DMODEL, FFN_DIM)
    down_shape = (2, STAGES, FFN_DIM, DMODEL)
    act_in = jax.random.normal(sub_keys[0], act_shape, jnp.float32)
    cot_out = jax.random.normal(sub_keys[1], act_shape, jnp.float32)
    w_gate = jax.random.normal(sub_keys[2], up_shape, jnp.float32) * DMODEL ** -0.5
    w_in = jax.random.normal(sub_keys[3], up_shape, jnp.float32) * DMODEL ** -0.5
    w_out = jax.random.normal(sub_keys[4], down_shape, jnp.float32) * FFN_DIM ** -0.5
    return dict(act_in=act_in.astype(jnp.bfloat16), cot_out=cot_out.astype(jnp.bfloat16), w_gate=w_gate.astype(jnp.bfloat16), w_in=w_in.astype(jnp.bfloat16), w_out=w_out.astype(jnp.bfloat16))


def layer_forward(rows_in, gate_w, lin_w, proj_w):
    rows_f32 = rows_in.astype(jnp.float32)
    inv_rms = lax.rsqrt(jnp.mean(rows_f32 * rows_f32, axis=-1, keepdims=True) + NORM_EPS)
    normed = (rows_f32 * inv_rms).astype(jnp.bfloat16)
    gate_pre = jnp.dot(normed, gate_w, preferred_element_type=jnp.float32)
    lin_pre = jnp.dot(normed, lin_w, preferred_element_type=jnp.float32)
    gate_act = gate_pre * jax.nn.sigmoid(gate_pre)
    hidden = (gate_act * lin_pre).astype(jnp.bfloat16)
    proj_out = jnp.dot(hidden, proj_w, preferred_element_type=jnp.float32)
    return (rows_f32 + proj_out).astype(jnp.bfloat16)


def layer_backward(rows_in, grad_rows, gate_w, lin_w, proj_w):
    rows_f32 = rows_in.astype(jnp.float32)
    inv_rms = lax.rsqrt(jnp.mean(rows_f32 * rows_f32, axis=-1, keepdims=True) + NORM_EPS)
    scaled = rows_f32 * inv_rms
    normed = scaled.astype(jnp.bfloat16)
    gate_pre = jnp.dot(normed, gate_w, preferred_element_type=jnp.float32)
    lin_pre = jnp.dot(normed, lin_w, preferred_element_type=jnp.float32)
    gate_sig = jax.nn.sigmoid(gate_pre)
    gate_act = gate_pre * gate_sig
    hidden = (gate_act * lin_pre).astype(jnp.bfloat16)
    grad_proj = jnp.dot(hidden.T, grad_rows, preferred_element_type=jnp.float32)
    grad_hidden = jnp.dot(grad_rows, proj_w.T, preferred_element_type=jnp.float32)
    d_gate = (grad_hidden * lin_pre * gate_sig * (1.0 + gate_pre * (1.0 - gate_sig))).astype(jnp.bfloat16)
    d_lin = (grad_hidden * gate_act).astype(jnp.bfloat16)
    grad_gate = jnp.dot(normed.T, d_gate, preferred_element_type=jnp.float32)
    grad_lin = jnp.dot(normed.T, d_lin, preferred_element_type=jnp.float32)
    grad_norm = jnp.dot(d_gate, gate_w.T, preferred_element_type=jnp.float32) + jnp.dot(d_lin, lin_w.T, preferred_element_type=jnp.float32)
    grad_in = grad_rows.astype(jnp.float32) + inv_rms * (grad_norm - scaled * jnp.mean(grad_norm * scaled, axis=-1, keepdims=True))
    return grad_in.astype(jnp.bfloat16), grad_gate, grad_lin, grad_proj


def reference(act_in, cot_out, w_gate, w_in, w_out):
    layers = 2 * STAGES
    tok_rows = BATCH_ROWS * SEQLEN
    gate_stack = w_gate.reshape(layers, DMODEL, FFN_DIM)
    lin_stack = w_in.reshape(layers, DMODEL, FFN_DIM)
    proj_stack = w_out.reshape(layers, FFN_DIM, DMODEL)
    act_micro = act_in.reshape(NUM_MICRO, tok_rows, DMODEL)
    cot_micro = cot_out.reshape(NUM_MICRO, tok_rows, DMODEL)

    def fwd_body(rows_in, weights):
        return layer_forward(rows_in, weights[0], weights[1], weights[2]), rows_in

    def bwd_body(grad_rows, packed):
        gate_w, lin_w, proj_w, rows_in = packed
        grad_in, grad_g, grad_l, grad_p = layer_backward(rows_in, grad_rows, gate_w, lin_w, proj_w)
        return grad_in, (grad_g, grad_l, grad_p)

    def micro_step(totals, pair):
        act_rows, cot_rows = pair
        last_rows, saved_in = lax.scan(fwd_body, act_rows, (gate_stack, lin_stack, proj_stack))
        grad_x, per_layer = lax.scan(bwd_body, cot_rows, (gate_stack, lin_stack, proj_stack, saved_in), reverse=True)
        new_totals = tuple(running + layer_part for running, layer_part in zip(totals, per_layer))
        return new_totals, grad_x

    zero_up = jnp.zeros((layers, DMODEL, FFN_DIM), jnp.float32)
    zero_down = jnp.zeros((layers, FFN_DIM, DMODEL), jnp.float32)
    totals, grad_act = lax.scan(micro_step, (zero_up, zero_up, zero_down), (act_micro, cot_micro))
    return (grad_act.reshape(NUM_MICRO, BATCH_ROWS, SEQLEN, DMODEL), totals[0].reshape(2, STAGES, DMODEL, FFN_DIM), totals[1].reshape(2, STAGES, DMODEL, FFN_DIM), totals[2].reshape(2, STAGES, FFN_DIM, DMODEL))
```

```python
import functools

import jax
import jax.numpy as jnp
from jax import lax
from jax.experimental import pallas as pl
from jax.experimental.pallas import tpu as pltpu
from jax.sharding import PartitionSpec as P

NORM_EPS = 1e-6
BF = jnp.bfloat16
F32 = jnp.float32
MESH = pl.DeviceIdType.MESH
X, Y, Z = 0, 1, 2
BLOCKS = COLOURS = HALVES = (0, 1)
NB, NA, NL = len(BLOCKS), 4, 64
RING = (1, 3, 2)
OPP = RING[-1]
PLUS, MINUS = RING[:-1]
QUARTERS = range(NA)
AXES = ((X, Y, Z), (Y, Z, X), (Z, X, Y))


def mm(left, right):
    return jnp.dot(left, right, preferred_element_type=F32)


def mm_nt(left, right):
    return lax.dot_general(left, right, (((1,), (1,)), ((), ())), preferred_element_type=F32)


def mm_tn(left, right):
    return lax.dot_general(left, right, (((0,), (0,)), ((), ())), preferred_element_type=F32)


def inv_rms(h):
    return lax.rsqrt(jnp.mean(h * h, axis=-1, keepdims=True) + NORM_EPS)


def kernel(act, cot, wg_in, wi_in, wo_in, gact, gg, gi, go,
           wg, wi, wo, hb, eb, xo, ga, ng, f1, f2, f1s, f2s, us, ub, da, db, das, dbs, qs, gs, is_, os_,
           gin, gout, fin, r3,
           lsem, ag_s, ag_r, lg_r, mc_s, mc_r, rl_s, ga_s, ga_r, rs_s, rs_r, r3_s, r3_r, turn, *rg):
    dm, fd = wo.shape[-1], wg.shape[-1]
    dr, fr = dm // NL, fd // NL
    fs = fd // NA
    pf = fs // NA
    rows = act.shape[0]
    wts = (wg, wi, wo)

    p = lax.axis_index("stage")
    d = lax.axis_index("data")
    zc, yc, xc = lax.div(d, 16), lax.rem(lax.div(d, 4), 4), lax.rem(d, 4)
    coord = (xc, yc, zc)
    stride = (1, 4, 16)
    ja = yc + p * (zc - yc)
    jb = zc + p * (yc - zc)
    sa, sb = 4 + 12 * p, 16 - 12 * p

    def rot(c, delta):
        return lax.rem(c + (delta % 4), 4)

    def peer(ax, delta):
        return d + (rot(coord[ax], delta) - coord[ax]) * stride[ax]

    def peer_a(delta):
        return d + (rot(ja, delta) - ja) * sa

    def peer_b(delta):
        return d + (rot(jb, delta) - jb) * sb

    def remote(src, dst, ssem, rsem, dev, core):
        return pltpu.make_async_remote_copy(src_ref=src, dst_ref=dst, send_sem=ssem, recv_sem=rsem,
                                            device_id=(dev, core), device_id_type=MESH)

    def send(src, dst, ssem, rsem, dev, core):
        remote(src, dst, ssem, rsem, dev, core).start()

    def wait_recv(ref, sem):
        remote(ref, ref, sem, sem, d, p).wait_recv()

    def wait_send(ref, sem):
        remote(ref, ref, sem, sem, d, p).wait_send()

    for v in BLOCKS:
        for k, shard in enumerate((wg_in, wi_in, wo_in)):
            pltpu.make_async_copy(shard.at[v], wts[k].at[v, zc, yc, xc], lsem.at[v, k]).start()

    @pl.when(p == 0)
    def _():
        pltpu.make_async_copy(act, hb.at[0, ja], lsem.at[0, 3]).start()

    @pl.when(p == 1)
    def _():
        pltpu.make_async_copy(cot, eb.at[1, ja], lsem.at[0, 3]).start()

    barrier = pltpu.get_barrier_semaphore()
    senders = [(peer(ax, delta), p) for ax in (X, Y, Z) for delta in RING]
    senders += [(d, 1 - p), (peer_a(1), 1 - p), (peer_a(-1), 1 - p)]
    for dev, core in senders:
        pl.semaphore_signal(barrier, inc=1, device_id=(dev, core), device_id_type=MESH)
    for v in BLOCKS:
        for k, shard in enumerate((wg_in, wi_in, wo_in)):
            pltpu.make_async_copy(shard.at[v], wts[k].at[v, zc, yc, xc], lsem.at[v, k]).wait()

    @pl.when(p == 0)
    def _():
        pltpu.make_async_copy(act, hb.at[0, ja], lsem.at[0, 3]).wait()

    @pl.when(p == 1)
    def _():
        pltpu.make_async_copy(cot, eb.at[1, ja], lsem.at[0, 3]).wait()

    pl.semaphore_wait(barrier, len(senders))

    FIRST, REST = ((0, PLUS, 0), (1, MINUS, 2)), ((1, PLUS, 1), (0, MINUS, 3))
    LARGE = 2

    def chunk(v, k, ph, q, half):
        if ph == 0:
            width = wts[k].shape[-1] // 2
            ix = tuple(q if ax == AXES[k][0] else coord[ax] for ax in (Z, Y, X)) + (slice(None), pl.ds(half * width, width))
        else:
            hs = pl.ds(2 * half, 2)
            ix = ((zc, q, hs), (q, hs, xc), (hs, yc, q))[k]
        return wts[k].at[(v,) + ix]

    def small_copy(v, k, ph, q, half, delta, slot):
        ref = chunk(v, k, ph, q, half)
        send(ref, ref, ag_s.at[v, k, ph], ag_r.at[v, k, ph, slot], peer(AXES[k][ph], delta), p)

    def small_wait(v, k, ph, back, half, slot):
        wait_recv(chunk(v, k, ph, rot(coord[AXES[k][ph]], back), half), ag_r.at[v, k, ph, slot])

    def small_send(v, ph):
        for half, delta, slot in FIRST + REST:
            for k in (X, Y, Z):
                small_copy(v, k, ph, coord[AXES[k][ph]], half, delta, slot)

    def small_relay(v, ph):
        for half, delta, slot in FIRST:
            for k in (X, Y, Z):
                small_wait(v, k, ph, -delta, half, slot)
                small_copy(v, k, ph, rot(coord[AXES[k][ph]], -delta), half, delta, 4 + half)

    def small_rest(v, ph):
        for half, delta, slot in REST:
            for k in (X, Y, Z):
                small_wait(v, k, ph, -delta, half, slot)

    def small_last(v, ph):
        for half in HALVES:
            for k in (X, Y, Z):
                small_wait(v, k, ph, OPP, half, 4 + half)

    UP, DOWN = (0, PLUS), (MINUS, OPP)
    RELAYS = ((UP[0], PLUS), (DOWN[0], MINUS), (UP[1], PLUS), (DOWN[1], MINUS))

    def row(v, k, q, r):
        m = rot(coord[AXES[k][1]], r)
        ix = ((q, m), (m, slice(None), q), (slice(None), q, m))[k]
        return wts[k].at[(v,) + ix]

    def large_slot(r, delta):
        return r if delta == PLUS else NA + r

    def large_send(v, up, down):
        for pair in zip(up, down):
            for r, delta in zip(pair, (PLUS, MINUS)):
                for k in (X, Y, Z):
                    ax = AXES[k][LARGE]
                    ref = row(v, k, coord[ax], r)
                    send(ref, ref, ag_s.at[v, k, LARGE], lg_r.at[v, k, large_slot(r, delta)], peer(ax, delta), p)

    def large_relay(v):
        for r, delta in RELAYS:
            for k in (X, Y, Z):
                ax = AXES[k][LARGE]
                ref = row(v, k, rot(coord[ax], -delta), r)
                wait_recv(ref, lg_r.at[v, k, large_slot(r, delta)])
                send(ref, ref, ag_s.at[v, k, LARGE], lg_r.at[v, k, 2 * NA + r], peer(ax, delta), p)

    def large_finish(v):
        for pieces, delta in ((DOWN, PLUS), (UP, MINUS)):
            for r in pieces:
                for k in (X, Y, Z):
                    wait_recv(row(v, k, rot(coord[AXES[k][LARGE]], -delta), r), lg_r.at[v, k, large_slot(r, delta)])
        for r in QUARTERS:
            for k in (X, Y, Z):
                wait_recv(row(v, k, rot(coord[AXES[k][LARGE]], OPP), r), lg_r.at[v, k, 2 * NA + r])

    half_rows = rows // 2

    def spread_near(src, buf, which, vd, ssem):
        send(src, buf.at[vd, jb], ssem, mc_r.at[which, vd, 0], d, 1 - p)

    def spread_far(src, buf, which, vd, ssem):
        send(src, buf.at[vd, jb], ssem, mc_r.at[which, vd, 1], peer_b(1), 1 - p)
        send(src, buf.at[vd, jb], ssem, mc_r.at[which, vd, 2], peer_b(-1), 1 - p)

    def spread_same(buf, which, v, ssem):
        own = buf.at[v, ja]
        send(own, own, ssem, mc_r.at[which, v, 1], peer_a(1), p)
        send(own, own, ssem, mc_r.at[which, v, 2], peer_a(-1), p)

    def spread_relay(buf, which, v):
        for half, delta in ((0, 1), (1, 3)):
            slot = rot(ja, -delta)
            wait_recv(buf.at[v, slot], mc_r.at[which, v, 1 + half])
            ref = buf.at[v, slot, pl.ds(half * half_rows, half_rows)]
            send(ref, ref, rl_s.at[which, v], mc_r.at[which, v, 3 + half], peer_a(delta), p)

    def spread_finish(buf, which, v):
        for half in HALVES:
            wait_recv(buf.at[v, rot(ja, 2), pl.ds(half * half_rows, half_rows)], mc_r.at[which, v, 3 + half])

    def spread_own(buf, which, v):
        wait_recv(buf.at[v, ja], mc_r.at[which, v, 0])

    def gates(n, wgt, wlin):
        a, b = mm(n, wgt), mm(n, wlin)
        s = jax.nn.sigmoid(a)
        act_a = a * s
        return (act_a * b).astype(BF), b * s * (1.0 + a * (1.0 - s)), act_a

    def block_gates(v):
        h = hb[v, ja].astype(F32)
        n = (h * inv_rms(h)).astype(BF)

        def tile(i, carry):
            wide = fs // 2
            cols = pl.ds(pl.multiple_of(i * wide, wide), wide)
            u, t1, t2 = gates(n, wg[v, :, :, :, :, cols].reshape(dm, wide), wi[v, :, :, :, :, cols].reshape(dm, wide))
            ub[:, cols] = u
            f1[v, :, cols] = t1
            f2[v, :, cols] = t2
            return carry

        lax.fori_loop(0, 2 * NA, tile, 0, unroll=True)

    def block_out(v, dst):
        half_dm = dm // 2
        for i in HALVES:
            cols = pl.ds(i * half_dm, half_dm)
            out = mm(ub[...], wo[v, :, :, :, :, cols].reshape(fd, half_dm))
            dst[:, cols] = (hb[v, ja, :, cols].astype(F32) + out).astype(BF)

    def block_backward(v, dst):
        e = eb[v, ja]

        def tile(i, carry):
            cols = pl.ds(pl.multiple_of(i * fs, fs), fs)
            t = mm_nt(e, wo[v, i].reshape(fs, dm))
            da[:, cols] = (t * f1[v, :, cols]).astype(BF)
            db[:, cols] = (t * f2[v, :, cols]).astype(BF)
            return carry

        lax.fori_loop(0, NA, tile, 0, unroll=True)
        half_dm = dm // 2
        for i in HALVES:
            q = mm_nt(da[...], wg[v, pl.ds(2 * i, 2)].reshape(half_dm, fd))
            q += mm_nt(db[...], wi[v, pl.ds(2 * i, 2)].reshape(half_dm, fd))
            qs[:, pl.ds(i * half_dm, half_dm)] = q
        h = hb[v, ja].astype(F32)
        r = inv_rms(h)
        hr = h * r
        q = qs[...]
        dst[...] = (e.astype(F32) + r * (q - hr * jnp.mean(q * hr, axis=-1, keepdims=True))).astype(BF)

    def piece(j, i):
        z = i + p * (j - i)
        y = j + p * (i - j)
        return z, y

    def grad_first(v):
        for i in QUARTERS:
            z, y = piece(ja, i)
            cols = pl.ds(pl.multiple_of((z * NA + y) * pf, pf), pf)
            gs[:, pl.ds(i * pf, pf)] = wg[v, :, :, :, :, cols].reshape(dm, pf)
            is_[:, pl.ds(i * pf, pf)] = wi[v, :, :, :, :, cols].reshape(dm, pf)

        def tile(s, carry):
            h = hb[v, s].astype(F32)
            n = (h * inv_rms(h)).astype(BF)
            ng[v, s] = n
            u, t1, t2 = gates(n, gs[...], is_[...])
            us[v, s] = u
            f1s[v, s] = t1
            f2s[v, s] = t2
            return carry

        lax.fori_loop(0, NA, tile, 0, unroll=True)

    def grad_hidden(v):
        for i in QUARTERS:
            z, y = piece(ja, i)
            os_[pl.ds(i * pf, pf), :] = wo[v, z, y].reshape(pf, dm)

        def tile(s, carry):
            t = mm_nt(eb[v, s], os_[...])
            das[s] = (t * f1s[v, s]).astype(BF)
            dbs[s] = (t * f2s[v, s]).astype(BF)
            return carry

        lax.fori_loop(0, NA, tile, 0, unroll=True)

    def grad_out(v):
        def tile(i, carry):
            cols = pl.ds(pl.multiple_of(i * 2 * pf, 2 * pf), 2 * pf)
            g = mm_tn(us[v, :, :, cols].reshape(NA * rows, 2 * pf), eb[v].reshape(NA * rows, dm))
            gout[v, pl.ds(2 * i, 2)] = g.reshape(2, 4, fr, dm)
            return carry

        lax.fori_loop(0, 2, tile, 0, unroll=True)

    def grad_in(v):
        for which, dref in enumerate((das, dbs)):

            def tile(i, carry, which=which, dref=dref):
                cols = pl.ds(pl.multiple_of(i * (dm // NA), dm // NA), dm // NA)
                g = mm_tn(ng[v, :, :, cols].reshape(NA * rows, dm // NA), dref[...].reshape(NA * rows, fs)).reshape(4, 4, dr, fs)

                for y in QUARTERS:
                    gin[v, which, y + p * (i - y), i + p * (y - i)] = g[y]
                return carry

            lax.fori_loop(0, NA, tile, 0, unroll=True)

    IN, OUT = 0, 1

    def split(width):
        return pl.ds(0, width - pf), pl.ds(width - pf, pf)

    def view(which, st, v, colour, t, half):
        along_b = colour == st
        if which == IN:
            cols = split(fs)[colour]
            b, x = (t, slice(None) if st == 0 else xc) if along_b else (slice(None) if st == 0 else jb, t)
            return gin.at[v, half, :, b, x, :, cols]
        cols = split(dm)[colour]
        if st == 0:
            hs = pl.ds(2 * half, 2)
            return gout.at[v, t, hs, :, cols] if along_b else gout.at[v, hs, t, :, cols]
        hs = pl.ds(half * (fr // 2), fr // 2)
        return gout.at[v, t, xc, hs, cols] if along_b else gout.at[v, jb, t, hs, cols]

    RECV = (((rg[0], rg[1]), (rg[2], rg[3])), ((rg[4], rg[5]), (rg[6], rg[7])))
    MERGED, DIRECT = ((0, OPP, PLUS, 0), (1, OPP, MINUS, 1)), ((1, PLUS, PLUS, 2), (0, MINUS, MINUS, 3))
    RELAYED = ((0, PLUS, PLUS, 4), (1, MINUS, MINUS, 5))

    def axis_of(colour, st):
        return (jb, peer_b) if colour == st else (xc, functools.partial(peer, X))

    def scatter_send(v, which, st, copies):
        for colour in COLOURS:
            q, to = axis_of(colour, st)
            for half, c, delta, slot in copies:
                send(view(which, st, v, colour, rot(q, c), half), RECV[st][which][colour].at[v, slot],
                     rs_s.at[st, v, colour, which], rs_r.at[st, v, colour, which, slot], to(delta), p)

    def scatter_relay(v, which, st):
        for colour in COLOURS:
            q, _ = axis_of(colour, st)
            recv = RECV[st][which][colour]
            for half, c, _, slot in RELAYED:
                wait_recv(recv.at[v, slot - 4], rs_r.at[st, v, colour, which, slot - 4])
                ref = view(which, st, v, colour, rot(q, c), half)
                ref[...] = ref[...] + recv[v, slot - 4]
        scatter_send(v, which, st, RELAYED)

    def scatter_sum(v, which, st):
        for colour in COLOURS:
            q, _ = axis_of(colour, st)
            recv = RECV[st][which][colour]
            for half in HALVES:
                direct, merged = 3 - half, 4 + half
                for slot in (direct, merged):
                    wait_recv(recv.at[v, slot], rs_r.at[st, v, colour, which, slot])
                ref = view(which, st, v, colour, q, half)
                ref[...] = ref[...] + recv[v, direct] + recv[v, merged]

    def scatter_turn(v, which):
        scatter_sum(v, which, 0)
        scatter_send(v, which, 1, MERGED + DIRECT)

    def scatter_last(v):
        scatter_sum(v, OUT, 1)
        go[v] = gout[v, jb, xc]
        scatter_sum(v, IN, 1)
        for which in HALVES:
            fin[v, :, which] = gin[v, which, :, jb, xc]
        for delta in RING:
            send(fin.at[v, rot(ja, delta)], r3.at[v, delta - 1], r3_s.at[v], r3_r.at[v, delta - 1], peer_a(delta), p)

    def scatter_finish(v):
        def put(j, vals):
            for i in QUARTERS:
                z, y = piece(j, i)
                cols = pl.ds(pl.multiple_of((z * NA + y) * pf, pf), pf)
                gg[v, :, cols] = vals(0)[:, i * pf:(i + 1) * pf]
                gi[v, :, cols] = vals(1)[:, i * pf:(i + 1) * pf]

        put(ja, lambda w: fin[v, ja, w])
        for delta in RING:
            wait_recv(r3.at[v, delta - 1], r3_r.at[v, delta - 1])
            put(rot(ja, -delta), lambda w, delta=delta: r3[v, delta - 1, w])

    def step(fn, *args):
        with jax.named_scope(fn.__name__):
            fn(*args)

    def on(core):
        return pl.when(p == core)

    def take_turn():
        pl.semaphore_wait(turn, 1)

    def give_turn():
        pl.semaphore_signal(turn, inc=1, device_id=(d, 1 - p), device_id_type=MESH)

    h_mid, h_late, e_first, e_last = ((xo.at[i], mc_s.at[1 + i]) for i in QUARTERS)

    def pass_on(part, item, buf, which, vd):
        step(part, item[0], buf, which, vd, item[1])

    ALL = UP + (MINUS, OPP), DOWN + (0, PLUS)
    for v in BLOCKS:
        step(small_send, v, 0)
    for v in BLOCKS:
        step(small_relay, v, 0)
    step(small_rest, 0, 0)
    step(small_last, 0, 0)
    step(small_send, 0, 1)
    step(large_send, 0, (0,), (0,))
    step(small_rest, 1, 0)
    step(small_last, 1, 0)
    step(small_send, 1, 1)
    step(small_relay, 0, 1)
    step(small_relay, 1, 1)
    step(small_rest, 0, 1)
    step(large_send, 0, (PLUS, MINUS), (MINUS, PLUS))
    step(small_last, 0, 1)
    step(large_send, 0, (OPP,), (OPP,))
    step(small_rest, 1, 1)
    step(small_last, 1, 1)
    step(large_relay, 0)

    @on(0)
    def _():
        step(large_send, 1, *ALL)

    step(large_finish, 0)

    @on(1)
    def _():
        step(spread_own, hb, 0, 0)

    step(block_gates, 0)
    step(block_out, 0, h_mid[0])
    pass_on(spread_near, h_mid, hb, 0, p)

    @on(1)
    def _():
        step(take_turn)
        step(large_send, 1, *ALL)

    step(large_relay, 1)

    @on(0)
    def _():
        step(give_turn)
        step(spread_same, hb, 0, 0, mc_s.at[0])

    step(large_finish, 1)

    @on(1)
    def _():
        pass_on(spread_far, h_mid, hb, 0, p)

    step(spread_own, hb, 0, 1)
    step(block_gates, 1)

    @on(0)
    def _():
        step(block_out, 1, h_late[0])
        pass_on(spread_near, h_late, hb, 0, 1)
        pass_on(spread_far, h_late, hb, 0, 1)
        step(spread_relay, hb, 0, 0)
        step(spread_finish, hb, 0, 0)
        step(grad_first, 0)
        step(spread_own, eb, 1, 1)
        step(block_backward, 1, e_first[0])
        pass_on(spread_near, e_first, eb, 1, 0)
        pass_on(spread_far, e_first, eb, 1, 0)
        pass_on(spread_far, h_mid, hb, 0, p)
        step(spread_relay, eb, 1, 1)
        step(spread_relay, hb, 0, 1)
        step(spread_finish, hb, 0, 1)
        step(grad_first, 1)

    @on(1)
    def _():
        step(spread_relay, hb, 0, 1)
        step(block_backward, 1, e_first[0])
        pass_on(spread_near, e_first, eb, 1, 1)
        pass_on(spread_far, e_first, eb, 1, 1)
        step(spread_same, eb, 1, 1, mc_s.at[0])
        step(spread_finish, hb, 0, 1)
        step(grad_first, 1)
        step(spread_relay, eb, 1, 1)
        step(spread_own, eb, 1, 0)
        step(block_backward, 0, e_last[0])
        pass_on(spread_near, e_last, eb, 1, 0)
        pass_on(spread_far, e_last, eb, 1, 0)
        step(spread_relay, eb, 1, 0)

    step(spread_finish, eb, 1, 1)
    step(grad_hidden, 1)
    step(grad_out, 1)
    step(scatter_send, 1, OUT, 0, MERGED + DIRECT)
    step(grad_in, 1)

    @on(0)
    def _():
        step(spread_relay, eb, 1, 0)

    step(scatter_send, 1, IN, 0, MERGED + DIRECT)

    @on(0)
    def _():
        step(spread_own, eb, 1, 0)
        step(block_backward, 0, ga)
        send(ga, ga, ga_s, ga_r, d, 1)

    @on(1)
    def _():
        step(spread_relay, hb, 0, 0)
        step(spread_finish, hb, 0, 0)
        step(grad_first, 0)

    step(spread_finish, eb, 1, 0)
    step(scatter_relay, 1, OUT, 0)
    step(grad_hidden, 0)
    step(grad_out, 0)
    step(scatter_send, 0, OUT, 0, MERGED)
    step(scatter_relay, 1, IN, 0)
    step(grad_in, 0)
    step(scatter_send, 0, IN, 0, MERGED)
    step(scatter_send, 0, OUT, 0, DIRECT)
    step(scatter_turn, 1, OUT)
    step(scatter_turn, 1, IN)
    step(scatter_send, 0, IN, 0, DIRECT)
    step(scatter_relay, 0, OUT, 0)
    step(scatter_relay, 0, IN, 0)
    step(scatter_relay, 1, OUT, 1)
    step(scatter_relay, 1, IN, 1)

    @on(1)
    def _():
        wait_recv(ga, ga_r)

    gact[...] = ga[...]
    step(scatter_turn, 0, OUT)
    step(scatter_turn, 0, IN)
    step(scatter_last, 1)
    step(scatter_relay, 0, OUT, 1)
    step(scatter_relay, 0, IN, 1)
    step(scatter_finish, 1)
    step(scatter_last, 0)
    step(scatter_finish, 0)

    for v in BLOCKS:
        for k in (X, Y, Z):
            wait_send(wts[k].at[v, 0, 0, pl.ds(0, 3)], ag_s.at[v, k, 0])
            wait_send(wts[k].at[v, 0, pl.ds(0, 3)], ag_s.at[v, k, 1])
            wait_send(wts[k].at[v, pl.ds(0, 3)], ag_s.at[v, k, LARGE])
        for colour in COLOURS:
            for which in HALVES:
                for st in HALVES:
                    wait_send(RECV[st][which][colour].at[v], rs_s.at[st, v, colour, which])
        wait_send(r3.at[v], r3_s.at[v])
        wait_send(hb.at[v, 0], rl_s.at[0, v])
        wait_send(hb.at[v, 0], rl_s.at[1, v])
    wait_send(hb.at[0, pl.ds(0, 2)], mc_s.at[0])
    wait_send(hb.at[0, pl.ds(0, 3)], mc_s.at[1])
    wait_send(hb.at[0, pl.ds(0, 3)], mc_s.at[3])

    @pl.when(p == 0)
    def _():
        wait_send(hb.at[0, pl.ds(0, 3)], mc_s.at[2])
        wait_send(ga, ga_s)

    @pl.when(p == 1)
    def _():
        wait_send(hb.at[0, pl.ds(0, 3)], mc_s.at[4])


def hand_on(*refs):
    srcs, dsts, bufs = refs[:NA], refs[NA:2 * NA], refs[2 * NA:3 * NA]
    sem_in, sem_out = refs[3 * NA:]
    into = [pltpu.make_async_copy(srcs[i], bufs[i], sem_in.at[i]) for i in QUARTERS]
    onto = [pltpu.make_async_copy(bufs[i], dsts[i], sem_out.at[i]) for i in QUARTERS]
    for copy in into:
        copy.start()
    for i in QUARTERS:
        into[i].wait()
        onto[i].start()
    for copy in onto:
        copy.wait()


def solution(mesh):
    act_spec = P(None, "data", None, None)
    w_spec = P(None, "stage", "data", None)

    def body(act_in, cot_out, w_gate, w_in, w_out):
        shape = act_in.shape
        dm, fd = shape[3], w_gate.shape[3]
        rows = shape[0] * shape[1] * shape[2]
        dr, fr, fs = dm // NL, fd // NL, fd // NA
        pf = fs // NA
        vmem = pltpu.VMEM
        dma = pltpu.SemaphoreType.DMA
        n2, n3, na = NB, len(RING), NA
        ring = (na, na)
        scratch = [
            vmem((n2, na, *ring, dr, fd), BF), vmem((n2, na, *ring, dr, fd), BF), vmem((n2, na, *ring, fr, dm), BF),
            vmem((n2, na, rows, dm), BF), vmem((n2, na, rows, dm), BF), vmem((na, rows, dm), BF), vmem((rows, dm), BF),
            vmem((n2, na, rows, dm), BF),
            vmem((n2, rows, fd), F32), vmem((n2, rows, fd), F32),
            vmem((n2, na, rows, fs), F32), vmem((n2, na, rows, fs), F32),
            vmem((n2, na, rows, fs), BF),
            vmem((rows, fd), BF), vmem((rows, fd), BF), vmem((rows, fd), BF),
            vmem((na, rows, fs), BF), vmem((na, rows, fs), BF),
            vmem((rows, dm), F32),
            vmem((dm, fs), BF), vmem((dm, fs), BF), vmem((fs, dm), BF),
            vmem((n2, n2, na, *ring, dr, fs), F32), vmem((n2, *ring, fr, dm), F32),
            vmem((n2, na, n2, dr, fs), F32), vmem((n2, n3, n2, dr, fs), F32),
            dma((n2, na)), dma((n2, n3, n3)), dma((n2, n3, n2, 6)), dma((n2, n3, n3 * na)), dma((5,)), dma((n2, n2, 5)), dma((n2, n2)), dma, dma,
            dma((n2, n2, n2, n2)), dma((n2, n2, n2, n2, 6)), dma((n2,)), dma((n2, n3)), pltpu.SemaphoreType.REGULAR,
            *(vmem((n2, 6, *lead, width), F32)
              for lead_in, lead_out in (((*ring, dr), (n2, fr)), ((na, dr), (fr // n2,)))
              for lead, total in ((lead_in, fs), (lead_out, dm))
              for width in (total - pf, pf)),
        ]
        hbm = pl.BlockSpec(memory_space=pl.ANY)
        whole = pl.BlockSpec(memory_space=pltpu.VMEM)
        out = pl.pallas_call(
            kernel,
            out_shape=(
                jax.ShapeDtypeStruct((rows, dm), BF),
                jax.ShapeDtypeStruct((2, dr, fd), F32), jax.ShapeDtypeStruct((2, dr, fd), F32),
                jax.ShapeDtypeStruct((2, fr, dm), F32),
            ),
            in_specs=[hbm] * 5,
            out_specs=(whole,) * NA,
            scratch_shapes=scratch,
            compiler_params=pltpu.CompilerParams(collective_id=0, has_side_effects=True, vmem_limit_bytes=67043328),
            name="train_step",
        )(act_in.reshape(rows, dm), cot_out.reshape(rows, dm), w_gate[:, 0], w_in[:, 0], w_out[:, 0])
        grad_act, grad_gate, grad_lin, grad_proj = pl.pallas_call(
            hand_on, out_shape=tuple(jax.ShapeDtypeStruct(a.shape, a.dtype) for a in out), in_specs=[hbm] * NA, out_specs=(hbm,) * NA,
            scratch_shapes=[*(vmem(a.shape, a.dtype) for a in out), dma((NA,)), dma((NA,))], name="hand_on",
        )(*out)
        return grad_act.reshape(shape), grad_gate[:, None], grad_lin[:, None], grad_proj[:, None]

    return jax.shard_map(body, mesh=mesh, in_specs=(act_spec, act_spec, w_spec, w_spec, w_spec),
                         out_specs=(act_spec, w_spec, w_spec, w_spec), check_vma=False)
```

```python
import functools

import jax
import jax.numpy as jnp
from jax import lax
from jax.experimental import pallas as pl
from jax.experimental.pallas import tpu as pltpu
from jax.sharding import PartitionSpec as P

NORM_EPS = 1e-6
BF = jnp.bfloat16
F32 = jnp.float32
MESH = pl.DeviceIdType.MESH
X, Y, Z = 0, 1, 2
BLOCKS = COLOURS = HALVES = (0, 1)
NB, NA, NL = len(BLOCKS), 4, 64
RING = (1, 3, 2)
OPP = RING[-1]
PLUS, MINUS = RING[:-1]
QUARTERS = range(NA)
AXES = ((X, Y, Z), (Y, Z, X), (Z, X, Y))


def mm(left, right):
    return jnp.dot(left, right, preferred_element_type=F32)


def mm_nt(left, right):
    return lax.dot_general(left, right, (((1,), (1,)), ((), ())), preferred_element_type=F32)


def mm_tn(left, right):
    return lax.dot_general(left, right, (((0,), (0,)), ((), ())), preferred_element_type=F32)


def inv_rms(h):
    return lax.rsqrt(jnp.mean(h * h, axis=-1, keepdims=True) + NORM_EPS)


def kernel(act, cot, wg_in, wi_in, wo_in, gact, gg, gi, go,
           wg, wi, wo, hb, eb, xo, ga, ng, f1, f2, f1s, f2s, us, ub, da, db, das, dbs, qs, gs, is_, os_,
           gin, gout, fin, r3,
           lsem, ag_s, ag_r, lg_r, mc_s, mc_r, rl_s, ga_s, ga_r, rs_s, rs_r, r3_s, r3_r, turn, *rg):
    dm, fd = wo.shape[-1], wg.shape[-1]
    dr, fr = dm // NL, fd // NL
    fs = fd // NA
    pf = fs // NA
    rows = act.shape[0]
    wts = (wg, wi, wo)

    p = lax.axis_index("stage")
    d = lax.axis_index("data")
    zc, yc, xc = lax.div(d, 16), lax.rem(lax.div(d, 4), 4), lax.rem(d, 4)
    coord = (xc, yc, zc)
    stride = (1, 4, 16)
    ja = yc + p * (zc - yc)
    jb = zc + p * (yc - zc)
    sa, sb = 4 + 12 * p, 16 - 12 * p

    def rot(c, delta):
        return lax.rem(c + (delta % 4), 4)

    def peer(ax, delta):
        return d + (rot(coord[ax], delta) - coord[ax]) * stride[ax]

    def peer_a(delta):
        return d + (rot(ja, delta) - ja) * sa

    def peer_b(delta):
        return d + (rot(jb, delta) - jb) * sb

    def remote(src, dst, ssem, rsem, dev, core):
        return pltpu.make_async_remote_copy(src_ref=src, dst_ref=dst, send_sem=ssem, recv_sem=rsem,
                                            device_id=(dev, core), device_id_type=MESH)

    def send(src, dst, ssem, rsem, dev, core):
        remote(src, dst, ssem, rsem, dev, core).start()

    def wait_recv(ref, sem):
        remote(ref, ref, sem, sem, d, p).wait_recv()

    def wait_send(ref, sem):
        remote(ref, ref, sem, sem, d, p).wait_send()

    for v in BLOCKS:
        for k, shard in enumerate((wg_in, wi_in, wo_in)):
            pltpu.make_async_copy(shard.at[v], wts[k].at[v, zc, yc, xc], lsem.at[v, k]).start()

    @pl.when(p == 0)
    def _():
        pltpu.make_async_copy(act, hb.at[0, ja], lsem.at[0, 3]).start()

    @pl.when(p == 1)
    def _():
        pltpu.make_async_copy(cot, eb.at[1, ja], lsem.at[0, 3]).start()

    barrier = pltpu.get_barrier_semaphore()
    senders = [(peer(ax, delta), p) for ax in (X, Y, Z) for delta in RING]
    senders += [(d, 1 - p), (peer_a(1), 1 - p), (peer_a(-1), 1 - p)]
    for dev, core in senders:
        pl.semaphore_signal(barrier, inc=1, device_id=(dev, core), device_id_type=MESH)
    for v in BLOCKS:
        for k, shard in enumerate((wg_in, wi_in, wo_in)):
            pltpu.make_async_copy(shard.at[v], wts[k].at[v, zc, yc, xc], lsem.at[v, k]).wait()

    @pl.when(p == 0)
    def _():
        pltpu.make_async_copy(act, hb.at[0, ja], lsem.at[0, 3]).wait()

    @pl.when(p == 1)
    def _():
        pltpu.make_async_copy(cot, eb.at[1, ja], lsem.at[0, 3]).wait()

    pl.semaphore_wait(barrier, len(senders))

    FIRST, REST = ((0, PLUS, 0), (1, MINUS, 2)), ((1, PLUS, 1), (0, MINUS, 3))
    LARGE = 2

    def chunk(v, k, ph, q, half):
        if ph == 0:
            width = wts[k].shape[-1] // 2
            ix = tuple(q if ax == AXES[k][0] else coord[ax] for ax in (Z, Y, X)) + (slice(None), pl.ds(half * width, width))
        else:
            hs = pl.ds(2 * half, 2)
            ix = ((zc, q, hs), (q, hs, xc), (hs, yc, q))[k]
        return wts[k].at[(v,) + ix]

    def small_copy(v, k, ph, q, half, delta, slot):
        ref = chunk(v, k, ph, q, half)
        send(ref, ref, ag_s.at[v, k, ph], ag_r.at[v, k, ph, slot], peer(AXES[k][ph], delta), p)

    def small_wait(v, k, ph, back, half, slot):
        wait_recv(chunk(v, k, ph, rot(coord[AXES[k][ph]], back), half), ag_r.at[v, k, ph, slot])

    def small_send(v, ph):
        for half, delta, slot in FIRST + REST:
            for k in (X, Y, Z):
                small_copy(v, k, ph, coord[AXES[k][ph]], half, delta, slot)

    def small_relay(v, ph):
        for half, delta, slot in FIRST:
            for k in (X, Y, Z):
                small_wait(v, k, ph, -delta, half, slot)
                small_copy(v, k, ph, rot(coord[AXES[k][ph]], -delta), half, delta, 4 + half)

    def small_rest(v, ph):
        for half, delta, slot in REST:
            for k in (X, Y, Z):
                small_wait(v, k, ph, -delta, half, slot)

    def small_last(v, ph):
        for half in HALVES:
            for k in (X, Y, Z):
                small_wait(v, k, ph, OPP, half, 4 + half)

    UP, DOWN = (0, PLUS), (MINUS, OPP)
    RELAYS = ((UP[0], PLUS), (DOWN[0], MINUS), (UP[1], PLUS), (DOWN[1], MINUS))

    def row(v, k, q, r):
        m = rot(coord[AXES[k][1]], r)
        ix = ((q, m), (m, slice(None), q), (slice(None), q, m))[k]
        return wts[k].at[(v,) + ix]

    def large_slot(r, delta):
        return r if delta == PLUS else NA + r

    def large_send(v, up, down):
        for pair in zip(up, down):
            for r, delta in zip(pair, (PLUS, MINUS)):
                for k in (X, Y, Z):
                    ax = AXES[k][LARGE]
                    ref = row(v, k, coord[ax], r)
                    send(ref, ref, ag_s.at[v, k, LARGE], lg_r.at[v, k, large_slot(r, delta)], peer(ax, delta), p)

    def large_relay(v):
        for r, delta in RELAYS:
            for k in (X, Y, Z):
                ax = AXES[k][LARGE]
                ref = row(v, k, rot(coord[ax], -delta), r)
                wait_recv(ref, lg_r.at[v, k, large_slot(r, delta)])
                send(ref, ref, ag_s.at[v, k, LARGE], lg_r.at[v, k, 2 * NA + r], peer(ax, delta), p)

    def large_finish(v):
        for pieces, delta in ((DOWN, PLUS), (UP, MINUS)):
            for r in pieces:
                for k in (X, Y, Z):
                    wait_recv(row(v, k, rot(coord[AXES[k][LARGE]], -delta), r), lg_r.at[v, k, large_slot(r, delta)])
        for r in QUARTERS:
            for k in (X, Y, Z):
                wait_recv(row(v, k, rot(coord[AXES[k][LARGE]], OPP), r), lg_r.at[v, k, 2 * NA + r])

    half_rows = rows // 2

    def spread_near(src, buf, which, vd, ssem):
        send(src, buf.at[vd, jb], ssem, mc_r.at[which, vd, 0], d, 1 - p)

    def spread_far(src, buf, which, vd, ssem):
        send(src, buf.at[vd, jb], ssem, mc_r.at[which, vd, 1], peer_b(1), 1 - p)
        send(src, buf.at[vd, jb], ssem, mc_r.at[which, vd, 2], peer_b(-1), 1 - p)

    def spread_same(buf, which, v, ssem):
        own = buf.at[v, ja]
        send(own, own, ssem, mc_r.at[which, v, 1], peer_a(1), p)
        send(own, own, ssem, mc_r.at[which, v, 2], peer_a(-1), p)

    def spread_relay(buf, which, v):
        for half, delta in ((0, 1), (1, 3)):
            slot = rot(ja, -delta)
            wait_recv(buf.at[v, slot], mc_r.at[which, v, 1 + half])
            ref = buf.at[v, slot, pl.ds(half * half_rows, half_rows)]
            send(ref, ref, rl_s.at[which, v], mc_r.at[which, v, 3 + half], peer_a(delta), p)

    def spread_finish(buf, which, v):
        for half in HALVES:
            wait_recv(buf.at[v, rot(ja, 2), pl.ds(half * half_rows, half_rows)], mc_r.at[which, v, 3 + half])

    def spread_own(buf, which, v):
        wait_recv(buf.at[v, ja], mc_r.at[which, v, 0])

    def gates(n, wgt, wlin):
        a, b = mm(n, wgt), mm(n, wlin)
        s = jax.nn.sigmoid(a)
        act_a = a * s
        return (act_a * b).astype(BF), b * s * (1.0 + a * (1.0 - s)), act_a

    def block_gates(v):
        h = hb[v, ja].astype(F32)
        n = (h * inv_rms(h)).astype(BF)

        def tile(i, carry):
            wide = fs // 2
            cols = pl.ds(pl.multiple_of(i * wide, wide), wide)
            u, t1, t2 = gates(n, wg[v, :, :, :, :, cols].reshape(dm, wide), wi[v, :, :, :, :, cols].reshape(dm, wide))
            ub[:, cols] = u
            f1[v, :, cols] = t1
            f2[v, :, cols] = t2
            return carry

        lax.fori_loop(0, 2 * NA, tile, 0, unroll=True)

    def block_out(v, dst):
        half_dm = dm // 2
        for i in HALVES:
            cols = pl.ds(i * half_dm, half_dm)
            out = mm(ub[...], wo[v, :, :, :, :, cols].reshape(fd, half_dm))
            dst[:, cols] = (hb[v, ja, :, cols].astype(F32) + out).astype(BF)

    def block_backward(v, dst):
        e = eb[v, ja]

        def tile(i, carry):
            cols = pl.ds(pl.multiple_of(i * fs, fs), fs)
            t = mm_nt(e, wo[v, i].reshape(fs, dm))
            da[:, cols] = (t * f1[v, :, cols]).astype(BF)
            db[:, cols] = (t * f2[v, :, cols]).astype(BF)
            return carry

        lax.fori_loop(0, NA, tile, 0, unroll=True)
        half_dm = dm // 2
        for i in HALVES:
            q = mm_nt(da[...], wg[v, pl.ds(2 * i, 2)].reshape(half_dm, fd))
            q += mm_nt(db[...], wi[v, pl.ds(2 * i, 2)].reshape(half_dm, fd))
            qs[:, pl.ds(i * half_dm, half_dm)] = q
        h = hb[v, ja].astype(F32)
        r = inv_rms(h)
        hr = h * r
        q = qs[...]
        dst[...] = (e.astype(F32) + r * (q - hr * jnp.mean(q * hr, axis=-1, keepdims=True))).astype(BF)

    def piece(j, i):
        z = i + p * (j - i)
        y = j + p * (i - j)
        return z, y

    def grad_first(v):
        for i in QUARTERS:
            z, y = piece(ja, i)
            cols = pl.ds(pl.multiple_of((z * NA + y) * pf, pf), pf)
            gs[:, pl.ds(i * pf, pf)] = wg[v, :, :, :, :, cols].reshape(dm, pf)
            is_[:, pl.ds(i * pf, pf)] = wi[v, :, :, :, :, cols].reshape(dm, pf)

        def tile(s, carry):
            h = hb[v, s].astype(F32)
            n = (h * inv_rms(h)).astype(BF)
            ng[v, s] = n
            u, t1, t2 = gates(n, gs[...], is_[...])
            us[v, s] = u
            f1s[v, s] = t1
            f2s[v, s] = t2
            return carry

        lax.fori_loop(0, NA, tile, 0, unroll=True)

    def grad_hidden(v):
        for i in QUARTERS:
            z, y = piece(ja, i)
            os_[pl.ds(i * pf, pf), :] = wo[v, z, y].reshape(pf, dm)

        def tile(s, carry):
            t = mm_nt(eb[v, s], os_[...])
            das[s] = (t * f1s[v, s]).astype(BF)
            dbs[s] = (t * f2s[v, s]).astype(BF)
            return carry

        lax.fori_loop(0, NA, tile, 0, unroll=True)

    def grad_out(v):
        def tile(i, carry):
            cols = pl.ds(pl.multiple_of(i * 2 * pf, 2 * pf), 2 * pf)
            g = mm_tn(us[v, :, :, cols].reshape(NA * rows, 2 * pf), eb[v].reshape(NA * rows, dm))
            gout[v, pl.ds(2 * i, 2)] = g.reshape(2, 4, fr, dm)
            return carry

        lax.fori_loop(0, 2, tile, 0, unroll=True)

    def grad_in(v):
        for which, dref in enumerate((das, dbs)):

            def tile(i, carry, which=which, dref=dref):
                cols = pl.ds(pl.multiple_of(i * (dm // NA), dm // NA), dm // NA)
                g = mm_tn(ng[v, :, :, cols].reshape(NA * rows, dm // NA), dref[...].reshape(NA * rows, fs)).reshape(4, 4, dr, fs)

                for y in QUARTERS:
                    gin[v, which, y + p * (i - y), i + p * (y - i)] = g[y]
                return carry

            lax.fori_loop(0, NA, tile, 0, unroll=True)

    IN, OUT = 0, 1

    def split(width):
        return pl.ds(0, width - pf), pl.ds(width - pf, pf)

    def view(which, st, v, colour, t, half):
        along_b = colour == st
        if which == IN:
            cols = split(fs)[colour]
            b, x = (t, slice(None) if st == 0 else xc) if along_b else (slice(None) if st == 0 else jb, t)
            return gin.at[v, half, :, b, x, :, cols]
        cols = split(dm)[colour]
        if st == 0:
            hs = pl.ds(2 * half, 2)
            return gout.at[v, t, hs, :, cols] if along_b else gout.at[v, hs, t, :, cols]
        hs = pl.ds(half * (fr // 2), fr // 2)
        return gout.at[v, t, xc, hs, cols] if along_b else gout.at[v, jb, t, hs, cols]

    RECV = (((rg[0], rg[1]), (rg[2], rg[3])), ((rg[4], rg[5]), (rg[6], rg[7])))
    MERGED, DIRECT = ((0, OPP, PLUS, 0), (1, OPP, MINUS, 1)), ((1, PLUS, PLUS, 2), (0, MINUS, MINUS, 3))
    RELAYED = ((0, PLUS, PLUS, 4), (1, MINUS, MINUS, 5))

    def axis_of(colour, st):
        return (jb, peer_b) if colour == st else (xc, functools.partial(peer, X))

    def scatter_send(v, which, st, copies):
        for colour in COLOURS:
            q, to = axis_of(colour, st)
            for half, c, delta, slot in copies:
                send(view(which, st, v, colour, rot(q, c), half), RECV[st][which][colour].at[v, slot],
                     rs_s.at[st, v, colour, which], rs_r.at[st, v, colour, which, slot], to(delta), p)

    def scatter_relay(v, which, st):
        for colour in COLOURS:
            q, _ = axis_of(colour, st)
            recv = RECV[st][which][colour]
            for half, c, _, slot in RELAYED:
                wait_recv(recv.at[v, slot - 4], rs_r.at[st, v, colour, which, slot - 4])
                ref = view(which, st, v, colour, rot(q, c), half)
                ref[...] = ref[...] + recv[v, slot - 4]
        scatter_send(v, which, st, RELAYED)

    def scatter_sum(v, which, st):
        for colour in COLOURS:
            q, _ = axis_of(colour, st)
            recv = RECV[st][which][colour]
            for half in HALVES:
                direct, merged = 3 - half, 4 + half
                for slot in (direct, merged):
                    wait_recv(recv.at[v, slot], rs_r.at[st, v, colour, which, slot])
                ref = view(which, st, v, colour, q, half)
                ref[...] = ref[...] + recv[v, direct] + recv[v, merged]

    def scatter_turn(v, which):
        scatter_sum(v, which, 0)
        scatter_send(v, which, 1, MERGED + DIRECT)

    def scatter_last(v):
        scatter_sum(v, OUT, 1)
        go[v] = gout[v, jb, xc]
        scatter_sum(v, IN, 1)
        for which in HALVES:
            fin[v, :, which] = gin[v, which, :, jb, xc]
        for delta in RING:
            send(fin.at[v, rot(ja, delta)], r3.at[v, delta - 1], r3_s.at[v], r3_r.at[v, delta - 1], peer_a(delta), p)

    def scatter_finish(v):
        def put(j, vals):
            for i in QUARTERS:
                z, y = piece(j, i)
                cols = pl.ds(pl.multiple_of((z * NA + y) * pf, pf), pf)
                gg[v, :, cols] = vals(0)[:, i * pf:(i + 1) * pf]
                gi[v, :, cols] = vals(1)[:, i * pf:(i + 1) * pf]

        put(ja, lambda w: fin[v, ja, w])
        for delta in RING:
            wait_recv(r3.at[v, delta - 1], r3_r.at[v, delta - 1])
            put(rot(ja, -delta), lambda w, delta=delta: r3[v, delta - 1, w])

    def step(fn, *args):
        with jax.named_scope(fn.__name__):
            fn(*args)

    def on(core):
        return pl.when(p == core)

    def take_turn():
        pl.semaphore_wait(turn, 1)

    def give_turn():
        pl.semaphore_signal(turn, inc=1, device_id=(d, 1 - p), device_id_type=MESH)

    h_mid, h_late, e_first, e_last = ((xo.at[i], mc_s.at[1 + i]) for i in QUARTERS)

    def pass_on(part, item, buf, which, vd):
        step(part, item[0], buf, which, vd, item[1])

    ALL = UP + (MINUS, OPP), DOWN + (0, PLUS)
    for v in BLOCKS:
        step(small_send, v, 0)

    @on(0)
    def _():
        step(spread_same, hb, 0, 0, mc_s.at[0])

    @on(1)
    def _():
        step(spread_same, eb, 1, 1, mc_s.at[0])

    for v in BLOCKS:
        step(small_relay, v, 0)
    step(small_rest, 0, 0)
    step(small_last, 0, 0)
    step(small_send, 0, 1)
    step(large_send, 0, (0,), (0,))
    step(small_rest, 1, 0)
    step(small_last, 1, 0)
    step(small_send, 1, 1)
    step(small_relay, 0, 1)
    step(small_relay, 1, 1)
    step(small_rest, 0, 1)
    step(large_send, 0, (PLUS, MINUS), (MINUS, PLUS))
    step(small_last, 0, 1)
    step(large_send, 0, (OPP,), (OPP,))
    step(small_rest, 1, 1)
    step(small_last, 1, 1)
    step(large_relay, 0)

    @on(0)
    def _():
        step(large_send, 1, *ALL)

    step(large_finish, 0)

    @on(1)
    def _():
        step(spread_own, hb, 0, 0)

    step(block_gates, 0)
    step(block_out, 0, h_mid[0])
    pass_on(spread_near, h_mid, hb, 0, p)

    @on(1)
    def _():
        step(take_turn)
        step(large_send, 1, *ALL)

    step(large_relay, 1)

    @on(0)
    def _():
        step(give_turn)
        step(spread_relay, hb, 0, 0)

    step(large_finish, 1)

    @on(1)
    def _():
        step(give_turn)
        step(spread_relay, eb, 1, 1)
        pass_on(spread_far, h_mid, hb, 0, p)

    step(spread_own, hb, 0, 1)

    @on(1)
    def _():
        step(spread_relay, hb, 0, 1)

    step(block_gates, 1)

    @on(0)
    def _():
        step(block_out, 1, h_late[0])
        pass_on(spread_near, h_late, hb, 0, 1)
        pass_on(spread_far, h_late, hb, 0, 1)
        step(spread_finish, hb, 0, 0)
        step(grad_first, 0)
        step(take_turn)
        pass_on(spread_far, h_mid, hb, 0, p)
        step(spread_relay, hb, 0, 1)
        step(spread_own, eb, 1, 1)
        step(block_backward, 1, e_first[0])
        pass_on(spread_near, e_first, eb, 1, 0)
        pass_on(spread_far, e_first, eb, 1, 0)
        step(spread_relay, eb, 1, 1)
        step(spread_finish, hb, 0, 1)
        step(grad_first, 1)

    @on(1)
    def _():
        step(block_backward, 1, e_first[0])
        pass_on(spread_near, e_first, eb, 1, 1)
        pass_on(spread_far, e_first, eb, 1, 1)
        step(spread_finish, hb, 0, 1)
        step(grad_first, 1)

    step(spread_finish, eb, 1, 1)
    step(grad_hidden, 1)
    step(grad_out, 1)
    step(scatter_send, 1, OUT, 0, MERGED + DIRECT)

    @on(1)
    def _():
        step(spread_own, eb, 1, 0)
        step(block_backward, 0, e_last[0])
        pass_on(spread_near, e_last, eb, 1, 0)
        pass_on(spread_far, e_last, eb, 1, 0)

    step(grad_in, 1)

    @on(0)
    def _():
        step(spread_relay, eb, 1, 0)

    step(scatter_send, 1, IN, 0, MERGED + DIRECT)

    @on(0)
    def _():
        step(spread_own, eb, 1, 0)
        step(block_backward, 0, ga)
        send(ga, ga, ga_s, ga_r, d, 1)

    @on(1)
    def _():
        step(spread_relay, hb, 0, 0)
        step(spread_relay, eb, 1, 0)
        step(spread_finish, hb, 0, 0)
        step(grad_first, 0)

    step(scatter_relay, 1, OUT, 0)
    step(spread_finish, eb, 1, 0)
    step(grad_hidden, 0)
    step(grad_out, 0)
    step(scatter_send, 0, OUT, 0, MERGED)
    step(scatter_relay, 1, IN, 0)
    step(grad_in, 0)
    step(scatter_send, 0, IN, 0, MERGED)
    step(scatter_send, 0, OUT, 0, DIRECT)
    step(scatter_turn, 1, OUT)
    step(scatter_send, 0, IN, 0, DIRECT)
    step(scatter_relay, 0, OUT, 0)
    step(scatter_turn, 1, IN)
    step(scatter_relay, 0, IN, 0)
    step(scatter_relay, 1, OUT, 1)

    @on(1)
    def _():
        wait_recv(ga, ga_r)

    gact[...] = ga[...]
    step(scatter_turn, 0, OUT)
    step(scatter_relay, 1, IN, 1)
    step(scatter_turn, 0, IN)
    step(scatter_last, 1)
    step(scatter_relay, 0, OUT, 1)
    step(scatter_relay, 0, IN, 1)
    step(scatter_finish, 1)
    step(scatter_last, 0)
    step(scatter_finish, 0)

    for v in BLOCKS:
        for k in (X, Y, Z):
            wait_send(wts[k].at[v, 0, 0, pl.ds(0, 3)], ag_s.at[v, k, 0])
            wait_send(wts[k].at[v, 0, pl.ds(0, 3)], ag_s.at[v, k, 1])
            wait_send(wts[k].at[v, pl.ds(0, 3)], ag_s.at[v, k, LARGE])
        for colour in COLOURS:
            for which in HALVES:
                for st in HALVES:
                    wait_send(RECV[st][which][colour].at[v], rs_s.at[st, v, colour, which])
        wait_send(r3.at[v], r3_s.at[v])
        wait_send(hb.at[v, 0], rl_s.at[0, v])
        wait_send(hb.at[v, 0], rl_s.at[1, v])
    wait_send(hb.at[0, pl.ds(0, 2)], mc_s.at[0])
    wait_send(hb.at[0, pl.ds(0, 3)], mc_s.at[1])
    wait_send(hb.at[0, pl.ds(0, 3)], mc_s.at[3])

    @pl.when(p == 0)
    def _():
        wait_send(hb.at[0, pl.ds(0, 3)], mc_s.at[2])
        wait_send(ga, ga_s)

    @pl.when(p == 1)
    def _():
        wait_send(hb.at[0, pl.ds(0, 3)], mc_s.at[4])


def hand_on(*refs):
    srcs, dsts, bufs = refs[:NA], refs[NA:2 * NA], refs[2 * NA:3 * NA]
    sem_in, sem_out = refs[3 * NA:]
    into = [pltpu.make_async_copy(srcs[i], bufs[i], sem_in.at[i]) for i in QUARTERS]
    onto = [pltpu.make_async_copy(bufs[i], dsts[i], sem_out.at[i]) for i in QUARTERS]
    for copy in into:
        copy.start()
    for i in QUARTERS:
        into[i].wait()
        onto[i].start()
    for copy in onto:
        copy.wait()


def solution(mesh):
    act_spec = P(None, "data", None, None)
    w_spec = P(None, "stage", "data", None)

    def body(act_in, cot_out, w_gate, w_in, w_out):
        shape = act_in.shape
        dm, fd = shape[3], w_gate.shape[3]
        rows = shape[0] * shape[1] * shape[2]
        dr, fr, fs = dm // NL, fd // NL, fd // NA
        pf = fs // NA
        vmem = pltpu.VMEM
        dma = pltpu.SemaphoreType.DMA
        n2, n3, na = NB, len(RING), NA
        ring = (na, na)
        scratch = [
            vmem((n2, na, *ring, dr, fd), BF), vmem((n2, na, *ring, dr, fd), BF), vmem((n2, na, *ring, fr, dm), BF),
            vmem((n2, na, rows, dm), BF), vmem((n2, na, rows, dm), BF), vmem((na, rows, dm), BF), vmem((rows, dm), BF),
            vmem((n2, na, rows, dm), BF),
            vmem((n2, rows, fd), F32), vmem((n2, rows, fd), F32),
            vmem((n2, na, rows, fs), F32), vmem((n2, na, rows, fs), F32),
            vmem((n2, na, rows, fs), BF),
            vmem((rows, fd), BF), vmem((rows, fd), BF), vmem((rows, fd), BF),
            vmem((na, rows, fs), BF), vmem((na, rows, fs), BF),
            vmem((rows, dm), F32),
            vmem((dm, fs), BF), vmem((dm, fs), BF), vmem((fs, dm), BF),
            vmem((n2, n2, na, *ring, dr, fs), F32), vmem((n2, *ring, fr, dm), F32),
            vmem((n2, na, n2, dr, fs), F32), vmem((n2, n3, n2, dr, fs), F32),
            dma((n2, na)), dma((n2, n3, n3)), dma((n2, n3, n2, 6)), dma((n2, n3, n3 * na)), dma((5,)), dma((n2, n2, 5)), dma((n2, n2)), dma, dma,
            dma((n2, n2, n2, n2)), dma((n2, n2, n2, n2, 6)), dma((n2,)), dma((n2, n3)), pltpu.SemaphoreType.REGULAR,
            *(vmem((n2, 6, *lead, width), F32)
              for lead_in, lead_out in (((*ring, dr), (n2, fr)), ((na, dr), (fr // n2,)))
              for lead, total in ((lead_in, fs), (lead_out, dm))
              for width in (total - pf, pf)),
        ]
        hbm = pl.BlockSpec(memory_space=pl.ANY)
        whole = pl.BlockSpec(memory_space=pltpu.VMEM)
        out = pl.pallas_call(
            kernel,
            out_shape=(
                jax.ShapeDtypeStruct((rows, dm), BF),
                jax.ShapeDtypeStruct((2, dr, fd), F32), jax.ShapeDtypeStruct((2, dr, fd), F32),
                jax.ShapeDtypeStruct((2, fr, dm), F32),
            ),
            in_specs=[hbm] * 5,
            out_specs=(whole,) * NA,
            scratch_shapes=scratch,
            compiler_params=pltpu.CompilerParams(collective_id=0, has_side_effects=True, vmem_limit_bytes=67043328),
            name="train_step",
        )(act_in.reshape(rows, dm), cot_out.reshape(rows, dm), w_gate[:, 0], w_in[:, 0], w_out[:, 0])
        grad_act, grad_gate, grad_lin, grad_proj = pl.pallas_call(
            hand_on, out_shape=tuple(jax.ShapeDtypeStruct(a.shape, a.dtype) for a in out), in_specs=[hbm] * NA, out_specs=(hbm,) * NA,
            scratch_shapes=[*(vmem(a.shape, a.dtype) for a in out), dma((NA,)), dma((NA,))], name="hand_on",
        )(*out)
        return grad_act.reshape(shape), grad_gate[:, None], grad_lin[:, None], grad_proj[:, None]

    return jax.shard_map(body, mesh=mesh, in_specs=(act_spec, act_spec, w_spec, w_spec, w_spec),
                         out_specs=(act_spec, w_spec, w_spec, w_spec), check_vma=False)
```

```python
import functools

import jax
import jax.numpy as jnp
from jax import lax
from jax.experimental import pallas as pl
from jax.experimental.pallas import tpu as pltpu
from jax.sharding import PartitionSpec as P

NORM_EPS = 1e-6
BF = jnp.bfloat16
F32 = jnp.float32
MESH = pl.DeviceIdType.MESH
X, Y, Z = 0, 1, 2
BLOCKS = COLOURS = HALVES = (0, 1)
NB, NA, NL = len(BLOCKS), 4, 64
RING = (1, 3, 2)
OPP = RING[-1]
PLUS, MINUS = RING[:-1]
QUARTERS = range(NA)
AXES = ((X, Y, Z), (Y, Z, X), (Z, X, Y))


def mm(left, right):
    return jnp.dot(left, right, preferred_element_type=F32)


def mm_nt(left, right):
    return lax.dot_general(left, right, (((1,), (1,)), ((), ())), preferred_element_type=F32)


def mm_tn(left, right):
    return lax.dot_general(left, right, (((0,), (0,)), ((), ())), preferred_element_type=F32)


def inv_rms(h):
    return lax.rsqrt(jnp.mean(h * h, axis=-1, keepdims=True) + NORM_EPS)


def kernel(act, cot, wg_in, wi_in, wo_in, gact, gg, gi, go,
           wg, wi, wo, hb, eb, xo, ga, ng, f1, f2, f1s, f2s, us, ub, da, db, das, dbs, qs, gs, is_, os_,
           gin, gout, fin, r3,
           lsem, ag_s, ag_r, lg_r, mc_s, mc_r, rl_s, ga_s, ga_r, rs_s, rs_r, r3_s, r3_r, turn, *rg):
    dm, fd = wo.shape[-1], wg.shape[-1]
    dr, fr = dm // NL, fd // NL
    fs = fd // NA
    pf = fs // NA
    rows = act.shape[0]
    wts = (wg, wi, wo)

    p = lax.axis_index("stage")
    d = lax.axis_index("data")
    zc, yc, xc = lax.div(d, 16), lax.rem(lax.div(d, 4), 4), lax.rem(d, 4)
    coord = (xc, yc, zc)
    stride = (1, 4, 16)
    ja = yc + p * (zc - yc)
    jb = zc + p * (yc - zc)
    sa, sb = 4 + 12 * p, 16 - 12 * p

    def rot(c, delta):
        return lax.rem(c + (delta % 4), 4)

    def peer(ax, delta):
        return d + (rot(coord[ax], delta) - coord[ax]) * stride[ax]

    def peer_a(delta):
        return d + (rot(ja, delta) - ja) * sa

    def peer_b(delta):
        return d + (rot(jb, delta) - jb) * sb

    def remote(src, dst, ssem, rsem, dev, core):
        return pltpu.make_async_remote_copy(src_ref=src, dst_ref=dst, send_sem=ssem, recv_sem=rsem,
                                            device_id=(dev, core), device_id_type=MESH)

    def send(src, dst, ssem, rsem, dev, core):
        remote(src, dst, ssem, rsem, dev, core).start()

    def wait_recv(ref, sem):
        remote(ref, ref, sem, sem, d, p).wait_recv()

    def wait_send(ref, sem):
        remote(ref, ref, sem, sem, d, p).wait_send()

    for v in BLOCKS:
        for k, shard in enumerate((wg_in, wi_in, wo_in)):
            pltpu.make_async_copy(shard.at[v], wts[k].at[v, zc, yc, xc], lsem.at[v, k]).start()

    @pl.when(p == 0)
    def _():
        pltpu.make_async_copy(act, hb.at[0, ja], lsem.at[0, 3]).start()

    @pl.when(p == 1)
    def _():
        pltpu.make_async_copy(cot, eb.at[1, ja], lsem.at[0, 3]).start()

    barrier = pltpu.get_barrier_semaphore()
    senders = [(peer(ax, delta), p) for ax in (X, Y, Z) for delta in RING]
    senders += [(d, 1 - p), (peer_a(1), 1 - p), (peer_a(-1), 1 - p)]
    for dev, core in senders:
        pl.semaphore_signal(barrier, inc=1, device_id=(dev, core), device_id_type=MESH)
    for v in BLOCKS:
        for k, shard in enumerate((wg_in, wi_in, wo_in)):
            pltpu.make_async_copy(shard.at[v], wts[k].at[v, zc, yc, xc], lsem.at[v, k]).wait()

    @pl.when(p == 0)
    def _():
        pltpu.make_async_copy(act, hb.at[0, ja], lsem.at[0, 3]).wait()

    @pl.when(p == 1)
    def _():
        pltpu.make_async_copy(cot, eb.at[1, ja], lsem.at[0, 3]).wait()

    pl.semaphore_wait(barrier, len(senders))

    FIRST, REST = ((0, PLUS, 0), (1, MINUS, 2)), ((1, PLUS, 1), (0, MINUS, 3))
    LARGE = 2

    def chunk(v, k, ph, q, half):
        if ph == 0:
            width = wts[k].shape[-1] // 2
            ix = tuple(q if ax == AXES[k][0] else coord[ax] for ax in (Z, Y, X)) + (slice(None), pl.ds(half * width, width))
        else:
            hs = pl.ds(2 * half, 2)
            ix = ((zc, q, hs), (q, hs, xc), (hs, yc, q))[k]
        return wts[k].at[(v,) + ix]

    def small_copy(v, k, ph, q, half, delta, slot):
        ref = chunk(v, k, ph, q, half)
        send(ref, ref, ag_s.at[v, k, ph], ag_r.at[v, k, ph, slot], peer(AXES[k][ph], delta), p)

    def small_wait(v, k, ph, back, half, slot):
        wait_recv(chunk(v, k, ph, rot(coord[AXES[k][ph]], back), half), ag_r.at[v, k, ph, slot])

    def small_send(v, ph):
        for half, delta, slot in FIRST + REST:
            for k in (X, Y, Z):
                small_copy(v, k, ph, coord[AXES[k][ph]], half, delta, slot)

    def small_relay(v, ph):
        for half, delta, slot in FIRST:
            for k in (X, Y, Z):
                small_wait(v, k, ph, -delta, half, slot)
                small_copy(v, k, ph, rot(coord[AXES[k][ph]], -delta), half, delta, 4 + half)

    def small_rest(v, ph):
        for half, delta, slot in REST:
            for k in (X, Y, Z):
                small_wait(v, k, ph, -delta, half, slot)

    def small_last(v, ph):
        for half in HALVES:
            for k in (X, Y, Z):
                small_wait(v, k, ph, OPP, half, 4 + half)

    UP, DOWN = (0, PLUS), (MINUS, OPP)
    RELAYS = ((UP[0], PLUS), (DOWN[0], MINUS), (UP[1], PLUS), (DOWN[1], MINUS))

    def row(v, k, q, r):
        m = rot(coord[AXES[k][1]], r)
        ix = ((q, m), (m, slice(None), q), (slice(None), q, m))[k]
        return wts[k].at[(v,) + ix]

    def large_slot(r, delta):
        return r if delta == PLUS else NA + r

    def large_send(v, up, down):
        for pair in zip(up, down):
            for r, delta in zip(pair, (PLUS, MINUS)):
                for k in (X, Y, Z):
                    ax = AXES[k][LARGE]
                    ref = row(v, k, coord[ax], r)
                    send(ref, ref, ag_s.at[v, k, LARGE], lg_r.at[v, k, large_slot(r, delta)], peer(ax, delta), p)

    def large_relay(v):
        for r, delta in RELAYS:
            for k in (X, Y, Z):
                ax = AXES[k][LARGE]
                ref = row(v, k, rot(coord[ax], -delta), r)
                wait_recv(ref, lg_r.at[v, k, large_slot(r, delta)])
                send(ref, ref, ag_s.at[v, k, LARGE], lg_r.at[v, k, 2 * NA + r], peer(ax, delta), p)

    def large_finish(v):
        for pieces, delta in ((DOWN, PLUS), (UP, MINUS)):
            for r in pieces:
                for k in (X, Y, Z):
                    wait_recv(row(v, k, rot(coord[AXES[k][LARGE]], -delta), r), lg_r.at[v, k, large_slot(r, delta)])
        for r in QUARTERS:
            for k in (X, Y, Z):
                wait_recv(row(v, k, rot(coord[AXES[k][LARGE]], OPP), r), lg_r.at[v, k, 2 * NA + r])

    half_rows = rows // 2

    def spread_near(src, buf, which, vd, ssem):
        send(src, buf.at[vd, jb], ssem, mc_r.at[which, vd, 0], d, 1 - p)

    def spread_far(src, buf, which, vd, ssem):
        send(src, buf.at[vd, jb], ssem, mc_r.at[which, vd, 1], peer_b(1), 1 - p)
        send(src, buf.at[vd, jb], ssem, mc_r.at[which, vd, 2], peer_b(-1), 1 - p)

    def spread_same(buf, which, v, ssem):
        own = buf.at[v, ja]
        send(own, own, ssem, mc_r.at[which, v, 1], peer_a(1), p)
        send(own, own, ssem, mc_r.at[which, v, 2], peer_a(-1), p)

    def spread_relay(buf, which, v):
        for half, delta in ((0, 1), (1, 3)):
            slot = rot(ja, -delta)
            wait_recv(buf.at[v, slot], mc_r.at[which, v, 1 + half])
            ref = buf.at[v, slot, pl.ds(half * half_rows, half_rows)]
            send(ref, ref, rl_s.at[which, v], mc_r.at[which, v, 3 + half], peer_a(delta), p)

    def spread_finish(buf, which, v):
        for half in HALVES:
            wait_recv(buf.at[v, rot(ja, 2), pl.ds(half * half_rows, half_rows)], mc_r.at[which, v, 3 + half])

    def spread_own(buf, which, v):
        wait_recv(buf.at[v, ja], mc_r.at[which, v, 0])

    def gates(n, wgt, wlin):
        a, b = mm(n, wgt), mm(n, wlin)
        s = jax.nn.sigmoid(a)
        act_a = a * s
        return (act_a * b).astype(BF), b * s * (1.0 + a * (1.0 - s)), act_a

    def block_gates(v):
        h = hb[v, ja].astype(F32)
        n = (h * inv_rms(h)).astype(BF)

        def tile(i, carry):
            wide = fs // 2
            cols = pl.ds(pl.multiple_of(i * wide, wide), wide)
            u, t1, t2 = gates(n, wg[v, :, :, :, :, cols].reshape(dm, wide), wi[v, :, :, :, :, cols].reshape(dm, wide))
            ub[:, cols] = u
            f1[v, :, cols] = t1
            f2[v, :, cols] = t2
            return carry

        lax.fori_loop(0, 2 * NA, tile, 0, unroll=True)

    def block_out(v, dst):
        half_dm = dm // 2
        for i in HALVES:
            cols = pl.ds(i * half_dm, half_dm)
            out = mm(ub[...], wo[v, :, :, :, :, cols].reshape(fd, half_dm))
            dst[:, cols] = (hb[v, ja, :, cols].astype(F32) + out).astype(BF)

    def block_backward(v, dst):
        e = eb[v, ja]

        def tile(i, carry):
            cols = pl.ds(pl.multiple_of(i * fs, fs), fs)
            t = mm_nt(e, wo[v, i].reshape(fs, dm))
            da[:, cols] = (t * f1[v, :, cols]).astype(BF)
            db[:, cols] = (t * f2[v, :, cols]).astype(BF)
            return carry

        lax.fori_loop(0, NA, tile, 0, unroll=True)
        half_dm = dm // 2
        for i in HALVES:
            q = mm_nt(da[...], wg[v, pl.ds(2 * i, 2)].reshape(half_dm, fd))
            q += mm_nt(db[...], wi[v, pl.ds(2 * i, 2)].reshape(half_dm, fd))
            qs[:, pl.ds(i * half_dm, half_dm)] = q
        h = hb[v, ja].astype(F32)
        r = inv_rms(h)
        hr = h * r
        q = qs[...]
        dst[...] = (e.astype(F32) + r * (q - hr * jnp.mean(q * hr, axis=-1, keepdims=True))).astype(BF)

    def piece(j, i):
        z = i + p * (j - i)
        y = j + p * (i - j)
        return z, y

    def grad_first(v):
        for i in QUARTERS:
            z, y = piece(ja, i)
            cols = pl.ds(pl.multiple_of((z * NA + y) * pf, pf), pf)
            gs[:, pl.ds(i * pf, pf)] = wg[v, :, :, :, :, cols].reshape(dm, pf)
            is_[:, pl.ds(i * pf, pf)] = wi[v, :, :, :, :, cols].reshape(dm, pf)

        def tile(s, carry):
            h = hb[v, s].astype(F32)
            n = (h * inv_rms(h)).astype(BF)
            ng[v, s] = n
            u, t1, t2 = gates(n, gs[...], is_[...])
            us[v, s] = u
            f1s[v, s] = t1
            f2s[v, s] = t2
            return carry

        lax.fori_loop(0, NA, tile, 0, unroll=True)

    def grad_hidden(v):
        for i in QUARTERS:
            z, y = piece(ja, i)
            os_[pl.ds(i * pf, pf), :] = wo[v, z, y].reshape(pf, dm)

        def tile(s, carry):
            t = mm_nt(eb[v, s], os_[...])
            das[s] = (t * f1s[v, s]).astype(BF)
            dbs[s] = (t * f2s[v, s]).astype(BF)
            return carry

        lax.fori_loop(0, NA, tile, 0, unroll=True)

    def grad_out(v):
        def tile(i, carry):
            cols = pl.ds(pl.multiple_of(i * 2 * pf, 2 * pf), 2 * pf)
            g = mm_tn(us[v, :, :, cols].reshape(NA * rows, 2 * pf), eb[v].reshape(NA * rows, dm))
            gout[v, pl.ds(2 * i, 2)] = g.reshape(2, 4, fr, dm)
            return carry

        lax.fori_loop(0, 2, tile, 0, unroll=True)

    def grad_in(v):
        for which, dref in enumerate((das, dbs)):

            def tile(i, carry, which=which, dref=dref):
                cols = pl.ds(pl.multiple_of(i * (dm // NA), dm // NA), dm // NA)
                g = mm_tn(ng[v, :, :, cols].reshape(NA * rows, dm // NA), dref[...].reshape(NA * rows, fs)).reshape(4, 4, dr, fs)

                for y in QUARTERS:
                    gin[v, which, y + p * (i - y), i + p * (y - i)] = g[y]
                return carry

            lax.fori_loop(0, NA, tile, 0, unroll=True)

    IN, OUT = 0, 1

    def split(width):
        return pl.ds(0, width - pf), pl.ds(width - pf, pf)

    def view(which, st, v, colour, t, half):
        along_b = colour == st
        if which == IN:
            cols = split(fs)[colour]
            b, x = (t, slice(None) if st == 0 else xc) if along_b else (slice(None) if st == 0 else jb, t)
            return gin.at[v, half, :, b, x, :, cols]
        cols = split(dm)[colour]
        if st == 0:
            hs = pl.ds(2 * half, 2)
            return gout.at[v, t, hs, :, cols] if along_b else gout.at[v, hs, t, :, cols]
        hs = pl.ds(half * (fr // 2), fr // 2)
        return gout.at[v, t, xc, hs, cols] if along_b else gout.at[v, jb, t, hs, cols]

    RECV = (((rg[0], rg[1]), (rg[2], rg[3])), ((rg[4], rg[5]), (rg[6], rg[7])))
    MERGED, DIRECT = ((0, OPP, PLUS, 0), (1, OPP, MINUS, 1)), ((1, PLUS, PLUS, 2), (0, MINUS, MINUS, 3))
    RELAYED = ((0, PLUS, PLUS, 4), (1, MINUS, MINUS, 5))

    def axis_of(colour, st):
        return (jb, peer_b) if colour == st else (xc, functools.partial(peer, X))

    def scatter_send(v, which, st, copies):
        for colour in COLOURS:
            q, to = axis_of(colour, st)
            for half, c, delta, slot in copies:
                send(view(which, st, v, colour, rot(q, c), half), RECV[st][which][colour].at[v, slot],
                     rs_s.at[st, v, colour, which], rs_r.at[st, v, colour, which, slot], to(delta), p)

    def scatter_relay(v, which, st):
        for colour in COLOURS:
            q, _ = axis_of(colour, st)
            recv = RECV[st][which][colour]
            for half, c, _, slot in RELAYED:
                wait_recv(recv.at[v, slot - 4], rs_r.at[st, v, colour, which, slot - 4])
                ref = view(which, st, v, colour, rot(q, c), half)
                ref[...] = ref[...] + recv[v, slot - 4]
        scatter_send(v, which, st, RELAYED + DIRECT)

    def scatter_sum(v, which, st):
        for colour in COLOURS:
            q, _ = axis_of(colour, st)
            recv = RECV[st][which][colour]
            for half in HALVES:
                direct, merged = 3 - half, 4 + half
                for slot in (direct, merged):
                    wait_recv(recv.at[v, slot], rs_r.at[st, v, colour, which, slot])
                ref = view(which, st, v, colour, q, half)
                ref[...] = ref[...] + recv[v, direct] + recv[v, merged]

    def scatter_turn(v, which):
        scatter_sum(v, which, 0)
        scatter_send(v, which, 1, MERGED)

    def scatter_last(v):
        scatter_sum(v, OUT, 1)
        go[v] = gout[v, jb, xc]
        scatter_sum(v, IN, 1)
        for which in HALVES:
            fin[v, :, which] = gin[v, which, :, jb, xc]
        for delta in RING:
            send(fin.at[v, rot(ja, delta)], r3.at[v, delta - 1], r3_s.at[v], r3_r.at[v, delta - 1], peer_a(delta), p)

    def scatter_finish(v):
        def put(j, vals):
            for i in QUARTERS:
                z, y = piece(j, i)
                cols = pl.ds(pl.multiple_of((z * NA + y) * pf, pf), pf)
                gg[v, :, cols] = vals(0)[:, i * pf:(i + 1) * pf]
                gi[v, :, cols] = vals(1)[:, i * pf:(i + 1) * pf]

        put(ja, lambda w: fin[v, ja, w])
        for delta in RING:
            wait_recv(r3.at[v, delta - 1], r3_r.at[v, delta - 1])
            put(rot(ja, -delta), lambda w, delta=delta: r3[v, delta - 1, w])

    def step(fn, *args):
        with jax.named_scope(fn.__name__):
            fn(*args)

    def on(core):
        return pl.when(p == core)

    def take_turn():
        pl.semaphore_wait(turn, 1)

    def give_turn():
        pl.semaphore_signal(turn, inc=1, device_id=(d, 1 - p), device_id_type=MESH)

    h_mid, h_late, e_first, e_last = ((xo.at[i], mc_s.at[1 + i]) for i in QUARTERS)

    def pass_on(part, item, buf, which, vd):
        step(part, item[0], buf, which, vd, item[1])

    ALL = UP + (MINUS, OPP), DOWN + (0, PLUS)
    for v in BLOCKS:
        step(small_send, v, 0)

    @on(0)
    def _():
        step(spread_same, hb, 0, 0, mc_s.at[0])

    @on(1)
    def _():
        step(spread_same, eb, 1, 1, mc_s.at[0])

    for v in BLOCKS:
        step(small_relay, v, 0)
    step(small_rest, 0, 0)
    step(small_last, 0, 0)
    step(small_send, 0, 1)
    step(large_send, 0, (0,), (0,))
    step(small_rest, 1, 0)
    step(small_last, 1, 0)
    step(small_send, 1, 1)
    step(small_relay, 0, 1)
    step(small_relay, 1, 1)
    step(small_rest, 0, 1)
    step(large_send, 0, (PLUS, MINUS), (MINUS, PLUS))
    step(small_last, 0, 1)
    step(large_send, 0, (OPP,), (OPP,))
    step(small_rest, 1, 1)
    step(small_last, 1, 1)
    step(large_relay, 0)

    @on(0)
    def _():
        step(large_send, 1, *ALL)

    step(large_finish, 0)

    @on(1)
    def _():
        step(take_turn)
        step(large_send, 1, *ALL)
        step(spread_own, hb, 0, 0)

    step(block_gates, 0)
    step(block_out, 0, h_mid[0])
    pass_on(spread_near, h_mid, hb, 0, p)
    step(large_relay, 1)

    @on(0)
    def _():
        step(give_turn)
        step(spread_relay, hb, 0, 0)

    step(large_finish, 1)

    @on(1)
    def _():
        step(spread_relay, hb, 0, 1)
        pass_on(spread_far, h_mid, hb, 0, p)

    step(spread_own, hb, 0, 1)
    step(block_gates, 1)

    @on(0)
    def _():
        step(block_out, 1, h_late[0])
        pass_on(spread_near, h_late, hb, 0, 1)
        pass_on(spread_far, h_late, hb, 0, 1)
        step(spread_finish, hb, 0, 0)
        step(grad_first, 0)
        step(spread_relay, hb, 0, 1)
        step(spread_own, eb, 1, 1)
        step(block_backward, 1, e_first[0])
        pass_on(spread_near, e_first, eb, 1, 0)
        pass_on(spread_far, e_first, eb, 1, 0)
        pass_on(spread_far, h_mid, hb, 0, p)
        step(spread_relay, eb, 1, 1)
        step(spread_finish, hb, 0, 1)
        step(grad_first, 1)

    @on(1)
    def _():
        step(spread_relay, eb, 1, 1)
        step(block_backward, 1, e_first[0])
        pass_on(spread_near, e_first, eb, 1, 1)
        pass_on(spread_far, e_first, eb, 1, 1)
        step(spread_finish, hb, 0, 1)
        step(grad_first, 1)

    step(spread_finish, eb, 1, 1)
    step(grad_hidden, 1)
    step(grad_out, 1)
    step(scatter_send, 1, OUT, 0, MERGED)

    @on(1)
    def _():
        step(spread_own, eb, 1, 0)
        step(block_backward, 0, e_last[0])
        pass_on(spread_near, e_last, eb, 1, 0)
        pass_on(spread_far, e_last, eb, 1, 0)

    step(grad_in, 1)

    @on(0)
    def _():
        step(spread_relay, eb, 1, 0)

    step(scatter_send, 1, IN, 0, MERGED)

    @on(0)
    def _():
        step(spread_own, eb, 1, 0)
        step(block_backward, 0, ga)
        send(ga, ga, ga_s, ga_r, d, 1)

    step(scatter_relay, 1, OUT, 0)

    @on(1)
    def _():
        step(spread_relay, hb, 0, 0)
        step(spread_relay, eb, 1, 0)
        step(spread_finish, hb, 0, 0)
        step(grad_first, 0)

    step(scatter_relay, 1, IN, 0)
    step(spread_finish, eb, 1, 0)
    step(grad_hidden, 0)
    step(grad_out, 0)
    step(scatter_send, 0, OUT, 0, MERGED)
    step(grad_in, 0)
    step(scatter_send, 0, IN, 0, MERGED)
    step(scatter_turn, 1, OUT)
    step(scatter_relay, 0, OUT, 0)
    step(scatter_relay, 0, IN, 0)
    step(scatter_turn, 1, IN)
    step(scatter_turn, 0, OUT)
    step(scatter_relay, 1, OUT, 1)

    @on(1)
    def _():
        wait_recv(ga, ga_r)

    gact[...] = ga[...]
    step(scatter_turn, 0, IN)
    step(scatter_relay, 1, IN, 1)
    step(scatter_relay, 0, OUT, 1)
    step(scatter_relay, 0, IN, 1)
    step(scatter_last, 1)
    step(scatter_last, 0)
    step(scatter_finish, 1)
    step(scatter_finish, 0)

    for v in BLOCKS:
        for k in (X, Y, Z):
            wait_send(wts[k].at[v, 0, 0, pl.ds(0, 3)], ag_s.at[v, k, 0])
            wait_send(wts[k].at[v, 0, pl.ds(0, 3)], ag_s.at[v, k, 1])
            wait_send(wts[k].at[v, pl.ds(0, 3)], ag_s.at[v, k, LARGE])
        for colour in COLOURS:
            for which in HALVES:
                for st in HALVES:
                    wait_send(RECV[st][which][colour].at[v], rs_s.at[st, v, colour, which])
        wait_send(r3.at[v], r3_s.at[v])
        wait_send(hb.at[v, 0], rl_s.at[0, v])
        wait_send(hb.at[v, 0], rl_s.at[1, v])
    wait_send(hb.at[0, pl.ds(0, 2)], mc_s.at[0])
    wait_send(hb.at[0, pl.ds(0, 3)], mc_s.at[1])
    wait_send(hb.at[0, pl.ds(0, 3)], mc_s.at[3])

    @pl.when(p == 0)
    def _():
        wait_send(hb.at[0, pl.ds(0, 3)], mc_s.at[2])
        wait_send(ga, ga_s)

    @pl.when(p == 1)
    def _():
        wait_send(hb.at[0, pl.ds(0, 3)], mc_s.at[4])


def hand_on(*refs):
    srcs, dsts, bufs = refs[:NA], refs[NA:2 * NA], refs[2 * NA:3 * NA]
    sem_in, sem_out = refs[3 * NA:]
    into = [pltpu.make_async_copy(srcs[i], bufs[i], sem_in.at[i]) for i in QUARTERS]
    onto = [pltpu.make_async_copy(bufs[i], dsts[i], sem_out.at[i]) for i in QUARTERS]
    for copy in into:
        copy.start()
    for i in QUARTERS:
        into[i].wait()
        onto[i].start()
    for copy in onto:
        copy.wait()


def solution(mesh):
    act_spec = P(None, "data", None, None)
    w_spec = P(None, "stage", "data", None)

    def body(act_in, cot_out, w_gate, w_in, w_out):
        shape = act_in.shape
        dm, fd = shape[3], w_gate.shape[3]
        rows = shape[0] * shape[1] * shape[2]
        dr, fr, fs = dm // NL, fd // NL, fd // NA
        pf = fs // NA
        vmem = pltpu.VMEM
        dma = pltpu.SemaphoreType.DMA
        n2, n3, na = NB, len(RING), NA
        ring = (na, na)
        scratch = [
            vmem((n2, na, *ring, dr, fd), BF), vmem((n2, na, *ring, dr, fd), BF), vmem((n2, na, *ring, fr, dm), BF),
            vmem((n2, na, rows, dm), BF), vmem((n2, na, rows, dm), BF), vmem((na, rows, dm), BF), vmem((rows, dm), BF),
            vmem((n2, na, rows, dm), BF),
            vmem((n2, rows, fd), F32), vmem((n2, rows, fd), F32),
            vmem((n2, na, rows, fs), F32), vmem((n2, na, rows, fs), F32),
            vmem((n2, na, rows, fs), BF),
            vmem((rows, fd), BF), vmem((rows, fd), BF), vmem((rows, fd), BF),
            vmem((na, rows, fs), BF), vmem((na, rows, fs), BF),
            vmem((rows, dm), F32),
            vmem((dm, fs), BF), vmem((dm, fs), BF), vmem((fs, dm), BF),
            vmem((n2, n2, na, *ring, dr, fs), F32), vmem((n2, *ring, fr, dm), F32),
            vmem((n2, na, n2, dr, fs), F32), vmem((n2, n3, n2, dr, fs), F32),
            dma((n2, na)), dma((n2, n3, n3)), dma((n2, n3, n2, 6)), dma((n2, n3, n3 * na)), dma((5,)), dma((n2, n2, 5)), dma((n2, n2)), dma, dma,
            dma((n2, n2, n2, n2)), dma((n2, n2, n2, n2, 6)), dma((n2,)), dma((n2, n3)), pltpu.SemaphoreType.REGULAR,
            *(vmem((n2, 6, *lead, width), F32)
              for lead_in, lead_out in (((*ring, dr), (n2, fr)), ((na, dr), (fr // n2,)))
              for lead, total in ((lead_in, fs), (lead_out, dm))
              for width in (total - pf, pf)),
        ]
        hbm = pl.BlockSpec(memory_space=pl.ANY)
        whole = pl.BlockSpec(memory_space=pltpu.VMEM)
        out = pl.pallas_call(
            kernel,
            out_shape=(
                jax.ShapeDtypeStruct((rows, dm), BF),
                jax.ShapeDtypeStruct((2, dr, fd), F32), jax.ShapeDtypeStruct((2, dr, fd), F32),
                jax.ShapeDtypeStruct((2, fr, dm), F32),
            ),
            in_specs=[hbm] * 5,
            out_specs=(whole,) * NA,
            scratch_shapes=scratch,
            compiler_params=pltpu.CompilerParams(collective_id=0, has_side_effects=True, vmem_limit_bytes=67043328),
            name="train_step",
        )(act_in.reshape(rows, dm), cot_out.reshape(rows, dm), w_gate[:, 0], w_in[:, 0], w_out[:, 0])
        grad_act, grad_gate, grad_lin, grad_proj = pl.pallas_call(
            hand_on, out_shape=tuple(jax.ShapeDtypeStruct(a.shape, a.dtype) for a in out), in_specs=[hbm] * NA, out_specs=(hbm,) * NA,
            scratch_shapes=[*(vmem(a.shape, a.dtype) for a in out), dma((NA,)), dma((NA,))], name="hand_on",
        )(*out)
        return grad_act.reshape(shape), grad_gate[:, None], grad_lin[:, None], grad_proj[:, None]

    return jax.shard_map(body, mesh=mesh, in_specs=(act_spec, act_spec, w_spec, w_spec, w_spec),
                         out_specs=(act_spec, w_spec, w_spec, w_spec), check_vma=False)
```

```python
import functools

import jax
import jax.numpy as jnp
from jax import lax
from jax.experimental import pallas as pl
from jax.experimental.pallas import tpu as pltpu
from jax.sharding import PartitionSpec as P

NORM_EPS = 1e-6
BF = jnp.bfloat16
F32 = jnp.float32
MESH = pl.DeviceIdType.MESH
X, Y, Z = 0, 1, 2
BLOCKS = COLOURS = HALVES = (0, 1)
NB, NA, NL = len(BLOCKS), 4, 64
RING = (1, 3, 2)
OPP = RING[-1]
PLUS, MINUS = RING[:-1]
QUARTERS = range(NA)
OWN = 0
AXES = ((X, Y, Z), (Y, Z, X), (Z, X, Y))


def mm(left, right):
    return jnp.dot(left, right, preferred_element_type=F32)


def mm_nt(left, right):
    return lax.dot_general(left, right, (((1,), (1,)), ((), ())), preferred_element_type=F32)


def mm_tn(left, right):
    return lax.dot_general(left, right, (((0,), (0,)), ((), ())), preferred_element_type=F32)


def inv_rms(h):
    return lax.rsqrt(jnp.mean(h * h, axis=-1, keepdims=True) + NORM_EPS)


def kernel(act, cot, wg_in, wi_in, wo_in, gact, gg, gi, go,
           wg, wi, wo, hb, eb, xo, ga, ng, f1, f2, f1s, f2s, us, ub, da, db, das, dbs, qs, gs, is_, os_,
           gin, gout, fin, r3,
           lsem, ag_s, ag_r, lg_r, mc_s, mc_r, rl_s, ga_s, ga_r, rs_s, rs_r, r3_s, r3_r, turn, *rg):
    dm, fd = wo.shape[-1], wg.shape[-1]
    dr, fr = dm // NL, fd // NL
    fs = fd // NA
    pf = fs // NA
    rows = act.shape[0]
    wts = (wg, wi, wo)

    p = lax.axis_index("stage")
    d = lax.axis_index("data")
    zc, yc, xc = lax.div(d, 16), lax.rem(lax.div(d, 4), 4), lax.rem(d, 4)
    coord = (xc, yc, zc)
    stride = (1, 4, 16)
    ja = yc + p * (zc - yc)
    jb = zc + p * (yc - zc)
    sa, sb = 4 + 12 * p, 16 - 12 * p

    def rot(c, delta):
        return lax.rem(c + (delta % 4), 4)

    def peer(ax, delta):
        return d + (rot(coord[ax], delta) - coord[ax]) * stride[ax]

    def peer_a(delta):
        return d + (rot(ja, delta) - ja) * sa

    def peer_b(delta):
        return d + (rot(jb, delta) - jb) * sb

    def remote(src, dst, ssem, rsem, dev, core):
        return pltpu.make_async_remote_copy(src_ref=src, dst_ref=dst, send_sem=ssem, recv_sem=rsem,
                                            device_id=(dev, core), device_id_type=MESH)

    def send(src, dst, ssem, rsem, dev, core):
        remote(src, dst, ssem, rsem, dev, core).start()

    def wait_recv(ref, sem):
        remote(ref, ref, sem, sem, d, p).wait_recv()

    def wait_send(ref, sem):
        remote(ref, ref, sem, sem, d, p).wait_send()

    for v in BLOCKS:
        for k, shard in enumerate((wg_in, wi_in, wo_in)):
            pltpu.make_async_copy(shard.at[v], wts[k].at[v, zc, yc, xc], lsem.at[v, k]).start()

    @pl.when(p == 0)
    def _():
        pltpu.make_async_copy(act, hb.at[0, OWN], lsem.at[0, 3]).start()

    @pl.when(p == 1)
    def _():
        pltpu.make_async_copy(cot, eb.at[1, OWN], lsem.at[0, 3]).start()

    barrier = pltpu.get_barrier_semaphore()
    senders = [(peer(ax, delta), p) for ax in (X, Y, Z) for delta in RING]
    senders += [(d, 1 - p), (peer_a(1), 1 - p), (peer_a(-1), 1 - p)]
    for dev, core in senders:
        pl.semaphore_signal(barrier, inc=1, device_id=(dev, core), device_id_type=MESH)
    for v in BLOCKS:
        for k, shard in enumerate((wg_in, wi_in, wo_in)):
            pltpu.make_async_copy(shard.at[v], wts[k].at[v, zc, yc, xc], lsem.at[v, k]).wait()

    @pl.when(p == 0)
    def _():
        pltpu.make_async_copy(act, hb.at[0, OWN], lsem.at[0, 3]).wait()

    @pl.when(p == 1)
    def _():
        pltpu.make_async_copy(cot, eb.at[1, OWN], lsem.at[0, 3]).wait()

    pl.semaphore_wait(barrier, len(senders))

    FIRST, REST = ((0, PLUS, 0), (1, MINUS, 2)), ((1, PLUS, 1), (0, MINUS, 3))
    LARGE = 2

    def chunk(v, k, ph, q, half):
        if ph == 0:
            width = wts[k].shape[-1] // 2
            ix = tuple(q if ax == AXES[k][0] else coord[ax] for ax in (Z, Y, X)) + (slice(None), pl.ds(half * width, width))
        else:
            hs = pl.ds(2 * half, 2)
            ix = ((zc, q, hs), (q, hs, xc), (hs, yc, q))[k]
        return wts[k].at[(v,) + ix]

    def small_copy(v, k, ph, q, half, delta, slot):
        ref = chunk(v, k, ph, q, half)
        send(ref, ref, ag_s.at[v, k, ph], ag_r.at[v, k, ph, slot], peer(AXES[k][ph], delta), p)

    def small_wait(v, k, ph, back, half, slot):
        wait_recv(chunk(v, k, ph, rot(coord[AXES[k][ph]], back), half), ag_r.at[v, k, ph, slot])

    def small_send(v, ph):
        for half, delta, slot in FIRST + REST:
            for k in (X, Y, Z):
                small_copy(v, k, ph, coord[AXES[k][ph]], half, delta, slot)

    def small_relay(v, ph):
        for half, delta, slot in FIRST:
            for k in (X, Y, Z):
                small_wait(v, k, ph, -delta, half, slot)
                small_copy(v, k, ph, rot(coord[AXES[k][ph]], -delta), half, delta, 4 + half)

    def small_rest(v, ph):
        for half, delta, slot in REST:
            for k in (X, Y, Z):
                small_wait(v, k, ph, -delta, half, slot)

    def small_last(v, ph):
        for half in HALVES:
            for k in (X, Y, Z):
                small_wait(v, k, ph, OPP, half, 4 + half)

    UP, DOWN = (0, PLUS), (MINUS, OPP)
    RELAYS = ((UP[0], PLUS), (DOWN[0], MINUS), (UP[1], PLUS), (DOWN[1], MINUS))

    def row(v, k, q, r):
        m = rot(coord[AXES[k][1]], r)
        ix = ((q, m), (m, slice(None), q), (slice(None), q, m))[k]
        return wts[k].at[(v,) + ix]

    def large_slot(r, delta):
        return r if delta == PLUS else NA + r

    def large_send(v, up, down):
        for pair in zip(up, down):
            for r, delta in zip(pair, (PLUS, MINUS)):
                for k in (X, Y, Z):
                    ax = AXES[k][LARGE]
                    ref = row(v, k, coord[ax], r)
                    send(ref, ref, ag_s.at[v, k, LARGE], lg_r.at[v, k, large_slot(r, delta)], peer(ax, delta), p)

    def large_relay(v):
        for r, delta in RELAYS:
            for k in (X, Y, Z):
                ax = AXES[k][LARGE]
                ref = row(v, k, rot(coord[ax], -delta), r)
                wait_recv(ref, lg_r.at[v, k, large_slot(r, delta)])
                send(ref, ref, ag_s.at[v, k, LARGE], lg_r.at[v, k, 2 * NA + r], peer(ax, delta), p)

    def large_finish(v):
        for pieces, delta in ((DOWN, PLUS), (UP, MINUS)):
            for r in pieces:
                for k in (X, Y, Z):
                    wait_recv(row(v, k, rot(coord[AXES[k][LARGE]], -delta), r), lg_r.at[v, k, large_slot(r, delta)])
        for r in QUARTERS:
            for k in (X, Y, Z):
                wait_recv(row(v, k, rot(coord[AXES[k][LARGE]], OPP), r), lg_r.at[v, k, 2 * NA + r])

    half_rows = rows // 2
    BACK, AHEAD, FAR = 1, 2, 3

    def spread_near(src, buf, which, vd, ssem):
        send(src, buf.at[vd, OWN], ssem, mc_r.at[which, vd, OWN], d, 1 - p)

    def spread_far(src, buf, which, vd, ssem):
        send(src, buf.at[vd, BACK], ssem, mc_r.at[which, vd, BACK], peer_b(PLUS), 1 - p)
        send(src, buf.at[vd, AHEAD], ssem, mc_r.at[which, vd, AHEAD], peer_b(MINUS), 1 - p)

    def spread_same(buf, which, v, ssem):
        send(buf.at[v, OWN], buf.at[v, BACK], ssem, mc_r.at[which, v, BACK], peer_a(PLUS), p)
        send(buf.at[v, OWN], buf.at[v, AHEAD], ssem, mc_r.at[which, v, AHEAD], peer_a(MINUS), p)

    def spread_relay(buf, which, v):
        for half, slot, delta in ((0, BACK, PLUS), (1, AHEAD, MINUS)):
            wait_recv(buf.at[v, slot], mc_r.at[which, v, slot])
            part = pl.ds(half * half_rows, half_rows)
            send(buf.at[v, slot, part], buf.at[v, FAR, part], rl_s.at[which, v], mc_r.at[which, v, FAR + half], peer_a(delta), p)

    def spread_finish(buf, which, v):
        for half in HALVES:
            wait_recv(buf.at[v, FAR, pl.ds(half * half_rows, half_rows)], mc_r.at[which, v, FAR + half])

    def spread_own(buf, which, v):
        wait_recv(buf.at[v, OWN], mc_r.at[which, v, OWN])

    def gates(n, wgt, wlin):
        a, b = mm(n, wgt), mm(n, wlin)
        s = jax.nn.sigmoid(a)
        act_a = a * s
        return (act_a * b).astype(BF), b * s * (1.0 + a * (1.0 - s)), act_a

    def block_gates(v):
        h = hb[v, OWN].astype(F32)
        n = (h * inv_rms(h)).astype(BF)

        def tile(i, carry):
            wide = fs // 2
            cols = pl.ds(pl.multiple_of(i * wide, wide), wide)
            u, t1, t2 = gates(n, wg[v, :, :, :, :, cols].reshape(dm, wide), wi[v, :, :, :, :, cols].reshape(dm, wide))
            ub[:, cols] = u
            f1[v, :, cols] = t1
            f2[v, :, cols] = t2
            return carry

        lax.fori_loop(0, 2 * NA, tile, 0, unroll=True)

    def block_out(v, dst):
        half_dm = dm // 2
        for i in HALVES:
            cols = pl.ds(i * half_dm, half_dm)
            out = mm(ub[...], wo[v, :, :, :, :, cols].reshape(fd, half_dm))
            dst[:, cols] = (hb[v, OWN, :, cols].astype(F32) + out).astype(BF)

    def block_backward(v, dst):
        e = eb[v, OWN]

        def tile(i, carry):
            cols = pl.ds(pl.multiple_of(i * fs, fs), fs)
            t = mm_nt(e, wo[v, i].reshape(fs, dm))
            da[:, cols] = (t * f1[v, :, cols]).astype(BF)
            db[:, cols] = (t * f2[v, :, cols]).astype(BF)
            return carry

        lax.fori_loop(0, NA, tile, 0, unroll=True)
        half_dm = dm // 2
        for i in HALVES:
            q = mm_nt(da[...], wg[v, pl.ds(2 * i, 2)].reshape(half_dm, fd))
            q += mm_nt(db[...], wi[v, pl.ds(2 * i, 2)].reshape(half_dm, fd))
            qs[:, pl.ds(i * half_dm, half_dm)] = q
        h = hb[v, OWN].astype(F32)
        r = inv_rms(h)
        hr = h * r
        q = qs[...]
        dst[...] = (e.astype(F32) + r * (q - hr * jnp.mean(q * hr, axis=-1, keepdims=True))).astype(BF)

    def piece(j, i):
        z = i + p * (j - i)
        y = j + p * (i - j)
        return z, y

    EARLY, LATE = range(FAR), range(FAR, NA)

    def grad_first(v, slots):
        for i in QUARTERS if OWN in slots else ():
            z, y = piece(ja, i)
            cols = pl.ds(pl.multiple_of((z * NA + y) * pf, pf), pf)
            gs[v, :, pl.ds(i * pf, pf)] = wg[v, :, :, :, :, cols].reshape(dm, pf)
            is_[v, :, pl.ds(i * pf, pf)] = wi[v, :, :, :, :, cols].reshape(dm, pf)
        for s in slots:
            h = hb[v, s].astype(F32)
            n = (h * inv_rms(h)).astype(BF)
            ng[v, s] = n
            u, t1, t2 = gates(n, gs[v], is_[v])
            us[v, s] = u
            f1s[v, s] = t1
            f2s[v, s] = t2

    def grad_hidden(v, slots):
        for i in QUARTERS if OWN in slots else ():
            z, y = piece(ja, i)
            os_[pl.ds(i * pf, pf), :] = wo[v, z, y].reshape(pf, dm)
        for s in slots:
            t = mm_nt(eb[v, s], os_[...])
            das[s] = (t * f1s[v, s]).astype(BF)
            dbs[s] = (t * f2s[v, s]).astype(BF)

    def rows_of(slots):
        return pl.ds(slots[0], len(slots)), len(slots) * rows

    def grad_out(v, slots):
        some, count = rows_of(slots)
        for i in HALVES:
            cols, to = pl.ds(i * 2 * pf, 2 * pf), pl.ds(2 * i, 2)
            g = mm_tn(us[v, some, :, cols].reshape(count, 2 * pf), eb[v, some].reshape(count, dm)).reshape(2, 4, fr, dm)
            gout[v, to] = g if OWN in slots else gout[v, to] + g

    def grad_in(v, slots):
        some, count = rows_of(slots)
        for which, dref in enumerate((das, dbs)):
            for i in QUARTERS:
                cols = pl.ds(i * (dm // NA), dm // NA)
                g = mm_tn(ng[v, some, :, cols].reshape(count, dm // NA), dref[some].reshape(count, fs)).reshape(4, 4, dr, fs)
                for y in QUARTERS:
                    at = (v, which, y + p * (i - y), i + p * (y - i))
                    gin[at] = g[y] if OWN in slots else gin[at] + g[y]

    IN, OUT = 0, 1

    def split(width):
        return pl.ds(0, width - pf), pl.ds(width - pf, pf)

    def view(which, st, v, colour, t, half):
        along_b = colour == st
        if which == IN:
            cols = split(fs)[colour]
            b, x = (t, slice(None) if st == 0 else xc) if along_b else (slice(None) if st == 0 else jb, t)
            return gin.at[v, half, :, b, x, :, cols]
        cols = pl.ds(colour * (dm // 2), dm // 2)
        if st == 0:
            hs = pl.ds(2 * half, 2)
            return gout.at[v, t, hs, :, cols] if along_b else gout.at[v, hs, t, :, cols]
        hs = pl.ds(half * (fr // 2), fr // 2)
        return gout.at[v, t, xc, hs, cols] if along_b else gout.at[v, jb, t, hs, cols]

    RECV = (((rg[0], rg[1]), (rg[2], rg[3])), ((rg[4], rg[5]), (rg[6], rg[7])))
    MERGED, DIRECT = ((0, OPP, PLUS, 0), (1, OPP, MINUS, 1)), ((1, PLUS, PLUS, 2), (0, MINUS, MINUS, 3))
    RELAYED = ((0, PLUS, PLUS, 4), (1, MINUS, MINUS, 5))

    def axis_of(colour, st):
        return (jb, peer_b) if colour == st else (xc, functools.partial(peer, X))

    def scatter_send(v, which, st, copies):
        for colour in COLOURS:
            q, to = axis_of(colour, st)
            for half, c, delta, slot in copies:
                send(view(which, st, v, colour, rot(q, c), half), RECV[st][which][colour].at[v, slot],
                     rs_s.at[st, v, colour, which], rs_r.at[st, v, colour, which, slot], to(delta), p)

    def scatter_relay(v, which, st):
        for colour in COLOURS:
            q, _ = axis_of(colour, st)
            recv = RECV[st][which][colour]
            for half, c, _, slot in RELAYED:
                wait_recv(recv.at[v, slot - 4], rs_r.at[st, v, colour, which, slot - 4])
                ref = view(which, st, v, colour, rot(q, c), half)
                ref[...] = ref[...] + recv[v, slot - 4]
        scatter_send(v, which, st, RELAYED)

    def scatter_sum(v, which, st):
        for colour in COLOURS:
            q, _ = axis_of(colour, st)
            recv = RECV[st][which][colour]
            for half in HALVES:
                direct, merged = 3 - half, 4 + half
                for slot in (direct, merged):
                    wait_recv(recv.at[v, slot], rs_r.at[st, v, colour, which, slot])
                ref = view(which, st, v, colour, q, half)
                ref[...] = ref[...] + recv[v, direct] + recv[v, merged]

    def scatter_turn(v, which):
        scatter_sum(v, which, 0)
        scatter_send(v, which, 1, MERGED + DIRECT)

    def scatter_last(v):
        scatter_sum(v, OUT, 1)
        go[v] = gout[v, jb, xc]
        scatter_sum(v, IN, 1)
        for which in HALVES:
            fin[v, :, which] = gin[v, which, :, jb, xc]
        for delta in RING:
            send(fin.at[v, rot(ja, delta)], r3.at[v, delta - 1], r3_s.at[v], r3_r.at[v, delta - 1], peer_a(delta), p)

    def scatter_finish(v):
        def put(j, vals):
            for i in QUARTERS:
                z, y = piece(j, i)
                cols = pl.ds(pl.multiple_of((z * NA + y) * pf, pf), pf)
                gg[v, :, cols] = vals(0)[:, i * pf:(i + 1) * pf]
                gi[v, :, cols] = vals(1)[:, i * pf:(i + 1) * pf]

        put(ja, lambda w: fin[v, ja, w])
        for delta in RING:
            wait_recv(r3.at[v, delta - 1], r3_r.at[v, delta - 1])
            put(rot(ja, -delta), lambda w, delta=delta: r3[v, delta - 1, w])

    def step(fn, *args):
        with jax.named_scope(fn.__name__):
            fn(*args)

    def on(core):
        return pl.when(p == core)

    def take_turn():
        pl.semaphore_wait(turn, 1)

    def give_turn():
        pl.semaphore_signal(turn, inc=1, device_id=(d, 1 - p), device_id_type=MESH)

    h_mid, h_late, e_first, e_last = ((xo.at[i], mc_s.at[1 + i]) for i in QUARTERS)

    def pass_on(part, item, buf, which, vd):
        step(part, item[0], buf, which, vd, item[1])

    ALL = UP + (MINUS, OPP), DOWN + (0, PLUS)
    for v in BLOCKS:
        step(small_send, v, 0)

    @on(0)
    def _():
        step(spread_same, hb, 0, 0, mc_s.at[0])

    @on(1)
    def _():
        step(spread_same, eb, 1, 1, mc_s.at[0])

    for v in BLOCKS:
        step(small_relay, v, 0)
    step(small_rest, 0, 0)
    step(small_last, 0, 0)
    step(small_send, 0, 1)
    step(large_send, 0, (0,), (0,))
    step(small_rest, 1, 0)
    step(small_last, 1, 0)
    step(small_send, 1, 1)
    step(small_relay, 0, 1)
    step(small_relay, 1, 1)
    step(small_rest, 0, 1)
    step(large_send, 0, (PLUS, MINUS), (MINUS, PLUS))
    step(small_last, 0, 1)
    step(large_send, 0, (OPP,), (OPP,))
    step(small_rest, 1, 1)
    step(small_last, 1, 1)
    step(large_relay, 0)

    @on(0)
    def _():
        step(large_send, 1, *ALL)

    step(large_finish, 0)

    @on(1)
    def _():
        step(take_turn)
        step(large_send, 1, *ALL)
        step(spread_own, hb, 0, 0)

    step(block_gates, 0)
    step(block_out, 0, h_mid[0])
    pass_on(spread_near, h_mid, hb, 0, p)
    step(large_relay, 1)

    @on(0)
    def _():
        step(give_turn)
        step(spread_relay, hb, 0, 0)

    step(large_finish, 1)

    @on(1)
    def _():
        step(give_turn)
        step(spread_relay, hb, 0, 1)
        pass_on(spread_far, h_mid, hb, 0, p)

    step(spread_own, hb, 0, 1)
    step(block_gates, 1)

    @on(0)
    def _():
        step(block_out, 1, h_late[0])
        pass_on(spread_near, h_late, hb, 0, 1)
        pass_on(spread_far, h_late, hb, 0, 1)
        step(spread_finish, hb, 0, 0)
        step(grad_first, 0, EARLY)
        step(grad_first, 0, LATE)
        step(take_turn)
        pass_on(spread_far, h_mid, hb, 0, p)
        step(spread_relay, hb, 0, 1)
        step(spread_own, eb, 1, 1)
        step(block_backward, 1, e_first[0])
        pass_on(spread_near, e_first, eb, 1, 0)
        pass_on(spread_far, e_first, eb, 1, 0)

    @on(1)
    def _():
        step(spread_relay, eb, 1, 1)
        step(block_backward, 1, e_first[0])
        pass_on(spread_near, e_first, eb, 1, 1)
        pass_on(spread_far, e_first, eb, 1, 1)

    step(grad_first, 1, EARLY)

    @on(0)
    def _():
        step(spread_relay, eb, 1, 1)

    step(grad_hidden, 1, EARLY)
    step(grad_out, 1, EARLY)

    @on(0)
    def _():
        step(grad_in, 1, EARLY)

    step(spread_finish, hb, 0, 1)
    step(grad_first, 1, LATE)

    @on(0)
    def _():
        step(spread_own, eb, 1, 0)
        step(block_backward, 0, ga)
        send(ga, ga, ga_s, ga_r, d, 1)

    step(spread_finish, eb, 1, 1)
    step(grad_hidden, 1, LATE)
    step(grad_out, 1, LATE)
    step(scatter_send, 1, OUT, 0, MERGED)

    @on(1)
    def _():
        step(spread_relay, hb, 0, 0)
        step(grad_first, 0, EARLY)
        step(spread_own, eb, 1, 0)
        step(block_backward, 0, e_last[0])
        pass_on(spread_near, e_last, eb, 1, 0)
        pass_on(spread_far, e_last, eb, 1, 0)
        step(grad_in, 1, EARLY)

    step(grad_in, 1, LATE)
    step(scatter_send, 1, IN, 0, MERGED)
    step(scatter_send, 1, OUT, 0, DIRECT)
    step(spread_relay, eb, 1, 0)

    @on(1)
    def _():
        step(spread_finish, hb, 0, 0)
        step(grad_first, 0, LATE)

    step(grad_hidden, 0, EARLY)
    step(scatter_send, 1, IN, 0, DIRECT)
    step(grad_out, 0, EARLY)
    step(scatter_relay, 1, OUT, 0)
    step(grad_in, 0, EARLY)
    step(spread_finish, eb, 1, 0)
    step(grad_hidden, 0, LATE)
    step(grad_out, 0, LATE)
    step(scatter_send, 0, OUT, 0, MERGED)
    step(grad_in, 0, LATE)
    step(scatter_send, 0, IN, 0, MERGED)
    step(scatter_relay, 1, IN, 0)
    step(scatter_send, 0, OUT, 0, DIRECT)
    step(scatter_turn, 1, OUT)
    step(scatter_send, 0, IN, 0, DIRECT)
    step(scatter_relay, 0, OUT, 0)
    step(scatter_turn, 1, IN)
    step(scatter_relay, 0, IN, 0)
    step(scatter_relay, 1, OUT, 1)

    @on(1)
    def _():
        wait_recv(ga, ga_r)

    gact[...] = ga[...]
    step(scatter_turn, 0, OUT)
    step(scatter_relay, 1, IN, 1)
    step(scatter_turn, 0, IN)
    step(scatter_relay, 0, OUT, 1)
    step(scatter_last, 1)
    step(scatter_relay, 0, IN, 1)
    step(scatter_last, 0)
    step(scatter_finish, 1)
    step(scatter_finish, 0)

    for v in BLOCKS:
        for k in (X, Y, Z):
            wait_send(wts[k].at[v, 0, 0, pl.ds(0, 3)], ag_s.at[v, k, 0])
            wait_send(wts[k].at[v, 0, pl.ds(0, 3)], ag_s.at[v, k, 1])
            wait_send(wts[k].at[v, pl.ds(0, 3)], ag_s.at[v, k, LARGE])
        for colour in COLOURS:
            for which in HALVES:
                for st in HALVES:
                    wait_send(RECV[st][which][colour].at[v], rs_s.at[st, v, colour, which])
        wait_send(r3.at[v], r3_s.at[v])
        wait_send(hb.at[v, 0], rl_s.at[0, v])
        wait_send(hb.at[v, 0], rl_s.at[1, v])
    wait_send(hb.at[0, pl.ds(0, 2)], mc_s.at[0])
    wait_send(hb.at[0, pl.ds(0, 3)], mc_s.at[1])
    wait_send(hb.at[0, pl.ds(0, 3)], mc_s.at[3])

    @pl.when(p == 0)
    def _():
        wait_send(hb.at[0, pl.ds(0, 3)], mc_s.at[2])
        wait_send(ga, ga_s)

    @pl.when(p == 1)
    def _():
        wait_send(hb.at[0, pl.ds(0, 3)], mc_s.at[4])


def hand_on(*refs):
    srcs, dsts, bufs = refs[:NA], refs[NA:2 * NA], refs[2 * NA:3 * NA]
    sem_in, sem_out = refs[3 * NA:]
    into = [pltpu.make_async_copy(srcs[i], bufs[i], sem_in.at[i]) for i in QUARTERS]
    onto = [pltpu.make_async_copy(bufs[i], dsts[i], sem_out.at[i]) for i in QUARTERS]
    for copy in into:
        copy.start()
    for i in QUARTERS:
        into[i].wait()
        onto[i].start()
    for copy in onto:
        copy.wait()


def solution(mesh):
    act_spec = P(None, "data", None, None)
    w_spec = P(None, "stage", "data", None)

    def body(act_in, cot_out, w_gate, w_in, w_out):
        shape = act_in.shape
        dm, fd = shape[3], w_gate.shape[3]
        rows = shape[0] * shape[1] * shape[2]
        dr, fr, fs = dm // NL, fd // NL, fd // NA
        pf = fs // NA
        vmem = pltpu.VMEM
        dma = pltpu.SemaphoreType.DMA
        n2, n3, na = NB, len(RING), NA
        ring = (na, na)
        scratch = [
            vmem((n2, na, *ring, dr, fd), BF), vmem((n2, na, *ring, dr, fd), BF), vmem((n2, na, *ring, fr, dm), BF),
            vmem((n2, na, rows, dm), BF), vmem((n2, na, rows, dm), BF), vmem((na, rows, dm), BF), vmem((rows, dm), BF),
            vmem((n2, na, rows, dm), BF),
            vmem((n2, rows, fd), F32), vmem((n2, rows, fd), F32),
            vmem((n2, na, rows, fs), F32), vmem((n2, na, rows, fs), F32),
            vmem((n2, na, rows, fs), BF),
            vmem((rows, fd), BF), vmem((rows, fd), BF), vmem((rows, fd), BF),
            vmem((na, rows, fs), BF), vmem((na, rows, fs), BF),
            vmem((rows, dm), F32),
            vmem((n2, dm, fs), BF), vmem((n2, dm, fs), BF), vmem((fs, dm), BF),
            vmem((n2, n2, na, *ring, dr, fs), F32), vmem((n2, *ring, fr, dm), F32),
            vmem((n2, na, n2, dr, fs), F32), vmem((n2, n3, n2, dr, fs), F32),
            dma((n2, na)), dma((n2, n3, n3)), dma((n2, n3, n2, 6)), dma((n2, n3, n3 * na)), dma((5,)), dma((n2, n2, 5)), dma((n2, n2)), dma, dma,
            dma((n2, n2, n2, n2)), dma((n2, n2, n2, n2, 6)), dma((n2,)), dma((n2, n3)), pltpu.SemaphoreType.REGULAR,
            *(vmem((n2, 6, *lead, width), F32)
              for lead_in, lead_out in (((*ring, dr), (n2, fr)), ((na, dr), (fr // n2,)))
              for lead, width in ((lead_in, fs - pf), (lead_in, pf), (lead_out, dm // n2), (lead_out, dm // n2))),
        ]
        hbm = pl.BlockSpec(memory_space=pl.ANY)
        whole = pl.BlockSpec(memory_space=pltpu.VMEM)
        out = pl.pallas_call(
            kernel,
            out_shape=(
                jax.ShapeDtypeStruct((rows, dm), BF),
                jax.ShapeDtypeStruct((2, dr, fd), F32), jax.ShapeDtypeStruct((2, dr, fd), F32),
                jax.ShapeDtypeStruct((2, fr, dm), F32),
            ),
            in_specs=[hbm] * 5,
            out_specs=(whole,) * NA,
            scratch_shapes=scratch,
            compiler_params=pltpu.CompilerParams(collective_id=0, has_side_effects=True, vmem_limit_bytes=67043328),
            name="train_step",
        )(act_in.reshape(rows, dm), cot_out.reshape(rows, dm), w_gate[:, 0], w_in[:, 0], w_out[:, 0])
        grad_act, grad_gate, grad_lin, grad_proj = pl.pallas_call(
            hand_on, out_shape=tuple(jax.ShapeDtypeStruct(a.shape, a.dtype) for a in out), in_specs=[hbm] * NA, out_specs=(hbm,) * NA,
            scratch_shapes=[*(vmem(a.shape, a.dtype) for a in out), dma((NA,)), dma((NA,))], name="hand_on",
        )(*out)
        return grad_act.reshape(shape), grad_gate[:, None], grad_lin[:, None], grad_proj[:, None]

    return jax.shard_map(body, mesh=mesh, in_specs=(act_spec, act_spec, w_spec, w_spec, w_spec),
                         out_specs=(act_spec, w_spec, w_spec, w_spec), check_vma=False)
```

```python
import functools

import jax
import jax.numpy as jnp
from jax import lax
from jax.experimental import pallas as pl
from jax.experimental.pallas import tpu as pltpu
from jax.sharding import PartitionSpec as P

NORM_EPS = 1e-6
BF = jnp.bfloat16
F32 = jnp.float32
MESH = pl.DeviceIdType.MESH
X, Y, Z = 0, 1, 2
BLOCKS = COLOURS = HALVES = (0, 1)
NB, NA, NL = len(BLOCKS), 4, 64
RING = (1, 3, 2)
OPP = RING[-1]
PLUS, MINUS = RING[:-1]
QUARTERS = range(NA)
OWN = 0
AXES = ((X, Y, Z), (Y, Z, X), (Z, X, Y))


def mm(left, right):
    return jnp.dot(left, right, preferred_element_type=F32)


def mm_nt(left, right):
    return lax.dot_general(left, right, (((1,), (1,)), ((), ())), preferred_element_type=F32)


def mm_tn(left, right):
    return lax.dot_general(left, right, (((0,), (0,)), ((), ())), preferred_element_type=F32)


def inv_rms(h):
    return lax.rsqrt(jnp.mean(h * h, axis=-1, keepdims=True) + NORM_EPS)


def kernel(act, cot, wg_in, wi_in, wo_in, gact, gg, gi, go,
           wg, wi, wo, hb, eb, xo, ga, ng, f1, f2, f1s, f2s, us, ub, da, db, das, dbs, qs, gs, is_, os_,
           gin, gout, fin, r3,
           lsem, ag_s, ag_r, lg_r, mc_s, mc_r, rl_s, ga_s, ga_r, rs_s, rs_r, r3_s, r3_r, turn, *rg):
    dm, fd = wo.shape[-1], wg.shape[-1]
    dr, fr = dm // NL, fd // NL
    fs = fd // NA
    pf = fs // NA
    rows = act.shape[0]
    wts = (wg, wi, wo)

    p = lax.axis_index("stage")
    d = lax.axis_index("data")
    zc, yc, xc = lax.div(d, 16), lax.rem(lax.div(d, 4), 4), lax.rem(d, 4)
    coord = (xc, yc, zc)
    stride = (1, 4, 16)
    ja = yc + p * (zc - yc)
    jb = zc + p * (yc - zc)
    sa, sb = 4 + 12 * p, 16 - 12 * p

    def rot(c, delta):
        return lax.rem(c + (delta % 4), 4)

    def peer(ax, delta):
        return d + (rot(coord[ax], delta) - coord[ax]) * stride[ax]

    def peer_a(delta):
        return d + (rot(ja, delta) - ja) * sa

    def peer_b(delta):
        return d + (rot(jb, delta) - jb) * sb

    def remote(src, dst, ssem, rsem, dev, core):
        return pltpu.make_async_remote_copy(src_ref=src, dst_ref=dst, send_sem=ssem, recv_sem=rsem,
                                            device_id=(dev, core), device_id_type=MESH)

    def send(src, dst, ssem, rsem, dev, core):
        remote(src, dst, ssem, rsem, dev, core).start()

    def wait_recv(ref, sem):
        remote(ref, ref, sem, sem, d, p).wait_recv()

    def wait_send(ref, sem):
        remote(ref, ref, sem, sem, d, p).wait_send()

    for v in BLOCKS:
        for k, shard in enumerate((wg_in, wi_in, wo_in)):
            pltpu.make_async_copy(shard.at[v], wts[k].at[v, zc, yc, xc], lsem.at[v, k]).start()

    @pl.when(p == 0)
    def _():
        pltpu.make_async_copy(act, hb.at[0, OWN], lsem.at[0, 3]).start()

    @pl.when(p == 1)
    def _():
        pltpu.make_async_copy(cot, eb.at[1, OWN], lsem.at[0, 3]).start()

    barrier = pltpu.get_barrier_semaphore()
    senders = [(peer(ax, delta), p) for ax in (X, Y, Z) for delta in RING]
    senders += [(d, 1 - p), (peer_a(1), 1 - p), (peer_a(-1), 1 - p)]
    for dev, core in senders:
        pl.semaphore_signal(barrier, inc=1, device_id=(dev, core), device_id_type=MESH)
    for v in BLOCKS:
        for k, shard in enumerate((wg_in, wi_in, wo_in)):
            pltpu.make_async_copy(shard.at[v], wts[k].at[v, zc, yc, xc], lsem.at[v, k]).wait()

    @pl.when(p == 0)
    def _():
        pltpu.make_async_copy(act, hb.at[0, OWN], lsem.at[0, 3]).wait()

    @pl.when(p == 1)
    def _():
        pltpu.make_async_copy(cot, eb.at[1, OWN], lsem.at[0, 3]).wait()

    pl.semaphore_wait(barrier, len(senders))

    FIRST, REST = ((0, PLUS, 0), (1, MINUS, 2)), ((1, PLUS, 1), (0, MINUS, 3))
    LARGE = 2

    def chunk(v, k, ph, q, half):
        if ph == 0:
            width = wts[k].shape[-1] // 2
            ix = tuple(q if ax == AXES[k][0] else coord[ax] for ax in (Z, Y, X)) + (slice(None), pl.ds(half * width, width))
        else:
            hs = pl.ds(2 * half, 2)
            ix = ((zc, q, hs), (q, hs, xc), (hs, yc, q))[k]
        return wts[k].at[(v,) + ix]

    def small_copy(v, k, ph, q, half, delta, slot):
        ref = chunk(v, k, ph, q, half)
        send(ref, ref, ag_s.at[v, k, ph], ag_r.at[v, k, ph, slot], peer(AXES[k][ph], delta), p)

    def small_wait(v, k, ph, back, half, slot):
        wait_recv(chunk(v, k, ph, rot(coord[AXES[k][ph]], back), half), ag_r.at[v, k, ph, slot])

    def small_send(v, ph):
        for half, delta, slot in FIRST + REST:
            for k in (X, Y, Z):
                small_copy(v, k, ph, coord[AXES[k][ph]], half, delta, slot)

    def small_relay(v, ph):
        for half, delta, slot in FIRST:
            for k in (X, Y, Z):
                small_wait(v, k, ph, -delta, half, slot)
                small_copy(v, k, ph, rot(coord[AXES[k][ph]], -delta), half, delta, 4 + half)

    def small_rest(v, ph):
        for half, delta, slot in REST:
            for k in (X, Y, Z):
                small_wait(v, k, ph, -delta, half, slot)

    def small_last(v, ph):
        for half in HALVES:
            for k in (X, Y, Z):
                small_wait(v, k, ph, OPP, half, 4 + half)

    UP, DOWN = (0, PLUS), (MINUS, OPP)
    RELAYS = ((UP[0], PLUS), (DOWN[0], MINUS), (UP[1], PLUS), (DOWN[1], MINUS))

    def row(v, k, q, r):
        m = rot(coord[AXES[k][1]], r)
        ix = ((q, m), (m, slice(None), q), (slice(None), q, m))[k]
        return wts[k].at[(v,) + ix]

    def large_slot(r, delta):
        return r if delta == PLUS else NA + r

    def large_send(v, up, down):
        for pair in zip(up, down):
            for r, delta in zip(pair, (PLUS, MINUS)):
                for k in (X, Y, Z):
                    ax = AXES[k][LARGE]
                    ref = row(v, k, coord[ax], r)
                    send(ref, ref, ag_s.at[v, k, LARGE], lg_r.at[v, k, large_slot(r, delta)], peer(ax, delta), p)

    def large_relay(v):
        for r, delta in RELAYS:
            for k in (X, Y, Z):
                ax = AXES[k][LARGE]
                ref = row(v, k, rot(coord[ax], -delta), r)
                wait_recv(ref, lg_r.at[v, k, large_slot(r, delta)])
                send(ref, ref, ag_s.at[v, k, LARGE], lg_r.at[v, k, 2 * NA + r], peer(ax, delta), p)

    def large_finish(v):
        for pieces, delta in ((DOWN, PLUS), (UP, MINUS)):
            for r in pieces:
                for k in (X, Y, Z):
                    wait_recv(row(v, k, rot(coord[AXES[k][LARGE]], -delta), r), lg_r.at[v, k, large_slot(r, delta)])
        for r in QUARTERS:
            for k in (X, Y, Z):
                wait_recv(row(v, k, rot(coord[AXES[k][LARGE]], OPP), r), lg_r.at[v, k, 2 * NA + r])

    half_rows = rows // 2
    BACK, AHEAD, FAR = 1, 2, 3

    def spread_near(src, buf, which, vd, ssem):
        send(src, buf.at[vd, OWN], ssem, mc_r.at[which, vd, OWN], d, 1 - p)

    def spread_far(src, buf, which, vd, ssem):
        send(src, buf.at[vd, BACK], ssem, mc_r.at[which, vd, BACK], peer_b(PLUS), 1 - p)
        send(src, buf.at[vd, AHEAD], ssem, mc_r.at[which, vd, AHEAD], peer_b(MINUS), 1 - p)

    def spread_same(buf, which, v, ssem):
        send(buf.at[v, OWN], buf.at[v, BACK], ssem, mc_r.at[which, v, BACK], peer_a(PLUS), p)
        send(buf.at[v, OWN], buf.at[v, AHEAD], ssem, mc_r.at[which, v, AHEAD], peer_a(MINUS), p)

    def spread_relay(buf, which, v):
        for half, slot, delta in ((0, BACK, PLUS), (1, AHEAD, MINUS)):
            wait_recv(buf.at[v, slot], mc_r.at[which, v, slot])
            part = pl.ds(half * half_rows, half_rows)
            send(buf.at[v, slot, part], buf.at[v, FAR, part], rl_s.at[which, v], mc_r.at[which, v, FAR + half], peer_a(delta), p)

    def spread_finish(buf, which, v):
        for half in HALVES:
            wait_recv(buf.at[v, FAR, pl.ds(half * half_rows, half_rows)], mc_r.at[which, v, FAR + half])

    def spread_own(buf, which, v):
        wait_recv(buf.at[v, OWN], mc_r.at[which, v, OWN])

    def gates(n, wgt, wlin):
        a, b = mm(n, wgt), mm(n, wlin)
        s = jax.nn.sigmoid(a)
        act_a = a * s
        return (act_a * b).astype(BF), b * s * (1.0 + a * (1.0 - s)), act_a

    def block_gates(v):
        h = hb[v, OWN].astype(F32)
        n = (h * inv_rms(h)).astype(BF)

        def tile(i, carry):
            wide = fs // 2
            cols = pl.ds(pl.multiple_of(i * wide, wide), wide)
            u, t1, t2 = gates(n, wg[v, :, :, :, :, cols].reshape(dm, wide), wi[v, :, :, :, :, cols].reshape(dm, wide))
            ub[:, cols] = u
            f1[v, :, cols] = t1
            f2[v, :, cols] = t2
            return carry

        lax.fori_loop(0, 2 * NA, tile, 0, unroll=True)

    def block_out(v, dst):
        half_dm = dm // 2
        for i in HALVES:
            cols = pl.ds(i * half_dm, half_dm)
            out = mm(ub[...], wo[v, :, :, :, :, cols].reshape(fd, half_dm))
            dst[:, cols] = (hb[v, OWN, :, cols].astype(F32) + out).astype(BF)

    def block_backward(v, dst):
        e = eb[v, OWN]

        def tile(i, carry):
            cols = pl.ds(pl.multiple_of(i * fs, fs), fs)
            t = mm_nt(e, wo[v, i].reshape(fs, dm))
            da[:, cols] = (t * f1[v, :, cols]).astype(BF)
            db[:, cols] = (t * f2[v, :, cols]).astype(BF)
            return carry

        lax.fori_loop(0, NA, tile, 0, unroll=True)
        half_dm = dm // 2
        for i in HALVES:
            q = mm_nt(da[...], wg[v, pl.ds(2 * i, 2)].reshape(half_dm, fd))
            q += mm_nt(db[...], wi[v, pl.ds(2 * i, 2)].reshape(half_dm, fd))
            qs[:, pl.ds(i * half_dm, half_dm)] = q
        h = hb[v, OWN].astype(F32)
        r = inv_rms(h)
        hr = h * r
        q = qs[...]
        dst[...] = (e.astype(F32) + r * (q - hr * jnp.mean(q * hr, axis=-1, keepdims=True))).astype(BF)

    def piece(j, i):
        z = i + p * (j - i)
        y = j + p * (i - j)
        return z, y

    EARLY, LATE = range(FAR), range(FAR, NA)

    def grad_first(v, slots):
        for i in QUARTERS if OWN in slots else ():
            z, y = piece(ja, i)
            cols = pl.ds(pl.multiple_of((z * NA + y) * pf, pf), pf)
            gs[v, :, pl.ds(i * pf, pf)] = wg[v, :, :, :, :, cols].reshape(dm, pf)
            is_[v, :, pl.ds(i * pf, pf)] = wi[v, :, :, :, :, cols].reshape(dm, pf)
        for s in slots:
            h = hb[v, s].astype(F32)
            n = (h * inv_rms(h)).astype(BF)
            ng[v, s] = n
            u, t1, t2 = gates(n, gs[v], is_[v])
            us[v, s] = u
            f1s[v, s] = t1
            f2s[v, s] = t2

    def grad_hidden(v, slots):
        for i in QUARTERS if OWN in slots else ():
            z, y = piece(ja, i)
            os_[pl.ds(i * pf, pf), :] = wo[v, z, y].reshape(pf, dm)
        for s in slots:
            t = mm_nt(eb[v, s], os_[...])
            das[s] = (t * f1s[v, s]).astype(BF)
            dbs[s] = (t * f2s[v, s]).astype(BF)

    def rows_of(slots):
        return pl.ds(slots[0], len(slots)), len(slots) * rows

    def grad_out(v, slots):
        some, count = rows_of(slots)
        for i in HALVES:
            cols, to = pl.ds(i * 2 * pf, 2 * pf), pl.ds(2 * i, 2)
            g = mm_tn(us[v, some, :, cols].reshape(count, 2 * pf), eb[v, some].reshape(count, dm)).reshape(2, 4, fr, dm)
            gout[v, to] = g if OWN in slots else gout[v, to] + g

    def grad_in(v, slots):
        some, count = rows_of(slots)
        for which, dref in enumerate((das, dbs)):
            for i in QUARTERS:
                cols = pl.ds(i * (dm // NA), dm // NA)
                g = mm_tn(ng[v, some, :, cols].reshape(count, dm // NA), dref[some].reshape(count, fs)).reshape(4, 4, dr, fs)
                for y in QUARTERS:
                    at = (v, which, y + p * (i - y), i + p * (y - i))
                    gin[at] = g[y] if OWN in slots else gin[at] + g[y]

    IN, OUT = 0, 1

    def split(width):
        return pl.ds(0, width - pf), pl.ds(width - pf, pf)

    def view(which, st, v, colour, t, half):
        along_b = colour == st
        if which == IN:
            cols = split(fs)[colour]
            b, x = (t, slice(None) if st == 0 else xc) if along_b else (slice(None) if st == 0 else jb, t)
            return gin.at[v, half, :, b, x, :, cols]
        cols = pl.ds(colour * (dm // 2), dm // 2)
        if st == 0:
            hs = pl.ds(2 * half, 2)
            return gout.at[v, t, hs, :, cols] if along_b else gout.at[v, hs, t, :, cols]
        hs = pl.ds(half * (fr // 2), fr // 2)
        return gout.at[v, t, xc, hs, cols] if along_b else gout.at[v, jb, t, hs, cols]

    RECV = (((rg[0], rg[1]), (rg[2], rg[3])), ((rg[4], rg[5]), (rg[6], rg[7])))
    MERGED, DIRECT = ((0, OPP, PLUS, 0), (1, OPP, MINUS, 1)), ((1, PLUS, PLUS, 2), (0, MINUS, MINUS, 3))
    RELAYED = ((0, PLUS, PLUS, 4), (1, MINUS, MINUS, 5))

    def axis_of(colour, st):
        return (jb, peer_b) if colour == st else (xc, functools.partial(peer, X))

    def scatter_send(v, which, st, copies):
        for colour in COLOURS:
            q, to = axis_of(colour, st)
            for half, c, delta, slot in copies:
                send(view(which, st, v, colour, rot(q, c), half), RECV[st][which][colour].at[v, slot],
                     rs_s.at[st, v, colour, which], rs_r.at[st, v, colour, which, slot], to(delta), p)

    def scatter_relay(v, which, st):
        for colour in COLOURS:
            q, _ = axis_of(colour, st)
            recv = RECV[st][which][colour]
            for half, c, _, slot in RELAYED:
                wait_recv(recv.at[v, slot - 4], rs_r.at[st, v, colour, which, slot - 4])
                ref = view(which, st, v, colour, rot(q, c), half)
                ref[...] = ref[...] + recv[v, slot - 4]
        scatter_send(v, which, st, RELAYED)

    def scatter_sum(v, which, st):
        for colour in COLOURS:
            q, _ = axis_of(colour, st)
            recv = RECV[st][which][colour]
            for half in HALVES:
                direct, merged = 3 - half, 4 + half
                for slot in (direct, merged):
                    wait_recv(recv.at[v, slot], rs_r.at[st, v, colour, which, slot])
                ref = view(which, st, v, colour, q, half)
                ref[...] = ref[...] + recv[v, direct] + recv[v, merged]

    def scatter_turn(v, which):
        scatter_sum(v, which, 0)
        scatter_send(v, which, 1, MERGED + DIRECT)

    def scatter_last(v):
        scatter_sum(v, OUT, 1)
        go[v] = gout[v, jb, xc]
        scatter_sum(v, IN, 1)
        for which in HALVES:
            fin[v, :, which] = gin[v, which, :, jb, xc]
        for delta in (OPP, PLUS, MINUS):
            send(fin.at[v, rot(ja, delta)], r3.at[v, delta - 1], r3_s.at[v], r3_r.at[v, delta - 1], peer_a(delta), p)

    def scatter_finish(v):
        def put(j, vals):
            for i in QUARTERS:
                z, y = piece(j, i)
                cols = pl.ds(pl.multiple_of((z * NA + y) * pf, pf), pf)
                gg[v, :, cols] = vals(0)[:, i * pf:(i + 1) * pf]
                gi[v, :, cols] = vals(1)[:, i * pf:(i + 1) * pf]

        put(ja, lambda w: fin[v, ja, w])
        for delta in RING:
            wait_recv(r3.at[v, delta - 1], r3_r.at[v, delta - 1])
            put(rot(ja, -delta), lambda w, delta=delta: r3[v, delta - 1, w])

    def step(fn, *args):
        with jax.named_scope(fn.__name__):
            fn(*args)

    def on(core):
        return pl.when(p == core)

    def take_turn():
        pl.semaphore_wait(turn, 1)

    def give_turn():
        pl.semaphore_signal(turn, inc=1, device_id=(d, 1 - p), device_id_type=MESH)

    h_mid, h_late, e_first, e_last = ((xo.at[i], mc_s.at[1 + i]) for i in QUARTERS)

    def pass_on(part, item, buf, which, vd):
        step(part, item[0], buf, which, vd, item[1])

    ALL = UP + (MINUS, OPP), DOWN + (0, PLUS)
    for v in BLOCKS:
        step(small_send, v, 0)

    @on(0)
    def _():
        step(spread_same, hb, 0, 0, mc_s.at[0])

    @on(1)
    def _():
        step(spread_same, eb, 1, 1, mc_s.at[0])

    for v in BLOCKS:
        step(small_relay, v, 0)
    step(small_rest, 0, 0)
    step(small_last, 0, 0)
    step(small_send, 0, 1)
    step(large_send, 0, (0,), (0,))
    step(small_rest, 1, 0)
    step(small_last, 1, 0)
    step(small_send, 1, 1)
    step(small_relay, 0, 1)
    step(small_relay, 1, 1)
    step(small_rest, 0, 1)
    step(large_send, 0, (PLUS, MINUS), (MINUS, PLUS))
    step(small_last, 0, 1)
    step(large_send, 0, (OPP,), (OPP,))
    step(small_rest, 1, 1)
    step(small_last, 1, 1)
    step(large_relay, 0)

    @on(0)
    def _():
        step(large_send, 1, *ALL)

    step(large_finish, 0)

    @on(1)
    def _():
        step(take_turn)
        step(large_send, 1, *ALL)
        step(spread_own, hb, 0, 0)

    step(block_gates, 0)
    step(block_out, 0, h_mid[0])
    pass_on(spread_near, h_mid, hb, 0, p)
    step(large_relay, 1)

    @on(0)
    def _():
        step(give_turn)
        step(spread_relay, hb, 0, 0)

    step(large_finish, 1)

    @on(1)
    def _():
        step(give_turn)
        pass_on(spread_far, h_mid, hb, 0, p)

    step(spread_own, hb, 0, 1)
    step(block_gates, 1)

    @on(0)
    def _():
        step(block_out, 1, h_late[0])
        pass_on(spread_near, h_late, hb, 0, 1)
        pass_on(spread_far, h_late, hb, 0, 1)
        step(spread_finish, hb, 0, 0)
        step(grad_first, 0, EARLY)
        step(grad_first, 0, LATE)
        step(take_turn)
        pass_on(spread_far, h_mid, hb, 0, p)
        step(spread_own, eb, 1, 1)
        step(block_backward, 1, e_first[0])
        pass_on(spread_near, e_first, eb, 1, 0)
        pass_on(spread_far, e_first, eb, 1, 0)
        step(spread_relay, hb, 0, 1)

    @on(1)
    def _():
        step(spread_relay, hb, 0, 1)
        step(spread_relay, eb, 1, 1)
        step(block_backward, 1, e_first[0])
        pass_on(spread_near, e_first, eb, 1, 1)
        pass_on(spread_far, e_first, eb, 1, 1)

    step(grad_first, 1, EARLY)

    @on(0)
    def _():
        step(spread_relay, eb, 1, 1)

    @on(1)
    def _():
        step(spread_relay, hb, 0, 0)

    step(grad_hidden, 1, EARLY)
    step(grad_out, 1, EARLY)

    @on(0)
    def _():
        step(grad_in, 1, EARLY)

    step(spread_finish, hb, 0, 1)
    step(grad_first, 1, LATE)
    step(spread_finish, eb, 1, 1)
    step(grad_hidden, 1, LATE)
    step(grad_out, 1, LATE)
    step(scatter_send, 1, OUT, 0, MERGED)

    @on(1)
    def _():
        step(spread_own, eb, 1, 0)
        step(block_backward, 0, e_last[0])
        pass_on(spread_near, e_last, eb, 1, 0)
        pass_on(spread_far, e_last, eb, 1, 0)
        step(grad_in, 1, EARLY)

    step(grad_in, 1, LATE)
    step(scatter_send, 1, IN, 0, MERGED)

    @on(0)
    def _():
        step(spread_own, eb, 1, 0)
        step(block_backward, 0, ga)
        send(ga, ga, ga_s, ga_r, d, 1)

    @on(1)
    def _():
        step(grad_first, 0, EARLY)

    step(scatter_send, 1, OUT, 0, DIRECT)
    step(spread_relay, eb, 1, 0)

    @on(1)
    def _():
        step(spread_finish, hb, 0, 0)
        step(grad_first, 0, LATE)

    step(grad_hidden, 0, EARLY)
    step(scatter_send, 1, IN, 0, DIRECT)
    step(grad_out, 0, EARLY)
    step(scatter_relay, 1, OUT, 0)
    step(grad_in, 0, EARLY)
    step(spread_finish, eb, 1, 0)
    step(grad_hidden, 0, LATE)
    step(grad_out, 0, LATE)
    step(scatter_send, 0, OUT, 0, MERGED)
    step(grad_in, 0, LATE)
    step(scatter_send, 0, IN, 0, MERGED)
    step(scatter_relay, 1, IN, 0)
    step(scatter_send, 0, OUT, 0, DIRECT)
    step(scatter_turn, 1, OUT)
    step(scatter_send, 0, IN, 0, DIRECT)
    step(scatter_relay, 0, OUT, 0)
    step(scatter_turn, 1, IN)
    step(scatter_relay, 0, IN, 0)
    step(scatter_relay, 1, OUT, 1)

    @on(1)
    def _():
        wait_recv(ga, ga_r)

    gact[...] = ga[...]
    step(scatter_turn, 0, OUT)
    step(scatter_relay, 1, IN, 1)
    step(scatter_turn, 0, IN)
    step(scatter_relay, 0, OUT, 1)
    step(scatter_last, 1)
    step(scatter_relay, 0, IN, 1)
    step(scatter_last, 0)
    step(scatter_finish, 1)
    step(scatter_finish, 0)

    for v in BLOCKS:
        for k in (X, Y, Z):
            wait_send(wts[k].at[v, 0, 0, pl.ds(0, 3)], ag_s.at[v, k, 0])
            wait_send(wts[k].at[v, 0, pl.ds(0, 3)], ag_s.at[v, k, 1])
            wait_send(wts[k].at[v, pl.ds(0, 3)], ag_s.at[v, k, LARGE])
        for colour in COLOURS:
            for which in HALVES:
                for st in HALVES:
                    wait_send(RECV[st][which][colour].at[v], rs_s.at[st, v, colour, which])
        wait_send(r3.at[v], r3_s.at[v])
        wait_send(hb.at[v, 0], rl_s.at[0, v])
        wait_send(hb.at[v, 0], rl_s.at[1, v])
    wait_send(hb.at[0, pl.ds(0, 2)], mc_s.at[0])
    wait_send(hb.at[0, pl.ds(0, 3)], mc_s.at[1])
    wait_send(hb.at[0, pl.ds(0, 3)], mc_s.at[3])

    @pl.when(p == 0)
    def _():
        wait_send(hb.at[0, pl.ds(0, 3)], mc_s.at[2])
        wait_send(ga, ga_s)

    @pl.when(p == 1)
    def _():
        wait_send(hb.at[0, pl.ds(0, 3)], mc_s.at[4])


def hand_on(*refs):
    copies = [pltpu.make_async_copy(refs[i], refs[NA + i], refs[-1].at[i]) for i in QUARTERS]
    for copy in copies:
        copy.start()
    for copy in copies:
        copy.wait()


def solution(mesh):
    act_spec = P(None, "data", None, None)
    w_spec = P(None, "stage", "data", None)

    def body(act_in, cot_out, w_gate, w_in, w_out):
        shape = act_in.shape
        dm, fd = shape[3], w_gate.shape[3]
        rows = shape[0] * shape[1] * shape[2]
        dr, fr, fs = dm // NL, fd // NL, fd // NA
        pf = fs // NA
        vmem = pltpu.VMEM
        dma = pltpu.SemaphoreType.DMA
        n2, n3, na = NB, len(RING), NA
        ring = (na, na)
        scratch = [
            vmem((n2, na, *ring, dr, fd), BF), vmem((n2, na, *ring, dr, fd), BF), vmem((n2, na, *ring, fr, dm), BF),
            vmem((n2, na, rows, dm), BF), vmem((n2, na, rows, dm), BF), vmem((na, rows, dm), BF), vmem((rows, dm), BF),
            vmem((n2, na, rows, dm), BF),
            vmem((n2, rows, fd), F32), vmem((n2, rows, fd), F32),
            vmem((n2, na, rows, fs), F32), vmem((n2, na, rows, fs), F32),
            vmem((n2, na, rows, fs), BF),
            vmem((rows, fd), BF), vmem((rows, fd), BF), vmem((rows, fd), BF),
            vmem((na, rows, fs), BF), vmem((na, rows, fs), BF),
            vmem((rows, dm), F32),
            vmem((n2, dm, fs), BF), vmem((n2, dm, fs), BF), vmem((fs, dm), BF),
            vmem((n2, n2, na, *ring, dr, fs), F32), vmem((n2, *ring, fr, dm), F32),
            vmem((n2, na, n2, dr, fs), F32), vmem((n2, n3, n2, dr, fs), F32),
            dma((n2, na)), dma((n2, n3, n3)), dma((n2, n3, n2, 6)), dma((n2, n3, n3 * na)), dma((5,)), dma((n2, n2, 5)), dma((n2, n2)), dma, dma,
            dma((n2, n2, n2, n2)), dma((n2, n2, n2, n2, 6)), dma((n2,)), dma((n2, n3)), pltpu.SemaphoreType.REGULAR,
            *(vmem((n2, 6, *lead, width), F32)
              for lead_in, lead_out in (((*ring, dr), (n2, fr)), ((na, dr), (fr // n2,)))
              for lead, width in ((lead_in, fs - pf), (lead_in, pf), (lead_out, dm // n2), (lead_out, dm // n2))),
        ]
        hbm = pl.BlockSpec(memory_space=pl.ANY)
        whole = pl.BlockSpec(memory_space=pltpu.VMEM)
        out = pl.pallas_call(
            kernel,
            out_shape=(
                vmem((rows, dm), BF), vmem((n2, dr, fd), F32), vmem((n2, dr, fd), F32), vmem((n2, fr, dm), F32),
            ),
            in_specs=[hbm] * 5,
            out_specs=(whole,) * NA,
            scratch_shapes=scratch,
            compiler_params=pltpu.CompilerParams(collective_id=0, has_side_effects=True, vmem_limit_bytes=66300000),
            name="train_step",
        )(act_in.reshape(rows, dm), cot_out.reshape(rows, dm), w_gate[:, 0], w_in[:, 0], w_out[:, 0])
        grad_act, grad_gate, grad_lin, grad_proj = pl.pallas_call(
            hand_on, out_shape=tuple(jax.ShapeDtypeStruct(a.shape, a.dtype) for a in out), in_specs=[whole] * NA, out_specs=(hbm,) * NA,
            scratch_shapes=[dma((NA,))], compiler_params=pltpu.CompilerParams(vmem_limit_bytes=2 ** 20), name="hand_on",
        )(*(pltpu.with_memory_space_constraint(a, vmem) for a in out))
        return grad_act.reshape(shape), grad_gate[:, None], grad_lin[:, None], grad_proj[:, None]

    return jax.shard_map(body, mesh=mesh, in_specs=(act_spec, act_spec, w_spec, w_spec, w_spec),
                         out_specs=(act_spec, w_spec, w_spec, w_spec), check_vma=False)
```

```python
import functools

import jax
import jax.numpy as jnp
from jax import lax
from jax.experimental import pallas as pl
from jax.experimental.pallas import tpu as pltpu
from jax.sharding import PartitionSpec as P

NORM_EPS = 1e-6
BF = jnp.bfloat16
F32 = jnp.float32
MESH = pl.DeviceIdType.MESH
X, Y, Z = 0, 1, 2
BLOCKS = COLOURS = HALVES = (0, 1)
NB, NA, NL = len(BLOCKS), 4, 64
RING = (1, 3, 2)
OPP = RING[-1]
PLUS, MINUS = RING[:-1]
QUARTERS = range(NA)
OWN = 0
AXES = ((X, Y, Z), (Y, Z, X), (Z, X, Y))


def mm(left, right):
    return jnp.dot(left, right, preferred_element_type=F32)


def mm_nt(left, right):
    return lax.dot_general(left, right, (((1,), (1,)), ((), ())), preferred_element_type=F32)


def mm_tn(left, right):
    return lax.dot_general(left, right, (((0,), (0,)), ((), ())), preferred_element_type=F32)


def inv_rms(h):
    return lax.rsqrt(jnp.mean(h * h, axis=-1, keepdims=True) + NORM_EPS)


def kernel(act, cot, wg_in, wi_in, wo_in, gact, gg, gi, go,
           wg, wi, wo, hb, eb, xo, ga, ng, f1, f2, f1s, f2s, us, ub, da, db, das, dbs, qs, gs, is_, os_,
           gin, gout, fin, r3,
           lsem, ag_s, ag_r, lg_r, mc_s, mc_r, rl_s, ga_s, ga_r, rs_s, rs_r, r3_s, r3_r, turn, *rg):
    dm, fd = wo.shape[-1], wg.shape[-1]
    dr, fr = dm // NL, fd // NL
    fs = fd // NA
    pf = fs // NA
    rows = act.shape[0]
    wts = (wg, wi, wo)

    p = lax.axis_index("stage")
    d = lax.axis_index("data")
    zc, yc, xc = lax.div(d, 16), lax.rem(lax.div(d, 4), 4), lax.rem(d, 4)
    coord = (xc, yc, zc)
    stride = (1, 4, 16)
    ja = yc + p * (zc - yc)
    jb = zc + p * (yc - zc)
    sa, sb = 4 + 12 * p, 16 - 12 * p

    def rot(c, delta):
        return lax.rem(c + (delta % 4), 4)

    def peer(ax, delta):
        return d + (rot(coord[ax], delta) - coord[ax]) * stride[ax]

    def peer_a(delta):
        return d + (rot(ja, delta) - ja) * sa

    def peer_b(delta):
        return d + (rot(jb, delta) - jb) * sb

    def remote(src, dst, ssem, rsem, dev, core):
        return pltpu.make_async_remote_copy(src_ref=src, dst_ref=dst, send_sem=ssem, recv_sem=rsem,
                                            device_id=(dev, core), device_id_type=MESH)

    def send(src, dst, ssem, rsem, dev, core):
        remote(src, dst, ssem, rsem, dev, core).start()

    def wait_recv(ref, sem):
        remote(ref, ref, sem, sem, d, p).wait_recv()

    def wait_send(ref, sem):
        remote(ref, ref, sem, sem, d, p).wait_send()

    for v in BLOCKS:
        for k, shard in enumerate((wg_in, wi_in, wo_in)):
            pltpu.make_async_copy(shard.at[v], wts[k].at[v, zc, yc, xc], lsem.at[v, k]).start()

    @pl.when(p == 0)
    def _():
        pltpu.make_async_copy(act, hb.at[0, OWN], lsem.at[0, 3]).start()

    @pl.when(p == 1)
    def _():
        pltpu.make_async_copy(cot, eb.at[1, OWN], lsem.at[0, 3]).start()

    barrier = pltpu.get_barrier_semaphore()
    senders = [(peer(ax, delta), p) for ax in (X, Y, Z) for delta in RING]
    senders += [(d, 1 - p), (peer_a(1), 1 - p), (peer_a(-1), 1 - p)]
    for dev, core in senders:
        pl.semaphore_signal(barrier, inc=1, device_id=(dev, core), device_id_type=MESH)
    for v in BLOCKS:
        for k, shard in enumerate((wg_in, wi_in, wo_in)):
            pltpu.make_async_copy(shard.at[v], wts[k].at[v, zc, yc, xc], lsem.at[v, k]).wait()

    @pl.when(p == 0)
    def _():
        pltpu.make_async_copy(act, hb.at[0, OWN], lsem.at[0, 3]).wait()

    @pl.when(p == 1)
    def _():
        pltpu.make_async_copy(cot, eb.at[1, OWN], lsem.at[0, 3]).wait()

    pl.semaphore_wait(barrier, len(senders))

    FIRST, REST = ((0, PLUS, 0), (1, MINUS, 2)), ((1, PLUS, 1), (0, MINUS, 3))
    LARGE = 2

    def chunk(v, k, ph, q, half):
        if ph == 0:
            width = wts[k].shape[-1] // 2
            ix = tuple(q if ax == AXES[k][0] else coord[ax] for ax in (Z, Y, X)) + (slice(None), pl.ds(half * width, width))
        else:
            hs = pl.ds(2 * half, 2)
            ix = ((zc, q, hs), (q, hs, xc), (hs, yc, q))[k]
        return wts[k].at[(v,) + ix]

    def small_copy(v, k, ph, q, half, delta, slot):
        ref = chunk(v, k, ph, q, half)
        send(ref, ref, ag_s.at[v, k, ph], ag_r.at[v, k, ph, slot], peer(AXES[k][ph], delta), p)

    def small_wait(v, k, ph, back, half, slot):
        wait_recv(chunk(v, k, ph, rot(coord[AXES[k][ph]], back), half), ag_r.at[v, k, ph, slot])

    def small_send(v, ph):
        for half, delta, slot in FIRST + REST:
            for k in (X, Y, Z):
                small_copy(v, k, ph, coord[AXES[k][ph]], half, delta, slot)

    def small_relay(v, ph):
        for half, delta, slot in FIRST:
            for k in (X, Y, Z):
                small_wait(v, k, ph, -delta, half, slot)
                small_copy(v, k, ph, rot(coord[AXES[k][ph]], -delta), half, delta, 4 + half)

    def small_rest(v, ph):
        for half, delta, slot in REST:
            for k in (X, Y, Z):
                small_wait(v, k, ph, -delta, half, slot)

    def small_last(v, ph):
        for half in HALVES:
            for k in (X, Y, Z):
                small_wait(v, k, ph, OPP, half, 4 + half)

    def direct_send(v):
        for delta in (OPP, PLUS, MINUS):
            for k in (X, Y, Z):
                own = wts[k].at[v, zc, yc, xc]
                send(own, own, ag_s.at[v, k, 0], ag_r.at[v, k, 0, delta], peer(AXES[k][0], delta), p)

    def direct_wait(v):
        for delta in RING:
            for k in (X, Y, Z):
                at = tuple(rot(coord[ax], -delta) if ax == AXES[k][0] else coord[ax] for ax in (Z, Y, X))
                wait_recv(wts[k].at[(v,) + at], ag_r.at[v, k, 0, delta])

    UP, DOWN = (0, PLUS), (MINUS, OPP)
    RELAYS = ((UP[0], PLUS), (DOWN[0], MINUS), (UP[1], PLUS), (DOWN[1], MINUS))

    def row(v, k, q, r):
        m = rot(coord[AXES[k][1]], r)
        ix = ((q, m), (m, slice(None), q), (slice(None), q, m))[k]
        return wts[k].at[(v,) + ix]

    def large_slot(r, delta):
        return r if delta == PLUS else NA + r

    def large_send(v, up, down):
        for pair in zip(up, down):
            for r, delta in zip(pair, (PLUS, MINUS)):
                for k in (X, Y, Z):
                    ax = AXES[k][LARGE]
                    ref = row(v, k, coord[ax], r)
                    send(ref, ref, ag_s.at[v, k, LARGE], lg_r.at[v, k, large_slot(r, delta)], peer(ax, delta), p)

    def large_relay(v):
        for r, delta in RELAYS:
            for k in (X, Y, Z):
                ax = AXES[k][LARGE]
                ref = row(v, k, rot(coord[ax], -delta), r)
                wait_recv(ref, lg_r.at[v, k, large_slot(r, delta)])
                send(ref, ref, ag_s.at[v, k, LARGE], lg_r.at[v, k, 2 * NA + r], peer(ax, delta), p)

    def large_finish(v):
        for pieces, delta in ((DOWN, PLUS), (UP, MINUS)):
            for r in pieces:
                for k in (X, Y, Z):
                    wait_recv(row(v, k, rot(coord[AXES[k][LARGE]], -delta), r), lg_r.at[v, k, large_slot(r, delta)])
        for r in QUARTERS:
            for k in (X, Y, Z):
                wait_recv(row(v, k, rot(coord[AXES[k][LARGE]], OPP), r), lg_r.at[v, k, 2 * NA + r])

    half_rows = rows // 2
    BACK, AHEAD, FAR = 1, 2, 3

    def spread_near(src, buf, which, vd, ssem):
        send(src, buf.at[vd, OWN], ssem, mc_r.at[which, vd, OWN], d, 1 - p)

    def spread_far(src, buf, which, vd, ssem):
        send(src, buf.at[vd, BACK], ssem, mc_r.at[which, vd, BACK], peer_b(PLUS), 1 - p)
        send(src, buf.at[vd, AHEAD], ssem, mc_r.at[which, vd, AHEAD], peer_b(MINUS), 1 - p)

    def spread_same(buf, which, v, ssem):
        send(buf.at[v, OWN], buf.at[v, BACK], ssem, mc_r.at[which, v, BACK], peer_a(PLUS), p)
        send(buf.at[v, OWN], buf.at[v, AHEAD], ssem, mc_r.at[which, v, AHEAD], peer_a(MINUS), p)

    def spread_relay(buf, which, v):
        for half, slot, delta in ((0, BACK, PLUS), (1, AHEAD, MINUS)):
            wait_recv(buf.at[v, slot], mc_r.at[which, v, slot])
            part = pl.ds(half * half_rows, half_rows)
            send(buf.at[v, slot, part], buf.at[v, FAR, part], rl_s.at[which, v], mc_r.at[which, v, FAR + half], peer_a(delta), p)

    def spread_finish(buf, which, v):
        for half in HALVES:
            wait_recv(buf.at[v, FAR, pl.ds(half * half_rows, half_rows)], mc_r.at[which, v, FAR + half])

    def spread_own(buf, which, v):
        wait_recv(buf.at[v, OWN], mc_r.at[which, v, OWN])

    def gates(n, wgt, wlin):
        a, b = mm(n, wgt), mm(n, wlin)
        s = jax.nn.sigmoid(a)
        act_a = a * s
        return (act_a * b).astype(BF), b * s * (1.0 + a * (1.0 - s)), act_a

    def block_gates(v):
        h = hb[v, OWN].astype(F32)
        n = (h * inv_rms(h)).astype(BF)

        def tile(i, carry):
            wide = fs // 2
            cols = pl.ds(pl.multiple_of(i * wide, wide), wide)
            u, t1, t2 = gates(n, wg[v, :, :, :, :, cols].reshape(dm, wide), wi[v, :, :, :, :, cols].reshape(dm, wide))
            ub[:, cols] = u
            f1[v, :, cols] = t1
            f2[v, :, cols] = t2
            return carry

        lax.fori_loop(0, 2 * NA, tile, 0, unroll=True)

    def block_out(v, dst):
        half_dm = dm // 2
        for i in HALVES:
            cols = pl.ds(i * half_dm, half_dm)
            out = mm(ub[...], wo[v, :, :, :, :, cols].reshape(fd, half_dm))
            dst[:, cols] = (hb[v, OWN, :, cols].astype(F32) + out).astype(BF)

    def block_backward(v, dst):
        e = eb[v, OWN]

        def tile(i, carry):
            cols = pl.ds(pl.multiple_of(i * fs, fs), fs)
            t = mm_nt(e, wo[v, i].reshape(fs, dm))
            da[:, cols] = (t * f1[v, :, cols]).astype(BF)
            db[:, cols] = (t * f2[v, :, cols]).astype(BF)
            return carry

        lax.fori_loop(0, NA, tile, 0, unroll=True)
        half_dm = dm // 2
        for i in HALVES:
            q = mm_nt(da[...], wg[v, pl.ds(2 * i, 2)].reshape(half_dm, fd))
            q += mm_nt(db[...], wi[v, pl.ds(2 * i, 2)].reshape(half_dm, fd))
            qs[:, pl.ds(i * half_dm, half_dm)] = q
        h = hb[v, OWN].astype(F32)
        r = inv_rms(h)
        hr = h * r
        q = qs[...]
        dst[...] = (e.astype(F32) + r * (q - hr * jnp.mean(q * hr, axis=-1, keepdims=True))).astype(BF)

    def piece(j, i):
        z = i + p * (j - i)
        y = j + p * (i - j)
        return z, y

    EARLY, LATE = range(FAR), range(FAR, NA)

    def grad_first(v, slots):
        for i in QUARTERS if OWN in slots else ():
            z, y = piece(ja, i)
            cols = pl.ds(pl.multiple_of((z * NA + y) * pf, pf), pf)
            gs[v, :, pl.ds(i * pf, pf)] = wg[v, :, :, :, :, cols].reshape(dm, pf)
            is_[v, :, pl.ds(i * pf, pf)] = wi[v, :, :, :, :, cols].reshape(dm, pf)
        for s in slots:
            h = hb[v, s].astype(F32)
            n = (h * inv_rms(h)).astype(BF)
            ng[v, s] = n
            u, t1, t2 = gates(n, gs[v], is_[v])
            us[v, s] = u
            f1s[v, s] = t1
            f2s[v, s] = t2

    def grad_hidden(v, slots):
        for i in QUARTERS if OWN in slots else ():
            z, y = piece(ja, i)
            os_[pl.ds(i * pf, pf), :] = wo[v, z, y].reshape(pf, dm)
        for s in slots:
            t = mm_nt(eb[v, s], os_[...])
            das[s] = (t * f1s[v, s]).astype(BF)
            dbs[s] = (t * f2s[v, s]).astype(BF)

    def rows_of(slots):
        return pl.ds(slots[0], len(slots)), len(slots) * rows

    def grad_out(v, slots):
        some, count = rows_of(slots)
        for i in HALVES:
            cols, to = pl.ds(i * 2 * pf, 2 * pf), pl.ds(2 * i, 2)
            g = mm_tn(us[v, some, :, cols].reshape(count, 2 * pf), eb[v, some].reshape(count, dm)).reshape(2, 4, fr, dm)
            gout[v, to] = g if OWN in slots else gout[v, to] + g

    def grad_in(v, slots):
        some, count = rows_of(slots)
        for which, dref in enumerate((das, dbs)):
            for i in QUARTERS:
                cols = pl.ds(i * (dm // NA), dm // NA)
                g = mm_tn(ng[v, some, :, cols].reshape(count, dm // NA), dref[some].reshape(count, fs)).reshape(4, 4, dr, fs)
                for y in QUARTERS:
                    at = (v, which, y + p * (i - y), i + p * (y - i))
                    gin[at] = g[y] if OWN in slots else gin[at] + g[y]

    IN, OUT = 0, 1

    def split(width):
        return pl.ds(0, width - pf), pl.ds(width - pf, pf)

    def view(which, st, v, colour, t, half):
        along_b = colour == st
        if which == IN:
            cols = split(fs)[colour]
            b, x = (t, slice(None) if st == 0 else xc) if along_b else (slice(None) if st == 0 else jb, t)
            return gin.at[v, half, :, b, x, :, cols]
        cols = pl.ds(colour * (dm // 2), dm // 2)
        if st == 0:
            hs = pl.ds(2 * half, 2)
            return gout.at[v, t, hs, :, cols] if along_b else gout.at[v, hs, t, :, cols]
        hs = pl.ds(half * (fr // 2), fr // 2)
        return gout.at[v, t, xc, hs, cols] if along_b else gout.at[v, jb, t, hs, cols]

    RECV = (((rg[0], rg[1]), (rg[2], rg[3])), ((rg[4], rg[5]), (rg[6], rg[7])))
    MERGED, DIRECT = ((0, OPP, PLUS, 0), (1, OPP, MINUS, 1)), ((1, PLUS, PLUS, 2), (0, MINUS, MINUS, 3))
    RELAYED = ((0, PLUS, PLUS, 4), (1, MINUS, MINUS, 5))

    def axis_of(colour, st):
        return (jb, peer_b) if colour == st else (xc, functools.partial(peer, X))

    def scatter_send(v, which, st, copies):
        for colour in COLOURS:
            q, to = axis_of(colour, st)
            for half, c, delta, slot in copies:
                send(view(which, st, v, colour, rot(q, c), half), RECV[st][which][colour].at[v, slot],
                     rs_s.at[st, v, colour, which], rs_r.at[st, v, colour, which, slot], to(delta), p)

    def scatter_relay(v, which, st):
        for colour in COLOURS:
            q, _ = axis_of(colour, st)
            recv = RECV[st][which][colour]
            for half, c, _, slot in RELAYED:
                wait_recv(recv.at[v, slot - 4], rs_r.at[st, v, colour, which, slot - 4])
                ref = view(which, st, v, colour, rot(q, c), half)
                ref[...] = ref[...] + recv[v, slot - 4]
        scatter_send(v, which, st, RELAYED)

    def scatter_sum(v, which, st):
        for colour in COLOURS:
            q, _ = axis_of(colour, st)
            recv = RECV[st][which][colour]
            for half in HALVES:
                direct, merged = 3 - half, 4 + half
                for slot in (direct, merged):
                    wait_recv(recv.at[v, slot], rs_r.at[st, v, colour, which, slot])
                ref = view(which, st, v, colour, q, half)
                ref[...] = ref[...] + recv[v, direct] + recv[v, merged]

    def scatter_turn(v, which):
        scatter_sum(v, which, 0)
        scatter_send(v, which, 1, MERGED + DIRECT)

    def scatter_out(v):
        scatter_sum(v, OUT, 1)
        go[v] = gout[v, jb, xc]

    def scatter_last(v):
        scatter_sum(v, IN, 1)
        for which in HALVES:
            fin[v, :, which] = gin[v, which, :, jb, xc]
        for delta in (OPP, PLUS, MINUS):
            send(fin.at[v, rot(ja, delta)], r3.at[v, delta - 1], r3_s.at[v], r3_r.at[v, delta - 1], peer_a(delta), p)

    def scatter_finish(v):
        def put(j, vals):
            for i in QUARTERS:
                z, y = piece(j, i)
                cols = pl.ds(pl.multiple_of((z * NA + y) * pf, pf), pf)
                gg[v, :, cols] = vals(0)[:, i * pf:(i + 1) * pf]
                gi[v, :, cols] = vals(1)[:, i * pf:(i + 1) * pf]

        put(ja, lambda w: fin[v, ja, w])
        for delta in RING:
            wait_recv(r3.at[v, delta - 1], r3_r.at[v, delta - 1])
            put(rot(ja, -delta), lambda w, delta=delta: r3[v, delta - 1, w])

    def step(fn, *args):
        with jax.named_scope(fn.__name__):
            fn(*args)

    def on(core):
        return pl.when(p == core)

    def take_turn():
        pl.semaphore_wait(turn, 1)

    def give_turn():
        pl.semaphore_signal(turn, inc=1, device_id=(d, 1 - p), device_id_type=MESH)

    h_mid, h_late, e_first, e_last = ((xo.at[i], mc_s.at[1 + i]) for i in QUARTERS)

    def pass_on(part, item, buf, which, vd):
        step(part, item[0], buf, which, vd, item[1])

    AFTER = (MINUS, OPP), (0, PLUS)
    step(direct_send, 0)
    step(small_send, 1, 0)

    @on(0)
    def _():
        step(spread_same, hb, 0, 0, mc_s.at[0])

    @on(1)
    def _():
        step(spread_same, eb, 1, 1, mc_s.at[0])

    step(direct_wait, 0)
    step(small_send, 0, 1)
    step(small_relay, 1, 0)
    step(large_send, 0, (0,), (0,))
    step(small_rest, 1, 0)
    step(small_last, 1, 0)
    step(small_send, 1, 1)
    step(small_relay, 0, 1)
    step(small_relay, 1, 1)
    step(small_rest, 0, 1)
    step(large_send, 0, (PLUS, MINUS), (MINUS, PLUS))
    step(small_last, 0, 1)
    step(large_send, 0, (OPP,), (OPP,))
    step(small_rest, 1, 1)
    step(small_last, 1, 1)
    step(large_relay, 0)

    @on(0)
    def _():
        step(large_send, 1, UP, DOWN)

    step(large_finish, 0)

    @on(0)
    def _():
        step(large_send, 1, *AFTER)

    @on(1)
    def _():
        step(take_turn)
        step(large_send, 1, UP, DOWN)
        step(spread_own, hb, 0, 0)

    step(block_gates, 0)

    @on(1)
    def _():
        step(large_send, 1, *AFTER)

    step(block_out, 0, h_mid[0])
    pass_on(spread_near, h_mid, hb, 0, p)
    step(large_relay, 1)

    @on(0)
    def _():
        step(give_turn)
        step(spread_relay, hb, 0, 0)

    step(large_finish, 1)

    @on(1)
    def _():
        step(give_turn)
        pass_on(spread_far, h_mid, hb, 0, p)

    step(spread_own, hb, 0, 1)
    step(block_gates, 1)

    @on(0)
    def _():
        step(block_out, 1, h_late[0])
        pass_on(spread_near, h_late, hb, 0, 1)
        pass_on(spread_far, h_late, hb, 0, 1)
        step(spread_finish, hb, 0, 0)
        step(grad_first, 0, EARLY)
        step(grad_first, 0, LATE)
        step(take_turn)
        pass_on(spread_far, h_mid, hb, 0, p)
        step(spread_own, eb, 1, 1)
        step(block_backward, 1, e_first[0])
        pass_on(spread_near, e_first, eb, 1, 0)
        pass_on(spread_far, e_first, eb, 1, 0)
        step(spread_relay, hb, 0, 1)

    @on(1)
    def _():
        step(spread_relay, hb, 0, 1)
        step(spread_relay, eb, 1, 1)
        step(block_backward, 1, e_first[0])
        pass_on(spread_near, e_first, eb, 1, 1)
        pass_on(spread_far, e_first, eb, 1, 1)

    step(grad_first, 1, EARLY)

    @on(0)
    def _():
        step(spread_relay, eb, 1, 1)

    step(grad_hidden, 1, EARLY)
    step(grad_out, 1, EARLY)

    @on(0)
    def _():
        step(grad_in, 1, EARLY)

    step(spread_finish, hb, 0, 1)
    step(grad_first, 1, LATE)
    step(spread_finish, eb, 1, 1)
    step(grad_hidden, 1, LATE)
    step(grad_out, 1, LATE)
    step(scatter_send, 1, OUT, 0, MERGED)

    @on(1)
    def _():
        step(spread_own, eb, 1, 0)
        step(block_backward, 0, e_last[0])
        pass_on(spread_near, e_last, eb, 1, 0)
        pass_on(spread_far, e_last, eb, 1, 0)
        step(grad_in, 1, EARLY)

    step(grad_in, 1, LATE)
    step(scatter_send, 1, IN, 0, MERGED)

    @on(0)
    def _():
        step(spread_own, eb, 1, 0)
        step(block_backward, 0, ga)
        send(ga, ga, ga_s, ga_r, d, 1)

    @on(1)
    def _():
        step(spread_relay, hb, 0, 0)
        step(grad_first, 0, EARLY)

    step(scatter_send, 1, OUT, 0, DIRECT)
    step(spread_relay, eb, 1, 0)

    @on(1)
    def _():
        step(spread_finish, hb, 0, 0)
        step(grad_first, 0, LATE)

    step(grad_hidden, 0, EARLY)
    step(scatter_send, 1, IN, 0, DIRECT)
    step(grad_in, 0, EARLY)
    step(scatter_relay, 1, OUT, 0)
    step(grad_out, 0, EARLY)
    step(spread_finish, eb, 1, 0)
    step(grad_hidden, 0, LATE)
    step(grad_in, 0, LATE)
    step(scatter_send, 0, IN, 0, MERGED)
    step(grad_out, 0, LATE)
    step(scatter_relay, 1, IN, 0)
    step(scatter_send, 0, OUT, 0, MERGED)
    step(scatter_send, 0, IN, 0, DIRECT)
    step(scatter_turn, 1, OUT)
    step(scatter_relay, 0, IN, 0)
    step(scatter_send, 0, OUT, 0, DIRECT)
    step(scatter_turn, 1, IN)
    step(scatter_relay, 0, OUT, 0)
    step(scatter_relay, 1, OUT, 1)

    @on(1)
    def _():
        wait_recv(ga, ga_r)

    gact[...] = ga[...]
    step(scatter_turn, 0, IN)
    step(scatter_relay, 1, IN, 1)
    step(scatter_turn, 0, OUT)
    step(scatter_out, 1)
    step(scatter_last, 1)
    step(scatter_relay, 0, IN, 1)
    step(scatter_relay, 0, OUT, 1)
    step(scatter_last, 0)
    step(scatter_finish, 1)
    step(scatter_out, 0)
    step(scatter_finish, 0)

    for v in BLOCKS:
        for k in (X, Y, Z):
            wait_send(wts[k].at[v, 0, 0, pl.ds(0, 3)], ag_s.at[v, k, 0])
            wait_send(wts[k].at[v, 0, pl.ds(0, 3)], ag_s.at[v, k, 1])
            wait_send(wts[k].at[v, pl.ds(0, 3)], ag_s.at[v, k, LARGE])
        for colour in COLOURS:
            for which in HALVES:
                for st in HALVES:
                    wait_send(RECV[st][which][colour].at[v], rs_s.at[st, v, colour, which])
        wait_send(r3.at[v], r3_s.at[v])
        wait_send(hb.at[v, 0], rl_s.at[0, v])
        wait_send(hb.at[v, 0], rl_s.at[1, v])
    wait_send(hb.at[0, pl.ds(0, 2)], mc_s.at[0])
    wait_send(hb.at[0, pl.ds(0, 3)], mc_s.at[1])
    wait_send(hb.at[0, pl.ds(0, 3)], mc_s.at[3])

    @pl.when(p == 0)
    def _():
        wait_send(hb.at[0, pl.ds(0, 3)], mc_s.at[2])
        wait_send(ga, ga_s)

    @pl.when(p == 1)
    def _():
        wait_send(hb.at[0, pl.ds(0, 3)], mc_s.at[4])


def hand_on(*refs):
    copies = [pltpu.make_async_copy(refs[i], refs[NA + i], refs[-1].at[i]) for i in QUARTERS]
    for copy in copies:
        copy.start()
    for copy in copies:
        copy.wait()


def solution(mesh):
    act_spec = P(None, "data", None, None)
    w_spec = P(None, "stage", "data", None)

    def body(act_in, cot_out, w_gate, w_in, w_out):
        shape = act_in.shape
        dm, fd = shape[3], w_gate.shape[3]
        rows = shape[0] * shape[1] * shape[2]
        dr, fr, fs = dm // NL, fd // NL, fd // NA
        pf = fs // NA
        vmem = pltpu.VMEM
        dma = pltpu.SemaphoreType.DMA
        n2, n3, na = NB, len(RING), NA
        ring = (na, na)
        scratch = [
            vmem((n2, na, *ring, dr, fd), BF), vmem((n2, na, *ring, dr, fd), BF), vmem((n2, na, *ring, fr, dm), BF),
            vmem((n2, na, rows, dm), BF), vmem((n2, na, rows, dm), BF), vmem((na, rows, dm), BF), vmem((rows, dm), BF),
            vmem((n2, na, rows, dm), BF),
            vmem((n2, rows, fd), F32), vmem((n2, rows, fd), F32),
            vmem((n2, na, rows, fs), F32), vmem((n2, na, rows, fs), F32),
            vmem((n2, na, rows, fs), BF),
            vmem((rows, fd), BF), vmem((rows, fd), BF), vmem((rows, fd), BF),
            vmem((na, rows, fs), BF), vmem((na, rows, fs), BF),
            vmem((rows, dm), F32),
            vmem((n2, dm, fs), BF), vmem((n2, dm, fs), BF), vmem((fs, dm), BF),
            vmem((n2, n2, na, *ring, dr, fs), F32), vmem((n2, *ring, fr, dm), F32),
            vmem((n2, na, n2, dr, fs), F32), vmem((n2, n3, n2, dr, fs), F32),
            dma((n2, na)), dma((n2, n3, n3)), dma((n2, n3, n2, 6)), dma((n2, n3, n3 * na)), dma((5,)), dma((n2, n2, 5)), dma((n2, n2)), dma, dma,
            dma((n2, n2, n2, n2)), dma((n2, n2, n2, n2, 6)), dma((n2,)), dma((n2, n3)), pltpu.SemaphoreType.REGULAR,
            *(vmem((n2, 6, *lead, width), F32)
              for lead_in, lead_out in (((*ring, dr), (n2, fr)), ((na, dr), (fr // n2,)))
              for lead, width in ((lead_in, fs - pf), (lead_in, pf), (lead_out, dm // n2), (lead_out, dm // n2))),
        ]
        hbm = pl.BlockSpec(memory_space=pl.ANY)
        whole = pl.BlockSpec(memory_space=pltpu.VMEM)
        out = pl.pallas_call(
            kernel,
            out_shape=(
                vmem((rows, dm), BF), vmem((n2, dr, fd), F32), vmem((n2, dr, fd), F32), vmem((n2, fr, dm), F32),
            ),
            in_specs=[hbm] * 5,
            out_specs=(whole,) * NA,
            scratch_shapes=scratch,
            compiler_params=pltpu.CompilerParams(collective_id=0, has_side_effects=True, vmem_limit_bytes=66300000),
            name="train_step",
        )(act_in.reshape(rows, dm), cot_out.reshape(rows, dm), w_gate[:, 0], w_in[:, 0], w_out[:, 0])
        grad_act, grad_gate, grad_lin, grad_proj = pl.pallas_call(
            hand_on, out_shape=tuple(jax.ShapeDtypeStruct(a.shape, a.dtype) for a in out), in_specs=[whole] * NA, out_specs=(hbm,) * NA,
            scratch_shapes=[dma((NA,))], compiler_params=pltpu.CompilerParams(vmem_limit_bytes=2 ** 20), name="hand_on",
        )(*(pltpu.with_memory_space_constraint(a, vmem) for a in out))
        return grad_act.reshape(shape), grad_gate[:, None], grad_lin[:, None], grad_proj[:, None]

    return jax.shard_map(body, mesh=mesh, in_specs=(act_spec, act_spec, w_spec, w_spec, w_spec),
                         out_specs=(act_spec, w_spec, w_spec, w_spec), check_vma=False)
```

```python
import functools

import jax
import jax.numpy as jnp
from jax import lax
from jax.experimental import pallas as pl
from jax.experimental.pallas import tpu as pltpu
from jax.sharding import PartitionSpec as P

NORM_EPS = 1e-6
BF = jnp.bfloat16
F32 = jnp.float32
MESH = pl.DeviceIdType.MESH
X, Y, Z = 0, 1, 2
BLOCKS = COLOURS = HALVES = (0, 1)
NB, NA, NL = len(BLOCKS), 4, 64
RING = (1, 3, 2)
OPP = RING[-1]
PLUS, MINUS = RING[:-1]
QUARTERS = range(NA)
OWN = 0
AXES = ((X, Y, Z), (Y, Z, X), (Z, X, Y))


def mm(left, right):
    return jnp.dot(left, right, preferred_element_type=F32)


def mm_nt(left, right):
    return lax.dot_general(left, right, (((1,), (1,)), ((), ())), preferred_element_type=F32)


def mm_tn(left, right):
    return lax.dot_general(left, right, (((0,), (0,)), ((), ())), preferred_element_type=F32)


def inv_rms(h):
    return lax.rsqrt(jnp.mean(h * h, axis=-1, keepdims=True) + NORM_EPS)


def kernel(act, cot, wg_in, wi_in, wo_in, gact, gg, gi, go,
           wg, wi, wo, hb, eb, xo, ga, ng, f1, f2, f1s, f2s, us, ub, da, db, das, dbs, qs, gs, is_, os_,
           gin, gout, fin, r3,
           lsem, ag_s, ag_r, lg_r, mc_s, mc_r, rl_s, ga_s, ga_r, rs_s, rs_r, r3_s, r3_r, turn, *rg):
    dm, fd = wo.shape[-1], wg.shape[-1]
    dr, fr = dm // NL, fd // NL
    fs = fd // NA
    pf = fs // NA
    rows = act.shape[0]
    wts = (wg, wi, wo)

    p = lax.axis_index("stage")
    d = lax.axis_index("data")
    zc, yc, xc = lax.div(d, 16), lax.rem(lax.div(d, 4), 4), lax.rem(d, 4)
    coord = (xc, yc, zc)
    stride = (1, 4, 16)
    ja = yc + p * (zc - yc)
    jb = zc + p * (yc - zc)
    sa, sb = 4 + 12 * p, 16 - 12 * p

    def rot(c, delta):
        return lax.rem(c + (delta % 4), 4)

    def peer(ax, delta):
        return d + (rot(coord[ax], delta) - coord[ax]) * stride[ax]

    def peer_a(delta):
        return d + (rot(ja, delta) - ja) * sa

    def peer_b(delta):
        return d + (rot(jb, delta) - jb) * sb

    def remote(src, dst, ssem, rsem, dev, core):
        return pltpu.make_async_remote_copy(src_ref=src, dst_ref=dst, send_sem=ssem, recv_sem=rsem,
                                            device_id=(dev, core), device_id_type=MESH)

    def send(src, dst, ssem, rsem, dev, core):
        remote(src, dst, ssem, rsem, dev, core).start()

    def wait_recv(ref, sem):
        remote(ref, ref, sem, sem, d, p).wait_recv()

    def wait_send(ref, sem):
        remote(ref, ref, sem, sem, d, p).wait_send()

    for v in BLOCKS:
        for k, shard in enumerate((wg_in, wi_in, wo_in)):
            pltpu.make_async_copy(shard.at[v], wts[k].at[v, zc, yc, xc], lsem.at[v, k]).start()

    @pl.when(p == 0)
    def _():
        pltpu.make_async_copy(act, hb.at[0, OWN], lsem.at[0, 3]).start()

    @pl.when(p == 1)
    def _():
        pltpu.make_async_copy(cot, eb.at[1, OWN], lsem.at[0, 3]).start()

    barrier = pltpu.get_barrier_semaphore()
    senders = [(peer(ax, delta), p) for ax in (X, Y, Z) for delta in RING]
    senders += [(d, 1 - p), (peer_a(1), 1 - p), (peer_a(-1), 1 - p)]
    for dev, core in senders:
        pl.semaphore_signal(barrier, inc=1, device_id=(dev, core), device_id_type=MESH)
    for v in BLOCKS:
        for k, shard in enumerate((wg_in, wi_in, wo_in)):
            pltpu.make_async_copy(shard.at[v], wts[k].at[v, zc, yc, xc], lsem.at[v, k]).wait()

    @pl.when(p == 0)
    def _():
        pltpu.make_async_copy(act, hb.at[0, OWN], lsem.at[0, 3]).wait()

    @pl.when(p == 1)
    def _():
        pltpu.make_async_copy(cot, eb.at[1, OWN], lsem.at[0, 3]).wait()

    pl.semaphore_wait(barrier, len(senders))

    FIRST, REST = ((0, PLUS, 0), (1, MINUS, 2)), ((1, PLUS, 1), (0, MINUS, 3))
    LARGE = 2

    def chunk(v, k, ph, q, half):
        if ph == 0:
            width = wts[k].shape[-1] // 2
            ix = tuple(q if ax == AXES[k][0] else coord[ax] for ax in (Z, Y, X)) + (slice(None), pl.ds(half * width, width))
        else:
            hs = pl.ds(2 * half, 2)
            ix = ((zc, q, hs), (q, hs, xc), (hs, yc, q))[k]
        return wts[k].at[(v,) + ix]

    def small_copy(v, k, ph, q, half, delta, slot):
        ref = chunk(v, k, ph, q, half)
        send(ref, ref, ag_s.at[v, k, ph], ag_r.at[v, k, ph, slot], peer(AXES[k][ph], delta), p)

    def small_wait(v, k, ph, back, half, slot):
        wait_recv(chunk(v, k, ph, rot(coord[AXES[k][ph]], back), half), ag_r.at[v, k, ph, slot])

    def small_send(v, ph):
        for half, delta, slot in FIRST + REST:
            for k in (X, Y, Z):
                small_copy(v, k, ph, coord[AXES[k][ph]], half, delta, slot)

    def small_relay(v, ph):
        for half, delta, slot in FIRST:
            for k in (X, Y, Z):
                small_wait(v, k, ph, -delta, half, slot)
                small_copy(v, k, ph, rot(coord[AXES[k][ph]], -delta), half, delta, 4 + half)

    def small_rest(v, ph):
        for half, delta, slot in REST:
            for k in (X, Y, Z):
                small_wait(v, k, ph, -delta, half, slot)

    def small_last(v, ph):
        for half in HALVES:
            for k in (X, Y, Z):
                small_wait(v, k, ph, OPP, half, 4 + half)

    def direct_send(v):
        for delta in (OPP, PLUS, MINUS):
            for k in (X, Y, Z):
                own = wts[k].at[v, zc, yc, xc]
                send(own, own, ag_s.at[v, k, 0], ag_r.at[v, k, 0, delta], peer(AXES[k][0], delta), p)

    def direct_wait(v):
        for delta in RING:
            for k in (X, Y, Z):
                at = tuple(rot(coord[ax], -delta) if ax == AXES[k][0] else coord[ax] for ax in (Z, Y, X))
                wait_recv(wts[k].at[(v,) + at], ag_r.at[v, k, 0, delta])

    UP, DOWN = (0, PLUS), (MINUS, OPP)
    RELAYS = ((UP[0], PLUS), (DOWN[0], MINUS), (UP[1], PLUS), (DOWN[1], MINUS))

    def row(v, k, q, r):
        m = rot(coord[AXES[k][1]], r)
        ix = ((q, m), (m, slice(None), q), (slice(None), q, m))[k]
        return wts[k].at[(v,) + ix]

    def large_slot(r, delta):
        return r if delta == PLUS else NA + r

    def large_send(v, up, down):
        for pair in zip(up, down):
            for r, delta in zip(pair, (PLUS, MINUS)):
                for k in (X, Y, Z):
                    ax = AXES[k][LARGE]
                    ref = row(v, k, coord[ax], r)
                    send(ref, ref, ag_s.at[v, k, LARGE], lg_r.at[v, k, large_slot(r, delta)], peer(ax, delta), p)

    def large_relay(v):
        for r, delta in RELAYS:
            for k in (X, Y, Z):
                ax = AXES[k][LARGE]
                ref = row(v, k, rot(coord[ax], -delta), r)
                wait_recv(ref, lg_r.at[v, k, large_slot(r, delta)])
                send(ref, ref, ag_s.at[v, k, LARGE], lg_r.at[v, k, 2 * NA + r], peer(ax, delta), p)

    def large_finish(v):
        for pieces, delta in ((DOWN, PLUS), (UP, MINUS)):
            for r in pieces:
                for k in (X, Y, Z):
                    wait_recv(row(v, k, rot(coord[AXES[k][LARGE]], -delta), r), lg_r.at[v, k, large_slot(r, delta)])
        for r in QUARTERS:
            for k in (X, Y, Z):
                wait_recv(row(v, k, rot(coord[AXES[k][LARGE]], OPP), r), lg_r.at[v, k, 2 * NA + r])

    half_rows = rows // 2
    BACK, AHEAD, FAR = 1, 2, 3

    def spread_near(src, buf, which, vd, ssem):
        send(src, buf.at[vd, OWN], ssem, mc_r.at[which, vd, OWN], d, 1 - p)

    def spread_far(src, buf, which, vd, ssem):
        send(src, buf.at[vd, BACK], ssem, mc_r.at[which, vd, BACK], peer_b(PLUS), 1 - p)
        send(src, buf.at[vd, AHEAD], ssem, mc_r.at[which, vd, AHEAD], peer_b(MINUS), 1 - p)

    def spread_same(buf, which, v, ssem):
        send(buf.at[v, OWN], buf.at[v, BACK], ssem, mc_r.at[which, v, BACK], peer_a(PLUS), p)
        send(buf.at[v, OWN], buf.at[v, AHEAD], ssem, mc_r.at[which, v, AHEAD], peer_a(MINUS), p)

    def spread_relay(buf, which, v):
        for half, slot, delta in ((0, BACK, PLUS), (1, AHEAD, MINUS)):
            wait_recv(buf.at[v, slot], mc_r.at[which, v, slot])
            part = pl.ds(half * half_rows, half_rows)
            send(buf.at[v, slot, part], buf.at[v, FAR, part], rl_s.at[which, v], mc_r.at[which, v, FAR + half], peer_a(delta), p)

    def spread_finish(buf, which, v):
        for half in HALVES:
            wait_recv(buf.at[v, FAR, pl.ds(half * half_rows, half_rows)], mc_r.at[which, v, FAR + half])

    def spread_own(buf, which, v):
        wait_recv(buf.at[v, OWN], mc_r.at[which, v, OWN])

    def gates(n, wgt, wlin):
        a, b = mm(n, wgt), mm(n, wlin)
        s = jax.nn.sigmoid(a)
        act_a = a * s
        return (act_a * b).astype(BF), b * s * (1.0 + a * (1.0 - s)), act_a

    def block_gates(v):
        h = hb[v, OWN].astype(F32)
        n = (h * inv_rms(h)).astype(BF)

        def tile(i, carry):
            wide = fs // 2
            cols = pl.ds(pl.multiple_of(i * wide, wide), wide)
            u, t1, t2 = gates(n, wg[v, :, :, :, :, cols].reshape(dm, wide), wi[v, :, :, :, :, cols].reshape(dm, wide))
            ub[:, cols] = u
            f1[v, :, cols] = t1
            f2[v, :, cols] = t2
            return carry

        lax.fori_loop(0, 2 * NA, tile, 0, unroll=True)

    def block_out(v, dst):
        half_dm = dm // 2
        for i in HALVES:
            cols = pl.ds(i * half_dm, half_dm)
            out = mm(ub[...], wo[v, :, :, :, :, cols].reshape(fd, half_dm))
            dst[:, cols] = (hb[v, OWN, :, cols].astype(F32) + out).astype(BF)

    def block_backward(v, dst):
        e = eb[v, OWN]

        def tile(i, carry):
            cols = pl.ds(pl.multiple_of(i * fs, fs), fs)
            t = mm_nt(e, wo[v, i].reshape(fs, dm))
            da[:, cols] = (t * f1[v, :, cols]).astype(BF)
            db[:, cols] = (t * f2[v, :, cols]).astype(BF)
            return carry

        lax.fori_loop(0, NA, tile, 0, unroll=True)
        half_dm = dm // 2
        for i in HALVES:
            q = mm_nt(da[...], wg[v, pl.ds(2 * i, 2)].reshape(half_dm, fd))
            q += mm_nt(db[...], wi[v, pl.ds(2 * i, 2)].reshape(half_dm, fd))
            qs[:, pl.ds(i * half_dm, half_dm)] = q
        h = hb[v, OWN].astype(F32)
        r = inv_rms(h)
        hr = h * r
        q = qs[...]
        dst[...] = (e.astype(F32) + r * (q - hr * jnp.mean(q * hr, axis=-1, keepdims=True))).astype(BF)

    def piece(j, i):
        z = i + p * (j - i)
        y = j + p * (i - j)
        return z, y

    EARLY, LATE = range(FAR), range(FAR, NA)

    def grad_first(v, slots):
        for i in QUARTERS if OWN in slots else ():
            z, y = piece(ja, i)
            cols = pl.ds(pl.multiple_of((z * NA + y) * pf, pf), pf)
            gs[v, :, pl.ds(i * pf, pf)] = wg[v, :, :, :, :, cols].reshape(dm, pf)
            is_[v, :, pl.ds(i * pf, pf)] = wi[v, :, :, :, :, cols].reshape(dm, pf)
        for s in slots:
            h = hb[v, s].astype(F32)
            n = (h * inv_rms(h)).astype(BF)
            ng[v, s] = n
            u, t1, t2 = gates(n, gs[v], is_[v])
            us[v, s] = u
            f1s[v, s] = t1
            f2s[v, s] = t2

    def grad_hidden(v, slots):
        for i in QUARTERS if OWN in slots else ():
            z, y = piece(ja, i)
            os_[pl.ds(i * pf, pf), :] = wo[v, z, y].reshape(pf, dm)
        for s in slots:
            t = mm_nt(eb[v, s], os_[...])
            das[s] = (t * f1s[v, s]).astype(BF)
            dbs[s] = (t * f2s[v, s]).astype(BF)

    def rows_of(slots):
        return pl.ds(slots[0], len(slots)), len(slots) * rows

    def grad_out(v, slots):
        some, count = rows_of(slots)
        for i in HALVES:
            cols, to = pl.ds(i * 2 * pf, 2 * pf), pl.ds(2 * i, 2)
            g = mm_tn(us[v, some, :, cols].reshape(count, 2 * pf), eb[v, some].reshape(count, dm)).reshape(2, 4, fr, dm)
            gout[v, to] = g if OWN in slots else gout[v, to] + g

    def grad_in(v, slots):
        some, count = rows_of(slots)
        for which, dref in enumerate((das, dbs)):
            for i in QUARTERS:
                cols = pl.ds(i * (dm // NA), dm // NA)
                g = mm_tn(ng[v, some, :, cols].reshape(count, dm // NA), dref[some].reshape(count, fs)).reshape(4, 4, dr, fs)
                for y in QUARTERS:
                    at = (v, which, y + p * (i - y), i + p * (y - i))
                    gin[at] = g[y] if OWN in slots else gin[at] + g[y]

    IN, OUT = 0, 1

    def split(width):
        return pl.ds(0, width - pf), pl.ds(width - pf, pf)

    def view(which, st, v, colour, t, half):
        along_b = colour == st
        if which == IN:
            cols = split(fs)[colour]
            b, x = (t, slice(None) if st == 0 else xc) if along_b else (slice(None) if st == 0 else jb, t)
            return gin.at[v, half, :, b, x, :, cols]
        cols = split(dm)[colour]
        if st == 0:
            hs = pl.ds(2 * half, 2)
            return gout.at[v, t, hs, :, cols] if along_b else gout.at[v, hs, t, :, cols]
        hs = pl.ds(half * (fr // 2), fr // 2)
        return gout.at[v, t, xc, hs, cols] if along_b else gout.at[v, jb, t, hs, cols]

    RECV = (((rg[0], rg[1]), (rg[2], rg[3])), ((rg[4], rg[5]), (rg[6], rg[7])))
    MERGED, DIRECT = ((0, OPP, PLUS, 0), (1, OPP, MINUS, 1)), ((1, PLUS, PLUS, 2), (0, MINUS, MINUS, 3))
    RELAYED = ((0, PLUS, PLUS, 4), (1, MINUS, MINUS, 5))

    def axis_of(colour, st):
        return (jb, peer_b) if colour == st else (xc, functools.partial(peer, X))

    def scatter_send(v, which, st, copies):
        for colour in COLOURS:
            q, to = axis_of(colour, st)
            for half, c, delta, slot in copies:
                send(view(which, st, v, colour, rot(q, c), half), RECV[st][which][colour].at[v, slot],
                     rs_s.at[st, v, colour, which], rs_r.at[st, v, colour, which, slot], to(delta), p)

    def scatter_relay(v, which, st):
        for colour in COLOURS:
            q, _ = axis_of(colour, st)
            recv = RECV[st][which][colour]
            for half, c, _, slot in RELAYED:
                wait_recv(recv.at[v, slot - 4], rs_r.at[st, v, colour, which, slot - 4])
                ref = view(which, st, v, colour, rot(q, c), half)
                ref[...] = ref[...] + recv[v, slot - 4]
        scatter_send(v, which, st, RELAYED)

    def scatter_sum(v, which, st):
        for colour in COLOURS:
            q, _ = axis_of(colour, st)
            recv = RECV[st][which][colour]
            for half in HALVES:
                direct, merged = 3 - half, 4 + half
                for slot in (direct, merged):
                    wait_recv(recv.at[v, slot], rs_r.at[st, v, colour, which, slot])
                ref = view(which, st, v, colour, q, half)
                ref[...] = ref[...] + recv[v, direct] + recv[v, merged]

    def scatter_turn(v, which):
        scatter_sum(v, which, 0)
        scatter_send(v, which, 1, MERGED + DIRECT)

    def scatter_out(v):
        scatter_sum(v, OUT, 1)
        go[v] = gout[v, jb, xc]

    def scatter_last(v):
        scatter_sum(v, IN, 1)
        for which in HALVES:
            fin[v, :, which] = gin[v, which, :, jb, xc]
        for delta in (OPP, PLUS, MINUS):
            send(fin.at[v, rot(ja, delta)], r3.at[v, delta - 1], r3_s.at[v], r3_r.at[v, delta - 1], peer_a(delta), p)

    def scatter_finish(v):
        def put(j, vals):
            for i in QUARTERS:
                z, y = piece(j, i)
                cols = pl.ds(pl.multiple_of((z * NA + y) * pf, pf), pf)
                gg[v, :, cols] = vals(0)[:, i * pf:(i + 1) * pf]
                gi[v, :, cols] = vals(1)[:, i * pf:(i + 1) * pf]

        put(ja, lambda w: fin[v, ja, w])
        for delta in RING:
            wait_recv(r3.at[v, delta - 1], r3_r.at[v, delta - 1])
            put(rot(ja, -delta), lambda w, delta=delta: r3[v, delta - 1, w])

    def step(fn, *args):
        with jax.named_scope(fn.__name__):
            fn(*args)

    def on(core):
        return pl.when(p == core)

    def take_turn():
        pl.semaphore_wait(turn, 1)

    def give_turn():
        pl.semaphore_signal(turn, inc=1, device_id=(d, 1 - p), device_id_type=MESH)

    h_mid, h_late, e_first, e_last = ((xo.at[i], mc_s.at[1 + i]) for i in QUARTERS)

    def pass_on(part, item, buf, which, vd):
        step(part, item[0], buf, which, vd, item[1])

    AFTER = (MINUS, OPP), (0, PLUS)
    step(direct_send, 0)
    step(small_send, 1, 0)

    @on(0)
    def _():
        step(spread_same, hb, 0, 0, mc_s.at[0])

    @on(1)
    def _():
        step(spread_same, eb, 1, 1, mc_s.at[0])

    step(direct_wait, 0)
    step(small_send, 0, 1)
    step(small_relay, 1, 0)
    step(large_send, 0, (0,), (0,))
    step(small_rest, 1, 0)
    step(small_last, 1, 0)
    step(small_send, 1, 1)
    step(small_relay, 0, 1)
    step(small_relay, 1, 1)
    step(small_rest, 0, 1)
    step(large_send, 0, (PLUS, MINUS), (MINUS, PLUS))
    step(small_last, 0, 1)
    step(large_send, 0, (OPP,), (OPP,))
    step(small_rest, 1, 1)
    step(small_last, 1, 1)
    step(large_relay, 0)

    @on(0)
    def _():
        step(large_send, 1, UP, DOWN)

    step(large_finish, 0)

    @on(0)
    def _():
        step(large_send, 1, *AFTER)
        step(give_turn)

    @on(1)
    def _():
        step(take_turn)
        step(large_send, 1, UP, DOWN)
        step(spread_own, hb, 0, 0)

    step(block_gates, 0)

    @on(1)
    def _():
        step(large_send, 1, *AFTER)

    step(block_out, 0, h_mid[0])
    pass_on(spread_near, h_mid, hb, 0, p)
    step(large_relay, 1)

    @on(0)
    def _():
        step(spread_relay, hb, 0, 0)

    step(large_finish, 1)

    @on(1)
    def _():
        pass_on(spread_far, h_mid, hb, 0, p)

    step(spread_own, hb, 0, 1)
    step(block_gates, 1)

    @on(0)
    def _():
        step(block_out, 1, h_late[0])
        pass_on(spread_near, h_late, hb, 0, 1)
        pass_on(spread_far, h_late, hb, 0, 1)
        step(spread_finish, hb, 0, 0)
        step(grad_first, 0, EARLY)
        step(grad_first, 0, LATE)
        step(spread_own, eb, 1, 1)
        pass_on(spread_far, h_mid, hb, 0, p)
        step(block_backward, 1, e_first[0])
        pass_on(spread_near, e_first, eb, 1, 0)
        pass_on(spread_far, e_first, eb, 1, 0)
        step(spread_relay, hb, 0, 1)

    @on(1)
    def _():
        step(spread_relay, hb, 0, 1)
        step(spread_relay, eb, 1, 1)
        step(block_backward, 1, e_first[0])
        pass_on(spread_near, e_first, eb, 1, 1)
        pass_on(spread_far, e_first, eb, 1, 1)

    step(grad_first, 1, EARLY)

    @on(0)
    def _():
        step(spread_relay, eb, 1, 1)

    step(grad_hidden, 1, EARLY)
    step(grad_out, 1, EARLY)

    @on(0)
    def _():
        step(grad_in, 1, EARLY)

    step(spread_finish, hb, 0, 1)
    step(grad_first, 1, LATE)
    step(spread_finish, eb, 1, 1)
    step(grad_hidden, 1, LATE)
    step(grad_out, 1, LATE)
    step(scatter_send, 1, OUT, 0, MERGED)

    @on(1)
    def _():
        step(spread_own, eb, 1, 0)
        step(block_backward, 0, e_last[0])
        pass_on(spread_near, e_last, eb, 1, 0)
        pass_on(spread_far, e_last, eb, 1, 0)
        step(grad_in, 1, EARLY)

    step(grad_in, 1, LATE)
    step(scatter_send, 1, IN, 0, MERGED)

    @on(0)
    def _():
        step(spread_relay, eb, 1, 0)
        step(spread_own, eb, 1, 0)
        step(block_backward, 0, ga)
        send(ga, ga, ga_s, ga_r, d, 1)

    @on(1)
    def _():
        step(spread_relay, hb, 0, 0)
        step(grad_first, 0, EARLY)

    step(scatter_send, 1, OUT, 0, DIRECT)

    @on(1)
    def _():
        step(spread_relay, eb, 1, 0)
        step(spread_finish, hb, 0, 0)
        step(grad_first, 0, LATE)

    step(grad_hidden, 0, EARLY)
    step(scatter_send, 1, IN, 0, DIRECT)
    step(grad_in, 0, EARLY)
    step(scatter_relay, 1, OUT, 0)
    step(grad_out, 0, EARLY)
    step(spread_finish, eb, 1, 0)
    step(grad_hidden, 0, LATE)
    step(grad_in, 0, LATE)
    step(scatter_send, 0, IN, 0, MERGED)
    step(grad_out, 0, LATE)
    step(scatter_relay, 1, IN, 0)
    step(scatter_send, 0, OUT, 0, MERGED)
    step(scatter_send, 0, IN, 0, DIRECT)
    step(scatter_turn, 1, OUT)
    step(scatter_relay, 0, IN, 0)
    step(scatter_send, 0, OUT, 0, DIRECT)
    step(scatter_turn, 1, IN)
    step(scatter_relay, 0, OUT, 0)
    step(scatter_relay, 1, OUT, 1)

    @on(1)
    def _():
        wait_recv(ga, ga_r)

    gact[...] = ga[...]
    step(scatter_turn, 0, IN)
    step(scatter_relay, 1, IN, 1)
    step(scatter_turn, 0, OUT)
    step(scatter_out, 1)
    step(scatter_last, 1)
    step(scatter_relay, 0, IN, 1)
    step(scatter_relay, 0, OUT, 1)
    step(scatter_last, 0)
    step(scatter_finish, 1)
    step(scatter_out, 0)
    step(scatter_finish, 0)

    for v in BLOCKS:
        for k in (X, Y, Z):
            wait_send(wts[k].at[v, 0, 0, pl.ds(0, 3)], ag_s.at[v, k, 0])
            wait_send(wts[k].at[v, 0, pl.ds(0, 3)], ag_s.at[v, k, 1])
            wait_send(wts[k].at[v, pl.ds(0, 3)], ag_s.at[v, k, LARGE])
        for colour in COLOURS:
            for which in HALVES:
                for st in HALVES:
                    wait_send(RECV[st][which][colour].at[v], rs_s.at[st, v, colour, which])
        wait_send(r3.at[v], r3_s.at[v])
        wait_send(hb.at[v, 0], rl_s.at[0, v])
        wait_send(hb.at[v, 0], rl_s.at[1, v])
    wait_send(hb.at[0, pl.ds(0, 2)], mc_s.at[0])
    wait_send(hb.at[0, pl.ds(0, 3)], mc_s.at[1])
    wait_send(hb.at[0, pl.ds(0, 3)], mc_s.at[3])

    @pl.when(p == 0)
    def _():
        wait_send(hb.at[0, pl.ds(0, 3)], mc_s.at[2])
        wait_send(ga, ga_s)

    @pl.when(p == 1)
    def _():
        wait_send(hb.at[0, pl.ds(0, 3)], mc_s.at[4])


def hand_on(*refs):
    copies = [pltpu.make_async_copy(refs[i], refs[NA + i], refs[-1].at[i]) for i in QUARTERS]
    for copy in copies:
        copy.start()
    for copy in copies:
        copy.wait()


def solution(mesh):
    act_spec = P(None, "data", None, None)
    w_spec = P(None, "stage", "data", None)

    def body(act_in, cot_out, w_gate, w_in, w_out):
        shape = act_in.shape
        dm, fd = shape[3], w_gate.shape[3]
        rows = shape[0] * shape[1] * shape[2]
        dr, fr, fs = dm // NL, fd // NL, fd // NA
        pf = fs // NA
        vmem = pltpu.VMEM
        dma = pltpu.SemaphoreType.DMA
        n2, n3, na = NB, len(RING), NA
        ring = (na, na)
        scratch = [
            vmem((n2, na, *ring, dr, fd), BF), vmem((n2, na, *ring, dr, fd), BF), vmem((n2, na, *ring, fr, dm), BF),
            vmem((n2, na, rows, dm), BF), vmem((n2, na, rows, dm), BF), vmem((na, rows, dm), BF), vmem((rows, dm), BF),
            vmem((n2, na, rows, dm), BF),
            vmem((n2, rows, fd), F32), vmem((n2, rows, fd), F32),
            vmem((n2, na, rows, fs), F32), vmem((n2, na, rows, fs), F32),
            vmem((n2, na, rows, fs), BF),
            vmem((rows, fd), BF), vmem((rows, fd), BF), vmem((rows, fd), BF),
            vmem((na, rows, fs), BF), vmem((na, rows, fs), BF),
            vmem((rows, dm), F32),
            vmem((n2, dm, fs), BF), vmem((n2, dm, fs), BF), vmem((fs, dm), BF),
            vmem((n2, n2, na, *ring, dr, fs), F32), vmem((n2, *ring, fr, dm), F32),
            vmem((n2, na, n2, dr, fs), F32), vmem((n2, n3, n2, dr, fs), F32),
            dma((n2, na)), dma((n2, n3, n3)), dma((n2, n3, n2, 6)), dma((n2, n3, n3 * na)), dma((5,)), dma((n2, n2, 5)), dma((n2, n2)), dma, dma,
            dma((n2, n2, n2, n2)), dma((n2, n2, n2, n2, 6)), dma((n2,)), dma((n2, n3)), pltpu.SemaphoreType.REGULAR,
            *(vmem((n2, 6, *lead, width), F32)
              for lead_in, lead_out in (((*ring, dr), (n2, fr)), ((na, dr), (fr // n2,)))
              for lead, width in ((lead_in, fs - pf), (lead_in, pf), (lead_out, dm - pf), (lead_out, pf))),
        ]
        hbm = pl.BlockSpec(memory_space=pl.ANY)
        whole = pl.BlockSpec(memory_space=pltpu.VMEM)
        out = pl.pallas_call(
            kernel,
            out_shape=(
                vmem((rows, dm), BF), vmem((n2, dr, fd), F32), vmem((n2, dr, fd), F32), vmem((n2, fr, dm), F32),
            ),
            in_specs=[hbm] * 5,
            out_specs=(whole,) * NA,
            scratch_shapes=scratch,
            compiler_params=pltpu.CompilerParams(collective_id=0, has_side_effects=True, vmem_limit_bytes=66300000),
            name="train_step",
        )(act_in.reshape(rows, dm), cot_out.reshape(rows, dm), w_gate[:, 0], w_in[:, 0], w_out[:, 0])
        grad_act, grad_gate, grad_lin, grad_proj = pl.pallas_call(
            hand_on, out_shape=tuple(jax.ShapeDtypeStruct(a.shape, a.dtype) for a in out), in_specs=[whole] * NA, out_specs=(hbm,) * NA,
            scratch_shapes=[dma((NA,))], compiler_params=pltpu.CompilerParams(vmem_limit_bytes=2 ** 20), name="hand_on",
        )(*(pltpu.with_memory_space_constraint(a, vmem) for a in out))
        return grad_act.reshape(shape), grad_gate[:, None], grad_lin[:, None], grad_proj[:, None]

    return jax.shard_map(body, mesh=mesh, in_specs=(act_spec, act_spec, w_spec, w_spec, w_spec),
                         out_specs=(act_spec, w_spec, w_spec, w_spec), check_vma=False)
```

```python
import functools

import jax
import jax.numpy as jnp
from jax import lax
from jax.experimental import pallas as pl
from jax.experimental.pallas import tpu as pltpu
from jax.sharding import PartitionSpec as P

NORM_EPS = 1e-6
BF = jnp.bfloat16
F32 = jnp.float32
MESH = pl.DeviceIdType.MESH
X, Y, Z = 0, 1, 2
BLOCKS = COLOURS = HALVES = (0, 1)
NB, NA, NL = len(BLOCKS), 4, 64
RING = (1, 3, 2)
OPP = RING[-1]
PLUS, MINUS = RING[:-1]
QUARTERS = range(NA)
OWN = 0
AXES = ((X, Y, Z), (Y, Z, X), (Z, X, Y), (Z, Y, X))


def mm(left, right):
    return jnp.dot(left, right, preferred_element_type=F32)


def mm_nt(left, right):
    return lax.dot_general(left, right, (((1,), (1,)), ((), ())), preferred_element_type=F32)


def mm_tn(left, right):
    return lax.dot_general(left, right, (((0,), (0,)), ((), ())), preferred_element_type=F32)


def inv_rms(h):
    return lax.rsqrt(jnp.mean(h * h, axis=-1, keepdims=True) + NORM_EPS)


def kernel(act, cot, wg_in, wi_in, wo_in, gact, gg, gi, go,
           wg, wi, wo, hb, eb, xo, ga, ng, f1, f2, f1s, f2s, us, ub, da, db, das, dbs, qs, gs, is_, os_,
           gin, gout, fin, r3,
           lsem, ag_s, ag_r, lg_r, mc_s, mc_r, rl_s, ga_s, ga_r, rs_s, rs_r, r3_s, r3_r, turn, *rg):
    dm, fd = wo.shape[-1], wg.shape[-1]
    dr, fr = dm // NL, fd // NL
    fs = fd // NA
    pf = fs // NA
    rows = act.shape[0]
    wts = (wg, wi, wo)

    p = lax.axis_index("stage")
    d = lax.axis_index("data")
    zc, yc, xc = lax.div(d, 16), lax.rem(lax.div(d, 4), 4), lax.rem(d, 4)
    coord = (xc, yc, zc)
    stride = (1, 4, 16)
    ja = yc + p * (zc - yc)
    jb = zc + p * (yc - zc)
    sa, sb = 4 + 12 * p, 16 - 12 * p

    def rot(c, delta):
        return lax.rem(c + (delta % 4), 4)

    def peer(ax, delta):
        return d + (rot(coord[ax], delta) - coord[ax]) * stride[ax]

    def peer_a(delta):
        return d + (rot(ja, delta) - ja) * sa

    def peer_b(delta):
        return d + (rot(jb, delta) - jb) * sb

    def remote(src, dst, ssem, rsem, dev, core):
        return pltpu.make_async_remote_copy(src_ref=src, dst_ref=dst, send_sem=ssem, recv_sem=rsem,
                                            device_id=(dev, core), device_id_type=MESH)

    def send(src, dst, ssem, rsem, dev, core):
        remote(src, dst, ssem, rsem, dev, core).start()

    def wait_recv(ref, sem):
        remote(ref, ref, sem, sem, d, p).wait_recv()

    def wait_send(ref, sem):
        remote(ref, ref, sem, sem, d, p).wait_send()

    for v in BLOCKS:
        for k, shard in enumerate((wg_in, wi_in, wo_in)):
            pltpu.make_async_copy(shard.at[v], wts[k].at[v, zc, yc, xc], lsem.at[v, k]).start()

    @pl.when(p == 0)
    def _():
        pltpu.make_async_copy(act, hb.at[0, OWN], lsem.at[0, 3]).start()

    @pl.when(p == 1)
    def _():
        pltpu.make_async_copy(cot, eb.at[1, OWN], lsem.at[0, 3]).start()

    barrier = pltpu.get_barrier_semaphore()
    senders = [(peer(ax, delta), p) for ax in (X, Y, Z) for delta in RING]
    senders += [(d, 1 - p), (peer_a(1), 1 - p), (peer_a(-1), 1 - p)]
    for dev, core in senders:
        pl.semaphore_signal(barrier, inc=1, device_id=(dev, core), device_id_type=MESH)
    for v in BLOCKS:
        for k, shard in enumerate((wg_in, wi_in, wo_in)):
            pltpu.make_async_copy(shard.at[v], wts[k].at[v, zc, yc, xc], lsem.at[v, k]).wait()

    @pl.when(p == 0)
    def _():
        pltpu.make_async_copy(act, hb.at[0, OWN], lsem.at[0, 3]).wait()

    @pl.when(p == 1)
    def _():
        pltpu.make_async_copy(cot, eb.at[1, OWN], lsem.at[0, 3]).wait()

    pl.semaphore_wait(barrier, len(senders))

    FIRST, REST = ((0, PLUS, 0), (1, MINUS, 2)), ((1, PLUS, 1), (0, MINUS, 3))
    LARGE = 2
    whole = slice(None)

    def parts(v):
        return range(len(AXES) - v)

    def part_at(v, k, small, middle, large, half=None):
        place = dict(zip(AXES[k], (small, middle, large)))
        cols = whole if v or k % 3 else (pl.ds(0, fd - fs), pl.ds(fd - fs, fs))[k // 3]
        if half is not None:
            width = wts[k].shape[-1] // 2
            cols = pl.ds(half * width, width)
        return wts[k % 3].at[v, place[Z], place[Y], place[X], :, cols]

    def own(k):
        return [coord[ax] for ax in AXES[k]]

    def chunk(v, k, ph, q, half):
        small, middle, large = own(k)
        return part_at(v, k, q, middle, large, half) if ph == 0 else part_at(v, k, pl.ds(2 * half, 2), q, large)

    def small_copy(v, k, ph, q, half, delta, slot):
        ref = chunk(v, k, ph, q, half)
        send(ref, ref, ag_s.at[v, k, ph], ag_r.at[v, k, ph, slot], peer(AXES[k][ph], delta), p)

    def small_wait(v, k, ph, back, half, slot):
        wait_recv(chunk(v, k, ph, rot(coord[AXES[k][ph]], back), half), ag_r.at[v, k, ph, slot])

    def small_send(v, ph):
        for half, delta, slot in FIRST + REST:
            for k in parts(v):
                small_copy(v, k, ph, coord[AXES[k][ph]], half, delta, slot)

    def small_relay(v, ph):
        for half, delta, slot in FIRST:
            for k in parts(v):
                small_wait(v, k, ph, -delta, half, slot)
                small_copy(v, k, ph, rot(coord[AXES[k][ph]], -delta), half, delta, 4 + half)

    def small_rest(v, ph):
        for half, delta, slot in REST:
            for k in parts(v):
                small_wait(v, k, ph, -delta, half, slot)

    def small_last(v, ph):
        for half in HALVES:
            for k in parts(v):
                small_wait(v, k, ph, OPP, half, 4 + half)

    def direct_send(v):
        for delta in (OPP, PLUS, MINUS):
            for k in parts(v):
                ref = part_at(v, k, *own(k))
                send(ref, ref, ag_s.at[v, k, 0], ag_r.at[v, k, 0, delta], peer(AXES[k][0], delta), p)

    def direct_wait(v):
        for delta in RING:
            for k in parts(v):
                small, middle, large = own(k)
                wait_recv(part_at(v, k, rot(small, -delta), middle, large), ag_r.at[v, k, 0, delta])

    UP, DOWN = (0, PLUS), (MINUS, OPP)
    RELAYS = ((UP[0], PLUS), (DOWN[0], MINUS), (UP[1], PLUS), (DOWN[1], MINUS))

    def row(v, k, q, r):
        return part_at(v, k, whole, rot(coord[AXES[k][1]], r), q)

    def large_slot(r, delta):
        return r if delta == PLUS else NA + r

    def large_send(v, up, down):
        for pair in zip(up, down):
            for r, delta in zip(pair, (PLUS, MINUS)):
                for k in parts(v):
                    ax = AXES[k][LARGE]
                    ref = row(v, k, coord[ax], r)
                    send(ref, ref, ag_s.at[v, k, LARGE], lg_r.at[v, k, large_slot(r, delta)], peer(ax, delta), p)

    def large_relay(v):
        for r, delta in RELAYS:
            for k in parts(v):
                ax = AXES[k][LARGE]
                ref = row(v, k, rot(coord[ax], -delta), r)
                wait_recv(ref, lg_r.at[v, k, large_slot(r, delta)])
                send(ref, ref, ag_s.at[v, k, LARGE], lg_r.at[v, k, 2 * NA + r], peer(ax, delta), p)

    def large_finish(v):
        for pieces, delta in ((DOWN, PLUS), (UP, MINUS)):
            for r in pieces:
                for k in parts(v):
                    wait_recv(row(v, k, rot(coord[AXES[k][LARGE]], -delta), r), lg_r.at[v, k, large_slot(r, delta)])
        for r in QUARTERS:
            for k in parts(v):
                wait_recv(row(v, k, rot(coord[AXES[k][LARGE]], OPP), r), lg_r.at[v, k, 2 * NA + r])

    half_rows = rows // 2
    BACK, AHEAD, FAR = 1, 2, 3

    def spread_near(src, buf, which, vd, ssem):
        send(src, buf.at[vd, OWN], ssem, mc_r.at[which, vd, OWN], d, 1 - p)

    def spread_far(src, buf, which, vd, ssem):
        send(src, buf.at[vd, BACK], ssem, mc_r.at[which, vd, BACK], peer_b(PLUS), 1 - p)
        send(src, buf.at[vd, AHEAD], ssem, mc_r.at[which, vd, AHEAD], peer_b(MINUS), 1 - p)

    def spread_same(buf, which, v, ssem):
        send(buf.at[v, OWN], buf.at[v, BACK], ssem, mc_r.at[which, v, BACK], peer_a(PLUS), p)
        send(buf.at[v, OWN], buf.at[v, AHEAD], ssem, mc_r.at[which, v, AHEAD], peer_a(MINUS), p)

    def spread_relay(buf, which, v):
        for half, slot, delta in ((0, BACK, PLUS), (1, AHEAD, MINUS)):
            wait_recv(buf.at[v, slot], mc_r.at[which, v, slot])
            part = pl.ds(half * half_rows, half_rows)
            send(buf.at[v, slot, part], buf.at[v, FAR, part], rl_s.at[which, v], mc_r.at[which, v, FAR + half], peer_a(delta), p)

    def spread_finish(buf, which, v):
        for half in HALVES:
            wait_recv(buf.at[v, FAR, pl.ds(half * half_rows, half_rows)], mc_r.at[which, v, FAR + half])

    def spread_own(buf, which, v):
        wait_recv(buf.at[v, OWN], mc_r.at[which, v, OWN])

    def gates(n, wgt, wlin):
        a, b = mm(n, wgt), mm(n, wlin)
        s = jax.nn.sigmoid(a)
        act_a = a * s
        return (act_a * b).astype(BF), b * s * (1.0 + a * (1.0 - s)), act_a

    def block_gates(v):
        h = hb[v, OWN].astype(F32)
        n = (h * inv_rms(h)).astype(BF)

        def tile(i, carry):
            wide = fs // 2
            cols = pl.ds(pl.multiple_of(i * wide, wide), wide)
            u, t1, t2 = gates(n, wg[v, :, :, :, :, cols].reshape(dm, wide), wi[v, :, :, :, :, cols].reshape(dm, wide))
            ub[:, cols] = u
            f1[v, :, cols] = t1
            f2[v, :, cols] = t2
            return carry

        lax.fori_loop(0, 2 * NA, tile, 0, unroll=True)

    def block_out(v, dst):
        half_dm = dm // 2
        for i in HALVES:
            cols = pl.ds(i * half_dm, half_dm)
            out = mm(ub[...], wo[v, :, :, :, :, cols].reshape(fd, half_dm))
            dst[:, cols] = (hb[v, OWN, :, cols].astype(F32) + out).astype(BF)

    def block_backward(v, dst):
        e = eb[v, OWN]

        def tile(i, carry):
            cols = pl.ds(pl.multiple_of(i * fs, fs), fs)
            t = mm_nt(e, wo[v, i].reshape(fs, dm))
            da[:, cols] = (t * f1[v, :, cols]).astype(BF)
            db[:, cols] = (t * f2[v, :, cols]).astype(BF)
            return carry

        lax.fori_loop(0, NA, tile, 0, unroll=True)
        half_dm = dm // 2
        for i in HALVES:
            q = mm_nt(da[...], wg[v, pl.ds(2 * i, 2)].reshape(half_dm, fd))
            q += mm_nt(db[...], wi[v, pl.ds(2 * i, 2)].reshape(half_dm, fd))
            qs[:, pl.ds(i * half_dm, half_dm)] = q
        h = hb[v, OWN].astype(F32)
        r = inv_rms(h)
        hr = h * r
        q = qs[...]
        dst[...] = (e.astype(F32) + r * (q - hr * jnp.mean(q * hr, axis=-1, keepdims=True))).astype(BF)

    def piece(j, i):
        z = i + p * (j - i)
        y = j + p * (i - j)
        return z, y

    EARLY, LATE = range(FAR), range(FAR, NA)

    def grad_first(v, slots):
        for i in QUARTERS if OWN in slots else ():
            z, y = piece(ja, i)
            cols = pl.ds(pl.multiple_of((z * NA + y) * pf, pf), pf)
            gs[v, :, pl.ds(i * pf, pf)] = wg[v, :, :, :, :, cols].reshape(dm, pf)
            is_[v, :, pl.ds(i * pf, pf)] = wi[v, :, :, :, :, cols].reshape(dm, pf)
        for s in slots:
            h = hb[v, s].astype(F32)
            n = (h * inv_rms(h)).astype(BF)
            ng[v, s] = n
            u, t1, t2 = gates(n, gs[v], is_[v])
            us[v, s] = u
            f1s[v, s] = t1
            f2s[v, s] = t2

    def grad_hidden(v, slots):
        for i in QUARTERS if OWN in slots else ():
            z, y = piece(ja, i)
            os_[pl.ds(i * pf, pf), :] = wo[v, z, y].reshape(pf, dm)
        for s in slots:
            t = mm_nt(eb[v, s], os_[...])
            das[s] = (t * f1s[v, s]).astype(BF)
            dbs[s] = (t * f2s[v, s]).astype(BF)

    def rows_of(slots):
        return pl.ds(slots[0], len(slots)), len(slots) * rows

    def grad_out(v, slots):
        some, count = rows_of(slots)
        for i in HALVES:
            cols, to = pl.ds(i * 2 * pf, 2 * pf), pl.ds(2 * i, 2)
            g = mm_tn(us[v, some, :, cols].reshape(count, 2 * pf), eb[v, some].reshape(count, dm)).reshape(2, 4, fr, dm)
            gout[v, to] = g if OWN in slots else gout[v, to] + g

    def grad_in(v, slots):
        some, count = rows_of(slots)
        for which, dref in enumerate((das, dbs)):
            for i in QUARTERS:
                cols = pl.ds(i * (dm // NA), dm // NA)
                g = mm_tn(ng[v, some, :, cols].reshape(count, dm // NA), dref[some].reshape(count, fs)).reshape(4, 4, dr, fs)
                for y in QUARTERS:
                    at = (v, which, y + p * (i - y), i + p * (y - i))
                    gin[at] = g[y] if OWN in slots else gin[at] + g[y]

    IN, OUT = 0, 1

    def split(width):
        return pl.ds(0, width - pf), pl.ds(width - pf, pf)

    def view(which, st, v, colour, t, half):
        along_b = colour == st
        if which == IN:
            cols = split(fs)[colour]
            b, x = (t, slice(None) if st == 0 else xc) if along_b else (slice(None) if st == 0 else jb, t)
            return gin.at[v, half, :, b, x, :, cols]
        cols = split(dm)[colour]
        if st == 0:
            hs = pl.ds(2 * half, 2)
            return gout.at[v, t, hs, :, cols] if along_b else gout.at[v, hs, t, :, cols]
        hs = pl.ds(half * (fr // 2), fr // 2)
        return gout.at[v, t, xc, hs, cols] if along_b else gout.at[v, jb, t, hs, cols]

    RECV = (((rg[0], rg[1]), (rg[2], rg[3])), ((rg[4], rg[5]), (rg[6], rg[7])))
    MERGED, DIRECT = ((0, OPP, PLUS, 0), (1, OPP, MINUS, 1)), ((1, PLUS, PLUS, 2), (0, MINUS, MINUS, 3))
    RELAYED = ((0, PLUS, PLUS, 4), (1, MINUS, MINUS, 5))

    def axis_of(colour, st):
        return (jb, peer_b) if colour == st else (xc, functools.partial(peer, X))

    def scatter_send(v, which, st, copies):
        for colour in COLOURS:
            q, to = axis_of(colour, st)
            for half, c, delta, slot in copies:
                send(view(which, st, v, colour, rot(q, c), half), RECV[st][which][colour].at[v, slot],
                     rs_s.at[st, v, colour, which], rs_r.at[st, v, colour, which, slot], to(delta), p)

    def scatter_relay(v, which, st):
        for colour in COLOURS:
            q, _ = axis_of(colour, st)
            recv = RECV[st][which][colour]
            for half, c, _, slot in RELAYED:
                wait_recv(recv.at[v, slot - 4], rs_r.at[st, v, colour, which, slot - 4])
                ref = view(which, st, v, colour, rot(q, c), half)
                ref[...] = ref[...] + recv[v, slot - 4]
        scatter_send(v, which, st, RELAYED)

    def scatter_sum(v, which, st):
        for colour in COLOURS:
            q, _ = axis_of(colour, st)
            recv = RECV[st][which][colour]
            for half in HALVES:
                direct, merged = 3 - half, 4 + half
                for slot in (direct, merged):
                    wait_recv(recv.at[v, slot], rs_r.at[st, v, colour, which, slot])
                ref = view(which, st, v, colour, q, half)
                ref[...] = ref[...] + recv[v, direct] + recv[v, merged]

    def scatter_turn(v, which):
        scatter_sum(v, which, 0)
        scatter_send(v, which, 1, MERGED + DIRECT)

    def scatter_out(v):
        scatter_sum(v, OUT, 1)
        go[v] = gout[v, jb, xc]

    def scatter_last(v):
        scatter_sum(v, IN, 1)
        for which in HALVES:
            fin[v, :, which] = gin[v, which, :, jb, xc]
        for delta in (OPP, PLUS, MINUS):
            send(fin.at[v, rot(ja, delta)], r3.at[v, delta - 1], r3_s.at[v], r3_r.at[v, delta - 1], peer_a(delta), p)

    def scatter_finish(v):
        def put(j, vals):
            for i in QUARTERS:
                z, y = piece(j, i)
                cols = pl.ds(pl.multiple_of((z * NA + y) * pf, pf), pf)
                gg[v, :, cols] = vals(0)[:, i * pf:(i + 1) * pf]
                gi[v, :, cols] = vals(1)[:, i * pf:(i + 1) * pf]

        put(ja, lambda w: fin[v, ja, w])
        for delta in RING:
            wait_recv(r3.at[v, delta - 1], r3_r.at[v, delta - 1])
            put(rot(ja, -delta), lambda w, delta=delta: r3[v, delta - 1, w])

    def step(fn, *args):
        with jax.named_scope(fn.__name__):
            fn(*args)

    def on(core):
        return pl.when(p == core)

    def take_turn():
        pl.semaphore_wait(turn, 1)

    def give_turn():
        pl.semaphore_signal(turn, inc=1, device_id=(d, 1 - p), device_id_type=MESH)

    h_mid, h_late, e_first, e_last = ((xo.at[i], mc_s.at[1 + i]) for i in QUARTERS)

    def pass_on(part, item, buf, which, vd):
        step(part, item[0], buf, which, vd, item[1])

    AFTER = (MINUS, OPP), (0, PLUS)
    step(direct_send, 0)
    step(small_send, 1, 0)

    @on(0)
    def _():
        step(spread_same, hb, 0, 0, mc_s.at[0])

    @on(1)
    def _():
        step(spread_same, eb, 1, 1, mc_s.at[0])

    step(direct_wait, 0)
    step(small_send, 0, 1)
    step(small_relay, 1, 0)
    step(large_send, 0, (0,), (0,))
    step(small_rest, 1, 0)
    step(small_last, 1, 0)
    step(small_send, 1, 1)
    step(small_relay, 0, 1)
    step(small_relay, 1, 1)
    step(small_rest, 0, 1)
    step(large_send, 0, (PLUS, MINUS), (MINUS, PLUS))
    step(small_last, 0, 1)
    step(large_send, 0, (OPP,), (OPP,))
    step(small_rest, 1, 1)
    step(small_last, 1, 1)
    step(large_relay, 0)

    @on(0)
    def _():
        step(large_send, 1, UP, DOWN)

    step(large_finish, 0)

    @on(0)
    def _():
        step(large_send, 1, *AFTER)

    @on(1)
    def _():
        step(take_turn)
        step(large_send, 1, UP, DOWN)
        step(spread_own, hb, 0, 0)

    step(block_gates, 0)

    @on(1)
    def _():
        step(large_send, 1, *AFTER)

    step(block_out, 0, h_mid[0])
    pass_on(spread_near, h_mid, hb, 0, p)
    step(large_relay, 1)

    @on(0)
    def _():
        step(give_turn)
        step(spread_relay, hb, 0, 0)

    step(large_finish, 1)

    @on(1)
    def _():
        pass_on(spread_far, h_mid, hb, 0, p)

    step(spread_own, hb, 0, 1)
    step(block_gates, 1)

    @on(0)
    def _():
        step(block_out, 1, h_late[0])
        pass_on(spread_near, h_late, hb, 0, 1)
        pass_on(spread_far, h_late, hb, 0, 1)
        step(spread_finish, hb, 0, 0)
        step(grad_first, 0, EARLY)
        step(grad_first, 0, LATE)
        step(spread_own, eb, 1, 1)
        pass_on(spread_far, h_mid, hb, 0, p)
        step(block_backward, 1, e_first[0])
        pass_on(spread_near, e_first, eb, 1, 0)
        pass_on(spread_far, e_first, eb, 1, 0)
        step(spread_relay, hb, 0, 1)

    @on(1)
    def _():
        step(spread_relay, hb, 0, 1)
        step(spread_relay, eb, 1, 1)
        step(block_backward, 1, e_first[0])
        pass_on(spread_near, e_first, eb, 1, 1)
        pass_on(spread_far, e_first, eb, 1, 1)

    step(grad_first, 1, EARLY)

    @on(0)
    def _():
        step(spread_relay, eb, 1, 1)

    step(grad_hidden, 1, EARLY)
    step(grad_out, 1, EARLY)

    @on(0)
    def _():
        step(grad_in, 1, EARLY)

    step(spread_finish, hb, 0, 1)
    step(grad_first, 1, LATE)
    step(spread_finish, eb, 1, 1)
    step(grad_hidden, 1, LATE)
    step(grad_out, 1, LATE)

    @on(0)
    def _():
        step(scatter_send, 1, OUT, 0, MERGED)

    @on(1)
    def _():
        step(spread_own, eb, 1, 0)
        step(block_backward, 0, e_last[0])
        pass_on(spread_near, e_last, eb, 1, 0)
        pass_on(spread_far, e_last, eb, 1, 0)
        step(scatter_send, 1, OUT, 0, MERGED)
        step(grad_in, 1, EARLY)

    step(grad_in, 1, LATE)
    step(scatter_send, 1, IN, 0, MERGED)

    @on(0)
    def _():
        step(spread_relay, eb, 1, 0)
        step(spread_own, eb, 1, 0)
        step(block_backward, 0, ga)
        send(ga, ga, ga_s, ga_r, d, 1)

    @on(1)
    def _():
        step(spread_relay, hb, 0, 0)
        step(grad_first, 0, EARLY)

    step(scatter_send, 1, OUT, 0, DIRECT)

    @on(1)
    def _():
        step(spread_relay, eb, 1, 0)
        step(spread_finish, hb, 0, 0)
        step(grad_first, 0, LATE)

    step(grad_hidden, 0, EARLY)
    step(scatter_send, 1, IN, 0, DIRECT)
    step(grad_in, 0, EARLY)
    step(scatter_relay, 1, OUT, 0)
    step(grad_out, 0, EARLY)
    step(spread_finish, eb, 1, 0)
    step(grad_hidden, 0, LATE)
    step(grad_in, 0, LATE)
    step(scatter_send, 0, IN, 0, MERGED)
    step(grad_out, 0, LATE)
    step(scatter_relay, 1, IN, 0)
    step(scatter_send, 0, OUT, 0, MERGED)
    step(scatter_send, 0, IN, 0, DIRECT)
    step(scatter_turn, 1, OUT)
    step(scatter_relay, 0, IN, 0)
    step(scatter_send, 0, OUT, 0, DIRECT)
    step(scatter_turn, 1, IN)
    step(scatter_relay, 0, OUT, 0)
    step(scatter_relay, 1, OUT, 1)

    @on(1)
    def _():
        wait_recv(ga, ga_r)

    gact[...] = ga[...]
    step(scatter_turn, 0, IN)
    step(scatter_relay, 1, IN, 1)
    step(scatter_turn, 0, OUT)
    step(scatter_out, 1)
    step(scatter_last, 1)
    step(scatter_relay, 0, IN, 1)
    step(scatter_relay, 0, OUT, 1)
    step(scatter_last, 0)
    step(scatter_finish, 1)
    step(scatter_out, 0)
    step(scatter_finish, 0)

    for v in BLOCKS:
        for k in parts(v):
            three = pl.ds(0, len(RING))
            wait_send(part_at(v, k, three, 0, 0), ag_s.at[v, k, 0])
            wait_send(part_at(v, k, whole, three, 0), ag_s.at[v, k, 1])
            wait_send(part_at(v, k, whole, whole, three), ag_s.at[v, k, LARGE])
        for colour in COLOURS:
            for which in HALVES:
                for st in HALVES:
                    wait_send(RECV[st][which][colour].at[v], rs_s.at[st, v, colour, which])
        wait_send(r3.at[v], r3_s.at[v])
        wait_send(hb.at[v, 0], rl_s.at[0, v])
        wait_send(hb.at[v, 0], rl_s.at[1, v])
    wait_send(hb.at[0, pl.ds(0, 2)], mc_s.at[0])
    wait_send(hb.at[0, pl.ds(0, 3)], mc_s.at[1])
    wait_send(hb.at[0, pl.ds(0, 3)], mc_s.at[3])

    @pl.when(p == 0)
    def _():
        wait_send(hb.at[0, pl.ds(0, 3)], mc_s.at[2])
        wait_send(ga, ga_s)

    @pl.when(p == 1)
    def _():
        wait_send(hb.at[0, pl.ds(0, 3)], mc_s.at[4])


def hand_on(*refs):
    copies = [pltpu.make_async_copy(refs[i], refs[NA + i], refs[-1].at[i]) for i in QUARTERS]
    for copy in copies:
        copy.start()
    for copy in copies:
        copy.wait()


def solution(mesh):
    act_spec = P(None, "data", None, None)
    w_spec = P(None, "stage", "data", None)

    def body(act_in, cot_out, w_gate, w_in, w_out):
        shape = act_in.shape
        dm, fd = shape[3], w_gate.shape[3]
        rows = shape[0] * shape[1] * shape[2]
        dr, fr, fs = dm // NL, fd // NL, fd // NA
        pf = fs // NA
        vmem = pltpu.VMEM
        dma = pltpu.SemaphoreType.DMA
        n2, n3, na = NB, len(RING), NA
        ring = (na, na)
        scratch = [
            vmem((n2, na, *ring, dr, fd), BF), vmem((n2, na, *ring, dr, fd), BF), vmem((n2, na, *ring, fr, dm), BF),
            vmem((n2, na, rows, dm), BF), vmem((n2, na, rows, dm), BF), vmem((na, rows, dm), BF), vmem((rows, dm), BF),
            vmem((n2, na, rows, dm), BF),
            vmem((n2, rows, fd), F32), vmem((n2, rows, fd), F32),
            vmem((n2, na, rows, fs), F32), vmem((n2, na, rows, fs), F32),
            vmem((n2, na, rows, fs), BF),
            vmem((rows, fd), BF), vmem((rows, fd), BF), vmem((rows, fd), BF),
            vmem((na, rows, fs), BF), vmem((na, rows, fs), BF),
            vmem((rows, dm), F32),
            vmem((n2, dm, fs), BF), vmem((n2, dm, fs), BF), vmem((fs, dm), BF),
            vmem((n2, n2, na, *ring, dr, fs), F32), vmem((n2, *ring, fr, dm), F32),
            vmem((n2, na, n2, dr, fs), F32), vmem((n2, n3, n2, dr, fs), F32),
            dma((n2, na)), dma((n2, na, n3)), dma((n2, na, n2, 6)), dma((n2, na, n3 * na)), dma((5,)), dma((n2, n2, 5)), dma((n2, n2)), dma, dma,
            dma((n2, n2, n2, n2)), dma((n2, n2, n2, n2, 6)), dma((n2,)), dma((n2, n3)), pltpu.SemaphoreType.REGULAR,
            *(vmem((n2, 6, *lead, width), F32)
              for lead_in, lead_out in (((*ring, dr), (n2, fr)), ((na, dr), (fr // n2,)))
              for lead, width in ((lead_in, fs - pf), (lead_in, pf), (lead_out, dm - pf), (lead_out, pf))),
        ]
        hbm = pl.BlockSpec(memory_space=pl.ANY)
        whole = pl.BlockSpec(memory_space=pltpu.VMEM)
        out = pl.pallas_call(
            kernel,
            out_shape=(
                vmem((rows, dm), BF), vmem((n2, dr, fd), F32), vmem((n2, dr, fd), F32), vmem((n2, fr, dm), F32),
            ),
            in_specs=[hbm] * 5,
            out_specs=(whole,) * NA,
            scratch_shapes=scratch,
            compiler_params=pltpu.CompilerParams(collective_id=0, has_side_effects=True, vmem_limit_bytes=66300000),
            name="train_step",
        )(act_in.reshape(rows, dm), cot_out.reshape(rows, dm), w_gate[:, 0], w_in[:, 0], w_out[:, 0])
        grad_act, grad_gate, grad_lin, grad_proj = pl.pallas_call(
            hand_on, out_shape=tuple(jax.ShapeDtypeStruct(a.shape, a.dtype) for a in out), in_specs=[whole] * NA, out_specs=(hbm,) * NA,
            scratch_shapes=[dma((NA,))], compiler_params=pltpu.CompilerParams(vmem_limit_bytes=2 ** 20), name="hand_on",
        )(*(pltpu.with_memory_space_constraint(a, vmem) for a in out))
        return grad_act.reshape(shape), grad_gate[:, None], grad_lin[:, None], grad_proj[:, None]

    return jax.shard_map(body, mesh=mesh, in_specs=(act_spec, act_spec, w_spec, w_spec, w_spec),
                         out_specs=(act_spec, w_spec, w_spec, w_spec), check_vma=False)
```

```python
import functools

import jax
import jax.numpy as jnp
from jax import lax
from jax.experimental import pallas as pl
from jax.experimental.pallas import tpu as pltpu
from jax.sharding import PartitionSpec as P

NORM_EPS = 1e-6
BF = jnp.bfloat16
F32 = jnp.float32
MESH = pl.DeviceIdType.MESH
X, Y, Z = 0, 1, 2
BLOCKS = COLOURS = HALVES = (0, 1)
NB, NA, NL = len(BLOCKS), 4, 64
RING = (1, 3, 2)
OPP = RING[-1]
PLUS, MINUS = RING[:-1]
QUARTERS = range(NA)
OWN = 0
AXES = ((Z, X, Y), (Y, Z, X), (X, Y, Z))
UP_MATS, OUT_MAT = (0, 1), (2,)
MATS = UP_MATS + OUT_MAT


def mm(left, right):
    return jnp.dot(left, right, preferred_element_type=F32)


def mm_nt(left, right):
    return lax.dot_general(left, right, (((1,), (1,)), ((), ())), preferred_element_type=F32)


def mm_tn(left, right):
    return lax.dot_general(left, right, (((0,), (0,)), ((), ())), preferred_element_type=F32)


def inv_rms(h):
    return lax.rsqrt(jnp.mean(h * h, axis=-1, keepdims=True) + NORM_EPS)


def kernel(act, cot, wg_in, wi_in, wo_in, gact, gg, gi, go,
           wg, wi, wo, hb, eb, xo, ga, ng, f1, f2, f1s, f2s, us, ub, da, db, das, dbs, qs, gs, is_, os_,
           gin, gout, fin, r3,
           lsem, ag_s, ag_r, lg_r, mc_s, mc_r, rl_s, ga_s, ga_r, rs_s, rs_r, r3_s, r3_r, turn, *rg):
    dm, fd = wo.shape[-1], wg.shape[-1]
    dr, fr = dm // NL, fd // NL
    fs = fd // NA
    pf = fs // NA
    rows = act.shape[0]
    wts = (wg, wi, wo)

    p = lax.axis_index("stage")
    d = lax.axis_index("data")
    zc, yc, xc = lax.div(d, 16), lax.rem(lax.div(d, 4), 4), lax.rem(d, 4)
    coord = (xc, yc, zc)
    stride = (1, 4, 16)
    ja = yc + p * (zc - yc)
    jb = zc + p * (yc - zc)
    sa, sb = 4 + 12 * p, 16 - 12 * p

    def rot(c, delta):
        return lax.rem(c + (delta % 4), 4)

    def peer(ax, delta):
        return d + (rot(coord[ax], delta) - coord[ax]) * stride[ax]

    def peer_a(delta):
        return d + (rot(ja, delta) - ja) * sa

    def peer_b(delta):
        return d + (rot(jb, delta) - jb) * sb

    def remote(src, dst, ssem, rsem, dev, core):
        return pltpu.make_async_remote_copy(src_ref=src, dst_ref=dst, send_sem=ssem, recv_sem=rsem,
                                            device_id=(dev, core), device_id_type=MESH)

    def send(src, dst, ssem, rsem, dev, core):
        remote(src, dst, ssem, rsem, dev, core).start()

    def wait_recv(ref, sem):
        remote(ref, ref, sem, sem, d, p).wait_recv()

    def wait_send(ref, sem):
        remote(ref, ref, sem, sem, d, p).wait_send()

    for v in BLOCKS:
        for k, shard in enumerate((wg_in, wi_in, wo_in)):
            pltpu.make_async_copy(shard.at[v], wts[k].at[v, zc, yc, xc], lsem.at[v, k]).start()

    @pl.when(p == 0)
    def _():
        pltpu.make_async_copy(act, hb.at[0, OWN], lsem.at[0, 3]).start()

    @pl.when(p == 1)
    def _():
        pltpu.make_async_copy(cot, eb.at[1, OWN], lsem.at[0, 3]).start()

    barrier = pltpu.get_barrier_semaphore()
    senders = [(peer(ax, delta), p) for ax in (X, Y, Z) for delta in RING]
    senders += [(d, 1 - p), (peer_a(1), 1 - p), (peer_a(-1), 1 - p)]
    for dev, core in senders:
        pl.semaphore_signal(barrier, inc=1, device_id=(dev, core), device_id_type=MESH)
    for v in BLOCKS:
        for k, shard in enumerate((wg_in, wi_in, wo_in)):
            pltpu.make_async_copy(shard.at[v], wts[k].at[v, zc, yc, xc], lsem.at[v, k]).wait()

    @pl.when(p == 0)
    def _():
        pltpu.make_async_copy(act, hb.at[0, OWN], lsem.at[0, 3]).wait()

    @pl.when(p == 1)
    def _():
        pltpu.make_async_copy(cot, eb.at[1, OWN], lsem.at[0, 3]).wait()

    pl.semaphore_wait(barrier, len(senders))

    FIRST, REST = ((0, PLUS, 0), (1, MINUS, 2)), ((1, PLUS, 1), (0, MINUS, 3))
    LARGE = 2
    whole = slice(None)

    def part_at(v, k, small, middle, large, half=None):
        place = dict(zip(AXES[k], (small, middle, large)))
        width = wts[k].shape[-1] // 2
        cols = whole if half is None else pl.ds(half * width, width)
        return wts[k].at[v, place[Z], place[Y], place[X], :, cols]

    def own(k):
        return [coord[ax] for ax in AXES[k]]

    def chunk(v, k, ph, q, half):
        small, middle, large = own(k)
        return part_at(v, k, q, middle, large, half) if ph == 0 else part_at(v, k, pl.ds(2 * half, 2), q, large)

    def small_copy(v, k, ph, q, half, delta, slot):
        ref = chunk(v, k, ph, q, half)
        send(ref, ref, ag_s.at[v, k, ph], ag_r.at[v, k, ph, slot], peer(AXES[k][ph], delta), p)

    def small_wait(v, k, ph, back, half, slot):
        wait_recv(chunk(v, k, ph, rot(coord[AXES[k][ph]], back), half), ag_r.at[v, k, ph, slot])

    def small_send(v, ph):
        for half, delta, slot in FIRST + REST:
            for k in MATS:
                small_copy(v, k, ph, coord[AXES[k][ph]], half, delta, slot)

    def small_relay(v, ph):
        for half, delta, slot in FIRST:
            for k in MATS:
                small_wait(v, k, ph, -delta, half, slot)
                small_copy(v, k, ph, rot(coord[AXES[k][ph]], -delta), half, delta, 4 + half)

    def small_rest(v, ph):
        for half, delta, slot in REST:
            for k in MATS:
                small_wait(v, k, ph, -delta, half, slot)

    def small_last(v, ph):
        for half in HALVES:
            for k in MATS:
                small_wait(v, k, ph, OPP, half, 4 + half)

    def direct_send(v):
        for delta in (OPP, PLUS, MINUS):
            for k in MATS:
                ref = part_at(v, k, *own(k))
                send(ref, ref, ag_s.at[v, k, 0], ag_r.at[v, k, 0, delta], peer(AXES[k][0], delta), p)

    def direct_wait(v):
        for delta in RING:
            for k in MATS:
                small, middle, large = own(k)
                wait_recv(part_at(v, k, rot(small, -delta), middle, large), ag_r.at[v, k, 0, delta])

    UP, DOWN = (0, PLUS), (MINUS, OPP)
    RELAYS = ((UP[0], PLUS), (DOWN[0], MINUS), (UP[1], PLUS), (DOWN[1], MINUS))

    def row(v, k, q, r):
        return part_at(v, k, whole, rot(coord[AXES[k][1]], r), q)

    def large_slot(r, delta):
        return r if delta == PLUS else NA + r

    def large_send(v, up, down):
        for pair in zip(up, down):
            for r, delta in zip(pair, (PLUS, MINUS)):
                for k in MATS:
                    ax = AXES[k][LARGE]
                    ref = row(v, k, coord[ax], r)
                    send(ref, ref, ag_s.at[v, k, LARGE], lg_r.at[v, k, large_slot(r, delta)], peer(ax, delta), p)

    def large_relay(v):
        for r, delta in RELAYS:
            for k in MATS:
                ax = AXES[k][LARGE]
                ref = row(v, k, rot(coord[ax], -delta), r)
                wait_recv(ref, lg_r.at[v, k, large_slot(r, delta)])
                send(ref, ref, ag_s.at[v, k, LARGE], lg_r.at[v, k, 2 * NA + r], peer(ax, delta), p)

    def large_finish(v, mats):
        for pieces, delta in ((DOWN, PLUS), (UP, MINUS)):
            for r in pieces:
                for k in mats:
                    wait_recv(row(v, k, rot(coord[AXES[k][LARGE]], -delta), r), lg_r.at[v, k, large_slot(r, delta)])
        for r in QUARTERS:
            for k in mats:
                wait_recv(row(v, k, rot(coord[AXES[k][LARGE]], OPP), r), lg_r.at[v, k, 2 * NA + r])

    half_rows = rows // 2
    BACK, AHEAD, FAR = 1, 2, 3

    def spread_near(src, buf, which, vd, ssem):
        send(src, buf.at[vd, OWN], ssem, mc_r.at[which, vd, OWN], d, 1 - p)

    def spread_far(src, buf, which, vd, ssem):
        send(src, buf.at[vd, BACK], ssem, mc_r.at[which, vd, BACK], peer_b(PLUS), 1 - p)
        send(src, buf.at[vd, AHEAD], ssem, mc_r.at[which, vd, AHEAD], peer_b(MINUS), 1 - p)

    def spread_same(buf, which, v, ssem):
        send(buf.at[v, OWN], buf.at[v, BACK], ssem, mc_r.at[which, v, BACK], peer_a(PLUS), p)
        send(buf.at[v, OWN], buf.at[v, AHEAD], ssem, mc_r.at[which, v, AHEAD], peer_a(MINUS), p)

    def spread_relay(buf, which, v):
        for half, slot, delta in ((0, BACK, PLUS), (1, AHEAD, MINUS)):
            wait_recv(buf.at[v, slot], mc_r.at[which, v, slot])
            part = pl.ds(half * half_rows, half_rows)
            send(buf.at[v, slot, part], buf.at[v, FAR, part], rl_s.at[which, v], mc_r.at[which, v, FAR + half], peer_a(delta), p)

    def spread_finish(buf, which, v):
        for half in HALVES:
            wait_recv(buf.at[v, FAR, pl.ds(half * half_rows, half_rows)], mc_r.at[which, v, FAR + half])

    def spread_own(buf, which, v):
        wait_recv(buf.at[v, OWN], mc_r.at[which, v, OWN])

    def gates(n, wgt, wlin):
        a, b = mm(n, wgt), mm(n, wlin)
        s = jax.nn.sigmoid(a)
        act_a = a * s
        return (act_a * b).astype(BF), b * s * (1.0 + a * (1.0 - s)), act_a

    def block_gates(v):
        h = hb[v, OWN].astype(F32)
        n = (h * inv_rms(h)).astype(BF)

        def tile(i, carry):
            wide = fs // 2
            cols = pl.ds(pl.multiple_of(i * wide, wide), wide)
            u, t1, t2 = gates(n, wg[v, :, :, :, :, cols].reshape(dm, wide), wi[v, :, :, :, :, cols].reshape(dm, wide))
            ub[:, cols] = u
            f1[v, :, cols] = t1
            f2[v, :, cols] = t2
            return carry

        lax.fori_loop(0, 2 * NA, tile, 0, unroll=True)

    def block_out(v, dst):
        half_dm = dm // 2
        for i in HALVES:
            cols = pl.ds(i * half_dm, half_dm)
            out = mm(ub[...], wo[v, :, :, :, :, cols].reshape(fd, half_dm))
            dst[:, cols] = (hb[v, OWN, :, cols].astype(F32) + out).astype(BF)

    def block_backward(v, dst):
        e = eb[v, OWN]

        def tile(i, carry):
            cols = pl.ds(pl.multiple_of(i * fs, fs), fs)
            t = mm_nt(e, wo[v, i].reshape(fs, dm))
            da[:, cols] = (t * f1[v, :, cols]).astype(BF)
            db[:, cols] = (t * f2[v, :, cols]).astype(BF)
            return carry

        lax.fori_loop(0, NA, tile, 0, unroll=True)
        half_dm = dm // 2
        for i in HALVES:
            q = mm_nt(da[...], wg[v, pl.ds(2 * i, 2)].reshape(half_dm, fd))
            q += mm_nt(db[...], wi[v, pl.ds(2 * i, 2)].reshape(half_dm, fd))
            qs[:, pl.ds(i * half_dm, half_dm)] = q
        h = hb[v, OWN].astype(F32)
        r = inv_rms(h)
        hr = h * r
        q = qs[...]
        dst[...] = (e.astype(F32) + r * (q - hr * jnp.mean(q * hr, axis=-1, keepdims=True))).astype(BF)

    def piece(j, i):
        z = i + p * (j - i)
        y = j + p * (i - j)
        return z, y

    EARLY, LATE = range(FAR), range(FAR, NA)

    def grad_first(v, slots):
        for i in QUARTERS if OWN in slots else ():
            z, y = piece(ja, i)
            cols = pl.ds(pl.multiple_of((z * NA + y) * pf, pf), pf)
            gs[v, :, pl.ds(i * pf, pf)] = wg[v, :, :, :, :, cols].reshape(dm, pf)
            is_[v, :, pl.ds(i * pf, pf)] = wi[v, :, :, :, :, cols].reshape(dm, pf)
        for s in slots:
            h = hb[v, s].astype(F32)
            n = (h * inv_rms(h)).astype(BF)
            ng[v, s] = n
            u, t1, t2 = gates(n, gs[v], is_[v])
            us[v, s] = u
            f1s[v, s] = t1
            f2s[v, s] = t2

    def grad_hidden(v, slots):
        for i in QUARTERS if OWN in slots else ():
            z, y = piece(ja, i)
            os_[pl.ds(i * pf, pf), :] = wo[v, z, y].reshape(pf, dm)
        for s in slots:
            t = mm_nt(eb[v, s], os_[...])
            das[s] = (t * f1s[v, s]).astype(BF)
            dbs[s] = (t * f2s[v, s]).astype(BF)

    def rows_of(slots):
        return pl.ds(slots[0], len(slots)), len(slots) * rows

    def grad_out(v, slots):
        some, count = rows_of(slots)
        for i in HALVES:
            cols, to = pl.ds(i * 2 * pf, 2 * pf), pl.ds(2 * i, 2)
            g = mm_tn(us[v, some, :, cols].reshape(count, 2 * pf), eb[v, some].reshape(count, dm)).reshape(2, 4, fr, dm)
            gout[v, to] = g if OWN in slots else gout[v, to] + g

    def grad_in(v, slots):
        some, count = rows_of(slots)
        for which, dref in enumerate((das, dbs)):
            for i in QUARTERS:
                cols = pl.ds(i * (dm // NA), dm // NA)
                g = mm_tn(ng[v, some, :, cols].reshape(count, dm // NA), dref[some].reshape(count, fs)).reshape(4, 4, dr, fs)
                for y in QUARTERS:
                    at = (v, which, y + p * (i - y), i + p * (y - i))
                    gin[at] = g[y] if OWN in slots else gin[at] + g[y]

    IN, OUT = 0, 1

    def split(width):
        return pl.ds(0, width - pf), pl.ds(width - pf, pf)

    def view(which, st, v, colour, t, half):
        along_b = colour == st
        if which == IN:
            cols = split(fs)[colour]
            b, x = (t, slice(None) if st == 0 else xc) if along_b else (slice(None) if st == 0 else jb, t)
            return gin.at[v, half, :, b, x, :, cols]
        cols = split(dm)[colour]
        if st == 0:
            hs = pl.ds(2 * half, 2)
            return gout.at[v, t, hs, :, cols] if along_b else gout.at[v, hs, t, :, cols]
        hs = pl.ds(half * (fr // 2), fr // 2)
        return gout.at[v, t, xc, hs, cols] if along_b else gout.at[v, jb, t, hs, cols]

    RECV = (((rg[0], rg[1]), (rg[2], rg[3])), ((rg[4], rg[5]), (rg[6], rg[7])))
    MERGED, DIRECT = ((0, OPP, PLUS, 0), (1, OPP, MINUS, 1)), ((1, PLUS, PLUS, 2), (0, MINUS, MINUS, 3))
    RELAYED = ((0, PLUS, PLUS, 4), (1, MINUS, MINUS, 5))

    def axis_of(colour, st):
        return (jb, peer_b) if colour == st else (xc, functools.partial(peer, X))

    def scatter_send(v, which, st, copies):
        for colour in COLOURS:
            q, to = axis_of(colour, st)
            for half, c, delta, slot in copies:
                send(view(which, st, v, colour, rot(q, c), half), RECV[st][which][colour].at[v, slot],
                     rs_s.at[st, v, colour, which], rs_r.at[st, v, colour, which, slot], to(delta), p)

    def scatter_relay(v, which, st):
        for colour in COLOURS:
            q, _ = axis_of(colour, st)
            recv = RECV[st][which][colour]
            for half, c, _, slot in RELAYED:
                wait_recv(recv.at[v, slot - 4], rs_r.at[st, v, colour, which, slot - 4])
                ref = view(which, st, v, colour, rot(q, c), half)
                ref[...] = ref[...] + recv[v, slot - 4]
        scatter_send(v, which, st, RELAYED)

    def scatter_sum(v, which, st):
        for colour in COLOURS:
            q, _ = axis_of(colour, st)
            recv = RECV[st][which][colour]
            for half in HALVES:
                direct, merged = 3 - half, 4 + half
                for slot in (direct, merged):
                    wait_recv(recv.at[v, slot], rs_r.at[st, v, colour, which, slot])
                ref = view(which, st, v, colour, q, half)
                ref[...] = ref[...] + recv[v, direct] + recv[v, merged]

    def scatter_turn(v, which):
        scatter_sum(v, which, 0)
        scatter_send(v, which, 1, MERGED + DIRECT)

    def scatter_out(v):
        scatter_sum(v, OUT, 1)
        go[v] = gout[v, jb, xc]

    def scatter_last(v):
        scatter_sum(v, IN, 1)
        for which in HALVES:
            fin[v, :, which] = gin[v, which, :, jb, xc]
        for delta in (OPP, PLUS, MINUS):
            send(fin.at[v, rot(ja, delta)], r3.at[v, delta - 1], r3_s.at[v], r3_r.at[v, delta - 1], peer_a(delta), p)

    def scatter_finish(v):
        def put(j, vals):
            for i in QUARTERS:
                z, y = piece(j, i)
                cols = pl.ds(pl.multiple_of((z * NA + y) * pf, pf), pf)
                gg[v, :, cols] = vals(0)[:, i * pf:(i + 1) * pf]
                gi[v, :, cols] = vals(1)[:, i * pf:(i + 1) * pf]

        put(ja, lambda w: fin[v, ja, w])
        for delta in RING:
            wait_recv(r3.at[v, delta - 1], r3_r.at[v, delta - 1])
            put(rot(ja, -delta), lambda w, delta=delta: r3[v, delta - 1, w])

    def step(fn, *args):
        with jax.named_scope(fn.__name__):
            fn(*args)

    def on(core):
        return pl.when(p == core)

    def take_turn():
        pl.semaphore_wait(turn, 1)

    def give_turn():
        pl.semaphore_signal(turn, inc=1, device_id=(d, 1 - p), device_id_type=MESH)

    h_mid, h_late, e_first, e_last = ((xo.at[i], mc_s.at[1 + i]) for i in QUARTERS)

    def pass_on(part, item, buf, which, vd):
        step(part, item[0], buf, which, vd, item[1])

    AFTER = (MINUS, OPP), (0, PLUS)
    step(direct_send, 0)
    step(small_send, 1, 0)
    step(direct_wait, 0)
    step(small_send, 0, 1)
    step(small_relay, 1, 0)
    step(large_send, 0, (0,), (0,))
    step(small_rest, 1, 0)
    step(small_last, 1, 0)
    step(small_send, 1, 1)
    step(small_relay, 0, 1)
    step(small_relay, 1, 1)
    step(small_rest, 0, 1)
    step(large_send, 0, (PLUS, MINUS), (MINUS, PLUS))
    step(small_last, 0, 1)
    step(large_send, 0, (OPP,), (OPP,))
    step(small_rest, 1, 1)
    step(small_last, 1, 1)
    step(large_relay, 0)

    @on(0)
    def _():
        step(large_send, 1, UP, DOWN)

    step(large_finish, 0, UP_MATS)

    @on(0)
    def _():
        step(large_send, 1, *AFTER)

    @on(1)
    def _():
        step(take_turn)
        step(large_send, 1, UP, DOWN)
        step(spread_own, hb, 0, 0)

    step(block_gates, 0)

    @on(1)
    def _():
        step(large_send, 1, *AFTER)

    step(large_finish, 0, OUT_MAT)
    step(block_out, 0, h_mid[0])
    pass_on(spread_near, h_mid, hb, 0, p)
    step(large_relay, 1)

    @on(0)
    def _():
        step(give_turn)

    step(spread_own, hb, 0, 1)
    step(large_finish, 1, UP_MATS)
    step(block_gates, 1)
    step(large_finish, 1, OUT_MAT)

    @on(0)
    def _():
        step(block_out, 1, h_late[0])
        pass_on(spread_near, h_late, hb, 0, 1)
        pass_on(spread_far, h_late, hb, 0, 1)
        step(spread_own, eb, 1, 1)
        pass_on(spread_far, h_mid, hb, 0, p)
        step(block_backward, 1, e_first[0])
        pass_on(spread_near, e_first, eb, 1, 0)
        pass_on(spread_far, e_first, eb, 1, 0)
        step(spread_same, hb, 0, 0, mc_s.at[0])
        step(spread_relay, hb, 0, 1)

    @on(1)
    def _():
        pass_on(spread_far, h_mid, hb, 0, p)
        step(spread_same, eb, 1, 1, mc_s.at[0])
        step(block_backward, 1, e_first[0])
        pass_on(spread_near, e_first, eb, 1, 1)
        pass_on(spread_far, e_first, eb, 1, 1)
        step(spread_relay, hb, 0, 1)

    step(grad_first, 1, EARLY)
    step(spread_relay, eb, 1, 1)

    step(grad_hidden, 1, EARLY)
    step(grad_out, 1, EARLY)

    @on(0)
    def _():
        step(grad_in, 1, EARLY)
        step(spread_relay, hb, 0, 0)

    @on(1)
    def _():
        step(spread_own, eb, 1, 0)
        step(block_backward, 0, e_last[0])
        pass_on(spread_near, e_last, eb, 1, 0)
        pass_on(spread_far, e_last, eb, 1, 0)
        step(grad_in, 1, EARLY)

    step(spread_finish, hb, 0, 1)
    step(grad_first, 1, LATE)

    @on(0)
    def _():
        step(grad_first, 0, EARLY)

    step(spread_finish, eb, 1, 1)
    step(grad_hidden, 1, LATE)
    step(grad_out, 1, LATE)
    step(scatter_send, 1, OUT, 0, MERGED)
    step(grad_in, 1, LATE)
    step(scatter_send, 1, IN, 0, MERGED)

    @on(0)
    def _():
        step(spread_relay, eb, 1, 0)
        step(spread_own, eb, 1, 0)
        step(block_backward, 0, ga)
        send(ga, ga, ga_s, ga_r, d, 1)

    @on(1)
    def _():
        step(spread_relay, hb, 0, 0)
        step(grad_first, 0, EARLY)

    step(scatter_send, 1, OUT, 0, DIRECT)

    @on(1)
    def _():
        step(spread_relay, eb, 1, 0)

    step(spread_finish, hb, 0, 0)
    step(grad_first, 0, LATE)

    step(grad_hidden, 0, EARLY)
    step(scatter_send, 1, IN, 0, DIRECT)
    step(grad_in, 0, EARLY)
    step(scatter_relay, 1, OUT, 0)
    step(grad_out, 0, EARLY)
    step(spread_finish, eb, 1, 0)
    step(grad_hidden, 0, LATE)
    step(grad_in, 0, LATE)
    step(scatter_send, 0, IN, 0, MERGED)
    step(grad_out, 0, LATE)
    step(scatter_relay, 1, IN, 0)
    step(scatter_send, 0, OUT, 0, MERGED)
    step(scatter_send, 0, IN, 0, DIRECT)
    step(scatter_turn, 1, OUT)
    step(scatter_relay, 0, IN, 0)
    step(scatter_send, 0, OUT, 0, DIRECT)
    step(scatter_turn, 1, IN)
    step(scatter_relay, 0, OUT, 0)
    step(scatter_relay, 1, OUT, 1)

    @on(1)
    def _():
        wait_recv(ga, ga_r)

    gact[...] = ga[...]
    step(scatter_turn, 0, IN)
    step(scatter_relay, 1, IN, 1)
    step(scatter_turn, 0, OUT)
    step(scatter_out, 1)
    step(scatter_last, 1)
    step(scatter_relay, 0, IN, 1)
    step(scatter_relay, 0, OUT, 1)
    step(scatter_last, 0)
    step(scatter_finish, 1)
    step(scatter_out, 0)
    step(scatter_finish, 0)

    for v in BLOCKS:
        for k in MATS:
            three = pl.ds(0, len(RING))
            wait_send(part_at(v, k, three, 0, 0), ag_s.at[v, k, 0])
            wait_send(part_at(v, k, whole, three, 0), ag_s.at[v, k, 1])
            wait_send(part_at(v, k, whole, whole, three), ag_s.at[v, k, LARGE])
        for colour in COLOURS:
            for which in HALVES:
                for st in HALVES:
                    wait_send(RECV[st][which][colour].at[v], rs_s.at[st, v, colour, which])
        wait_send(r3.at[v], r3_s.at[v])
        wait_send(hb.at[v, 0], rl_s.at[0, v])
        wait_send(hb.at[v, 0], rl_s.at[1, v])
    wait_send(hb.at[0, pl.ds(0, 2)], mc_s.at[0])
    wait_send(hb.at[0, pl.ds(0, 3)], mc_s.at[1])
    wait_send(hb.at[0, pl.ds(0, 3)], mc_s.at[3])

    @pl.when(p == 0)
    def _():
        wait_send(hb.at[0, pl.ds(0, 3)], mc_s.at[2])
        wait_send(ga, ga_s)

    @pl.when(p == 1)
    def _():
        wait_send(hb.at[0, pl.ds(0, 3)], mc_s.at[4])


def hand_on(*refs):
    copies = [pltpu.make_async_copy(refs[i], refs[NA + i], refs[-1].at[i]) for i in QUARTERS]
    for copy in copies:
        copy.start()
    for copy in copies:
        copy.wait()


def solution(mesh):
    act_spec = P(None, "data", None, None)
    w_spec = P(None, "stage", "data", None)

    def body(act_in, cot_out, w_gate, w_in, w_out):
        shape = act_in.shape
        dm, fd = shape[3], w_gate.shape[3]
        rows = shape[0] * shape[1] * shape[2]
        dr, fr, fs = dm // NL, fd // NL, fd // NA
        pf = fs // NA
        vmem = pltpu.VMEM
        dma = pltpu.SemaphoreType.DMA
        n2, n3, na = NB, len(RING), NA
        ring = (na, na)
        scratch = [
            vmem((n2, na, *ring, dr, fd), BF), vmem((n2, na, *ring, dr, fd), BF), vmem((n2, na, *ring, fr, dm), BF),
            vmem((n2, na, rows, dm), BF), vmem((n2, na, rows, dm), BF), vmem((na, rows, dm), BF), vmem((rows, dm), BF),
            vmem((n2, na, rows, dm), BF),
            vmem((n2, rows, fd), F32), vmem((n2, rows, fd), F32),
            vmem((n2, na, rows, fs), F32), vmem((n2, na, rows, fs), F32),
            vmem((n2, na, rows, fs), BF),
            vmem((rows, fd), BF), vmem((rows, fd), BF), vmem((rows, fd), BF),
            vmem((na, rows, fs), BF), vmem((na, rows, fs), BF),
            vmem((rows, dm), F32),
            vmem((n2, dm, fs), BF), vmem((n2, dm, fs), BF), vmem((fs, dm), BF),
            vmem((n2, n2, na, *ring, dr, fs), F32), vmem((n2, *ring, fr, dm), F32),
            vmem((n2, na, n2, dr, fs), F32), vmem((n2, n3, n2, dr, fs), F32),
            dma((n2, na)), dma((n2, n3, n3)), dma((n2, n3, n2, 6)), dma((n2, n3, n3 * na)), dma((5,)), dma((n2, n2, 5)), dma((n2, n2)), dma, dma,
            dma((n2, n2, n2, n2)), dma((n2, n2, n2, n2, 6)), dma((n2,)), dma((n2, n3)), pltpu.SemaphoreType.REGULAR,
            *(vmem((n2, 6, *lead, width), F32)
              for lead_in, lead_out in (((*ring, dr), (n2, fr)), ((na, dr), (fr // n2,)))
              for lead, width in ((lead_in, fs - pf), (lead_in, pf), (lead_out, dm - pf), (lead_out, pf))),
        ]
        hbm = pl.BlockSpec(memory_space=pl.ANY)
        whole = pl.BlockSpec(memory_space=pltpu.VMEM)
        out = pl.pallas_call(
            kernel,
            out_shape=(
                vmem((rows, dm), BF), vmem((n2, dr, fd), F32), vmem((n2, dr, fd), F32), vmem((n2, fr, dm), F32),
            ),
            in_specs=[hbm] * 5,
            out_specs=(whole,) * NA,
            scratch_shapes=scratch,
            compiler_params=pltpu.CompilerParams(collective_id=0, has_side_effects=True, vmem_limit_bytes=66300000),
            name="train_step",
        )(act_in.reshape(rows, dm), cot_out.reshape(rows, dm), w_gate[:, 0], w_in[:, 0], w_out[:, 0])
        grad_act, grad_gate, grad_lin, grad_proj = pl.pallas_call(
            hand_on, out_shape=tuple(jax.ShapeDtypeStruct(a.shape, a.dtype) for a in out), in_specs=[whole] * NA, out_specs=(hbm,) * NA,
            scratch_shapes=[dma((NA,))], compiler_params=pltpu.CompilerParams(vmem_limit_bytes=2 ** 20), name="hand_on",
        )(*(pltpu.with_memory_space_constraint(a, vmem) for a in out))
        return grad_act.reshape(shape), grad_gate[:, None], grad_lin[:, None], grad_proj[:, None]

    return jax.shard_map(body, mesh=mesh, in_specs=(act_spec, act_spec, w_spec, w_spec, w_spec),
                         out_specs=(act_spec, w_spec, w_spec, w_spec), check_vma=False)
```

```python
import functools

import jax
import jax.numpy as jnp
from jax import lax
from jax.experimental import pallas as pl
from jax.experimental.pallas import tpu as pltpu
from jax.sharding import PartitionSpec as P

NORM_EPS = 1e-6
BF = jnp.bfloat16
F32 = jnp.float32
MESH = pl.DeviceIdType.MESH
X, Y, Z = 0, 1, 2
BLOCKS = COLOURS = HALVES = (0, 1)
NB, NA, NL = len(BLOCKS), 4, 64
RING = (1, 3, 2)
OPP = RING[-1]
PLUS, MINUS = RING[:-1]
QUARTERS = range(NA)
OWN = 0
AXES = ((Z, X, Y), (Y, Z, X), (X, Y, Z))
UP_MATS, OUT_MAT = (0, 1), (2,)
MATS = UP_MATS + OUT_MAT


def mm(left, right):
    return jnp.dot(left, right, preferred_element_type=F32)


def mm_nt(left, right):
    return lax.dot_general(left, right, (((1,), (1,)), ((), ())), preferred_element_type=F32)


def mm_tn(left, right):
    return lax.dot_general(left, right, (((0,), (0,)), ((), ())), preferred_element_type=F32)


def inv_rms(h):
    return lax.rsqrt(jnp.mean(h * h, axis=-1, keepdims=True) + NORM_EPS)


def kernel(act, cot, wg_in, wi_in, wo_in, gact, gg, gi, go,
           wg, wi, wo, hb, eb, xo, ga, ng, f1, f2, f1s, f2s, us, ub, da, db, das, dbs, qs, gs, is_, os_,
           gin, gout, fin, r3,
           lsem, ag_s, ag_r, lg_r, mc_s, mc_r, rl_s, ga_s, ga_r, rs_s, rs_r, r3_s, r3_r, turn, *rg):
    dm, fd = wo.shape[-1], wg.shape[-1]
    dr, fr = dm // NL, fd // NL
    fs = fd // NA
    pf = fs // NA
    rows = act.shape[0]
    wts = (wg, wi, wo)

    p = lax.axis_index("stage")
    d = lax.axis_index("data")
    zc, yc, xc = lax.div(d, 16), lax.rem(lax.div(d, 4), 4), lax.rem(d, 4)
    coord = (xc, yc, zc)
    stride = (1, 4, 16)
    ja = yc + p * (zc - yc)
    jb = zc + p * (yc - zc)
    sa, sb = 4 + 12 * p, 16 - 12 * p

    def rot(c, delta):
        return lax.rem(c + (delta % 4), 4)

    def peer(ax, delta):
        return d + (rot(coord[ax], delta) - coord[ax]) * stride[ax]

    def peer_a(delta):
        return d + (rot(ja, delta) - ja) * sa

    def peer_b(delta):
        return d + (rot(jb, delta) - jb) * sb

    def remote(src, dst, ssem, rsem, dev, core):
        return pltpu.make_async_remote_copy(src_ref=src, dst_ref=dst, send_sem=ssem, recv_sem=rsem,
                                            device_id=(dev, core), device_id_type=MESH)

    def send(src, dst, ssem, rsem, dev, core):
        remote(src, dst, ssem, rsem, dev, core).start()

    def wait_recv(ref, sem):
        remote(ref, ref, sem, sem, d, p).wait_recv()

    def wait_send(ref, sem):
        remote(ref, ref, sem, sem, d, p).wait_send()

    for v in BLOCKS:
        for k, shard in enumerate((wg_in, wi_in, wo_in)):
            pltpu.make_async_copy(shard.at[v], wts[k].at[v, zc, yc, xc], lsem.at[v, k]).start()

    @pl.when(p == 0)
    def _():
        pltpu.make_async_copy(act, hb.at[0, OWN], lsem.at[0, 3]).start()

    @pl.when(p == 1)
    def _():
        pltpu.make_async_copy(cot, eb.at[1, OWN], lsem.at[0, 3]).start()

    barrier = pltpu.get_barrier_semaphore()
    senders = [(peer(ax, delta), p) for ax in (X, Y, Z) for delta in RING]
    senders += [(d, 1 - p), (peer_a(1), 1 - p), (peer_a(-1), 1 - p)]
    for dev, core in senders:
        pl.semaphore_signal(barrier, inc=1, device_id=(dev, core), device_id_type=MESH)
    for v in BLOCKS:
        for k, shard in enumerate((wg_in, wi_in, wo_in)):
            pltpu.make_async_copy(shard.at[v], wts[k].at[v, zc, yc, xc], lsem.at[v, k]).wait()

    @pl.when(p == 0)
    def _():
        pltpu.make_async_copy(act, hb.at[0, OWN], lsem.at[0, 3]).wait()

    @pl.when(p == 1)
    def _():
        pltpu.make_async_copy(cot, eb.at[1, OWN], lsem.at[0, 3]).wait()

    pl.semaphore_wait(barrier, len(senders))

    FIRST, REST = ((0, PLUS, 0), (1, MINUS, 2)), ((1, PLUS, 1), (0, MINUS, 3))
    LARGE = 2
    whole = slice(None)

    def part_at(v, k, small, middle, large, half=None):
        place = dict(zip(AXES[k], (small, middle, large)))
        width = wts[k].shape[-1] // 2
        cols = whole if half is None else pl.ds(half * width, width)
        return wts[k].at[v, place[Z], place[Y], place[X], :, cols]

    def own(k):
        return [coord[ax] for ax in AXES[k]]

    def chunk(v, k, ph, q, half):
        small, middle, large = own(k)
        return part_at(v, k, q, middle, large, half) if ph == 0 else part_at(v, k, pl.ds(2 * half, 2), q, large)

    def small_copy(v, k, ph, q, half, delta, slot):
        ref = chunk(v, k, ph, q, half)
        send(ref, ref, ag_s.at[v, k, ph], ag_r.at[v, k, ph, slot], peer(AXES[k][ph], delta), p)

    def small_wait(v, k, ph, back, half, slot):
        wait_recv(chunk(v, k, ph, rot(coord[AXES[k][ph]], back), half), ag_r.at[v, k, ph, slot])

    def small_send(v, ph):
        for half, delta, slot in FIRST + REST:
            for k in MATS:
                small_copy(v, k, ph, coord[AXES[k][ph]], half, delta, slot)

    def small_relay(v, ph):
        for half, delta, slot in FIRST:
            for k in MATS:
                small_wait(v, k, ph, -delta, half, slot)
                small_copy(v, k, ph, rot(coord[AXES[k][ph]], -delta), half, delta, 4 + half)

    def small_rest(v, ph):
        for half, delta, slot in REST:
            for k in MATS:
                small_wait(v, k, ph, -delta, half, slot)

    def small_last(v, ph):
        for half in HALVES:
            for k in MATS:
                small_wait(v, k, ph, OPP, half, 4 + half)

    def direct_send(v):
        for delta in (OPP, PLUS, MINUS):
            for k in MATS:
                ref = part_at(v, k, *own(k))
                send(ref, ref, ag_s.at[v, k, 0], ag_r.at[v, k, 0, delta], peer(AXES[k][0], delta), p)

    def direct_wait(v):
        for delta in RING:
            for k in MATS:
                small, middle, large = own(k)
                wait_recv(part_at(v, k, rot(small, -delta), middle, large), ag_r.at[v, k, 0, delta])

    UP, DOWN = (0, PLUS), (MINUS, OPP)
    RELAYS = ((UP[0], PLUS), (DOWN[0], MINUS), (UP[1], PLUS), (DOWN[1], MINUS))

    def row(v, k, q, r):
        return part_at(v, k, whole, rot(coord[AXES[k][1]], r), q)

    def large_slot(r, delta):
        return r if delta == PLUS else NA + r

    def large_send(v, up, down):
        for pair in zip(up, down):
            for r, delta in zip(pair, (PLUS, MINUS)):
                for k in MATS:
                    ax = AXES[k][LARGE]
                    ref = row(v, k, coord[ax], r)
                    send(ref, ref, ag_s.at[v, k, LARGE], lg_r.at[v, k, large_slot(r, delta)], peer(ax, delta), p)

    def large_relay(v):
        for r, delta in RELAYS:
            for k in MATS:
                ax = AXES[k][LARGE]
                ref = row(v, k, rot(coord[ax], -delta), r)
                wait_recv(ref, lg_r.at[v, k, large_slot(r, delta)])
                send(ref, ref, ag_s.at[v, k, LARGE], lg_r.at[v, k, 2 * NA + r], peer(ax, delta), p)

    def large_finish(v, mats):
        for pieces, delta in ((DOWN, PLUS), (UP, MINUS)):
            for r in pieces:
                for k in mats:
                    wait_recv(row(v, k, rot(coord[AXES[k][LARGE]], -delta), r), lg_r.at[v, k, large_slot(r, delta)])
        for r in QUARTERS:
            for k in mats:
                wait_recv(row(v, k, rot(coord[AXES[k][LARGE]], OPP), r), lg_r.at[v, k, 2 * NA + r])

    half_rows = rows // 2
    BACK, AHEAD, FAR = 1, 2, 3

    def spread_near(src, buf, which, vd, ssem):
        send(src, buf.at[vd, OWN], ssem, mc_r.at[which, vd, OWN], d, 1 - p)

    def spread_far(src, buf, which, vd, ssem):
        send(src, buf.at[vd, BACK], ssem, mc_r.at[which, vd, BACK], peer_b(PLUS), 1 - p)
        send(src, buf.at[vd, AHEAD], ssem, mc_r.at[which, vd, AHEAD], peer_b(MINUS), 1 - p)

    def spread_same(buf, which, v, ssem):
        send(buf.at[v, OWN], buf.at[v, BACK], ssem, mc_r.at[which, v, BACK], peer_a(PLUS), p)
        send(buf.at[v, OWN], buf.at[v, AHEAD], ssem, mc_r.at[which, v, AHEAD], peer_a(MINUS), p)

    def spread_relay(buf, which, v):
        for half, slot, delta in ((0, BACK, PLUS), (1, AHEAD, MINUS)):
            wait_recv(buf.at[v, slot], mc_r.at[which, v, slot])
            part = pl.ds(half * half_rows, half_rows)
            send(buf.at[v, slot, part], buf.at[v, FAR, part], rl_s.at[which, v], mc_r.at[which, v, FAR + half], peer_a(delta), p)

    def spread_finish(buf, which, v):
        for half in HALVES:
            wait_recv(buf.at[v, FAR, pl.ds(half * half_rows, half_rows)], mc_r.at[which, v, FAR + half])

    def spread_own(buf, which, v):
        wait_recv(buf.at[v, OWN], mc_r.at[which, v, OWN])

    def gates(n, wgt, wlin):
        a, b = mm(n, wgt), mm(n, wlin)
        s = jax.nn.sigmoid(a)
        act_a = a * s
        return (act_a * b).astype(BF), b * s * (1.0 + a * (1.0 - s)), act_a

    def block_gates(v):
        h = hb[v, OWN].astype(F32)
        n = (h * inv_rms(h)).astype(BF)

        def tile(i, carry):
            wide = fs // 2
            cols = pl.ds(pl.multiple_of(i * wide, wide), wide)
            u, t1, t2 = gates(n, wg[v, :, :, :, :, cols].reshape(dm, wide), wi[v, :, :, :, :, cols].reshape(dm, wide))
            ub[:, cols] = u
            f1[v, :, cols] = t1
            f2[v, :, cols] = t2
            return carry

        lax.fori_loop(0, 2 * NA, tile, 0, unroll=True)

    def block_out(v, dst):
        half_dm = dm // 2
        for i in HALVES:
            cols = pl.ds(i * half_dm, half_dm)
            out = mm(ub[...], wo[v, :, :, :, :, cols].reshape(fd, half_dm))
            dst[:, cols] = (hb[v, OWN, :, cols].astype(F32) + out).astype(BF)

    def block_backward(v, dst):
        e = eb[v, OWN]

        def tile(i, carry):
            cols = pl.ds(pl.multiple_of(i * fs, fs), fs)
            t = mm_nt(e, wo[v, i].reshape(fs, dm))
            da[:, cols] = (t * f1[v, :, cols]).astype(BF)
            db[:, cols] = (t * f2[v, :, cols]).astype(BF)
            return carry

        lax.fori_loop(0, NA, tile, 0, unroll=True)
        half_dm = dm // 2
        for i in HALVES:
            q = mm_nt(da[...], wg[v, pl.ds(2 * i, 2)].reshape(half_dm, fd))
            q += mm_nt(db[...], wi[v, pl.ds(2 * i, 2)].reshape(half_dm, fd))
            qs[:, pl.ds(i * half_dm, half_dm)] = q
        h = hb[v, OWN].astype(F32)
        r = inv_rms(h)
        hr = h * r
        q = qs[...]
        dst[...] = (e.astype(F32) + r * (q - hr * jnp.mean(q * hr, axis=-1, keepdims=True))).astype(BF)

    def piece(j, i):
        z = i + p * (j - i)
        y = j + p * (i - j)
        return z, y

    EARLY, LATE = range(FAR), range(FAR, NA)

    def grad_first(v, slots):
        for i in QUARTERS if OWN in slots else ():
            z, y = piece(ja, i)
            cols = pl.ds(pl.multiple_of((z * NA + y) * pf, pf), pf)
            gs[v, :, pl.ds(i * pf, pf)] = wg[v, :, :, :, :, cols].reshape(dm, pf)
            is_[v, :, pl.ds(i * pf, pf)] = wi[v, :, :, :, :, cols].reshape(dm, pf)
        for s in slots:
            h = hb[v, s].astype(F32)
            n = (h * inv_rms(h)).astype(BF)
            ng[v, s] = n
            u, t1, t2 = gates(n, gs[v], is_[v])
            us[v, s] = u
            f1s[v, s] = t1
            f2s[v, s] = t2

    def grad_hidden(v, slots):
        for i in QUARTERS if OWN in slots else ():
            z, y = piece(ja, i)
            os_[pl.ds(i * pf, pf), :] = wo[v, z, y].reshape(pf, dm)
        for s in slots:
            t = mm_nt(eb[v, s], os_[...])
            das[s] = (t * f1s[v, s]).astype(BF)
            dbs[s] = (t * f2s[v, s]).astype(BF)

    def rows_of(slots):
        return pl.ds(slots[0], len(slots)), len(slots) * rows

    def grad_out(v, slots):
        some, count = rows_of(slots)
        for i in HALVES:
            cols, to = pl.ds(i * 2 * pf, 2 * pf), pl.ds(2 * i, 2)
            g = mm_tn(us[v, some, :, cols].reshape(count, 2 * pf), eb[v, some].reshape(count, dm)).reshape(2, 4, fr, dm)
            gout[v, to] = g if OWN in slots else gout[v, to] + g

    def grad_in(v, slots):
        some, count = rows_of(slots)
        for which, dref in enumerate((das, dbs)):
            for i in QUARTERS:
                cols = pl.ds(i * (dm // NA), dm // NA)
                g = mm_tn(ng[v, some, :, cols].reshape(count, dm // NA), dref[some].reshape(count, fs)).reshape(4, 4, dr, fs)
                for y in QUARTERS:
                    at = (v, which, y + p * (i - y), i + p * (y - i))
                    gin[at] = g[y] if OWN in slots else gin[at] + g[y]

    IN, OUT = 0, 1

    def split(width):
        return pl.ds(0, width - pf), pl.ds(width - pf, pf)

    def view(which, st, v, colour, t, half):
        along_b = colour == st
        if which == IN:
            cols = split(fs)[colour]
            b, x = (t, slice(None) if st == 0 else xc) if along_b else (slice(None) if st == 0 else jb, t)
            return gin.at[v, half, :, b, x, :, cols]
        cols = split(dm)[colour]
        if st == 0:
            hs = pl.ds(2 * half, 2)
            return gout.at[v, t, hs, :, cols] if along_b else gout.at[v, hs, t, :, cols]
        hs = pl.ds(half * (fr // 2), fr // 2)
        return gout.at[v, t, xc, hs, cols] if along_b else gout.at[v, jb, t, hs, cols]

    RECV = (((rg[0], rg[1]), (rg[2], rg[3])), ((rg[4], rg[5]), (rg[6], rg[7])))
    MERGED, DIRECT = ((0, OPP, PLUS, 0), (1, OPP, MINUS, 1)), ((1, PLUS, PLUS, 2), (0, MINUS, MINUS, 3))
    RELAYED = ((0, PLUS, PLUS, 4), (1, MINUS, MINUS, 5))

    def axis_of(colour, st):
        return (jb, peer_b) if colour == st else (xc, functools.partial(peer, X))

    def scatter_send(v, which, st, copies):
        for colour in COLOURS:
            q, to = axis_of(colour, st)
            for half, c, delta, slot in copies:
                send(view(which, st, v, colour, rot(q, c), half), RECV[st][which][colour].at[v, slot],
                     rs_s.at[st, v, colour, which], rs_r.at[st, v, colour, which, slot], to(delta), p)

    def scatter_relay(v, which, st):
        for colour in COLOURS:
            q, _ = axis_of(colour, st)
            recv = RECV[st][which][colour]
            for half, c, _, slot in RELAYED:
                wait_recv(recv.at[v, slot - 4], rs_r.at[st, v, colour, which, slot - 4])
                ref = view(which, st, v, colour, rot(q, c), half)
                ref[...] = ref[...] + recv[v, slot - 4]
        scatter_send(v, which, st, RELAYED)

    def scatter_sum(v, which, st):
        for colour in COLOURS:
            q, _ = axis_of(colour, st)
            recv = RECV[st][which][colour]
            for half in HALVES:
                direct, merged = 3 - half, 4 + half
                for slot in (direct, merged):
                    wait_recv(recv.at[v, slot], rs_r.at[st, v, colour, which, slot])
                ref = view(which, st, v, colour, q, half)
                ref[...] = ref[...] + recv[v, direct] + recv[v, merged]

    def scatter_turn(v, which):
        scatter_sum(v, which, 0)
        scatter_send(v, which, 1, MERGED + DIRECT)

    def scatter_out(v):
        scatter_sum(v, OUT, 1)
        go[v] = gout[v, jb, xc]

    def scatter_last(v):
        scatter_sum(v, IN, 1)
        for which in HALVES:
            fin[v, :, which] = gin[v, which, :, jb, xc]
        for delta in (OPP, PLUS, MINUS):
            send(fin.at[v, rot(ja, delta)], r3.at[v, delta - 1], r3_s.at[v], r3_r.at[v, delta - 1], peer_a(delta), p)

    def scatter_finish(v):
        def put(j, vals):
            for i in QUARTERS:
                z, y = piece(j, i)
                cols = pl.ds(pl.multiple_of((z * NA + y) * pf, pf), pf)
                gg[v, :, cols] = vals(0)[:, i * pf:(i + 1) * pf]
                gi[v, :, cols] = vals(1)[:, i * pf:(i + 1) * pf]

        put(ja, lambda w: fin[v, ja, w])
        for delta in RING:
            wait_recv(r3.at[v, delta - 1], r3_r.at[v, delta - 1])
            put(rot(ja, -delta), lambda w, delta=delta: r3[v, delta - 1, w])

    def step(fn, *args):
        with jax.named_scope(fn.__name__):
            fn(*args)

    def on(core):
        return pl.when(p == core)

    def take_turn():
        pl.semaphore_wait(turn, 1)

    def give_turn():
        pl.semaphore_signal(turn, inc=1, device_id=(d, 1 - p), device_id_type=MESH)

    h_mid, h_late, e_first, e_last = ((xo.at[i], mc_s.at[1 + i]) for i in QUARTERS)

    def pass_on(part, item, buf, which, vd):
        step(part, item[0], buf, which, vd, item[1])

    AFTER = (MINUS, OPP), (0, PLUS)
    step(direct_send, 0)
    step(small_send, 1, 0)
    step(direct_wait, 0)
    step(small_send, 0, 1)
    step(small_relay, 1, 0)
    step(large_send, 0, (0,), (0,))
    step(small_rest, 1, 0)
    step(small_last, 1, 0)
    step(small_send, 1, 1)
    step(small_relay, 0, 1)
    step(small_relay, 1, 1)
    step(small_rest, 0, 1)
    step(large_send, 0, (PLUS, MINUS), (MINUS, PLUS))
    step(small_last, 0, 1)
    step(large_send, 0, (OPP,), (OPP,))
    step(small_rest, 1, 1)
    step(small_last, 1, 1)
    step(large_relay, 0)

    @on(0)
    def _():
        step(large_send, 1, UP, DOWN)

    step(large_finish, 0, UP_MATS)

    @on(0)
    def _():
        step(large_send, 1, *AFTER)

    @on(1)
    def _():
        step(take_turn)
        step(large_send, 1, UP, DOWN)
        step(spread_own, hb, 0, 0)

    step(block_gates, 0)

    @on(1)
    def _():
        step(large_send, 1, *AFTER)

    step(large_finish, 0, OUT_MAT)
    step(block_out, 0, h_mid[0])
    pass_on(spread_near, h_mid, hb, 0, p)
    step(large_relay, 1)

    @on(0)
    def _():
        step(give_turn)

    step(spread_own, hb, 0, 1)
    step(large_finish, 1, UP_MATS)
    step(block_gates, 1)
    step(large_finish, 1, OUT_MAT)

    @on(0)
    def _():
        step(block_out, 1, h_late[0])
        pass_on(spread_near, h_late, hb, 0, 1)
        pass_on(spread_far, h_late, hb, 0, 1)
        step(spread_own, eb, 1, 1)
        pass_on(spread_far, h_mid, hb, 0, p)
        step(block_backward, 1, e_first[0])
        pass_on(spread_near, e_first, eb, 1, 0)
        pass_on(spread_far, e_first, eb, 1, 0)
        step(spread_relay, hb, 0, 1)

    @on(1)
    def _():
        pass_on(spread_far, h_mid, hb, 0, p)
        step(spread_same, eb, 1, 1, mc_s.at[0])
        step(block_backward, 1, e_first[0])
        pass_on(spread_near, e_first, eb, 1, 1)
        pass_on(spread_far, e_first, eb, 1, 1)
        step(spread_relay, hb, 0, 1)

    step(grad_first, 1, EARLY)
    step(spread_relay, eb, 1, 1)

    step(grad_hidden, 1, EARLY)
    step(grad_out, 1, EARLY)

    @on(0)
    def _():
        step(grad_in, 1, EARLY)
        step(spread_same, hb, 0, 0, mc_s.at[0])

    @on(1)
    def _():
        step(spread_own, eb, 1, 0)
        step(block_backward, 0, e_last[0])
        pass_on(spread_near, e_last, eb, 1, 0)
        pass_on(spread_far, e_last, eb, 1, 0)
        step(grad_in, 1, EARLY)

    step(spread_finish, hb, 0, 1)
    step(grad_first, 1, LATE)

    step(spread_finish, eb, 1, 1)
    step(grad_hidden, 1, LATE)
    step(grad_out, 1, LATE)
    step(scatter_send, 1, OUT, 0, MERGED)
    step(grad_in, 1, LATE)
    step(scatter_send, 1, IN, 0, MERGED)

    @on(0)
    def _():
        step(spread_relay, eb, 1, 0)
        step(spread_own, eb, 1, 0)
        step(block_backward, 0, ga)
        send(ga, ga, ga_s, ga_r, d, 1)

    step(spread_relay, hb, 0, 0)
    step(scatter_send, 1, OUT, 0, DIRECT)
    step(grad_first, 0, EARLY)

    @on(1)
    def _():
        step(spread_relay, eb, 1, 0)

    step(grad_hidden, 0, EARLY)
    step(scatter_send, 1, IN, 0, DIRECT)
    step(grad_in, 0, EARLY)
    step(grad_out, 0, EARLY)
    step(spread_finish, hb, 0, 0)
    step(grad_first, 0, LATE)
    step(scatter_relay, 1, OUT, 0)
    step(spread_finish, eb, 1, 0)
    step(grad_hidden, 0, LATE)
    step(grad_in, 0, LATE)
    step(scatter_send, 0, IN, 0, MERGED)
    step(grad_out, 0, LATE)
    step(scatter_relay, 1, IN, 0)
    step(scatter_send, 0, OUT, 0, MERGED)
    step(scatter_send, 0, IN, 0, DIRECT)
    step(scatter_turn, 1, OUT)
    step(scatter_relay, 0, IN, 0)
    step(scatter_send, 0, OUT, 0, DIRECT)
    step(scatter_turn, 1, IN)
    step(scatter_relay, 0, OUT, 0)
    step(scatter_relay, 1, OUT, 1)

    @on(1)
    def _():
        wait_recv(ga, ga_r)

    gact[...] = ga[...]
    step(scatter_turn, 0, IN)
    step(scatter_relay, 1, IN, 1)
    step(scatter_turn, 0, OUT)
    step(scatter_out, 1)
    step(scatter_last, 1)
    step(scatter_relay, 0, IN, 1)
    step(scatter_relay, 0, OUT, 1)
    step(scatter_last, 0)
    step(scatter_finish, 1)
    step(scatter_out, 0)
    step(scatter_finish, 0)

    for v in BLOCKS:
        for k in MATS:
            three = pl.ds(0, len(RING))
            wait_send(part_at(v, k, three, 0, 0), ag_s.at[v, k, 0])
            wait_send(part_at(v, k, whole, three, 0), ag_s.at[v, k, 1])
            wait_send(part_at(v, k, whole, whole, three), ag_s.at[v, k, LARGE])
        for colour in COLOURS:
            for which in HALVES:
                for st in HALVES:
                    wait_send(RECV[st][which][colour].at[v], rs_s.at[st, v, colour, which])
        wait_send(r3.at[v], r3_s.at[v])
        wait_send(hb.at[v, 0], rl_s.at[0, v])
        wait_send(hb.at[v, 0], rl_s.at[1, v])
    wait_send(hb.at[0, pl.ds(0, 2)], mc_s.at[0])
    wait_send(hb.at[0, pl.ds(0, 3)], mc_s.at[1])
    wait_send(hb.at[0, pl.ds(0, 3)], mc_s.at[3])

    @pl.when(p == 0)
    def _():
        wait_send(hb.at[0, pl.ds(0, 3)], mc_s.at[2])
        wait_send(ga, ga_s)

    @pl.when(p == 1)
    def _():
        wait_send(hb.at[0, pl.ds(0, 3)], mc_s.at[4])


def hand_on(*refs):
    copies = [pltpu.make_async_copy(refs[i], refs[NA + i], refs[-1].at[i]) for i in QUARTERS]
    for copy in copies:
        copy.start()
    for copy in copies:
        copy.wait()


def solution(mesh):
    act_spec = P(None, "data", None, None)
    w_spec = P(None, "stage", "data", None)

    def body(act_in, cot_out, w_gate, w_in, w_out):
        shape = act_in.shape
        dm, fd = shape[3], w_gate.shape[3]
        rows = shape[0] * shape[1] * shape[2]
        dr, fr, fs = dm // NL, fd // NL, fd // NA
        pf = fs // NA
        vmem = pltpu.VMEM
        dma = pltpu.SemaphoreType.DMA
        n2, n3, na = NB, len(RING), NA
        ring = (na, na)
        scratch = [
            vmem((n2, na, *ring, dr, fd), BF), vmem((n2, na, *ring, dr, fd), BF), vmem((n2, na, *ring, fr, dm), BF),
            vmem((n2, na, rows, dm), BF), vmem((n2, na, rows, dm), BF), vmem((na, rows, dm), BF), vmem((rows, dm), BF),
            vmem((n2, na, rows, dm), BF),
            vmem((n2, rows, fd), F32), vmem((n2, rows, fd), F32),
            vmem((n2, na, rows, fs), F32), vmem((n2, na, rows, fs), F32),
            vmem((n2, na, rows, fs), BF),
            vmem((rows, fd), BF), vmem((rows, fd), BF), vmem((rows, fd), BF),
            vmem((na, rows, fs), BF), vmem((na, rows, fs), BF),
            vmem((rows, dm), F32),
            vmem((n2, dm, fs), BF), vmem((n2, dm, fs), BF), vmem((fs, dm), BF),
            vmem((n2, n2, na, *ring, dr, fs), F32), vmem((n2, *ring, fr, dm), F32),
            vmem((n2, na, n2, dr, fs), F32), vmem((n2, n3, n2, dr, fs), F32),
            dma((n2, na)), dma((n2, n3, n3)), dma((n2, n3, n2, 6)), dma((n2, n3, n3 * na)), dma((5,)), dma((n2, n2, 5)), dma((n2, n2)), dma, dma,
            dma((n2, n2, n2, n2)), dma((n2, n2, n2, n2, 6)), dma((n2,)), dma((n2, n3)), pltpu.SemaphoreType.REGULAR,
            *(vmem((n2, 6, *lead, width), F32)
              for lead_in, lead_out in (((*ring, dr), (n2, fr)), ((na, dr), (fr // n2,)))
              for lead, width in ((lead_in, fs - pf), (lead_in, pf), (lead_out, dm - pf), (lead_out, pf))),
        ]
        hbm = pl.BlockSpec(memory_space=pl.ANY)
        whole = pl.BlockSpec(memory_space=pltpu.VMEM)
        out = pl.pallas_call(
            kernel,
            out_shape=(
                vmem((rows, dm), BF), vmem((n2, dr, fd), F32), vmem((n2, dr, fd), F32), vmem((n2, fr, dm), F32),
            ),
            in_specs=[hbm] * 5,
            out_specs=(whole,) * NA,
            scratch_shapes=scratch,
            compiler_params=pltpu.CompilerParams(collective_id=0, has_side_effects=True, vmem_limit_bytes=66300000),
            name="train_step",
        )(act_in.reshape(rows, dm), cot_out.reshape(rows, dm), w_gate[:, 0], w_in[:, 0], w_out[:, 0])
        grad_act, grad_gate, grad_lin, grad_proj = pl.pallas_call(
            hand_on, out_shape=tuple(jax.ShapeDtypeStruct(a.shape, a.dtype) for a in out), in_specs=[whole] * NA, out_specs=(hbm,) * NA,
            scratch_shapes=[dma((NA,))], compiler_params=pltpu.CompilerParams(vmem_limit_bytes=2 ** 20), name="hand_on",
        )(*(pltpu.with_memory_space_constraint(a, vmem) for a in out))
        return grad_act.reshape(shape), grad_gate[:, None], grad_lin[:, None], grad_proj[:, None]

    return jax.shard_map(body, mesh=mesh, in_specs=(act_spec, act_spec, w_spec, w_spec, w_spec),
                         out_specs=(act_spec, w_spec, w_spec, w_spec), check_vma=False)
```

```python
import functools

import jax
import jax.numpy as jnp
from jax import lax
from jax.experimental import pallas as pl
from jax.experimental.pallas import tpu as pltpu
from jax.sharding import PartitionSpec as P

NORM_EPS = 1e-6
BF = jnp.bfloat16
F32 = jnp.float32
MESH = pl.DeviceIdType.MESH
X, Y, Z = 0, 1, 2
BLOCKS = COLOURS = HALVES = (0, 1)
NB, NA, NL = len(BLOCKS), 4, 64
RING = (1, 3, 2)
OPP = RING[-1]
PLUS, MINUS = RING[:-1]
QUARTERS = range(NA)
OWN = 0
AXES = ((Z, X, Y), (Y, Z, X), (X, Y, Z))
UP_MATS, OUT_MAT = (0, 1), (2,)
MATS = UP_MATS + OUT_MAT


def mm(left, right):
    return jnp.dot(left, right, preferred_element_type=F32)


def mm_nt(left, right):
    return lax.dot_general(left, right, (((1,), (1,)), ((), ())), preferred_element_type=F32)


def mm_tn(left, right):
    return lax.dot_general(left, right, (((0,), (0,)), ((), ())), preferred_element_type=F32)


def inv_rms(h):
    return lax.rsqrt(jnp.mean(h * h, axis=-1, keepdims=True) + NORM_EPS)


def kernel(act, cot, wg_in, wi_in, wo_in, gact, gg, gi, go,
           wg, wi, wo, hb, eb, xo, ga, ng, f1, f2, f1s, f2s, us, ub, da, db, das, dbs, qs, gs, is_, os_,
           gin0, gin1, gout0, gout1, fin, r3,
           lsem, ag_s, ag_r, lg_r, mc_s, mc_r, rl_s, ga_s, ga_r, rs_s, rs_r, r3_s, r3_r, turn, *rg):
    dm, fd = wo.shape[-1], wg.shape[-1]
    dr, fr = dm // NL, fd // NL
    fs = fd // NA
    pf = fs // NA
    rows = act.shape[0]
    wts = (wg, wi, wo)
    gin, gout = (gin0, gin1), (gout0, gout1)

    p = lax.axis_index("stage")
    d = lax.axis_index("data")
    zc, yc, xc = lax.div(d, 16), lax.rem(lax.div(d, 4), 4), lax.rem(d, 4)
    coord = (xc, yc, zc)
    stride = (1, 4, 16)
    ja = yc + p * (zc - yc)
    jb = zc + p * (yc - zc)
    sa, sb = 4 + 12 * p, 16 - 12 * p

    def rot(c, delta):
        return lax.rem(c + (delta % 4), 4)

    def peer(ax, delta):
        return d + (rot(coord[ax], delta) - coord[ax]) * stride[ax]

    def peer_a(delta):
        return d + (rot(ja, delta) - ja) * sa

    def peer_b(delta):
        return d + (rot(jb, delta) - jb) * sb

    def remote(src, dst, ssem, rsem, dev, core):
        return pltpu.make_async_remote_copy(src_ref=src, dst_ref=dst, send_sem=ssem, recv_sem=rsem,
                                            device_id=(dev, core), device_id_type=MESH)

    def send(src, dst, ssem, rsem, dev, core):
        remote(src, dst, ssem, rsem, dev, core).start()

    def wait_recv(ref, sem):
        remote(ref, ref, sem, sem, d, p).wait_recv()

    def wait_send(ref, sem):
        remote(ref, ref, sem, sem, d, p).wait_send()

    for v in BLOCKS:
        for k, shard in enumerate((wg_in, wi_in, wo_in)):
            pltpu.make_async_copy(shard.at[v], wts[k].at[v, zc, yc, xc], lsem.at[v, k]).start()

    @pl.when(p == 0)
    def _():
        pltpu.make_async_copy(act, hb.at[0, OWN], lsem.at[0, 3]).start()

    @pl.when(p == 1)
    def _():
        pltpu.make_async_copy(cot, eb.at[1, OWN], lsem.at[0, 3]).start()

    barrier = pltpu.get_barrier_semaphore()
    senders = [(peer(ax, delta), p) for ax in (X, Y, Z) for delta in RING]
    senders += [(d, 1 - p), (peer_a(1), 1 - p), (peer_a(-1), 1 - p)]
    for dev, core in senders:
        pl.semaphore_signal(barrier, inc=1, device_id=(dev, core), device_id_type=MESH)
    for v in BLOCKS:
        for k, shard in enumerate((wg_in, wi_in, wo_in)):
            pltpu.make_async_copy(shard.at[v], wts[k].at[v, zc, yc, xc], lsem.at[v, k]).wait()

    @pl.when(p == 0)
    def _():
        pltpu.make_async_copy(act, hb.at[0, OWN], lsem.at[0, 3]).wait()

    @pl.when(p == 1)
    def _():
        pltpu.make_async_copy(cot, eb.at[1, OWN], lsem.at[0, 3]).wait()

    pl.semaphore_wait(barrier, len(senders))

    FIRST, REST = ((0, PLUS, 0), (1, MINUS, 2)), ((1, PLUS, 1), (0, MINUS, 3))
    LARGE = 2
    whole = slice(None)

    def part_at(v, k, small, middle, large, half=None):
        place = dict(zip(AXES[k], (small, middle, large)))
        width = wts[k].shape[-1] // 2
        cols = whole if half is None else pl.ds(half * width, width)
        return wts[k].at[v, place[Z], place[Y], place[X], :, cols]

    def own(k):
        return [coord[ax] for ax in AXES[k]]

    def chunk(v, k, ph, q, half):
        small, middle, large = own(k)
        return part_at(v, k, q, middle, large, half) if ph == 0 else part_at(v, k, pl.ds(2 * half, 2), q, large)

    def small_copy(v, k, ph, q, half, delta, slot):
        ref = chunk(v, k, ph, q, half)
        send(ref, ref, ag_s.at[v, k, ph], ag_r.at[v, k, ph, slot], peer(AXES[k][ph], delta), p)

    def small_wait(v, k, ph, back, half, slot):
        wait_recv(chunk(v, k, ph, rot(coord[AXES[k][ph]], back), half), ag_r.at[v, k, ph, slot])

    def small_send(v, ph):
        for half, delta, slot in FIRST + REST:
            for k in MATS:
                small_copy(v, k, ph, coord[AXES[k][ph]], half, delta, slot)

    def small_relay(v, ph):
        for half, delta, slot in FIRST:
            for k in MATS:
                small_wait(v, k, ph, -delta, half, slot)
                small_copy(v, k, ph, rot(coord[AXES[k][ph]], -delta), half, delta, 4 + half)

    def small_rest(v, ph):
        for half, delta, slot in REST:
            for k in MATS:
                small_wait(v, k, ph, -delta, half, slot)

    def small_last(v, ph):
        for half in HALVES:
            for k in MATS:
                small_wait(v, k, ph, OPP, half, 4 + half)

    def direct_send(v):
        for delta in (OPP, PLUS, MINUS):
            for k in MATS:
                ref = part_at(v, k, *own(k))
                send(ref, ref, ag_s.at[v, k, 0], ag_r.at[v, k, 0, delta], peer(AXES[k][0], delta), p)

    def direct_wait(v):
        for delta in RING:
            for k in MATS:
                small, middle, large = own(k)
                wait_recv(part_at(v, k, rot(small, -delta), middle, large), ag_r.at[v, k, 0, delta])

    UP, DOWN = (0, PLUS), (MINUS, OPP)
    RELAYS = ((UP[0], PLUS), (DOWN[0], MINUS), (UP[1], PLUS), (DOWN[1], MINUS))

    def row(v, k, q, r):
        return part_at(v, k, whole, rot(coord[AXES[k][1]], r), q)

    def large_slot(r, delta):
        return r if delta == PLUS else NA + r

    def large_send(v, up, down):
        for pair in zip(up, down):
            for r, delta in zip(pair, (PLUS, MINUS)):
                for k in MATS:
                    ax = AXES[k][LARGE]
                    ref = row(v, k, coord[ax], r)
                    send(ref, ref, ag_s.at[v, k, LARGE], lg_r.at[v, k, large_slot(r, delta)], peer(ax, delta), p)

    def large_relay(v):
        for r, delta in RELAYS:
            for k in MATS:
                ax = AXES[k][LARGE]
                ref = row(v, k, rot(coord[ax], -delta), r)
                wait_recv(ref, lg_r.at[v, k, large_slot(r, delta)])
                send(ref, ref, ag_s.at[v, k, LARGE], lg_r.at[v, k, 2 * NA + r], peer(ax, delta), p)

    def large_finish(v, mats):
        for pieces, delta in ((DOWN, PLUS), (UP, MINUS)):
            for r in pieces:
                for k in mats:
                    wait_recv(row(v, k, rot(coord[AXES[k][LARGE]], -delta), r), lg_r.at[v, k, large_slot(r, delta)])
        for r in QUARTERS:
            for k in mats:
                wait_recv(row(v, k, rot(coord[AXES[k][LARGE]], OPP), r), lg_r.at[v, k, 2 * NA + r])

    half_rows = rows // 2
    BACK, AHEAD, FAR = 1, 2, 3

    def spread_near(src, buf, which, vd, ssem):
        send(src, buf.at[vd, OWN], ssem, mc_r.at[which, vd, OWN], d, 1 - p)

    def spread_far(src, buf, which, vd, ssem):
        send(src, buf.at[vd, BACK], ssem, mc_r.at[which, vd, BACK], peer_b(PLUS), 1 - p)
        send(src, buf.at[vd, AHEAD], ssem, mc_r.at[which, vd, AHEAD], peer_b(MINUS), 1 - p)

    def spread_same(buf, which, v, ssem):
        send(buf.at[v, OWN], buf.at[v, BACK], ssem, mc_r.at[which, v, BACK], peer_a(PLUS), p)
        send(buf.at[v, OWN], buf.at[v, AHEAD], ssem, mc_r.at[which, v, AHEAD], peer_a(MINUS), p)

    def spread_relay(buf, which, v):
        for half, slot, delta in ((0, BACK, PLUS), (1, AHEAD, MINUS)):
            wait_recv(buf.at[v, slot], mc_r.at[which, v, slot])
            part = pl.ds(half * half_rows, half_rows)
            send(buf.at[v, slot, part], buf.at[v, FAR, part], rl_s.at[which, v], mc_r.at[which, v, FAR + half], peer_a(delta), p)

    def spread_finish(buf, which, v):
        for half in HALVES:
            wait_recv(buf.at[v, FAR, pl.ds(half * half_rows, half_rows)], mc_r.at[which, v, FAR + half])

    def spread_own(buf, which, v):
        wait_recv(buf.at[v, OWN], mc_r.at[which, v, OWN])

    def gates(n, wgt, wlin):
        a, b = mm(n, wgt), mm(n, wlin)
        s = jax.nn.sigmoid(a)
        act_a = a * s
        return (act_a * b).astype(BF), b * s * (1.0 + a * (1.0 - s)), act_a

    def block_gates(v):
        h = hb[v, OWN].astype(F32)
        n = (h * inv_rms(h)).astype(BF)

        def tile(i, carry):
            wide = fs // 2
            cols = pl.ds(pl.multiple_of(i * wide, wide), wide)
            u, t1, t2 = gates(n, wg[v, :, :, :, :, cols].reshape(dm, wide), wi[v, :, :, :, :, cols].reshape(dm, wide))
            ub[:, cols] = u
            f1[v, :, cols] = t1
            f2[v, :, cols] = t2
            return carry

        lax.fori_loop(0, 2 * NA, tile, 0, unroll=True)

    def block_out(v, dst):
        half_dm = dm // 2
        for i in HALVES:
            cols = pl.ds(i * half_dm, half_dm)
            out = mm(ub[...], wo[v, :, :, :, :, cols].reshape(fd, half_dm))
            dst[:, cols] = (hb[v, OWN, :, cols].astype(F32) + out).astype(BF)

    def block_backward(v, dst):
        e = eb[v, OWN]

        def tile(i, carry):
            cols = pl.ds(pl.multiple_of(i * fs, fs), fs)
            t = mm_nt(e, wo[v, i].reshape(fs, dm))
            da[:, cols] = (t * f1[v, :, cols]).astype(BF)
            db[:, cols] = (t * f2[v, :, cols]).astype(BF)
            return carry

        lax.fori_loop(0, NA, tile, 0, unroll=True)
        half_dm = dm // 2
        for i in HALVES:
            q = mm_nt(da[...], wg[v, pl.ds(2 * i, 2)].reshape(half_dm, fd))
            q += mm_nt(db[...], wi[v, pl.ds(2 * i, 2)].reshape(half_dm, fd))
            qs[:, pl.ds(i * half_dm, half_dm)] = q
        h = hb[v, OWN].astype(F32)
        r = inv_rms(h)
        hr = h * r
        q = qs[...]
        dst[...] = (e.astype(F32) + r * (q - hr * jnp.mean(q * hr, axis=-1, keepdims=True))).astype(BF)

    def piece(j, i):
        z = i + p * (j - i)
        y = j + p * (i - j)
        return z, y

    EARLY, LATE = range(FAR), range(FAR, NA)

    def grad_first(v, slots):
        for i in QUARTERS if OWN in slots else ():
            z, y = piece(ja, i)
            cols = pl.ds(pl.multiple_of((z * NA + y) * pf, pf), pf)
            gs[v, :, pl.ds(i * pf, pf)] = wg[v, :, :, :, :, cols].reshape(dm, pf)
            is_[v, :, pl.ds(i * pf, pf)] = wi[v, :, :, :, :, cols].reshape(dm, pf)
        for s in slots:
            h = hb[v, s].astype(F32)
            n = (h * inv_rms(h)).astype(BF)
            ng[v, s] = n
            u, t1, t2 = gates(n, gs[v], is_[v])
            us[v, s] = u
            f1s[v, s] = t1
            f2s[v, s] = t2

    def grad_hidden(v, slots):
        for i in QUARTERS if OWN in slots else ():
            z, y = piece(ja, i)
            os_[pl.ds(i * pf, pf), :] = wo[v, z, y].reshape(pf, dm)
        for s in slots:
            t = mm_nt(eb[v, s], os_[...])
            das[s] = (t * f1s[v, s]).astype(BF)
            dbs[s] = (t * f2s[v, s]).astype(BF)

    def split(width):
        return pl.ds(0, width - pf), pl.ds(width - pf, pf)

    def keep(refs, v, place, tile, cols, first):
        b, rest = place[0], place[1:]
        lead = () if v is None else (v,)
        for colour in COLOURS:
            part = tile[..., cols[colour].start:cols[colour].start + cols[colour].size]
            at = lead + ((b, slice(None)) if colour == 0 else (slice(None), b)) + rest
            refs[colour][at] = part if first else refs[colour][at] + part

    def rows_of(slots):
        return pl.ds(slots[0], len(slots)), len(slots) * rows

    def grad_out(v, slots):
        some, count = rows_of(slots)
        for i in HALVES:
            cols = pl.ds(i * 2 * pf, 2 * pf)
            g = mm_tn(us[v, some, :, cols].reshape(count, 2 * pf), eb[v, some].reshape(count, dm)).reshape(2, NA, fr, dm)
            for b in HALVES:
                keep(gout, v, (2 * i + b,), g[b], split(dm), OWN in slots)

    def grad_in(v, slots):
        some, count = rows_of(slots)
        for which, dref in enumerate((das, dbs)):
            for i in QUARTERS:
                cols = pl.ds(i * (dm // NA), dm // NA)
                g = mm_tn(ng[v, some, :, cols].reshape(count, dm // NA), dref[some].reshape(count, fs)).reshape(NA, NA, dr, fs)
                for y in QUARTERS:
                    keep([ref.at[v, which] for ref in gin], None, (i + p * (y - i), y + p * (i - y)), g[y], split(fs), OWN in slots)

    IN, OUT = 0, 1

    def view(which, st, v, colour, t, half):
        own = jb if colour == 0 else xc
        if which == IN:
            ref = gin[colour].at[v, half]
            return ref.at[t] if st == 0 else ref.at[own, t]
        ref = gout[colour].at[v]
        return ref.at[t, pl.ds(2 * half, 2)] if st == 0 else ref.at[own, t, pl.ds(half * (fr // 2), fr // 2)]

    RECV = (((rg[0], rg[1]), (rg[2], rg[3])), ((rg[4], rg[5]), (rg[6], rg[7])))
    MERGED, DIRECT = ((0, OPP, PLUS, 0), (1, OPP, MINUS, 1)), ((1, PLUS, PLUS, 2), (0, MINUS, MINUS, 3))
    RELAYED = ((0, PLUS, PLUS, 4), (1, MINUS, MINUS, 5))

    def axis_of(colour, st):
        return (jb, peer_b) if colour == st else (xc, functools.partial(peer, X))

    def scatter_send(v, which, st, copies):
        for colour in COLOURS:
            q, to = axis_of(colour, st)
            for half, c, delta, slot in copies:
                send(view(which, st, v, colour, rot(q, c), half), RECV[st][which][colour].at[v, slot],
                     rs_s.at[st, v, colour, which], rs_r.at[st, v, colour, which, slot], to(delta), p)

    def scatter_relay(v, which, st):
        for colour in COLOURS:
            q, _ = axis_of(colour, st)
            recv = RECV[st][which][colour]
            for half, c, _, slot in RELAYED:
                wait_recv(recv.at[v, slot - 4], rs_r.at[st, v, colour, which, slot - 4])
                ref = view(which, st, v, colour, rot(q, c), half)
                ref[...] = ref[...] + recv[v, slot - 4]
        scatter_send(v, which, st, RELAYED)

    def scatter_sum(v, which, st):
        for colour in COLOURS:
            q, _ = axis_of(colour, st)
            recv = RECV[st][which][colour]
            for half in HALVES:
                direct, merged = 3 - half, 4 + half
                for slot in (direct, merged):
                    wait_recv(recv.at[v, slot], rs_r.at[st, v, colour, which, slot])
                ref = view(which, st, v, colour, q, half)
                ref[...] = ref[...] + recv[v, direct] + recv[v, merged]

    def scatter_turn(v, which):
        scatter_sum(v, which, 0)
        scatter_send(v, which, 1, MERGED + DIRECT)

    def scatter_out(v):
        scatter_sum(v, OUT, 1)
        for colour in COLOURS:
            go[v, :, split(dm)[colour]] = gout[colour][(v, jb, xc) if colour == 0 else (v, xc, jb)]

    def scatter_last(v):
        scatter_sum(v, IN, 1)
        for which in HALVES:
            for colour in COLOURS:
                fin[v, :, which, :, split(fs)[colour]] = gin[colour][(v, which, jb, xc) if colour == 0 else (v, which, xc, jb)]
        for delta in (OPP, PLUS, MINUS):
            send(fin.at[v, rot(ja, delta)], r3.at[v, delta - 1], r3_s.at[v], r3_r.at[v, delta - 1], peer_a(delta), p)

    def scatter_finish(v):
        def put(j, vals):
            for i in QUARTERS:
                z, y = piece(j, i)
                cols = pl.ds(pl.multiple_of((z * NA + y) * pf, pf), pf)
                gg[v, :, cols] = vals(0)[:, i * pf:(i + 1) * pf]
                gi[v, :, cols] = vals(1)[:, i * pf:(i + 1) * pf]

        put(ja, lambda w: fin[v, ja, w])
        for delta in RING:
            wait_recv(r3.at[v, delta - 1], r3_r.at[v, delta - 1])
            put(rot(ja, -delta), lambda w, delta=delta: r3[v, delta - 1, w])

    def step(fn, *args):
        with jax.named_scope(fn.__name__):
            fn(*args)

    def on(core):
        return pl.when(p == core)

    def take_turn():
        pl.semaphore_wait(turn, 1)

    def give_turn():
        pl.semaphore_signal(turn, inc=1, device_id=(d, 1 - p), device_id_type=MESH)

    h_mid, h_late, e_first, e_last = ((xo.at[i], mc_s.at[1 + i]) for i in QUARTERS)

    def pass_on(part, item, buf, which, vd):
        step(part, item[0], buf, which, vd, item[1])

    AFTER = (MINUS, OPP), (0, PLUS)
    step(direct_send, 0)
    step(small_send, 1, 0)

    @on(0)
    def _():
        step(spread_same, hb, 0, 0, mc_s.at[0])

    step(direct_wait, 0)
    step(small_send, 0, 1)
    step(small_relay, 1, 0)
    step(large_send, 0, (0,), (0,))
    step(small_rest, 1, 0)
    step(small_last, 1, 0)
    step(small_send, 1, 1)
    step(small_relay, 0, 1)
    step(small_relay, 1, 1)
    step(small_rest, 0, 1)
    step(large_send, 0, (PLUS, MINUS), (MINUS, PLUS))
    step(small_last, 0, 1)
    step(large_send, 0, (OPP,), (OPP,))
    step(small_rest, 1, 1)
    step(small_last, 1, 1)
    step(large_relay, 0)

    @on(0)
    def _():
        step(large_send, 1, UP, DOWN)

    step(large_finish, 0, UP_MATS)

    @on(0)
    def _():
        step(large_send, 1, *AFTER)

    @on(1)
    def _():
        step(take_turn)
        step(large_send, 1, UP, DOWN)
        step(spread_own, hb, 0, 0)

    step(block_gates, 0)

    @on(1)
    def _():
        step(large_send, 1, *AFTER)

    step(large_finish, 0, OUT_MAT)
    step(block_out, 0, h_mid[0])
    pass_on(spread_near, h_mid, hb, 0, p)
    step(large_relay, 1)

    @on(0)
    def _():
        step(give_turn)
        step(spread_relay, hb, 0, 0)

    step(spread_own, hb, 0, 1)
    step(large_finish, 1, UP_MATS)
    step(block_gates, 1)
    step(large_finish, 1, OUT_MAT)

    @on(0)
    def _():
        step(block_out, 1, h_late[0])
        pass_on(spread_near, h_late, hb, 0, 1)
        pass_on(spread_far, h_late, hb, 0, 1)
        step(spread_finish, hb, 0, 0)
        step(grad_first, 0, EARLY)
        step(grad_first, 0, LATE)
        step(spread_own, eb, 1, 1)
        pass_on(spread_far, h_mid, hb, 0, p)
        step(block_backward, 1, e_first[0])
        pass_on(spread_near, e_first, eb, 1, 0)
        pass_on(spread_far, e_first, eb, 1, 0)
        step(spread_relay, hb, 0, 1)

    @on(1)
    def _():
        pass_on(spread_far, h_mid, hb, 0, p)
        step(spread_same, eb, 1, 1, mc_s.at[0])
        step(block_backward, 1, e_first[0])
        pass_on(spread_near, e_first, eb, 1, 1)
        pass_on(spread_far, e_first, eb, 1, 1)
        step(spread_relay, hb, 0, 1)

    step(grad_first, 1, EARLY)
    step(spread_relay, eb, 1, 1)

    step(grad_hidden, 1, EARLY)
    step(grad_out, 1, EARLY)

    @on(0)
    def _():
        step(grad_in, 1, EARLY)

    @on(1)
    def _():
        step(spread_own, eb, 1, 0)
        step(block_backward, 0, e_last[0])
        pass_on(spread_near, e_last, eb, 1, 0)
        pass_on(spread_far, e_last, eb, 1, 0)
        step(grad_in, 1, EARLY)

    step(spread_finish, hb, 0, 1)
    step(grad_first, 1, LATE)

    step(spread_finish, eb, 1, 1)
    step(grad_hidden, 1, LATE)
    step(grad_out, 1, LATE)
    step(scatter_send, 1, OUT, 0, MERGED)
    step(grad_in, 1, LATE)
    step(scatter_send, 1, IN, 0, MERGED)

    @on(0)
    def _():
        step(spread_relay, eb, 1, 0)
        step(spread_own, eb, 1, 0)
        step(block_backward, 0, ga)
        send(ga, ga, ga_s, ga_r, d, 1)

    @on(1)
    def _():
        step(spread_relay, hb, 0, 0)
        step(grad_first, 0, EARLY)

    step(scatter_send, 1, OUT, 0, DIRECT)

    @on(1)
    def _():
        step(spread_relay, eb, 1, 0)
        step(spread_finish, hb, 0, 0)
        step(grad_first, 0, LATE)

    step(grad_hidden, 0, EARLY)
    step(scatter_send, 1, IN, 0, DIRECT)
    step(grad_in, 0, EARLY)
    step(grad_out, 0, EARLY)
    step(scatter_relay, 1, OUT, 0)
    step(spread_finish, eb, 1, 0)
    step(grad_hidden, 0, LATE)
    step(grad_in, 0, LATE)
    step(scatter_send, 0, IN, 0, MERGED)
    step(grad_out, 0, LATE)
    step(scatter_relay, 1, IN, 0)
    step(scatter_send, 0, OUT, 0, MERGED)
    step(scatter_send, 0, IN, 0, DIRECT)
    step(scatter_turn, 1, OUT)
    step(scatter_relay, 0, IN, 0)
    step(scatter_send, 0, OUT, 0, DIRECT)
    step(scatter_turn, 1, IN)
    step(scatter_relay, 0, OUT, 0)
    step(scatter_relay, 1, OUT, 1)

    @on(1)
    def _():
        wait_recv(ga, ga_r)

    gact[...] = ga[...]
    step(scatter_turn, 0, IN)
    step(scatter_relay, 1, IN, 1)
    step(scatter_turn, 0, OUT)
    step(scatter_out, 1)
    step(scatter_last, 1)
    step(scatter_relay, 0, IN, 1)
    step(scatter_relay, 0, OUT, 1)
    step(scatter_last, 0)
    step(scatter_finish, 1)
    step(scatter_out, 0)
    step(scatter_finish, 0)

    for v in BLOCKS:
        for k in MATS:
            three = pl.ds(0, len(RING))
            wait_send(part_at(v, k, three, 0, 0), ag_s.at[v, k, 0])
            wait_send(part_at(v, k, whole, three, 0), ag_s.at[v, k, 1])
            wait_send(part_at(v, k, whole, whole, three), ag_s.at[v, k, LARGE])
        for colour in COLOURS:
            for which in HALVES:
                for st in HALVES:
                    wait_send(RECV[st][which][colour].at[v], rs_s.at[st, v, colour, which])
        wait_send(r3.at[v], r3_s.at[v])
        wait_send(hb.at[v, 0], rl_s.at[0, v])
        wait_send(hb.at[v, 0], rl_s.at[1, v])
    wait_send(hb.at[0, pl.ds(0, 2)], mc_s.at[0])
    wait_send(hb.at[0, pl.ds(0, 3)], mc_s.at[1])
    wait_send(hb.at[0, pl.ds(0, 3)], mc_s.at[3])

    @pl.when(p == 0)
    def _():
        wait_send(hb.at[0, pl.ds(0, 3)], mc_s.at[2])
        wait_send(ga, ga_s)

    @pl.when(p == 1)
    def _():
        wait_send(hb.at[0, pl.ds(0, 3)], mc_s.at[4])


def hand_on(*refs):
    copies = [pltpu.make_async_copy(refs[i], refs[NA + i], refs[-1].at[i]) for i in QUARTERS]
    for copy in copies:
        copy.start()
    for copy in copies:
        copy.wait()


def solution(mesh):
    act_spec = P(None, "data", None, None)
    w_spec = P(None, "stage", "data", None)

    def body(act_in, cot_out, w_gate, w_in, w_out):
        shape = act_in.shape
        dm, fd = shape[3], w_gate.shape[3]
        rows = shape[0] * shape[1] * shape[2]
        dr, fr, fs = dm // NL, fd // NL, fd // NA
        pf = fs // NA
        vmem = pltpu.VMEM
        dma = pltpu.SemaphoreType.DMA
        n2, n3, na = NB, len(RING), NA
        ring = (na, na)
        scratch = [
            vmem((n2, na, *ring, dr, fd), BF), vmem((n2, na, *ring, dr, fd), BF), vmem((n2, na, *ring, fr, dm), BF),
            vmem((n2, na, rows, dm), BF), vmem((n2, na, rows, dm), BF), vmem((na, rows, dm), BF), vmem((rows, dm), BF),
            vmem((n2, na, rows, dm), BF),
            vmem((n2, rows, fd), F32), vmem((n2, rows, fd), F32),
            vmem((n2, na, rows, fs), F32), vmem((n2, na, rows, fs), F32),
            vmem((n2, na, rows, fs), BF),
            vmem((rows, fd), BF), vmem((rows, fd), BF), vmem((rows, fd), BF),
            vmem((na, rows, fs), BF), vmem((na, rows, fs), BF),
            vmem((rows, dm), F32),
            vmem((n2, dm, fs), BF), vmem((n2, dm, fs), BF), vmem((fs, dm), BF),
            *(vmem((n2, n2, *ring, na, dr, width), F32) for width in (fs - pf, pf)),
            *(vmem((n2, *ring, fr, width), F32) for width in (dm - pf, pf)),
            vmem((n2, na, n2, dr, fs), F32), vmem((n2, n3, n2, dr, fs), F32),
            dma((n2, na)), dma((n2, n3, n3)), dma((n2, n3, n2, 6)), dma((n2, n3, n3 * na)), dma((5,)), dma((n2, n2, 5)), dma((n2, n2)), dma, dma,
            dma((n2, n2, n2, n2)), dma((n2, n2, n2, n2, 6)), dma((n2,)), dma((n2, n3)), pltpu.SemaphoreType.REGULAR,
            *(vmem((n2, 6, *lead, width), F32)
              for lead_in, lead_out in (((*ring, dr), (n2, fr)), ((na, dr), (fr // n2,)))
              for lead, width in ((lead_in, fs - pf), (lead_in, pf), (lead_out, dm - pf), (lead_out, pf))),
        ]
        hbm = pl.BlockSpec(memory_space=pl.ANY)
        whole = pl.BlockSpec(memory_space=pltpu.VMEM)
        out = pl.pallas_call(
            kernel,
            out_shape=(
                vmem((rows, dm), BF), vmem((n2, dr, fd), F32), vmem((n2, dr, fd), F32), vmem((n2, fr, dm), F32),
            ),
            in_specs=[hbm] * 5,
            out_specs=(whole,) * NA,
            scratch_shapes=scratch,
            compiler_params=pltpu.CompilerParams(collective_id=0, has_side_effects=True, vmem_limit_bytes=66300000),
            name="train_step",
        )(act_in.reshape(rows, dm), cot_out.reshape(rows, dm), w_gate[:, 0], w_in[:, 0], w_out[:, 0])
        grad_act, grad_gate, grad_lin, grad_proj = pl.pallas_call(
            hand_on, out_shape=tuple(jax.ShapeDtypeStruct(a.shape, a.dtype) for a in out), in_specs=[whole] * NA, out_specs=(hbm,) * NA,
            scratch_shapes=[dma((NA,))], compiler_params=pltpu.CompilerParams(vmem_limit_bytes=2 ** 20), name="hand_on",
        )(*(pltpu.with_memory_space_constraint(a, vmem) for a in out))
        return grad_act.reshape(shape), grad_gate[:, None], grad_lin[:, None], grad_proj[:, None]

    return jax.shard_map(body, mesh=mesh, in_specs=(act_spec, act_spec, w_spec, w_spec, w_spec),
                         out_specs=(act_spec, w_spec, w_spec, w_spec), check_vma=False)
```

```python
import functools

import jax
import jax.numpy as jnp
from jax import lax
from jax.experimental import pallas as pl
from jax.experimental.pallas import tpu as pltpu
from jax.sharding import PartitionSpec as P

NORM_EPS = 1e-6
BF = jnp.bfloat16
F32 = jnp.float32
MESH = pl.DeviceIdType.MESH
X, Y, Z = 0, 1, 2
BLOCKS = COLOURS = HALVES = (0, 1)
NB, NA, NL = len(BLOCKS), 4, 64
RING = (1, 3, 2)
OPP = RING[-1]
PLUS, MINUS = RING[:-1]
QUARTERS = range(NA)
OWN = 0
AXES = ((Z, X, Y), (Y, Z, X), (X, Y, Z))
UP_MATS, OUT_MAT = (0, 1), (2,)
MATS = UP_MATS + OUT_MAT


def mm(left, right):
    return jnp.dot(left, right, preferred_element_type=F32)


def mm_nt(left, right):
    return lax.dot_general(left, right, (((1,), (1,)), ((), ())), preferred_element_type=F32)


def mm_tn(left, right):
    return lax.dot_general(left, right, (((0,), (0,)), ((), ())), preferred_element_type=F32)


def inv_rms(h):
    return lax.rsqrt(jnp.mean(h * h, axis=-1, keepdims=True) + NORM_EPS)


def kernel(act, cot, wg_in, wi_in, wo_in, gact, gg, gi, go,
           wg, wi, wo, hb, eb, xo, ga, ng, f1, f2, f1s, f2s, us, ub, da, db, das, dbs, qs, gs, is_, os_,
           gin0, gin1, gout0, gout1, fin, r3,
           lsem, ag_s, ag_r, lg_r, mc_s, mc_r, rl_s, ga_s, ga_r, rs_s, rs_r, r3_s, r3_r, turn, *rg):
    dm, fd = wo.shape[-1], wg.shape[-1]
    dr, fr = dm // NL, fd // NL
    fs = fd // NA
    pf = fs // NA
    rows = act.shape[0]
    wts = (wg, wi, wo)
    gin, gout = (gin0, gin1), (gout0, gout1)

    p = lax.axis_index("stage")
    d = lax.axis_index("data")
    zc, yc, xc = lax.div(d, 16), lax.rem(lax.div(d, 4), 4), lax.rem(d, 4)
    coord = (xc, yc, zc)
    stride = (1, 4, 16)
    ja = yc + p * (zc - yc)
    jb = zc + p * (yc - zc)
    sa, sb = 4 + 12 * p, 16 - 12 * p

    def rot(c, delta):
        return lax.rem(c + (delta % 4), 4)

    def peer(ax, delta):
        return d + (rot(coord[ax], delta) - coord[ax]) * stride[ax]

    def peer_a(delta):
        return d + (rot(ja, delta) - ja) * sa

    def peer_b(delta):
        return d + (rot(jb, delta) - jb) * sb

    def remote(src, dst, ssem, rsem, dev, core):
        return pltpu.make_async_remote_copy(src_ref=src, dst_ref=dst, send_sem=ssem, recv_sem=rsem,
                                            device_id=(dev, core), device_id_type=MESH)

    def send(src, dst, ssem, rsem, dev, core):
        remote(src, dst, ssem, rsem, dev, core).start()

    def wait_recv(ref, sem):
        remote(ref, ref, sem, sem, d, p).wait_recv()

    def wait_send(ref, sem):
        remote(ref, ref, sem, sem, d, p).wait_send()

    for v in BLOCKS:
        for k, shard in enumerate((wg_in, wi_in, wo_in)):
            pltpu.make_async_copy(shard.at[v], wts[k].at[v, zc, yc, xc], lsem.at[v, k]).start()

    @pl.when(p == 0)
    def _():
        pltpu.make_async_copy(act, hb.at[0, OWN], lsem.at[0, 3]).start()

    @pl.when(p == 1)
    def _():
        pltpu.make_async_copy(cot, eb.at[1, OWN], lsem.at[0, 3]).start()

    barrier = pltpu.get_barrier_semaphore()
    senders = [(peer(ax, delta), p) for ax in (X, Y, Z) for delta in RING]
    senders += [(d, 1 - p), (peer_a(1), 1 - p), (peer_a(-1), 1 - p)]
    for dev, core in senders:
        pl.semaphore_signal(barrier, inc=1, device_id=(dev, core), device_id_type=MESH)
    for v in BLOCKS:
        for k, shard in enumerate((wg_in, wi_in, wo_in)):
            pltpu.make_async_copy(shard.at[v], wts[k].at[v, zc, yc, xc], lsem.at[v, k]).wait()

    @pl.when(p == 0)
    def _():
        pltpu.make_async_copy(act, hb.at[0, OWN], lsem.at[0, 3]).wait()

    @pl.when(p == 1)
    def _():
        pltpu.make_async_copy(cot, eb.at[1, OWN], lsem.at[0, 3]).wait()

    pl.semaphore_wait(barrier, len(senders))

    FIRST, REST = ((0, PLUS, 0), (1, MINUS, 2)), ((1, PLUS, 1), (0, MINUS, 3))
    LARGE = 2
    whole = slice(None)

    def part_at(v, k, small, middle, large, half=None):
        place = dict(zip(AXES[k], (small, middle, large)))
        width = wts[k].shape[-1] // 2
        cols = whole if half is None else pl.ds(half * width, width)
        return wts[k].at[v, place[Z], place[Y], place[X], :, cols]

    def own(k):
        return [coord[ax] for ax in AXES[k]]

    def chunk(v, k, ph, q, half):
        small, middle, large = own(k)
        return part_at(v, k, q, middle, large, half) if ph == 0 else part_at(v, k, pl.ds(2 * half, 2), q, large)

    def small_copy(v, k, ph, q, half, delta, slot):
        ref = chunk(v, k, ph, q, half)
        send(ref, ref, ag_s.at[v, k, ph], ag_r.at[v, k, ph, slot], peer(AXES[k][ph], delta), p)

    def small_wait(v, k, ph, back, half, slot):
        wait_recv(chunk(v, k, ph, rot(coord[AXES[k][ph]], back), half), ag_r.at[v, k, ph, slot])

    def small_send(v, ph):
        for half, delta, slot in FIRST + REST:
            for k in MATS:
                small_copy(v, k, ph, coord[AXES[k][ph]], half, delta, slot)

    def small_relay(v, ph):
        for half, delta, slot in FIRST:
            for k in MATS:
                small_wait(v, k, ph, -delta, half, slot)
                small_copy(v, k, ph, rot(coord[AXES[k][ph]], -delta), half, delta, 4 + half)

    def small_rest(v, ph):
        for half, delta, slot in REST:
            for k in MATS:
                small_wait(v, k, ph, -delta, half, slot)

    def small_last(v, ph):
        for half in HALVES:
            for k in MATS:
                small_wait(v, k, ph, OPP, half, 4 + half)

    def direct_send(v):
        for delta in (OPP, PLUS, MINUS):
            for k in MATS:
                ref = part_at(v, k, *own(k))
                send(ref, ref, ag_s.at[v, k, 0], ag_r.at[v, k, 0, delta], peer(AXES[k][0], delta), p)

    def direct_wait(v):
        for delta in RING:
            for k in MATS:
                small, middle, large = own(k)
                wait_recv(part_at(v, k, rot(small, -delta), middle, large), ag_r.at[v, k, 0, delta])

    UP, DOWN = (0, PLUS), (MINUS, OPP)
    RELAYS = ((UP[0], PLUS), (DOWN[0], MINUS), (UP[1], PLUS), (DOWN[1], MINUS))

    def row(v, k, q, r):
        return part_at(v, k, whole, rot(coord[AXES[k][1]], r), q)

    def large_slot(r, delta):
        return r if delta == PLUS else NA + r

    def large_send(v, up, down):
        for pair in zip(up, down):
            for r, delta in zip(pair, (PLUS, MINUS)):
                for k in MATS:
                    ax = AXES[k][LARGE]
                    ref = row(v, k, coord[ax], r)
                    send(ref, ref, ag_s.at[v, k, LARGE], lg_r.at[v, k, large_slot(r, delta)], peer(ax, delta), p)

    def large_relay(v):
        for r, delta in RELAYS:
            for k in MATS:
                ax = AXES[k][LARGE]
                ref = row(v, k, rot(coord[ax], -delta), r)
                wait_recv(ref, lg_r.at[v, k, large_slot(r, delta)])
                send(ref, ref, ag_s.at[v, k, LARGE], lg_r.at[v, k, 2 * NA + r], peer(ax, delta), p)

    def large_finish(v, mats):
        for pieces, delta in ((DOWN, PLUS), (UP, MINUS)):
            for r in pieces:
                for k in mats:
                    wait_recv(row(v, k, rot(coord[AXES[k][LARGE]], -delta), r), lg_r.at[v, k, large_slot(r, delta)])
        for r in QUARTERS:
            for k in mats:
                wait_recv(row(v, k, rot(coord[AXES[k][LARGE]], OPP), r), lg_r.at[v, k, 2 * NA + r])

    half_rows = rows // 2
    BACK, AHEAD, FAR = 1, 2, 3

    def spread_near(src, buf, which, vd, ssem):
        send(src, buf.at[vd, OWN], ssem, mc_r.at[which, vd, OWN], d, 1 - p)

    def rows_half(half):
        return pl.ds(half * half_rows, half_rows)

    HALF_ORDER = [(half if first else 1 - half, slot, delta, slot if first else FAR + 1 + slot)
                  for first in (True, False) for half, slot, delta in ((0, BACK, PLUS), (1, AHEAD, MINUS))]

    def spread_far(src, buf, which, vd, ssem):
        for half, slot, delta, sem in HALF_ORDER:
            send(src.at[rows_half(half)], buf.at[vd, slot, rows_half(half)], ssem, mc_r.at[which, vd, sem], peer_b(delta), 1 - p)

    def spread_same(buf, which, v, ssem):
        for half, slot, delta, sem in HALF_ORDER:
            send(buf.at[v, OWN, rows_half(half)], buf.at[v, slot, rows_half(half)], ssem, mc_r.at[which, v, sem], peer_a(delta), p)

    def spread_relay(buf, which, v):
        for half, slot, delta, sem in HALF_ORDER:
            ref = buf.at[v, slot, rows_half(half)]
            wait_recv(ref, mc_r.at[which, v, sem])
            if sem == slot:
                send(ref, buf.at[v, FAR, rows_half(half)], rl_s.at[which, v], mc_r.at[which, v, FAR + half], peer_a(delta), p)

    def spread_finish(buf, which, v):
        for half in HALVES:
            wait_recv(buf.at[v, FAR, rows_half(half)], mc_r.at[which, v, FAR + half])

    def spread_own(buf, which, v):
        wait_recv(buf.at[v, OWN], mc_r.at[which, v, OWN])

    def gates(n, wgt, wlin):
        a, b = mm(n, wgt), mm(n, wlin)
        s = jax.nn.sigmoid(a)
        act_a = a * s
        return (act_a * b).astype(BF), b * s * (1.0 + a * (1.0 - s)), act_a

    def block_gates(v):
        h = hb[v, OWN].astype(F32)
        n = (h * inv_rms(h)).astype(BF)

        def tile(i, carry):
            wide = fs // 2
            cols = pl.ds(pl.multiple_of(i * wide, wide), wide)
            u, t1, t2 = gates(n, wg[v, :, :, :, :, cols].reshape(dm, wide), wi[v, :, :, :, :, cols].reshape(dm, wide))
            ub[:, cols] = u
            f1[v, :, cols] = t1
            f2[v, :, cols] = t2
            return carry

        lax.fori_loop(0, 2 * NA, tile, 0, unroll=True)

    def block_out(v, dst):
        half_dm = dm // 2
        for i in HALVES:
            cols = pl.ds(i * half_dm, half_dm)
            out = mm(ub[...], wo[v, :, :, :, :, cols].reshape(fd, half_dm))
            dst[:, cols] = (hb[v, OWN, :, cols].astype(F32) + out).astype(BF)

    def block_backward(v, dst):
        e = eb[v, OWN]

        def tile(i, carry):
            cols = pl.ds(pl.multiple_of(i * fs, fs), fs)
            t = mm_nt(e, wo[v, i].reshape(fs, dm))
            da[:, cols] = (t * f1[v, :, cols]).astype(BF)
            db[:, cols] = (t * f2[v, :, cols]).astype(BF)
            return carry

        lax.fori_loop(0, NA, tile, 0, unroll=True)
        half_dm = dm // 2
        for i in HALVES:
            q = mm_nt(da[...], wg[v, pl.ds(2 * i, 2)].reshape(half_dm, fd))
            q += mm_nt(db[...], wi[v, pl.ds(2 * i, 2)].reshape(half_dm, fd))
            qs[:, pl.ds(i * half_dm, half_dm)] = q
        h = hb[v, OWN].astype(F32)
        r = inv_rms(h)
        hr = h * r
        q = qs[...]
        dst[...] = (e.astype(F32) + r * (q - hr * jnp.mean(q * hr, axis=-1, keepdims=True))).astype(BF)

    def piece(j, i):
        z = i + p * (j - i)
        y = j + p * (i - j)
        return z, y

    EARLY, LATE = range(FAR), range(FAR, NA)

    def grad_first(v, slots):
        for i in QUARTERS if OWN in slots else ():
            z, y = piece(ja, i)
            cols = pl.ds(pl.multiple_of((z * NA + y) * pf, pf), pf)
            gs[v, :, pl.ds(i * pf, pf)] = wg[v, :, :, :, :, cols].reshape(dm, pf)
            is_[v, :, pl.ds(i * pf, pf)] = wi[v, :, :, :, :, cols].reshape(dm, pf)
        for s in slots:
            h = hb[v, s].astype(F32)
            n = (h * inv_rms(h)).astype(BF)
            ng[v, s] = n
            u, t1, t2 = gates(n, gs[v], is_[v])
            us[v, s] = u
            f1s[v, s] = t1
            f2s[v, s] = t2

    def grad_hidden(v, slots):
        for i in QUARTERS if OWN in slots else ():
            z, y = piece(ja, i)
            os_[pl.ds(i * pf, pf), :] = wo[v, z, y].reshape(pf, dm)
        for s in slots:
            t = mm_nt(eb[v, s], os_[...])
            das[s] = (t * f1s[v, s]).astype(BF)
            dbs[s] = (t * f2s[v, s]).astype(BF)

    def split(width):
        return pl.ds(0, width - pf), pl.ds(width - pf, pf)

    def keep(refs, v, place, tile, cols, first):
        b, rest = place[0], place[1:]
        lead = () if v is None else (v,)
        for colour in COLOURS:
            part = tile[..., cols[colour].start:cols[colour].start + cols[colour].size]
            at = lead + ((b, slice(None)) if colour == 0 else (slice(None), b)) + rest
            refs[colour][at] = part if first else refs[colour][at] + part

    def rows_of(slots):
        return pl.ds(slots[0], len(slots)), len(slots) * rows

    def grad_out(v, slots):
        some, count = rows_of(slots)
        for i in HALVES:
            cols = pl.ds(i * 2 * pf, 2 * pf)
            g = mm_tn(us[v, some, :, cols].reshape(count, 2 * pf), eb[v, some].reshape(count, dm)).reshape(2, NA, fr, dm)
            for b in HALVES:
                keep(gout, v, (2 * i + b,), g[b], split(dm), OWN in slots)

    def grad_in(v, slots):
        some, count = rows_of(slots)
        for which, dref in enumerate((das, dbs)):
            for i in QUARTERS:
                cols = pl.ds(i * (dm // NA), dm // NA)
                g = mm_tn(ng[v, some, :, cols].reshape(count, dm // NA), dref[some].reshape(count, fs)).reshape(NA, NA, dr, fs)
                for y in QUARTERS:
                    keep([ref.at[v, which] for ref in gin], None, (i + p * (y - i), y + p * (i - y)), g[y], split(fs), OWN in slots)

    IN, OUT = 0, 1

    def view(which, st, v, colour, t, half):
        own = jb if colour == 0 else xc
        if which == IN:
            ref = gin[colour].at[v, half]
            return ref.at[t] if st == 0 else ref.at[own, t]
        ref = gout[colour].at[v]
        return ref.at[t, pl.ds(2 * half, 2)] if st == 0 else ref.at[own, t, pl.ds(half * (fr // 2), fr // 2)]

    RECV = (((rg[0], rg[1]), (rg[2], rg[3])), ((rg[4], rg[5]), (rg[6], rg[7])))
    MERGED, DIRECT = ((0, OPP, PLUS, 0), (1, OPP, MINUS, 1)), ((1, PLUS, PLUS, 2), (0, MINUS, MINUS, 3))
    RELAYED = ((0, PLUS, PLUS, 4), (1, MINUS, MINUS, 5))

    def axis_of(colour, st):
        return (jb, peer_b) if colour == st else (xc, functools.partial(peer, X))

    def scatter_send(v, which, st, copies):
        for colour in COLOURS:
            q, to = axis_of(colour, st)
            for half, c, delta, slot in copies:
                send(view(which, st, v, colour, rot(q, c), half), RECV[st][which][colour].at[v, slot],
                     rs_s.at[st, v, colour, which], rs_r.at[st, v, colour, which, slot], to(delta), p)

    def scatter_relay(v, which, st):
        for colour in COLOURS:
            q, _ = axis_of(colour, st)
            recv = RECV[st][which][colour]
            for half, c, _, slot in RELAYED:
                wait_recv(recv.at[v, slot - 4], rs_r.at[st, v, colour, which, slot - 4])
                ref = view(which, st, v, colour, rot(q, c), half)
                ref[...] = ref[...] + recv[v, slot - 4]
        scatter_send(v, which, st, RELAYED)

    def scatter_sum(v, which, st):
        for colour in COLOURS:
            q, _ = axis_of(colour, st)
            recv = RECV[st][which][colour]
            for half in HALVES:
                direct, merged = 3 - half, 4 + half
                for slot in (direct, merged):
                    wait_recv(recv.at[v, slot], rs_r.at[st, v, colour, which, slot])
                ref = view(which, st, v, colour, q, half)
                ref[...] = ref[...] + recv[v, direct] + recv[v, merged]

    def scatter_turn(v, which):
        scatter_sum(v, which, 0)
        scatter_send(v, which, 1, MERGED + DIRECT)

    def scatter_out(v):
        scatter_sum(v, OUT, 1)
        for colour in COLOURS:
            go[v, :, split(dm)[colour]] = gout[colour][(v, jb, xc) if colour == 0 else (v, xc, jb)]

    def scatter_last(v):
        scatter_sum(v, IN, 1)
        for which in HALVES:
            for colour in COLOURS:
                fin[v, :, which, :, split(fs)[colour]] = gin[colour][(v, which, jb, xc) if colour == 0 else (v, which, xc, jb)]
        for delta in (OPP, PLUS, MINUS):
            send(fin.at[v, rot(ja, delta)], r3.at[v, delta - 1], r3_s.at[v], r3_r.at[v, delta - 1], peer_a(delta), p)

    def scatter_finish(v):
        def put(j, vals):
            for i in QUARTERS:
                z, y = piece(j, i)
                cols = pl.ds(pl.multiple_of((z * NA + y) * pf, pf), pf)
                gg[v, :, cols] = vals(0)[:, i * pf:(i + 1) * pf]
                gi[v, :, cols] = vals(1)[:, i * pf:(i + 1) * pf]

        put(ja, lambda w: fin[v, ja, w])
        for delta in RING:
            wait_recv(r3.at[v, delta - 1], r3_r.at[v, delta - 1])
            put(rot(ja, -delta), lambda w, delta=delta: r3[v, delta - 1, w])

    def step(fn, *args):
        with jax.named_scope(fn.__name__):
            fn(*args)

    def on(core):
        return pl.when(p == core)

    def take_turn():
        pl.semaphore_wait(turn, 1)

    def give_turn():
        pl.semaphore_signal(turn, inc=1, device_id=(d, 1 - p), device_id_type=MESH)

    h_mid, h_late, e_first, e_last = ((xo.at[i], mc_s.at[1 + i]) for i in QUARTERS)

    def pass_on(part, item, buf, which, vd):
        step(part, item[0], buf, which, vd, item[1])

    AFTER = (MINUS, OPP), (0, PLUS)
    step(direct_send, 0)
    step(small_send, 1, 0)

    @on(0)
    def _():
        step(spread_same, hb, 0, 0, mc_s.at[0])

    step(direct_wait, 0)
    step(small_send, 0, 1)
    step(small_relay, 1, 0)
    step(large_send, 0, (0,), (0,))
    step(small_rest, 1, 0)
    step(small_last, 1, 0)
    step(small_send, 1, 1)
    step(small_relay, 0, 1)
    step(small_relay, 1, 1)
    step(small_rest, 0, 1)
    step(large_send, 0, (PLUS, MINUS), (MINUS, PLUS))
    step(small_last, 0, 1)
    step(large_send, 0, (OPP,), (OPP,))
    step(small_rest, 1, 1)
    step(small_last, 1, 1)
    step(large_relay, 0)

    @on(0)
    def _():
        step(large_send, 1, UP, DOWN)

    step(large_finish, 0, UP_MATS)

    @on(0)
    def _():
        step(large_send, 1, *AFTER)

    @on(1)
    def _():
        step(take_turn)
        step(large_send, 1, UP, DOWN)
        step(spread_own, hb, 0, 0)

    step(block_gates, 0)

    @on(1)
    def _():
        step(large_send, 1, *AFTER)

    step(large_finish, 0, OUT_MAT)
    step(block_out, 0, h_mid[0])
    pass_on(spread_near, h_mid, hb, 0, p)
    step(large_relay, 1)

    @on(0)
    def _():
        step(give_turn)
        step(spread_relay, hb, 0, 0)

    step(spread_own, hb, 0, 1)
    step(large_finish, 1, UP_MATS)
    step(block_gates, 1)
    step(large_finish, 1, OUT_MAT)

    @on(0)
    def _():
        step(block_out, 1, h_late[0])
        pass_on(spread_near, h_late, hb, 0, 1)
        pass_on(spread_far, h_late, hb, 0, 1)
        step(spread_finish, hb, 0, 0)
        step(grad_first, 0, EARLY)
        step(grad_first, 0, LATE)
        step(spread_own, eb, 1, 1)
        pass_on(spread_far, h_mid, hb, 0, p)
        step(block_backward, 1, e_first[0])
        pass_on(spread_near, e_first, eb, 1, 0)
        pass_on(spread_far, e_first, eb, 1, 0)
        step(spread_relay, hb, 0, 1)

    @on(1)
    def _():
        pass_on(spread_far, h_mid, hb, 0, p)
        step(spread_same, eb, 1, 1, mc_s.at[0])
        step(block_backward, 1, e_first[0])
        pass_on(spread_near, e_first, eb, 1, 1)
        pass_on(spread_far, e_first, eb, 1, 1)
        step(spread_relay, hb, 0, 1)

    step(grad_first, 1, EARLY)
    step(spread_relay, eb, 1, 1)

    step(grad_hidden, 1, EARLY)
    step(grad_out, 1, EARLY)

    @on(0)
    def _():
        step(grad_in, 1, EARLY)

    @on(1)
    def _():
        step(spread_own, eb, 1, 0)
        step(block_backward, 0, e_last[0])
        pass_on(spread_near, e_last, eb, 1, 0)
        pass_on(spread_far, e_last, eb, 1, 0)
        step(grad_in, 1, EARLY)

    step(spread_finish, hb, 0, 1)
    step(grad_first, 1, LATE)

    step(spread_finish, eb, 1, 1)
    step(grad_hidden, 1, LATE)
    step(grad_out, 1, LATE)
    step(scatter_send, 1, OUT, 0, MERGED)
    step(grad_in, 1, LATE)
    step(scatter_send, 1, IN, 0, MERGED)

    @on(0)
    def _():
        step(spread_relay, eb, 1, 0)
        step(spread_own, eb, 1, 0)
        step(block_backward, 0, ga)
        send(ga, ga, ga_s, ga_r, d, 1)

    @on(1)
    def _():
        step(spread_relay, hb, 0, 0)
        step(grad_first, 0, EARLY)

    step(scatter_send, 1, OUT, 0, DIRECT)

    @on(1)
    def _():
        step(spread_relay, eb, 1, 0)
        step(spread_finish, hb, 0, 0)
        step(grad_first, 0, LATE)

    step(grad_hidden, 0, EARLY)
    step(scatter_send, 1, IN, 0, DIRECT)
    step(grad_in, 0, EARLY)
    step(grad_out, 0, EARLY)
    step(scatter_relay, 1, OUT, 0)
    step(spread_finish, eb, 1, 0)
    step(grad_hidden, 0, LATE)
    step(grad_in, 0, LATE)
    step(scatter_send, 0, IN, 0, MERGED)
    step(grad_out, 0, LATE)
    step(scatter_relay, 1, IN, 0)
    step(scatter_send, 0, OUT, 0, MERGED)
    step(scatter_send, 0, IN, 0, DIRECT)
    step(scatter_turn, 1, OUT)
    step(scatter_relay, 0, IN, 0)
    step(scatter_send, 0, OUT, 0, DIRECT)
    step(scatter_turn, 1, IN)
    step(scatter_relay, 0, OUT, 0)
    step(scatter_relay, 1, OUT, 1)

    @on(1)
    def _():
        wait_recv(ga, ga_r)

    gact[...] = ga[...]
    step(scatter_turn, 0, IN)
    step(scatter_relay, 1, IN, 1)
    step(scatter_turn, 0, OUT)
    step(scatter_relay, 0, IN, 1)
    step(scatter_out, 1)
    step(scatter_last, 1)
    step(scatter_relay, 0, OUT, 1)
    step(scatter_last, 0)
    step(scatter_finish, 1)
    step(scatter_out, 0)
    step(scatter_finish, 0)

    for v in BLOCKS:
        for k in MATS:
            three = pl.ds(0, len(RING))
            wait_send(part_at(v, k, three, 0, 0), ag_s.at[v, k, 0])
            wait_send(part_at(v, k, whole, three, 0), ag_s.at[v, k, 1])
            wait_send(part_at(v, k, whole, whole, three), ag_s.at[v, k, LARGE])
        for colour in COLOURS:
            for which in HALVES:
                for st in HALVES:
                    wait_send(RECV[st][which][colour].at[v], rs_s.at[st, v, colour, which])
        wait_send(r3.at[v], r3_s.at[v])
        wait_send(hb.at[v, 0], rl_s.at[0, v])
        wait_send(hb.at[v, 0], rl_s.at[1, v])
    wait_send(hb.at[0, pl.ds(0, 2)], mc_s.at[0])
    wait_send(hb.at[0, pl.ds(0, 3)], mc_s.at[1])
    wait_send(hb.at[0, pl.ds(0, 3)], mc_s.at[3])

    @pl.when(p == 0)
    def _():
        wait_send(hb.at[0, pl.ds(0, 3)], mc_s.at[2])
        wait_send(ga, ga_s)

    @pl.when(p == 1)
    def _():
        wait_send(hb.at[0, pl.ds(0, 3)], mc_s.at[4])


def hand_on(*refs):
    copies = [pltpu.make_async_copy(refs[i], refs[NA + i], refs[-1].at[i]) for i in QUARTERS]
    for copy in copies:
        copy.start()
    for copy in copies:
        copy.wait()


def solution(mesh):
    act_spec = P(None, "data", None, None)
    w_spec = P(None, "stage", "data", None)

    def body(act_in, cot_out, w_gate, w_in, w_out):
        shape = act_in.shape
        dm, fd = shape[3], w_gate.shape[3]
        rows = shape[0] * shape[1] * shape[2]
        dr, fr, fs = dm // NL, fd // NL, fd // NA
        pf = fs // NA
        vmem = pltpu.VMEM
        dma = pltpu.SemaphoreType.DMA
        n2, n3, na = NB, len(RING), NA
        ring = (na, na)
        scratch = [
            vmem((n2, na, *ring, dr, fd), BF), vmem((n2, na, *ring, dr, fd), BF), vmem((n2, na, *ring, fr, dm), BF),
            vmem((n2, na, rows, dm), BF), vmem((n2, na, rows, dm), BF), vmem((na, rows, dm), BF), vmem((rows, dm), BF),
            vmem((n2, na, rows, dm), BF),
            vmem((n2, rows, fd), F32), vmem((n2, rows, fd), F32),
            vmem((n2, na, rows, fs), F32), vmem((n2, na, rows, fs), F32),
            vmem((n2, na, rows, fs), BF),
            vmem((rows, fd), BF), vmem((rows, fd), BF), vmem((rows, fd), BF),
            vmem((na, rows, fs), BF), vmem((na, rows, fs), BF),
            vmem((rows, dm), F32),
            vmem((n2, dm, fs), BF), vmem((n2, dm, fs), BF), vmem((fs, dm), BF),
            *(vmem((n2, n2, *ring, na, dr, width), F32) for width in (fs - pf, pf)),
            *(vmem((n2, *ring, fr, width), F32) for width in (dm - pf, pf)),
            vmem((n2, na, n2, dr, fs), F32), vmem((n2, n3, n2, dr, fs), F32),
            dma((n2, na)), dma((n2, n3, n3)), dma((n2, n3, n2, 6)), dma((n2, n3, n3 * na)), dma((5,)), dma((n2, n2, 7)), dma((n2, n2)), dma, dma,
            dma((n2, n2, n2, n2)), dma((n2, n2, n2, n2, 6)), dma((n2,)), dma((n2, n3)), pltpu.SemaphoreType.REGULAR,
            *(vmem((n2, 6, *lead, width), F32)
              for lead_in, lead_out in (((*ring, dr), (n2, fr)), ((na, dr), (fr // n2,)))
              for lead, width in ((lead_in, fs - pf), (lead_in, pf), (lead_out, dm - pf), (lead_out, pf))),
        ]
        hbm = pl.BlockSpec(memory_space=pl.ANY)
        whole = pl.BlockSpec(memory_space=pltpu.VMEM)
        out = pl.pallas_call(
            kernel,
            out_shape=(
                vmem((rows, dm), BF), vmem((n2, dr, fd), F32), vmem((n2, dr, fd), F32), vmem((n2, fr, dm), F32),
            ),
            in_specs=[hbm] * 5,
            out_specs=(whole,) * NA,
            scratch_shapes=scratch,
            compiler_params=pltpu.CompilerParams(collective_id=0, has_side_effects=True, vmem_limit_bytes=66300000),
            name="train_step",
        )(act_in.reshape(rows, dm), cot_out.reshape(rows, dm), w_gate[:, 0], w_in[:, 0], w_out[:, 0])
        grad_act, grad_gate, grad_lin, grad_proj = pl.pallas_call(
            hand_on, out_shape=tuple(jax.ShapeDtypeStruct(a.shape, a.dtype) for a in out), in_specs=[whole] * NA, out_specs=(hbm,) * NA,
            scratch_shapes=[dma((NA,))], compiler_params=pltpu.CompilerParams(vmem_limit_bytes=2 ** 20), name="hand_on",
        )(*(pltpu.with_memory_space_constraint(a, vmem) for a in out))
        return grad_act.reshape(shape), grad_gate[:, None], grad_lin[:, None], grad_proj[:, None]

    return jax.shard_map(body, mesh=mesh, in_specs=(act_spec, act_spec, w_spec, w_spec, w_spec),
                         out_specs=(act_spec, w_spec, w_spec, w_spec), check_vma=False)
```

```python
import functools

import jax
import jax.numpy as jnp
from jax import lax
from jax.experimental import pallas as pl
from jax.experimental.pallas import tpu as pltpu
from jax.sharding import PartitionSpec as P

NORM_EPS = 1e-6
BF = jnp.bfloat16
F32 = jnp.float32
MESH = pl.DeviceIdType.MESH
X, Y, Z = 0, 1, 2
BLOCKS = COLOURS = HALVES = (0, 1)
NB, NA, NL = len(BLOCKS), 4, 64
RING = (1, 3, 2)
OPP = RING[-1]
PLUS, MINUS = RING[:-1]
QUARTERS = range(NA)
OWN = 0
AXES = ((Z, X, Y), (Y, Z, X), (X, Y, Z))
UP_MATS, OUT_MAT = (0, 1), (2,)
MATS = UP_MATS + OUT_MAT


def mm(left, right):
    return jnp.dot(left, right, preferred_element_type=F32)


def mm_nt(left, right):
    return lax.dot_general(left, right, (((1,), (1,)), ((), ())), preferred_element_type=F32)


def mm_tn(left, right):
    return lax.dot_general(left, right, (((0,), (0,)), ((), ())), preferred_element_type=F32)


def inv_rms(h):
    return lax.rsqrt(jnp.mean(h * h, axis=-1, keepdims=True) + NORM_EPS)


def kernel(act, cot, wg_in, wi_in, wo_in, gact, gg, gi, go,
           wg, wi, wo, hb, eb, xo, ga, ng, f1, f2, f1s, f2s, us, ub, da, db, das, dbs, qs, gs, is_, os_,
           gin0, gin1, gout0, gout1, fin, r3,
           lsem, ag_s, ag_r, lg_r, mc_s, mc_r, rl_s, ga_s, ga_r, rs_s, rs_r, r3_s, r3_r, turn, *rg):
    dm, fd = wo.shape[-1], wg.shape[-1]
    dr, fr = dm // NL, fd // NL
    fs = fd // NA
    pf = fs // NA
    rows = act.shape[0]
    wts = (wg, wi, wo)
    gin, gout = (gin0, gin1), (gout0, gout1)

    p = lax.axis_index("stage")
    d = lax.axis_index("data")
    zc, yc, xc = lax.div(d, 16), lax.rem(lax.div(d, 4), 4), lax.rem(d, 4)
    coord = (xc, yc, zc)
    stride = (1, 4, 16)
    ja = yc + p * (zc - yc)
    jb = zc + p * (yc - zc)
    sa, sb = 4 + 12 * p, 16 - 12 * p

    def rot(c, delta):
        return lax.rem(c + (delta % 4), 4)

    def peer(ax, delta):
        return d + (rot(coord[ax], delta) - coord[ax]) * stride[ax]

    def peer_a(delta):
        return d + (rot(ja, delta) - ja) * sa

    def peer_b(delta):
        return d + (rot(jb, delta) - jb) * sb

    def remote(src, dst, ssem, rsem, dev, core):
        return pltpu.make_async_remote_copy(src_ref=src, dst_ref=dst, send_sem=ssem, recv_sem=rsem,
                                            device_id=(dev, core), device_id_type=MESH)

    def send(src, dst, ssem, rsem, dev, core):
        remote(src, dst, ssem, rsem, dev, core).start()

    def wait_recv(ref, sem):
        remote(ref, ref, sem, sem, d, p).wait_recv()

    def wait_send(ref, sem):
        remote(ref, ref, sem, sem, d, p).wait_send()

    for v in BLOCKS:
        for k, shard in enumerate((wg_in, wi_in, wo_in)):
            pltpu.make_async_copy(shard.at[v], wts[k].at[v, zc, yc, xc], lsem.at[v, k]).start()

    @pl.when(p == 0)
    def _():
        pltpu.make_async_copy(act, hb.at[0, OWN], lsem.at[0, 3]).start()

    @pl.when(p == 1)
    def _():
        pltpu.make_async_copy(cot, eb.at[1, OWN], lsem.at[0, 3]).start()

    barrier = pltpu.get_barrier_semaphore()
    senders = [(peer(ax, delta), p) for ax in (X, Y, Z) for delta in RING]
    senders += [(d, 1 - p), (peer_a(1), 1 - p), (peer_a(-1), 1 - p)]
    for dev, core in senders:
        pl.semaphore_signal(barrier, inc=1, device_id=(dev, core), device_id_type=MESH)
    for v in BLOCKS:
        for k, shard in enumerate((wg_in, wi_in, wo_in)):
            pltpu.make_async_copy(shard.at[v], wts[k].at[v, zc, yc, xc], lsem.at[v, k]).wait()

    @pl.when(p == 0)
    def _():
        pltpu.make_async_copy(act, hb.at[0, OWN], lsem.at[0, 3]).wait()

    @pl.when(p == 1)
    def _():
        pltpu.make_async_copy(cot, eb.at[1, OWN], lsem.at[0, 3]).wait()

    pl.semaphore_wait(barrier, len(senders))

    FIRST, REST = ((0, PLUS, 0), (1, MINUS, 2)), ((1, PLUS, 1), (0, MINUS, 3))
    LARGE = 2
    whole = slice(None)

    def part_at(v, k, small, middle, large, half=None):
        place = dict(zip(AXES[k], (small, middle, large)))
        width = wts[k].shape[-1] // 2
        cols = whole if half is None else pl.ds(half * width, width)
        return wts[k].at[v, place[Z], place[Y], place[X], :, cols]

    def own(k):
        return [coord[ax] for ax in AXES[k]]

    def chunk(v, k, ph, q, half):
        small, middle, large = own(k)
        return part_at(v, k, q, middle, large, half) if ph == 0 else part_at(v, k, pl.ds(2 * half, 2), q, large)

    def small_copy(v, k, ph, q, half, delta, slot):
        ref = chunk(v, k, ph, q, half)
        send(ref, ref, ag_s.at[v, k, ph], ag_r.at[v, k, ph, slot], peer(AXES[k][ph], delta), p)

    def small_wait(v, k, ph, back, half, slot):
        wait_recv(chunk(v, k, ph, rot(coord[AXES[k][ph]], back), half), ag_r.at[v, k, ph, slot])

    def small_send(v, ph):
        for half, delta, slot in FIRST + REST:
            for k in MATS:
                small_copy(v, k, ph, coord[AXES[k][ph]], half, delta, slot)

    def small_relay(v, ph):
        for half, delta, slot in FIRST:
            for k in MATS:
                small_wait(v, k, ph, -delta, half, slot)
                small_copy(v, k, ph, rot(coord[AXES[k][ph]], -delta), half, delta, 4 + half)

    def small_rest(v, ph):
        for half, delta, slot in REST:
            for k in MATS:
                small_wait(v, k, ph, -delta, half, slot)

    def small_last(v, ph):
        for half in HALVES:
            for k in MATS:
                small_wait(v, k, ph, OPP, half, 4 + half)

    def direct_send(v):
        for delta in (OPP, PLUS, MINUS):
            for k in MATS:
                ref = part_at(v, k, *own(k))
                send(ref, ref, ag_s.at[v, k, 0], ag_r.at[v, k, 0, delta], peer(AXES[k][0], delta), p)

    def direct_wait(v):
        for delta in RING:
            for k in MATS:
                small, middle, large = own(k)
                wait_recv(part_at(v, k, rot(small, -delta), middle, large), ag_r.at[v, k, 0, delta])

    UP, DOWN = (0, PLUS), (MINUS, OPP)
    RELAYS = ((UP[0], PLUS), (DOWN[0], MINUS), (UP[1], PLUS), (DOWN[1], MINUS))

    def row(v, k, q, r):
        return part_at(v, k, whole, rot(coord[AXES[k][1]], r), q)

    def large_slot(r, delta):
        return r if delta == PLUS else NA + r

    def large_send(v, up, down):
        for pair in zip(up, down):
            for r, delta in zip(pair, (PLUS, MINUS)):
                for k in MATS:
                    ax = AXES[k][LARGE]
                    ref = row(v, k, coord[ax], r)
                    send(ref, ref, ag_s.at[v, k, LARGE], lg_r.at[v, k, large_slot(r, delta)], peer(ax, delta), p)

    def large_relay(v):
        for r, delta in RELAYS:
            for k in MATS:
                ax = AXES[k][LARGE]
                ref = row(v, k, rot(coord[ax], -delta), r)
                wait_recv(ref, lg_r.at[v, k, large_slot(r, delta)])
                send(ref, ref, ag_s.at[v, k, LARGE], lg_r.at[v, k, 2 * NA + r], peer(ax, delta), p)

    def large_finish(v, mats):
        for pieces, delta in ((DOWN, PLUS), (UP, MINUS)):
            for r in pieces:
                for k in mats:
                    wait_recv(row(v, k, rot(coord[AXES[k][LARGE]], -delta), r), lg_r.at[v, k, large_slot(r, delta)])
        for r in QUARTERS:
            for k in mats:
                wait_recv(row(v, k, rot(coord[AXES[k][LARGE]], OPP), r), lg_r.at[v, k, 2 * NA + r])

    half_rows = rows // 2
    BACK, AHEAD, FAR = 1, 2, 3

    def spread_near(src, buf, which, vd, ssem):
        send(src, buf.at[vd, OWN], ssem, mc_r.at[which, vd, OWN], d, 1 - p)

    def rows_half(half):
        return pl.ds(half * half_rows, half_rows)

    HALF_ORDER = [(half if first else 1 - half, slot, delta, slot if first else FAR + 1 + slot)
                  for first in (True, False) for half, slot, delta in ((0, BACK, PLUS), (1, AHEAD, MINUS))]

    def spread_far(src, buf, which, vd, ssem):
        for half, slot, delta, sem in HALF_ORDER:
            send(src.at[rows_half(half)], buf.at[vd, slot, rows_half(half)], ssem, mc_r.at[which, vd, sem], peer_b(delta), 1 - p)

    def spread_same(buf, which, v, ssem):
        for half, slot, delta, sem in HALF_ORDER:
            send(buf.at[v, OWN, rows_half(half)], buf.at[v, slot, rows_half(half)], ssem, mc_r.at[which, v, sem], peer_a(delta), p)

    def spread_relay(buf, which, v):
        for half, slot, delta, sem in HALF_ORDER:
            ref = buf.at[v, slot, rows_half(half)]
            wait_recv(ref, mc_r.at[which, v, sem])
            if sem == slot:
                send(ref, buf.at[v, FAR, rows_half(half)], rl_s.at[which, v], mc_r.at[which, v, FAR + half], peer_a(delta), p)

    def spread_finish(buf, which, v):
        for half in HALVES:
            wait_recv(buf.at[v, FAR, rows_half(half)], mc_r.at[which, v, FAR + half])

    def spread_own(buf, which, v):
        wait_recv(buf.at[v, OWN], mc_r.at[which, v, OWN])

    def gates(n, wgt, wlin):
        a, b = mm(n, wgt), mm(n, wlin)
        s = jax.nn.sigmoid(a)
        act_a = a * s
        return (act_a * b).astype(BF), b * s * (1.0 + a * (1.0 - s)), act_a

    def block_gates(v):
        h = hb[v, OWN].astype(F32)
        n = (h * inv_rms(h)).astype(BF)

        def tile(i, carry):
            wide = fs // 2
            cols = pl.ds(pl.multiple_of(i * wide, wide), wide)
            u, t1, t2 = gates(n, wg[v, :, :, :, :, cols].reshape(dm, wide), wi[v, :, :, :, :, cols].reshape(dm, wide))
            ub[:, cols] = u
            f1[v, :, cols] = t1
            f2[v, :, cols] = t2
            return carry

        lax.fori_loop(0, 2 * NA, tile, 0, unroll=True)

    def block_out(v, dst):
        half_dm = dm // 2
        for i in HALVES:
            cols = pl.ds(i * half_dm, half_dm)
            out = mm(ub[...], wo[v, :, :, :, :, cols].reshape(fd, half_dm))
            dst[:, cols] = (hb[v, OWN, :, cols].astype(F32) + out).astype(BF)

    def block_backward(v, dst):
        e = eb[v, OWN]

        def tile(i, carry):
            cols = pl.ds(pl.multiple_of(i * fs, fs), fs)
            t = mm_nt(e, wo[v, i].reshape(fs, dm))
            da[:, cols] = (t * f1[v, :, cols]).astype(BF)
            db[:, cols] = (t * f2[v, :, cols]).astype(BF)
            return carry

        lax.fori_loop(0, NA, tile, 0, unroll=True)
        half_dm = dm // 2
        for i in HALVES:
            q = mm_nt(da[...], wg[v, pl.ds(2 * i, 2)].reshape(half_dm, fd))
            q += mm_nt(db[...], wi[v, pl.ds(2 * i, 2)].reshape(half_dm, fd))
            qs[:, pl.ds(i * half_dm, half_dm)] = q
        h = hb[v, OWN].astype(F32)
        r = inv_rms(h)
        hr = h * r
        q = qs[...]
        dst[...] = (e.astype(F32) + r * (q - hr * jnp.mean(q * hr, axis=-1, keepdims=True))).astype(BF)

    def piece(j, i):
        z = i + p * (j - i)
        y = j + p * (i - j)
        return z, y

    EARLY, LATE = range(FAR), range(FAR, NA)

    def grad_first(v, slots):
        for i in QUARTERS if OWN in slots else ():
            z, y = piece(ja, i)
            cols = pl.ds(pl.multiple_of((z * NA + y) * pf, pf), pf)
            gs[v, :, pl.ds(i * pf, pf)] = wg[v, :, :, :, :, cols].reshape(dm, pf)
            is_[v, :, pl.ds(i * pf, pf)] = wi[v, :, :, :, :, cols].reshape(dm, pf)
        for s in slots:
            h = hb[v, s].astype(F32)
            n = (h * inv_rms(h)).astype(BF)
            ng[v, s] = n
            u, t1, t2 = gates(n, gs[v], is_[v])
            us[v, s] = u
            f1s[v, s] = t1
            f2s[v, s] = t2

    def grad_hidden(v, slots):
        for i in QUARTERS if OWN in slots else ():
            z, y = piece(ja, i)
            os_[pl.ds(i * pf, pf), :] = wo[v, z, y].reshape(pf, dm)
        for s in slots:
            t = mm_nt(eb[v, s], os_[...])
            das[s] = (t * f1s[v, s]).astype(BF)
            dbs[s] = (t * f2s[v, s]).astype(BF)

    def split(width):
        return pl.ds(0, width - pf), pl.ds(width - pf, pf)

    def keep(refs, v, place, tile, cols, first):
        b, rest = place[0], place[1:]
        lead = () if v is None else (v,)
        for colour in COLOURS:
            part = tile[..., cols[colour].start:cols[colour].start + cols[colour].size]
            at = lead + ((b, slice(None)) if colour == 0 else (slice(None), b)) + rest
            refs[colour][at] = part if first else refs[colour][at] + part

    def rows_of(slots):
        return pl.ds(slots[0], len(slots)), len(slots) * rows

    def grad_out(v, slots):
        some, count = rows_of(slots)
        for i in HALVES:
            cols = pl.ds(i * 2 * pf, 2 * pf)
            g = mm_tn(us[v, some, :, cols].reshape(count, 2 * pf), eb[v, some].reshape(count, dm)).reshape(2, NA, fr, dm)
            for b in HALVES:
                keep(gout, v, (2 * i + b,), g[b], split(dm), OWN in slots)

    def grad_in(v, slots):
        some, count = rows_of(slots)
        for which, dref in enumerate((das, dbs)):
            for i in QUARTERS:
                cols = pl.ds(i * (dm // NA), dm // NA)
                g = mm_tn(ng[v, some, :, cols].reshape(count, dm // NA), dref[some].reshape(count, fs)).reshape(NA, NA, dr, fs)
                for y in QUARTERS:
                    keep([ref.at[v, which] for ref in gin], None, (i + p * (y - i), y + p * (i - y)), g[y], split(fs), OWN in slots)

    IN, OUT = 0, 1

    def view(which, st, v, colour, t, half):
        own = jb if colour == 0 else xc
        if which == IN:
            ref = gin[colour].at[v, half]
            return ref.at[t] if st == 0 else ref.at[own, t]
        ref = gout[colour].at[v]
        return ref.at[t, pl.ds(2 * half, 2)] if st == 0 else ref.at[own, t, pl.ds(half * (fr // 2), fr // 2)]

    RECV = (((rg[0], rg[1]), (rg[2], rg[3])), ((rg[4], rg[5]), (rg[6], rg[7])))
    MERGED, DIRECT = ((0, OPP, PLUS, 0), (1, OPP, MINUS, 1)), ((1, PLUS, PLUS, 2), (0, MINUS, MINUS, 3))
    RELAYED = ((0, PLUS, PLUS, 4), (1, MINUS, MINUS, 5))

    def axis_of(colour, st):
        return (jb, peer_b) if colour == st else (xc, functools.partial(peer, X))

    def scatter_send(v, which, st, copies, colours):
        for colour in colours:
            q, to = axis_of(colour, st)
            for half, c, delta, slot in copies:
                send(view(which, st, v, colour, rot(q, c), half), RECV[st][which][colour].at[v, slot],
                     rs_s.at[st, v, colour, which], rs_r.at[st, v, colour, which, slot], to(delta), p)

    def scatter_relay(v, which, st, colours):
        for colour in colours:
            q, _ = axis_of(colour, st)
            recv = RECV[st][which][colour]
            for half, c, _, slot in RELAYED:
                wait_recv(recv.at[v, slot - 4], rs_r.at[st, v, colour, which, slot - 4])
                ref = view(which, st, v, colour, rot(q, c), half)
                ref[...] = ref[...] + recv[v, slot - 4]
        scatter_send(v, which, st, RELAYED, colours)

    def scatter_sum(v, which, st, colours):
        for colour in colours:
            q, _ = axis_of(colour, st)
            recv = RECV[st][which][colour]
            for half in HALVES:
                direct, merged = 3 - half, 4 + half
                for slot in (direct, merged):
                    wait_recv(recv.at[v, slot], rs_r.at[st, v, colour, which, slot])
                ref = view(which, st, v, colour, q, half)
                ref[...] = ref[...] + recv[v, direct] + recv[v, merged]

    def scatter_turn(v, which, colours):
        scatter_sum(v, which, 0, colours)
        scatter_send(v, which, 1, MERGED + DIRECT, colours)

    def scatter_out(v):
        scatter_sum(v, OUT, 1, COLOURS)
        for colour in COLOURS:
            go[v, :, split(dm)[colour]] = gout[colour][(v, jb, xc) if colour == 0 else (v, xc, jb)]

    def scatter_last(v):
        scatter_sum(v, IN, 1, COLOURS)
        for which in HALVES:
            for colour in COLOURS:
                fin[v, :, which, :, split(fs)[colour]] = gin[colour][(v, which, jb, xc) if colour == 0 else (v, which, xc, jb)]
        for delta in (OPP, PLUS, MINUS):
            send(fin.at[v, rot(ja, delta)], r3.at[v, delta - 1], r3_s.at[v], r3_r.at[v, delta - 1], peer_a(delta), p)

    def scatter_finish(v):
        def put(j, vals):
            for i in QUARTERS:
                z, y = piece(j, i)
                cols = pl.ds(pl.multiple_of((z * NA + y) * pf, pf), pf)
                gg[v, :, cols] = vals(0)[:, i * pf:(i + 1) * pf]
                gi[v, :, cols] = vals(1)[:, i * pf:(i + 1) * pf]

        put(ja, lambda w: fin[v, ja, w])
        for delta in RING:
            wait_recv(r3.at[v, delta - 1], r3_r.at[v, delta - 1])
            put(rot(ja, -delta), lambda w, delta=delta: r3[v, delta - 1, w])

    def step(fn, *args):
        with jax.named_scope(fn.__name__):
            fn(*args)

    def on(core):
        return pl.when(p == core)

    def take_turn():
        pl.semaphore_wait(turn, 1)

    def give_turn():
        pl.semaphore_signal(turn, inc=1, device_id=(d, 1 - p), device_id_type=MESH)

    h_mid, h_late, e_first, e_last = ((xo.at[i], mc_s.at[1 + i]) for i in QUARTERS)

    def pass_on(part, item, buf, which, vd):
        step(part, item[0], buf, which, vd, item[1])

    AFTER = (MINUS, OPP), (0, PLUS)
    step(direct_send, 0)
    step(small_send, 1, 0)

    @on(0)
    def _():
        step(spread_same, hb, 0, 0, mc_s.at[0])

    step(direct_wait, 0)
    step(small_send, 0, 1)
    step(small_relay, 1, 0)
    step(large_send, 0, (0,), (0,))
    step(small_rest, 1, 0)
    step(small_last, 1, 0)
    step(small_send, 1, 1)
    step(small_relay, 0, 1)
    step(small_relay, 1, 1)
    step(small_rest, 0, 1)
    step(large_send, 0, (PLUS, MINUS), (MINUS, PLUS))
    step(small_last, 0, 1)
    step(large_send, 0, (OPP,), (OPP,))
    step(small_rest, 1, 1)
    step(small_last, 1, 1)
    step(large_relay, 0)

    @on(0)
    def _():
        step(large_send, 1, UP, DOWN)

    step(large_finish, 0, UP_MATS)

    @on(0)
    def _():
        step(large_send, 1, *AFTER)

    @on(1)
    def _():
        step(take_turn)
        step(large_send, 1, UP, DOWN)
        step(spread_own, hb, 0, 0)

    step(block_gates, 0)

    @on(1)
    def _():
        step(large_send, 1, *AFTER)

    step(large_finish, 0, OUT_MAT)
    step(block_out, 0, h_mid[0])
    pass_on(spread_near, h_mid, hb, 0, p)
    step(large_relay, 1)

    @on(0)
    def _():
        step(give_turn)
        step(spread_relay, hb, 0, 0)

    step(spread_own, hb, 0, 1)
    step(large_finish, 1, UP_MATS)
    step(block_gates, 1)
    step(large_finish, 1, OUT_MAT)

    @on(0)
    def _():
        step(block_out, 1, h_late[0])
        pass_on(spread_near, h_late, hb, 0, 1)
        pass_on(spread_far, h_late, hb, 0, 1)
        step(spread_finish, hb, 0, 0)
        step(grad_first, 0, EARLY)
        step(grad_first, 0, LATE)
        step(spread_own, eb, 1, 1)
        pass_on(spread_far, h_mid, hb, 0, p)
        step(block_backward, 1, e_first[0])
        pass_on(spread_near, e_first, eb, 1, 0)
        pass_on(spread_far, e_first, eb, 1, 0)
        step(spread_relay, hb, 0, 1)

    @on(1)
    def _():
        pass_on(spread_far, h_mid, hb, 0, p)
        step(spread_same, eb, 1, 1, mc_s.at[0])
        step(block_backward, 1, e_first[0])
        pass_on(spread_near, e_first, eb, 1, 1)
        pass_on(spread_far, e_first, eb, 1, 1)
        step(spread_relay, hb, 0, 1)

    step(grad_first, 1, EARLY)
    step(spread_relay, eb, 1, 1)

    step(grad_hidden, 1, EARLY)
    step(grad_out, 1, EARLY)

    @on(0)
    def _():
        step(grad_in, 1, EARLY)

    @on(1)
    def _():
        step(spread_own, eb, 1, 0)
        step(block_backward, 0, e_last[0])
        pass_on(spread_near, e_last, eb, 1, 0)
        pass_on(spread_far, e_last, eb, 1, 0)
        step(grad_in, 1, EARLY)

    step(spread_finish, hb, 0, 1)
    step(grad_first, 1, LATE)

    step(spread_finish, eb, 1, 1)
    step(grad_hidden, 1, LATE)
    step(grad_out, 1, LATE)
    B_FIRST, X_FIRST = (0,), (1,)

    def scatter_start(v, which):
        scatter_send(v, which, 0, MERGED + DIRECT, X_FIRST)
        scatter_send(v, which, 0, MERGED, B_FIRST)

    step(scatter_start, 1, OUT)
    step(grad_in, 1, LATE)
    step(scatter_start, 1, IN)

    @on(0)
    def _():
        step(spread_relay, eb, 1, 0)
        step(spread_own, eb, 1, 0)
        step(block_backward, 0, ga)
        send(ga, ga, ga_s, ga_r, d, 1)

    @on(1)
    def _():
        step(spread_relay, hb, 0, 0)
        step(grad_first, 0, EARLY)

    step(scatter_send, 1, OUT, 0, DIRECT, B_FIRST)
    step(scatter_relay, 1, OUT, 0, X_FIRST)

    @on(1)
    def _():
        step(spread_relay, eb, 1, 0)
        step(spread_finish, hb, 0, 0)
        step(grad_first, 0, LATE)

    step(scatter_relay, 1, IN, 0, X_FIRST)
    step(grad_hidden, 0, EARLY)
    step(scatter_send, 1, IN, 0, DIRECT, B_FIRST)
    step(grad_in, 0, EARLY)
    step(scatter_turn, 1, OUT, X_FIRST)
    step(grad_out, 0, EARLY)
    step(scatter_turn, 1, IN, X_FIRST)
    step(scatter_relay, 1, OUT, 0, B_FIRST)
    step(spread_finish, eb, 1, 0)
    step(grad_hidden, 0, LATE)
    step(grad_in, 0, LATE)
    step(scatter_start, 0, IN)
    step(grad_out, 0, LATE)
    step(scatter_relay, 1, IN, 0, B_FIRST)
    step(scatter_start, 0, OUT)
    step(scatter_send, 0, IN, 0, DIRECT, B_FIRST)
    step(scatter_turn, 1, OUT, B_FIRST)
    step(scatter_relay, 0, IN, 0, X_FIRST)
    step(scatter_relay, 0, OUT, 0, X_FIRST)
    step(scatter_relay, 0, IN, 0, B_FIRST)
    step(scatter_send, 0, OUT, 0, DIRECT, B_FIRST)
    step(scatter_turn, 0, IN, X_FIRST)
    step(scatter_turn, 0, OUT, X_FIRST)
    step(scatter_turn, 1, IN, B_FIRST)
    step(scatter_relay, 1, OUT, 1, COLOURS)
    step(scatter_relay, 0, OUT, 0, B_FIRST)

    @on(1)
    def _():
        wait_recv(ga, ga_r)

    gact[...] = ga[...]
    step(scatter_relay, 1, IN, 1, COLOURS)
    step(scatter_out, 1)
    step(scatter_turn, 0, IN, B_FIRST)
    step(scatter_relay, 0, IN, 1, X_FIRST)
    step(scatter_turn, 0, OUT, B_FIRST)
    step(scatter_last, 1)
    step(scatter_relay, 0, IN, 1, B_FIRST)
    step(scatter_relay, 0, OUT, 1, COLOURS)
    step(scatter_finish, 1)
    step(scatter_last, 0)
    step(scatter_out, 0)
    step(scatter_finish, 0)

    for v in BLOCKS:
        for k in MATS:
            three = pl.ds(0, len(RING))
            wait_send(part_at(v, k, three, 0, 0), ag_s.at[v, k, 0])
            wait_send(part_at(v, k, whole, three, 0), ag_s.at[v, k, 1])
            wait_send(part_at(v, k, whole, whole, three), ag_s.at[v, k, LARGE])
        for colour in COLOURS:
            for which in HALVES:
                for st in HALVES:
                    wait_send(RECV[st][which][colour].at[v], rs_s.at[st, v, colour, which])
        wait_send(r3.at[v], r3_s.at[v])
        wait_send(hb.at[v, 0], rl_s.at[0, v])
        wait_send(hb.at[v, 0], rl_s.at[1, v])
    wait_send(hb.at[0, pl.ds(0, 2)], mc_s.at[0])
    wait_send(hb.at[0, pl.ds(0, 3)], mc_s.at[1])
    wait_send(hb.at[0, pl.ds(0, 3)], mc_s.at[3])

    @pl.when(p == 0)
    def _():
        wait_send(hb.at[0, pl.ds(0, 3)], mc_s.at[2])
        wait_send(ga, ga_s)

    @pl.when(p == 1)
    def _():
        wait_send(hb.at[0, pl.ds(0, 3)], mc_s.at[4])


def hand_on(*refs):
    copies = [pltpu.make_async_copy(refs[i], refs[NA + i], refs[-1].at[i]) for i in QUARTERS]
    for copy in copies:
        copy.start()
    for copy in copies:
        copy.wait()


def solution(mesh):
    act_spec = P(None, "data", None, None)
    w_spec = P(None, "stage", "data", None)

    def body(act_in, cot_out, w_gate, w_in, w_out):
        shape = act_in.shape
        dm, fd = shape[3], w_gate.shape[3]
        rows = shape[0] * shape[1] * shape[2]
        dr, fr, fs = dm // NL, fd // NL, fd // NA
        pf = fs // NA
        vmem = pltpu.VMEM
        dma = pltpu.SemaphoreType.DMA
        n2, n3, na = NB, len(RING), NA
        ring = (na, na)
        scratch = [
            vmem((n2, na, *ring, dr, fd), BF), vmem((n2, na, *ring, dr, fd), BF), vmem((n2, na, *ring, fr, dm), BF),
            vmem((n2, na, rows, dm), BF), vmem((n2, na, rows, dm), BF), vmem((na, rows, dm), BF), vmem((rows, dm), BF),
            vmem((n2, na, rows, dm), BF),
            vmem((n2, rows, fd), F32), vmem((n2, rows, fd), F32),
            vmem((n2, na, rows, fs), F32), vmem((n2, na, rows, fs), F32),
            vmem((n2, na, rows, fs), BF),
            vmem((rows, fd), BF), vmem((rows, fd), BF), vmem((rows, fd), BF),
            vmem((na, rows, fs), BF), vmem((na, rows, fs), BF),
            vmem((rows, dm), F32),
            vmem((n2, dm, fs), BF), vmem((n2, dm, fs), BF), vmem((fs, dm), BF),
            *(vmem((n2, n2, *ring, na, dr, width), F32) for width in (fs - pf, pf)),
            *(vmem((n2, *ring, fr, width), F32) for width in (dm - pf, pf)),
            vmem((n2, na, n2, dr, fs), F32), vmem((n2, n3, n2, dr, fs), F32),
            dma((n2, na)), dma((n2, n3, n3)), dma((n2, n3, n2, 6)), dma((n2, n3, n3 * na)), dma((5,)), dma((n2, n2, 7)), dma((n2, n2)), dma, dma,
            dma((n2, n2, n2, n2)), dma((n2, n2, n2, n2, 6)), dma((n2,)), dma((n2, n3)), pltpu.SemaphoreType.REGULAR,
            *(vmem((n2, 6, *lead, width), F32)
              for lead_in, lead_out in (((*ring, dr), (n2, fr)), ((na, dr), (fr // n2,)))
              for lead, width in ((lead_in, fs - pf), (lead_in, pf), (lead_out, dm - pf), (lead_out, pf))),
        ]
        hbm = pl.BlockSpec(memory_space=pl.ANY)
        whole = pl.BlockSpec(memory_space=pltpu.VMEM)
        out = pl.pallas_call(
            kernel,
            out_shape=(
                vmem((rows, dm), BF), vmem((n2, dr, fd), F32), vmem((n2, dr, fd), F32), vmem((n2, fr, dm), F32),
            ),
            in_specs=[hbm] * 5,
            out_specs=(whole,) * NA,
            scratch_shapes=scratch,
            compiler_params=pltpu.CompilerParams(collective_id=0, has_side_effects=True, vmem_limit_bytes=66300000),
            name="train_step",
        )(act_in.reshape(rows, dm), cot_out.reshape(rows, dm), w_gate[:, 0], w_in[:, 0], w_out[:, 0])
        grad_act, grad_gate, grad_lin, grad_proj = pl.pallas_call(
            hand_on, out_shape=tuple(jax.ShapeDtypeStruct(a.shape, a.dtype) for a in out), in_specs=[whole] * NA, out_specs=(hbm,) * NA,
            scratch_shapes=[dma((NA,))], compiler_params=pltpu.CompilerParams(vmem_limit_bytes=2 ** 20), name="hand_on",
        )(*(pltpu.with_memory_space_constraint(a, vmem) for a in out))
        return grad_act.reshape(shape), grad_gate[:, None], grad_lin[:, None], grad_proj[:, None]

    return jax.shard_map(body, mesh=mesh, in_specs=(act_spec, act_spec, w_spec, w_spec, w_spec),
                         out_specs=(act_spec, w_spec, w_spec, w_spec), check_vma=False)
```

```python
import functools

import jax
import jax.numpy as jnp
from jax import lax
from jax.experimental import pallas as pl
from jax.experimental.pallas import tpu as pltpu
from jax.sharding import PartitionSpec as P

NORM_EPS = 1e-6
BF = jnp.bfloat16
F32 = jnp.float32
MESH = pl.DeviceIdType.MESH
X, Y, Z = 0, 1, 2
BLOCKS = COLOURS = HALVES = (0, 1)
NB, NA, NL = len(BLOCKS), 4, 64
RING = (1, 3, 2)
OPP = RING[-1]
PLUS, MINUS = RING[:-1]
QUARTERS = range(NA)
OWN = 0
AXES = ((Z, X, Y), (Y, Z, X), (X, Y, Z))
UP_MATS, OUT_MAT = (0, 1), (2,)
MATS = UP_MATS + OUT_MAT


def mm(left, right):
    return jnp.dot(left, right, preferred_element_type=F32)


def mm_nt(left, right):
    return lax.dot_general(left, right, (((1,), (1,)), ((), ())), preferred_element_type=F32)


def mm_tn(left, right):
    return lax.dot_general(left, right, (((0,), (0,)), ((), ())), preferred_element_type=F32)


def inv_rms(h):
    return lax.rsqrt(jnp.mean(h * h, axis=-1, keepdims=True) + NORM_EPS)


def kernel(act, cot, wg_in, wi_in, wo_in, gact, gg, gi, go,
           wg, wi, wo, hb, eb, xo, ga, ng, f1, f2, f1s, f2s, us, ub, da, db, das, dbs, qs, gs, is_, os_,
           gin0, gin1, gout0, gout1, fin, r3,
           lsem, ag_s, ag_r, lg_r, mc_s, mc_r, rl_s, ga_s, ga_r, rs_s, rs_r, r3_s, r3_r, turn, *rg):
    dm, fd = wo.shape[-1], wg.shape[-1]
    dr, fr = dm // NL, fd // NL
    fs = fd // NA
    pf = fs // NA
    rows = act.shape[0]
    wts = (wg, wi, wo)
    gin, gout = (gin0, gin1), (gout0, gout1)

    p = lax.axis_index("stage")
    d = lax.axis_index("data")
    zc, yc, xc = lax.div(d, 16), lax.rem(lax.div(d, 4), 4), lax.rem(d, 4)
    coord = (xc, yc, zc)
    stride = (1, 4, 16)
    ja = yc + p * (zc - yc)
    jb = zc + p * (yc - zc)
    sa, sb = 4 + 12 * p, 16 - 12 * p

    def rot(c, delta):
        return lax.rem(c + (delta % 4), 4)

    def peer(ax, delta):
        return d + (rot(coord[ax], delta) - coord[ax]) * stride[ax]

    def peer_a(delta):
        return d + (rot(ja, delta) - ja) * sa

    def peer_b(delta):
        return d + (rot(jb, delta) - jb) * sb

    def remote(src, dst, ssem, rsem, dev, core):
        return pltpu.make_async_remote_copy(src_ref=src, dst_ref=dst, send_sem=ssem, recv_sem=rsem,
                                            device_id=(dev, core), device_id_type=MESH)

    def send(src, dst, ssem, rsem, dev, core):
        remote(src, dst, ssem, rsem, dev, core).start()

    def wait_recv(ref, sem):
        remote(ref, ref, sem, sem, d, p).wait_recv()

    def wait_send(ref, sem):
        remote(ref, ref, sem, sem, d, p).wait_send()

    for v in BLOCKS:
        for k, shard in enumerate((wg_in, wi_in, wo_in)):
            pltpu.make_async_copy(shard.at[v], wts[k].at[v, zc, yc, xc], lsem.at[v, k]).start()

    @pl.when(p == 0)
    def _():
        pltpu.make_async_copy(act, hb.at[0, OWN], lsem.at[0, 3]).start()

    @pl.when(p == 1)
    def _():
        pltpu.make_async_copy(cot, eb.at[1, OWN], lsem.at[0, 3]).start()

    barrier = pltpu.get_barrier_semaphore()
    senders = [(peer(ax, delta), p) for ax in (X, Y, Z) for delta in RING]
    senders += [(d, 1 - p), (peer_a(1), 1 - p), (peer_a(-1), 1 - p)]
    for dev, core in senders:
        pl.semaphore_signal(barrier, inc=1, device_id=(dev, core), device_id_type=MESH)
    for v in BLOCKS:
        for k, shard in enumerate((wg_in, wi_in, wo_in)):
            pltpu.make_async_copy(shard.at[v], wts[k].at[v, zc, yc, xc], lsem.at[v, k]).wait()

    @pl.when(p == 0)
    def _():
        pltpu.make_async_copy(act, hb.at[0, OWN], lsem.at[0, 3]).wait()

    @pl.when(p == 1)
    def _():
        pltpu.make_async_copy(cot, eb.at[1, OWN], lsem.at[0, 3]).wait()

    pl.semaphore_wait(barrier, len(senders))

    FIRST, REST = ((0, PLUS, 0), (1, MINUS, 2)), ((1, PLUS, 1), (0, MINUS, 3))
    LARGE = 2
    whole = slice(None)

    def part_at(v, k, small, middle, large, half=None):
        place = dict(zip(AXES[k], (small, middle, large)))
        width = wts[k].shape[-1] // 2
        cols = whole if half is None else pl.ds(half * width, width)
        return wts[k].at[v, place[Z], place[Y], place[X], :, cols]

    def own(k):
        return [coord[ax] for ax in AXES[k]]

    def chunk(v, k, ph, q, half):
        small, middle, large = own(k)
        return part_at(v, k, q, middle, large, half) if ph == 0 else part_at(v, k, pl.ds(2 * half, 2), q, large)

    def small_copy(v, k, ph, q, half, delta, slot):
        ref = chunk(v, k, ph, q, half)
        send(ref, ref, ag_s.at[v, k, ph], ag_r.at[v, k, ph, slot], peer(AXES[k][ph], delta), p)

    def small_wait(v, k, ph, back, half, slot):
        wait_recv(chunk(v, k, ph, rot(coord[AXES[k][ph]], back), half), ag_r.at[v, k, ph, slot])

    def small_send(v, ph):
        for half, delta, slot in FIRST + REST:
            for k in MATS:
                small_copy(v, k, ph, coord[AXES[k][ph]], half, delta, slot)

    def small_relay(v, ph):
        for half, delta, slot in FIRST:
            for k in MATS:
                small_wait(v, k, ph, -delta, half, slot)
                small_copy(v, k, ph, rot(coord[AXES[k][ph]], -delta), half, delta, 4 + half)

    def small_rest(v, ph):
        for half, delta, slot in REST:
            for k in MATS:
                small_wait(v, k, ph, -delta, half, slot)

    def small_last(v, ph):
        for half in HALVES:
            for k in MATS:
                small_wait(v, k, ph, OPP, half, 4 + half)

    def direct_send(v):
        for delta in (OPP, PLUS, MINUS):
            for k in MATS:
                ref = part_at(v, k, *own(k))
                send(ref, ref, ag_s.at[v, k, 0], ag_r.at[v, k, 0, delta], peer(AXES[k][0], delta), p)

    def direct_wait(v):
        for delta in RING:
            for k in MATS:
                small, middle, large = own(k)
                wait_recv(part_at(v, k, rot(small, -delta), middle, large), ag_r.at[v, k, 0, delta])

    UP, DOWN = (0, PLUS), (MINUS, OPP)
    RELAYS = ((UP[0], PLUS), (DOWN[0], MINUS), (UP[1], PLUS), (DOWN[1], MINUS))

    def row(v, k, q, r):
        return part_at(v, k, whole, rot(coord[AXES[k][1]], r), q)

    def large_slot(r, delta):
        return r if delta == PLUS else NA + r

    def large_send(v, up, down):
        for pair in zip(up, down):
            for r, delta in zip(pair, (PLUS, MINUS)):
                for k in MATS:
                    ax = AXES[k][LARGE]
                    ref = row(v, k, coord[ax], r)
                    send(ref, ref, ag_s.at[v, k, LARGE], lg_r.at[v, k, large_slot(r, delta)], peer(ax, delta), p)

    def large_relay(v):
        for r, delta in RELAYS:
            for k in MATS:
                ax = AXES[k][LARGE]
                ref = row(v, k, rot(coord[ax], -delta), r)
                wait_recv(ref, lg_r.at[v, k, large_slot(r, delta)])
                send(ref, ref, ag_s.at[v, k, LARGE], lg_r.at[v, k, 2 * NA + r], peer(ax, delta), p)

    def large_finish(v, mats):
        for pieces, delta in ((DOWN, PLUS), (UP, MINUS)):
            for r in pieces:
                for k in mats:
                    wait_recv(row(v, k, rot(coord[AXES[k][LARGE]], -delta), r), lg_r.at[v, k, large_slot(r, delta)])
        for r in QUARTERS:
            for k in mats:
                wait_recv(row(v, k, rot(coord[AXES[k][LARGE]], OPP), r), lg_r.at[v, k, 2 * NA + r])

    half_rows = rows // 2
    BACK, AHEAD, FAR = 1, 2, 3

    def spread_near(src, buf, which, vd, ssem):
        send(src, buf.at[vd, OWN], ssem, mc_r.at[which, vd, OWN], d, 1 - p)

    def rows_half(half):
        return pl.ds(half * half_rows, half_rows)

    HALF_ORDER = [(half if first else 1 - half, slot, delta, slot if first else FAR + 1 + slot)
                  for first in (True, False) for half, slot, delta in ((0, BACK, PLUS), (1, AHEAD, MINUS))]

    def spread_far(src, buf, which, vd, ssem):
        for half, slot, delta, sem in HALF_ORDER:
            send(src.at[rows_half(half)], buf.at[vd, slot, rows_half(half)], ssem, mc_r.at[which, vd, sem], peer_b(delta), 1 - p)

    def spread_same(buf, which, v, ssem):
        for half, slot, delta, sem in HALF_ORDER:
            send(buf.at[v, OWN, rows_half(half)], buf.at[v, slot, rows_half(half)], ssem, mc_r.at[which, v, sem], peer_a(delta), p)

    def spread_relay(buf, which, v):
        for half, slot, delta, sem in HALF_ORDER:
            ref = buf.at[v, slot, rows_half(half)]
            wait_recv(ref, mc_r.at[which, v, sem])
            if sem == slot:
                send(ref, buf.at[v, FAR, rows_half(half)], rl_s.at[which, v], mc_r.at[which, v, FAR + half], peer_a(delta), p)

    def spread_finish(buf, which, v):
        for half in HALVES:
            wait_recv(buf.at[v, FAR, rows_half(half)], mc_r.at[which, v, FAR + half])

    def spread_own(buf, which, v):
        wait_recv(buf.at[v, OWN], mc_r.at[which, v, OWN])

    def gates(n, wgt, wlin):
        a, b = mm(n, wgt), mm(n, wlin)
        s = jax.nn.sigmoid(a)
        act_a = a * s
        return (act_a * b).astype(BF), b * s * (1.0 + a * (1.0 - s)), act_a

    def block_gates(v):
        h = hb[v, OWN].astype(F32)
        n = (h * inv_rms(h)).astype(BF)

        def tile(i, carry):
            wide = fs // 2
            cols = pl.ds(pl.multiple_of(i * wide, wide), wide)
            u, t1, t2 = gates(n, wg[v, :, :, :, :, cols].reshape(dm, wide), wi[v, :, :, :, :, cols].reshape(dm, wide))
            ub[:, cols] = u
            f1[v, :, cols] = t1
            f2[v, :, cols] = t2
            return carry

        lax.fori_loop(0, 2 * NA, tile, 0, unroll=True)

    def block_out(v, dst):
        half_dm = dm // 2
        for i in HALVES:
            cols = pl.ds(i * half_dm, half_dm)
            out = mm(ub[...], wo[v, :, :, :, :, cols].reshape(fd, half_dm))
            dst[:, cols] = (hb[v, OWN, :, cols].astype(F32) + out).astype(BF)

    def block_backward(v, dst):
        e = eb[v, OWN]

        def tile(i, carry):
            cols = pl.ds(pl.multiple_of(i * fs, fs), fs)
            t = mm_nt(e, wo[v, i].reshape(fs, dm))
            da[:, cols] = (t * f1[v, :, cols]).astype(BF)
            db[:, cols] = (t * f2[v, :, cols]).astype(BF)
            return carry

        lax.fori_loop(0, NA, tile, 0, unroll=True)
        half_dm = dm // 2
        for i in HALVES:
            q = mm_nt(da[...], wg[v, pl.ds(2 * i, 2)].reshape(half_dm, fd))
            q += mm_nt(db[...], wi[v, pl.ds(2 * i, 2)].reshape(half_dm, fd))
            qs[:, pl.ds(i * half_dm, half_dm)] = q
        h = hb[v, OWN].astype(F32)
        r = inv_rms(h)
        hr = h * r
        q = qs[...]
        dst[...] = (e.astype(F32) + r * (q - hr * jnp.mean(q * hr, axis=-1, keepdims=True))).astype(BF)

    def piece(j, i):
        z = i + p * (j - i)
        y = j + p * (i - j)
        return z, y

    EARLY, LATE = range(FAR), range(FAR, NA)

    def grad_first(v, slots):
        for i in QUARTERS if OWN in slots else ():
            z, y = piece(ja, i)
            cols = pl.ds(pl.multiple_of((z * NA + y) * pf, pf), pf)
            gs[v, :, pl.ds(i * pf, pf)] = wg[v, :, :, :, :, cols].reshape(dm, pf)
            is_[v, :, pl.ds(i * pf, pf)] = wi[v, :, :, :, :, cols].reshape(dm, pf)
        for s in slots:
            h = hb[v, s].astype(F32)
            n = (h * inv_rms(h)).astype(BF)
            ng[v, s] = n
            u, t1, t2 = gates(n, gs[v], is_[v])
            us[v, s] = u
            f1s[v, s] = t1
            f2s[v, s] = t2

    def grad_hidden(v, slots):
        for i in QUARTERS if OWN in slots else ():
            z, y = piece(ja, i)
            os_[pl.ds(i * pf, pf), :] = wo[v, z, y].reshape(pf, dm)
        for s in slots:
            t = mm_nt(eb[v, s], os_[...])
            das[s] = (t * f1s[v, s]).astype(BF)
            dbs[s] = (t * f2s[v, s]).astype(BF)

    def split(width, second):
        return pl.ds(0, width - second), pl.ds(width - second, second)

    IN_COLS, OUT_COLS = split(fs, pf), split(dm, dm // 2)

    def keep(refs, v, place, tile, cols, first):
        b, rest = place[0], place[1:]
        lead = () if v is None else (v,)
        for colour in COLOURS:
            part = tile[..., cols[colour].start:cols[colour].start + cols[colour].size]
            at = lead + ((b, slice(None)) if colour == 0 else (slice(None), b)) + rest
            refs[colour][at] = part if first else refs[colour][at] + part

    def rows_of(slots):
        return pl.ds(slots[0], len(slots)), len(slots) * rows

    def grad_out(v, slots):
        some, count = rows_of(slots)
        for i in HALVES:
            cols = pl.ds(i * 2 * pf, 2 * pf)
            g = mm_tn(us[v, some, :, cols].reshape(count, 2 * pf), eb[v, some].reshape(count, dm)).reshape(2, NA, fr, dm)
            for b in HALVES:
                keep(gout, v, (2 * i + b,), g[b], OUT_COLS, OWN in slots)

    def grad_in(v, slots):
        some, count = rows_of(slots)
        for which, dref in enumerate((das, dbs)):
            for i in QUARTERS:
                cols = pl.ds(i * (dm // NA), dm // NA)
                g = mm_tn(ng[v, some, :, cols].reshape(count, dm // NA), dref[some].reshape(count, fs)).reshape(NA, NA, dr, fs)
                for y in QUARTERS:
                    keep([ref.at[v, which] for ref in gin], None, (i + p * (y - i), y + p * (i - y)), g[y], IN_COLS, OWN in slots)

    IN, OUT = 0, 1

    def view(which, st, v, colour, t, half):
        own = jb if colour == 0 else xc
        if which == IN:
            ref = gin[colour].at[v, half]
            return ref.at[t] if st == 0 else ref.at[own, t]
        ref = gout[colour].at[v]
        return ref.at[t, pl.ds(2 * half, 2)] if st == 0 else ref.at[own, t, pl.ds(half * (fr // 2), fr // 2)]

    RECV = (((rg[0], rg[1]), (rg[2], rg[3])), ((rg[4], rg[5]), (rg[6], rg[7])))
    MERGED, DIRECT = ((0, OPP, PLUS, 0), (1, OPP, MINUS, 1)), ((1, PLUS, PLUS, 2), (0, MINUS, MINUS, 3))
    RELAYED = ((0, PLUS, PLUS, 4), (1, MINUS, MINUS, 5))

    def axis_of(colour, st):
        return (jb, peer_b) if colour == st else (xc, functools.partial(peer, X))

    def scatter_send(v, which, st, copies):
        for colour in COLOURS:
            q, to = axis_of(colour, st)
            for half, c, delta, slot in copies:
                send(view(which, st, v, colour, rot(q, c), half), RECV[st][which][colour].at[v, slot],
                     rs_s.at[st, v, colour, which], rs_r.at[st, v, colour, which, slot], to(delta), p)

    def scatter_relay(v, which, st):
        for colour in COLOURS:
            q, _ = axis_of(colour, st)
            recv = RECV[st][which][colour]
            for half, c, _, slot in RELAYED:
                wait_recv(recv.at[v, slot - 4], rs_r.at[st, v, colour, which, slot - 4])
                ref = view(which, st, v, colour, rot(q, c), half)
                ref[...] = ref[...] + recv[v, slot - 4]
        scatter_send(v, which, st, RELAYED)

    def scatter_sum(v, which, st):
        for colour in COLOURS:
            q, _ = axis_of(colour, st)
            recv = RECV[st][which][colour]
            for half in HALVES:
                direct, merged = 3 - half, 4 + half
                for slot in (direct, merged):
                    wait_recv(recv.at[v, slot], rs_r.at[st, v, colour, which, slot])
                ref = view(which, st, v, colour, q, half)
                ref[...] = ref[...] + recv[v, direct] + recv[v, merged]

    def scatter_turn(v, which):
        scatter_sum(v, which, 0)
        scatter_send(v, which, 1, MERGED + DIRECT)

    def scatter_out(v):
        scatter_sum(v, OUT, 1)
        for colour in COLOURS:
            go[v, :, OUT_COLS[colour]] = gout[colour][(v, jb, xc) if colour == 0 else (v, xc, jb)]

    def scatter_last(v):
        scatter_sum(v, IN, 1)
        for which in HALVES:
            for colour in COLOURS:
                fin[v, :, which, :, IN_COLS[colour]] = gin[colour][(v, which, jb, xc) if colour == 0 else (v, which, xc, jb)]
        for delta in (OPP, PLUS, MINUS):
            send(fin.at[v, rot(ja, delta)], r3.at[v, delta - 1], r3_s.at[v], r3_r.at[v, delta - 1], peer_a(delta), p)

    def scatter_finish(v):
        def put(j, vals):
            for i in QUARTERS:
                z, y = piece(j, i)
                cols = pl.ds(pl.multiple_of((z * NA + y) * pf, pf), pf)
                gg[v, :, cols] = vals(0)[:, i * pf:(i + 1) * pf]
                gi[v, :, cols] = vals(1)[:, i * pf:(i + 1) * pf]

        put(ja, lambda w: fin[v, ja, w])
        for delta in RING:
            wait_recv(r3.at[v, delta - 1], r3_r.at[v, delta - 1])
            put(rot(ja, -delta), lambda w, delta=delta: r3[v, delta - 1, w])

    def step(fn, *args):
        with jax.named_scope(fn.__name__):
            fn(*args)

    def on(core):
        return pl.when(p == core)

    def take_turn():
        pl.semaphore_wait(turn, 1)

    def give_turn():
        pl.semaphore_signal(turn, inc=1, device_id=(d, 1 - p), device_id_type=MESH)

    h_mid, h_late, e_first, e_last = ((xo.at[i], mc_s.at[1 + i]) for i in QUARTERS)

    def pass_on(part, item, buf, which, vd):
        step(part, item[0], buf, which, vd, item[1])

    AFTER = (MINUS, OPP), (0, PLUS)
    step(direct_send, 0)
    step(small_send, 1, 0)

    @on(0)
    def _():
        step(spread_same, hb, 0, 0, mc_s.at[0])

    step(direct_wait, 0)
    step(small_send, 0, 1)
    step(small_relay, 1, 0)
    step(large_send, 0, (0,), (0,))
    step(small_rest, 1, 0)
    step(small_last, 1, 0)
    step(small_send, 1, 1)
    step(small_relay, 0, 1)
    step(small_relay, 1, 1)
    step(small_rest, 0, 1)
    step(large_send, 0, (PLUS, MINUS), (MINUS, PLUS))
    step(small_last, 0, 1)
    step(large_send, 0, (OPP,), (OPP,))
    step(small_rest, 1, 1)
    step(small_last, 1, 1)
    step(large_relay, 0)

    @on(0)
    def _():
        step(large_send, 1, UP, DOWN)

    step(large_finish, 0, UP_MATS)

    @on(0)
    def _():
        step(large_send, 1, *AFTER)

    @on(1)
    def _():
        step(take_turn)
        step(large_send, 1, UP, DOWN)
        step(spread_own, hb, 0, 0)

    step(block_gates, 0)

    @on(1)
    def _():
        step(large_send, 1, *AFTER)

    step(large_finish, 0, OUT_MAT)
    step(block_out, 0, h_mid[0])
    pass_on(spread_near, h_mid, hb, 0, p)
    step(large_relay, 1)

    @on(0)
    def _():
        step(give_turn)
        step(spread_relay, hb, 0, 0)

    step(spread_own, hb, 0, 1)
    step(large_finish, 1, UP_MATS)
    step(block_gates, 1)
    step(large_finish, 1, OUT_MAT)

    @on(0)
    def _():
        step(block_out, 1, h_late[0])
        pass_on(spread_near, h_late, hb, 0, 1)
        pass_on(spread_far, h_late, hb, 0, 1)
        step(spread_finish, hb, 0, 0)
        step(grad_first, 0, EARLY)
        step(grad_first, 0, LATE)
        step(spread_own, eb, 1, 1)
        pass_on(spread_far, h_mid, hb, 0, p)
        step(block_backward, 1, e_first[0])
        pass_on(spread_near, e_first, eb, 1, 0)
        pass_on(spread_far, e_first, eb, 1, 0)
        step(spread_relay, hb, 0, 1)

    @on(1)
    def _():
        pass_on(spread_far, h_mid, hb, 0, p)
        step(spread_same, eb, 1, 1, mc_s.at[0])
        step(block_backward, 1, e_first[0])
        pass_on(spread_near, e_first, eb, 1, 1)
        pass_on(spread_far, e_first, eb, 1, 1)
        step(spread_relay, hb, 0, 1)

    step(grad_first, 1, EARLY)
    step(spread_relay, eb, 1, 1)

    step(grad_hidden, 1, EARLY)
    step(grad_out, 1, EARLY)

    @on(0)
    def _():
        step(grad_in, 1, EARLY)

    @on(1)
    def _():
        step(spread_own, eb, 1, 0)
        step(block_backward, 0, e_last[0])
        pass_on(spread_near, e_last, eb, 1, 0)
        pass_on(spread_far, e_last, eb, 1, 0)
        step(spread_relay, hb, 0, 0)
        step(grad_in, 1, EARLY)

    step(spread_finish, hb, 0, 1)
    step(grad_first, 1, LATE)

    step(spread_finish, eb, 1, 1)
    step(grad_hidden, 1, LATE)
    step(grad_out, 1, LATE)
    step(scatter_send, 1, OUT, 0, MERGED)
    step(grad_in, 1, LATE)
    step(scatter_send, 1, IN, 0, MERGED)
    step(scatter_send, 1, OUT, 0, DIRECT)
    step(scatter_send, 1, IN, 0, DIRECT)

    @on(0)
    def _():
        step(spread_relay, eb, 1, 0)
        step(spread_own, eb, 1, 0)

    @on(1)
    def _():
        step(grad_first, 0, EARLY)
        step(spread_relay, eb, 1, 0)
        step(spread_finish, hb, 0, 0)
        step(grad_first, 0, LATE)

    step(grad_hidden, 0, EARLY)
    step(grad_in, 0, EARLY)
    step(grad_out, 0, EARLY)
    step(scatter_relay, 1, OUT, 0)
    step(spread_finish, eb, 1, 0)
    step(grad_hidden, 0, LATE)
    step(grad_in, 0, LATE)
    step(scatter_send, 0, IN, 0, MERGED)
    step(grad_out, 0, LATE)
    step(scatter_relay, 1, IN, 0)
    step(scatter_send, 0, OUT, 0, MERGED)
    step(scatter_send, 0, IN, 0, DIRECT)

    @on(0)
    def _():
        step(block_backward, 0, ga)
        send(ga, ga, ga_s, ga_r, d, 1)

    step(scatter_turn, 1, OUT)
    step(scatter_relay, 0, IN, 0)
    step(scatter_send, 0, OUT, 0, DIRECT)
    step(scatter_turn, 1, IN)
    step(scatter_relay, 0, OUT, 0)
    step(scatter_relay, 1, OUT, 1)

    @on(1)
    def _():
        wait_recv(ga, ga_r)

    gact[...] = ga[...]
    step(scatter_turn, 0, IN)
    step(scatter_relay, 1, IN, 1)
    step(scatter_turn, 0, OUT)
    step(scatter_relay, 0, IN, 1)
    step(scatter_out, 1)
    step(scatter_last, 1)
    step(scatter_relay, 0, OUT, 1)
    step(scatter_last, 0)
    step(scatter_finish, 1)
    step(scatter_out, 0)
    step(scatter_finish, 0)

    for v in BLOCKS:
        for k in MATS:
            three = pl.ds(0, len(RING))
            wait_send(part_at(v, k, three, 0, 0), ag_s.at[v, k, 0])
            wait_send(part_at(v, k, whole, three, 0), ag_s.at[v, k, 1])
            wait_send(part_at(v, k, whole, whole, three), ag_s.at[v, k, LARGE])
        for colour in COLOURS:
            for which in HALVES:
                for st in HALVES:
                    wait_send(RECV[st][which][colour].at[v], rs_s.at[st, v, colour, which])
        wait_send(r3.at[v], r3_s.at[v])
        wait_send(hb.at[v, 0], rl_s.at[0, v])
        wait_send(hb.at[v, 0], rl_s.at[1, v])
    wait_send(hb.at[0, pl.ds(0, 2)], mc_s.at[0])
    wait_send(hb.at[0, pl.ds(0, 3)], mc_s.at[1])
    wait_send(hb.at[0, pl.ds(0, 3)], mc_s.at[3])

    @pl.when(p == 0)
    def _():
        wait_send(hb.at[0, pl.ds(0, 3)], mc_s.at[2])
        wait_send(ga, ga_s)

    @pl.when(p == 1)
    def _():
        wait_send(hb.at[0, pl.ds(0, 3)], mc_s.at[4])


def hand_on(*refs):
    copies = [pltpu.make_async_copy(refs[i], refs[NA + i], refs[-1].at[i]) for i in QUARTERS]
    for copy in copies:
        copy.start()
    for copy in copies:
        copy.wait()


def solution(mesh):
    act_spec = P(None, "data", None, None)
    w_spec = P(None, "stage", "data", None)

    def body(act_in, cot_out, w_gate, w_in, w_out):
        shape = act_in.shape
        dm, fd = shape[3], w_gate.shape[3]
        rows = shape[0] * shape[1] * shape[2]
        dr, fr, fs = dm // NL, fd // NL, fd // NA
        pf = fs // NA
        vmem = pltpu.VMEM
        dma = pltpu.SemaphoreType.DMA
        n2, n3, na = NB, len(RING), NA
        ring = (na, na)
        scratch = [
            vmem((n2, na, *ring, dr, fd), BF), vmem((n2, na, *ring, dr, fd), BF), vmem((n2, na, *ring, fr, dm), BF),
            vmem((n2, na, rows, dm), BF), vmem((n2, na, rows, dm), BF), vmem((na, rows, dm), BF), vmem((rows, dm), BF),
            vmem((n2, na, rows, dm), BF),
            vmem((n2, rows, fd), F32), vmem((n2, rows, fd), F32),
            vmem((n2, na, rows, fs), F32), vmem((n2, na, rows, fs), F32),
            vmem((n2, na, rows, fs), BF),
            vmem((rows, fd), BF), vmem((rows, fd), BF), vmem((rows, fd), BF),
            vmem((na, rows, fs), BF), vmem((na, rows, fs), BF),
            vmem((rows, dm), F32),
            vmem((n2, dm, fs), BF), vmem((n2, dm, fs), BF), vmem((fs, dm), BF),
            *(vmem((n2, n2, *ring, na, dr, width), F32) for width in (fs - pf, pf)),
            *(vmem((n2, *ring, fr, width), F32) for width in (dm // n2, dm // n2)),
            vmem((n2, na, n2, dr, fs), F32), vmem((n2, n3, n2, dr, fs), F32),
            dma((n2, na)), dma((n2, n3, n3)), dma((n2, n3, n2, 6)), dma((n2, n3, n3 * na)), dma((5,)), dma((n2, n2, 7)), dma((n2, n2)), dma, dma,
            dma((n2, n2, n2, n2)), dma((n2, n2, n2, n2, 6)), dma((n2,)), dma((n2, n3)), pltpu.SemaphoreType.REGULAR,
            *(vmem((n2, 6, *lead, width), F32)
              for lead_in, lead_out in (((*ring, dr), (n2, fr)), ((na, dr), (fr // n2,)))
              for lead, width in ((lead_in, fs - pf), (lead_in, pf), (lead_out, dm // n2), (lead_out, dm // n2))),
        ]
        hbm = pl.BlockSpec(memory_space=pl.ANY)
        whole = pl.BlockSpec(memory_space=pltpu.VMEM)
        out = pl.pallas_call(
            kernel,
            out_shape=(
                vmem((rows, dm), BF), vmem((n2, dr, fd), F32), vmem((n2, dr, fd), F32), vmem((n2, fr, dm), F32),
            ),
            in_specs=[hbm] * 5,
            out_specs=(whole,) * NA,
            scratch_shapes=scratch,
            compiler_params=pltpu.CompilerParams(collective_id=0, has_side_effects=True, vmem_limit_bytes=66300000),
            name="train_step",
        )(act_in.reshape(rows, dm), cot_out.reshape(rows, dm), w_gate[:, 0], w_in[:, 0], w_out[:, 0])
        grad_act, grad_gate, grad_lin, grad_proj = pl.pallas_call(
            hand_on, out_shape=tuple(jax.ShapeDtypeStruct(a.shape, a.dtype) for a in out), in_specs=[whole] * NA, out_specs=(hbm,) * NA,
            scratch_shapes=[dma((NA,))], compiler_params=pltpu.CompilerParams(vmem_limit_bytes=2 ** 20), name="hand_on",
        )(*(pltpu.with_memory_space_constraint(a, vmem) for a in out))
        return grad_act.reshape(shape), grad_gate[:, None], grad_lin[:, None], grad_proj[:, None]

    return jax.shard_map(body, mesh=mesh, in_specs=(act_spec, act_spec, w_spec, w_spec, w_spec),
                         out_specs=(act_spec, w_spec, w_spec, w_spec), check_vma=False)
```

```python
import functools

import jax
import jax.numpy as jnp
from jax import lax
from jax.experimental import pallas as pl
from jax.experimental.pallas import tpu as pltpu
from jax.sharding import PartitionSpec as P

NORM_EPS = 1e-6
BF = jnp.bfloat16
F32 = jnp.float32
MESH = pl.DeviceIdType.MESH
X, Y, Z = 0, 1, 2
BLOCKS = COLOURS = HALVES = (0, 1)
NB, NA, NL = len(BLOCKS), 4, 64
RING = (1, 3, 2)
OPP = RING[-1]
PLUS, MINUS = RING[:-1]
QUARTERS = range(NA)
OWN = 0
AXES = ((Z, X, Y), (Y, Z, X), (X, Y, Z))
UP_MATS, OUT_MAT = (0, 1), (2,)
MATS = UP_MATS + OUT_MAT


def mm(left, right):
    return jnp.dot(left, right, preferred_element_type=F32)


def mm_nt(left, right):
    return lax.dot_general(left, right, (((1,), (1,)), ((), ())), preferred_element_type=F32)


def mm_tn(left, right):
    return lax.dot_general(left, right, (((0,), (0,)), ((), ())), preferred_element_type=F32)


def inv_rms(h):
    return lax.rsqrt(jnp.mean(h * h, axis=-1, keepdims=True) + NORM_EPS)


def kernel(act, cot, wg_in, wi_in, wo_in, gact, gg, gi, go,
           wg, wi, wo, hb, eb, xo, ga, ng, f1, f2, f1s, f2s, us, ub, da, db, das, dbs, qs, gs, is_, os_,
           gout0, gout1, fin, r3,
           lsem, ag_s, ag_r, lg_r, mc_s, mc_r, rl_s, ga_s, ga_r, rs_s, rs_r, r3_s, r3_r, turn, *more):
    dm, fd = wo.shape[-1], wg.shape[-1]
    dr, fr = dm // NL, fd // NL
    fs = fd // NA
    pf = fs // NA
    rows = act.shape[0]
    wts = (wg, wi, wo)
    gins, rg = more[:4], more[4:]
    gin, gout = (gins[:2], gins[2:]), (gout0, gout1)

    p = lax.axis_index("stage")
    d = lax.axis_index("data")
    zc, yc, xc = lax.div(d, 16), lax.rem(lax.div(d, 4), 4), lax.rem(d, 4)
    coord = (xc, yc, zc)
    stride = (1, 4, 16)
    ja = yc + p * (zc - yc)
    jb = zc + p * (yc - zc)
    sa, sb = 4 + 12 * p, 16 - 12 * p

    def rot(c, delta):
        return lax.rem(c + (delta % 4), 4)

    def peer(ax, delta):
        return d + (rot(coord[ax], delta) - coord[ax]) * stride[ax]

    def peer_a(delta):
        return d + (rot(ja, delta) - ja) * sa

    def peer_b(delta):
        return d + (rot(jb, delta) - jb) * sb

    def remote(src, dst, ssem, rsem, dev, core):
        return pltpu.make_async_remote_copy(src_ref=src, dst_ref=dst, send_sem=ssem, recv_sem=rsem,
                                            device_id=(dev, core), device_id_type=MESH)

    def send(src, dst, ssem, rsem, dev, core):
        remote(src, dst, ssem, rsem, dev, core).start()

    def wait_recv(ref, sem):
        remote(ref, ref, sem, sem, d, p).wait_recv()

    def wait_send(ref, sem):
        remote(ref, ref, sem, sem, d, p).wait_send()

    for v in BLOCKS:
        for k, shard in enumerate((wg_in, wi_in, wo_in)):
            pltpu.make_async_copy(shard.at[v], wts[k].at[v, zc, yc, xc], lsem.at[v, k]).start()

    @pl.when(p == 0)
    def _():
        pltpu.make_async_copy(act, hb.at[0, OWN], lsem.at[0, 3]).start()

    @pl.when(p == 1)
    def _():
        pltpu.make_async_copy(cot, eb.at[1, OWN], lsem.at[0, 3]).start()

    barrier = pltpu.get_barrier_semaphore()
    senders = [(peer(ax, delta), p) for ax in (X, Y, Z) for delta in RING]
    senders += [(d, 1 - p), (peer_a(1), 1 - p), (peer_a(-1), 1 - p)]
    for dev, core in senders:
        pl.semaphore_signal(barrier, inc=1, device_id=(dev, core), device_id_type=MESH)
    for v in BLOCKS:
        for k, shard in enumerate((wg_in, wi_in, wo_in)):
            pltpu.make_async_copy(shard.at[v], wts[k].at[v, zc, yc, xc], lsem.at[v, k]).wait()

    @pl.when(p == 0)
    def _():
        pltpu.make_async_copy(act, hb.at[0, OWN], lsem.at[0, 3]).wait()

    @pl.when(p == 1)
    def _():
        pltpu.make_async_copy(cot, eb.at[1, OWN], lsem.at[0, 3]).wait()

    pl.semaphore_wait(barrier, len(senders))

    FIRST, REST = ((0, PLUS, 0), (1, MINUS, 2)), ((1, PLUS, 1), (0, MINUS, 3))
    LARGE = 2
    whole = slice(None)

    def part_at(v, k, small, middle, large, half=None):
        place = dict(zip(AXES[k], (small, middle, large)))
        width = wts[k].shape[-1] // 2
        cols = whole if half is None else pl.ds(half * width, width)
        return wts[k].at[v, place[Z], place[Y], place[X], :, cols]

    def own(k):
        return [coord[ax] for ax in AXES[k]]

    def chunk(v, k, ph, q, half):
        small, middle, large = own(k)
        return part_at(v, k, q, middle, large, half) if ph == 0 else part_at(v, k, pl.ds(2 * half, 2), q, large)

    def small_copy(v, k, ph, q, half, delta, slot):
        ref = chunk(v, k, ph, q, half)
        send(ref, ref, ag_s.at[v, k, ph], ag_r.at[v, k, ph, slot], peer(AXES[k][ph], delta), p)

    def small_wait(v, k, ph, back, half, slot):
        wait_recv(chunk(v, k, ph, rot(coord[AXES[k][ph]], back), half), ag_r.at[v, k, ph, slot])

    def small_send(v, ph):
        for half, delta, slot in FIRST + REST:
            for k in MATS:
                small_copy(v, k, ph, coord[AXES[k][ph]], half, delta, slot)

    def small_relay(v, ph):
        for half, delta, slot in FIRST:
            for k in MATS:
                small_wait(v, k, ph, -delta, half, slot)
                small_copy(v, k, ph, rot(coord[AXES[k][ph]], -delta), half, delta, 4 + half)

    def small_rest(v, ph):
        for half, delta, slot in REST:
            for k in MATS:
                small_wait(v, k, ph, -delta, half, slot)

    def small_last(v, ph):
        for half in HALVES:
            for k in MATS:
                small_wait(v, k, ph, OPP, half, 4 + half)

    def direct_send(v):
        for delta in (OPP, PLUS, MINUS):
            for k in MATS:
                ref = part_at(v, k, *own(k))
                send(ref, ref, ag_s.at[v, k, 0], ag_r.at[v, k, 0, delta], peer(AXES[k][0], delta), p)

    def direct_wait(v):
        for delta in RING:
            for k in MATS:
                small, middle, large = own(k)
                wait_recv(part_at(v, k, rot(small, -delta), middle, large), ag_r.at[v, k, 0, delta])

    UP, DOWN = (0, PLUS), (MINUS, OPP)
    RELAYS = ((UP[0], PLUS), (DOWN[0], MINUS), (UP[1], PLUS), (DOWN[1], MINUS))

    def row(v, k, q, r):
        return part_at(v, k, whole, rot(coord[AXES[k][1]], r), q)

    def large_slot(r, delta):
        return r if delta == PLUS else NA + r

    def large_send(v, up, down):
        for pair in zip(up, down):
            for r, delta in zip(pair, (PLUS, MINUS)):
                for k in MATS:
                    ax = AXES[k][LARGE]
                    ref = row(v, k, coord[ax], r)
                    send(ref, ref, ag_s.at[v, k, LARGE], lg_r.at[v, k, large_slot(r, delta)], peer(ax, delta), p)

    def large_relay(v):
        for r, delta in RELAYS:
            for k in MATS:
                ax = AXES[k][LARGE]
                ref = row(v, k, rot(coord[ax], -delta), r)
                wait_recv(ref, lg_r.at[v, k, large_slot(r, delta)])
                send(ref, ref, ag_s.at[v, k, LARGE], lg_r.at[v, k, 2 * NA + r], peer(ax, delta), p)

    def large_finish(v, mats):
        for pieces, delta in ((DOWN, PLUS), (UP, MINUS)):
            for r in pieces:
                for k in mats:
                    wait_recv(row(v, k, rot(coord[AXES[k][LARGE]], -delta), r), lg_r.at[v, k, large_slot(r, delta)])
        for r in QUARTERS:
            for k in mats:
                wait_recv(row(v, k, rot(coord[AXES[k][LARGE]], OPP), r), lg_r.at[v, k, 2 * NA + r])

    half_rows = rows // 2
    BACK, AHEAD, FAR = 1, 2, 3

    def spread_near(src, buf, which, vd, ssem):
        send(src, buf.at[vd, OWN], ssem, mc_r.at[which, vd, OWN], d, 1 - p)

    def rows_half(half):
        return pl.ds(half * half_rows, half_rows)

    HALF_ORDER = [(half if first else 1 - half, slot, delta, slot if first else FAR + 1 + slot)
                  for first in (True, False) for half, slot, delta in ((0, BACK, PLUS), (1, AHEAD, MINUS))]

    def spread_far(src, buf, which, vd, ssem):
        for half, slot, delta, sem in HALF_ORDER:
            send(src.at[rows_half(half)], buf.at[vd, slot, rows_half(half)], ssem, mc_r.at[which, vd, sem], peer_b(delta), 1 - p)

    def spread_same(buf, which, v, ssem):
        for half, slot, delta, sem in HALF_ORDER:
            send(buf.at[v, OWN, rows_half(half)], buf.at[v, slot, rows_half(half)], ssem, mc_r.at[which, v, sem], peer_a(delta), p)

    def spread_relay(buf, which, v):
        for half, slot, delta, sem in HALF_ORDER:
            ref = buf.at[v, slot, rows_half(half)]
            wait_recv(ref, mc_r.at[which, v, sem])
            if sem == slot:
                send(ref, buf.at[v, FAR, rows_half(half)], rl_s.at[which, v], mc_r.at[which, v, FAR + half], peer_a(delta), p)

    def spread_finish(buf, which, v):
        for half in HALVES:
            wait_recv(buf.at[v, FAR, rows_half(half)], mc_r.at[which, v, FAR + half])

    def spread_own(buf, which, v):
        wait_recv(buf.at[v, OWN], mc_r.at[which, v, OWN])

    def gates(n, wgt, wlin):
        a, b = mm(n, wgt), mm(n, wlin)
        s = jax.nn.sigmoid(a)
        act_a = a * s
        return (act_a * b).astype(BF), b * s * (1.0 + a * (1.0 - s)), act_a

    def block_gates(v):
        h = hb[v, OWN].astype(F32)
        n = (h * inv_rms(h)).astype(BF)

        def tile(i, carry):
            wide = fs // 2
            cols = pl.ds(pl.multiple_of(i * wide, wide), wide)
            u, t1, t2 = gates(n, wg[v, :, :, :, :, cols].reshape(dm, wide), wi[v, :, :, :, :, cols].reshape(dm, wide))
            ub[:, cols] = u
            f1[v, :, cols] = t1
            f2[v, :, cols] = t2
            return carry

        lax.fori_loop(0, 2 * NA, tile, 0, unroll=True)

    def block_out(v, dst):
        half_dm = dm // 2
        for i in HALVES:
            cols = pl.ds(i * half_dm, half_dm)
            out = mm(ub[...], wo[v, :, :, :, :, cols].reshape(fd, half_dm))
            dst[:, cols] = (hb[v, OWN, :, cols].astype(F32) + out).astype(BF)

    def block_backward(v, dst):
        e = eb[v, OWN]

        def tile(i, carry):
            cols = pl.ds(pl.multiple_of(i * fs, fs), fs)
            t = mm_nt(e, wo[v, i].reshape(fs, dm))
            da[:, cols] = (t * f1[v, :, cols]).astype(BF)
            db[:, cols] = (t * f2[v, :, cols]).astype(BF)
            return carry

        lax.fori_loop(0, NA, tile, 0, unroll=True)
        half_dm = dm // 2
        for i in HALVES:
            q = mm_nt(da[...], wg[v, pl.ds(2 * i, 2)].reshape(half_dm, fd))
            q += mm_nt(db[...], wi[v, pl.ds(2 * i, 2)].reshape(half_dm, fd))
            qs[:, pl.ds(i * half_dm, half_dm)] = q
        h = hb[v, OWN].astype(F32)
        r = inv_rms(h)
        hr = h * r
        q = qs[...]
        dst[...] = (e.astype(F32) + r * (q - hr * jnp.mean(q * hr, axis=-1, keepdims=True))).astype(BF)

    def piece(j, i):
        z = i + p * (j - i)
        y = j + p * (i - j)
        return z, y

    EARLY, LATE = range(FAR), range(FAR, NA)

    def grad_first(v, slots):
        for i in QUARTERS if OWN in slots else ():
            z, y = piece(ja, i)
            cols = pl.ds(pl.multiple_of((z * NA + y) * pf, pf), pf)
            gs[v, :, pl.ds(i * pf, pf)] = wg[v, :, :, :, :, cols].reshape(dm, pf)
            is_[v, :, pl.ds(i * pf, pf)] = wi[v, :, :, :, :, cols].reshape(dm, pf)
        for s in slots:
            h = hb[v, s].astype(F32)
            n = (h * inv_rms(h)).astype(BF)
            ng[v, s] = n
            u, t1, t2 = gates(n, gs[v], is_[v])
            us[v, s] = u
            f1s[v, s] = t1
            f2s[v, s] = t2

    def grad_hidden(v, slots):
        for i in QUARTERS if OWN in slots else ():
            z, y = piece(ja, i)
            os_[pl.ds(i * pf, pf), :] = wo[v, z, y].reshape(pf, dm)
        for s in slots:
            t = mm_nt(eb[v, s], os_[...])
            das[s] = (t * f1s[v, s]).astype(BF)
            dbs[s] = (t * f2s[v, s]).astype(BF)

    def split(width, second):
        return pl.ds(0, width - second), pl.ds(width - second, second)

    IN_COLS, OUT_COLS = (split(fs, fs // 2), split(fs, pf)), split(dm, dm // 2)

    def keep(refs, lead, place, tile, cols, first):
        b, rest = place[0], place[1:]
        for colour in COLOURS:
            part = tile[..., cols[colour].start:cols[colour].start + cols[colour].size]
            at = lead + ((b, slice(None)) if colour == 0 else (slice(None), b)) + rest
            refs[colour][at] = part if first else refs[colour][at] + part

    def rows_of(slots):
        return pl.ds(slots[0], len(slots)), len(slots) * rows

    def grad_out(v, slots):
        some, count = rows_of(slots)
        for i in HALVES:
            cols = pl.ds(i * 2 * pf, 2 * pf)
            g = mm_tn(us[v, some, :, cols].reshape(count, 2 * pf), eb[v, some].reshape(count, dm)).reshape(2, NA, fr, dm)
            for b in HALVES:
                keep(gout, (v,), (2 * i + b,), g[b], OUT_COLS, OWN in slots)

    def grad_in(v, slots):
        some, count = rows_of(slots)
        for which, dref in enumerate((das, dbs)):
            for i in QUARTERS:
                cols = pl.ds(i * (dm // NA), dm // NA)
                g = mm_tn(ng[v, some, :, cols].reshape(count, dm // NA), dref[some].reshape(count, fs)).reshape(NA, NA, dr, fs)
                for y in QUARTERS:
                    keep(gin[v], (which,), (i + p * (y - i), y + p * (i - y)), g[y], IN_COLS[v], OWN in slots)

    IN, OUT = 0, 1

    def view(which, st, v, colour, t, half):
        own = jb if colour == 0 else xc
        if which == IN:
            ref = gin[v][colour].at[half]
            return ref.at[t] if st == 0 else ref.at[own, t]
        ref = gout[colour].at[v]
        return ref.at[t, pl.ds(2 * half, 2)] if st == 0 else ref.at[own, t, pl.ds(half * (fr // 2), fr // 2)]

    def landing(v, st, which, colour):
        return rg[4 * v + 2 * st + colour] if which == IN else rg[8 + 2 * st + colour].at[v]

    MERGED, DIRECT = ((0, OPP, PLUS, 0), (1, OPP, MINUS, 1)), ((1, PLUS, PLUS, 2), (0, MINUS, MINUS, 3))
    RELAYED = ((0, PLUS, PLUS, 4), (1, MINUS, MINUS, 5))

    def axis_of(colour, st):
        return (jb, peer_b) if colour == st else (xc, functools.partial(peer, X))

    def scatter_send(v, which, st, copies):
        for colour in COLOURS:
            q, to = axis_of(colour, st)
            for half, c, delta, slot in copies:
                send(view(which, st, v, colour, rot(q, c), half), landing(v, st, which, colour).at[slot],
                     rs_s.at[st, v, colour, which], rs_r.at[st, v, colour, which, slot], to(delta), p)

    def scatter_relay(v, which, st):
        for colour in COLOURS:
            q, _ = axis_of(colour, st)
            recv = landing(v, st, which, colour)
            for half, c, _, slot in RELAYED:
                wait_recv(recv.at[slot - 4], rs_r.at[st, v, colour, which, slot - 4])
                ref = view(which, st, v, colour, rot(q, c), half)
                ref[...] = ref[...] + recv[slot - 4]
        scatter_send(v, which, st, RELAYED)

    def scatter_sum(v, which, st):
        for colour in COLOURS:
            q, _ = axis_of(colour, st)
            recv = landing(v, st, which, colour)
            for half in HALVES:
                direct, merged = 3 - half, 4 + half
                for slot in (direct, merged):
                    wait_recv(recv.at[slot], rs_r.at[st, v, colour, which, slot])
                ref = view(which, st, v, colour, q, half)
                ref[...] = ref[...] + recv[direct] + recv[merged]

    def scatter_turn(v, which):
        scatter_sum(v, which, 0)
        scatter_send(v, which, 1, MERGED + DIRECT)

    def scatter_out(v):
        scatter_sum(v, OUT, 1)
        for colour in COLOURS:
            go[v, :, OUT_COLS[colour]] = gout[colour][(v, jb, xc) if colour == 0 else (v, xc, jb)]

    def scatter_last(v):
        scatter_sum(v, IN, 1)
        for which in HALVES:
            for colour in COLOURS:
                fin[v, :, which, :, IN_COLS[v][colour]] = gin[v][colour][(which, jb, xc) if colour == 0 else (which, xc, jb)]
        for delta in (OPP, PLUS, MINUS):
            send(fin.at[v, rot(ja, delta)], r3.at[v, delta - 1], r3_s.at[v], r3_r.at[v, delta - 1], peer_a(delta), p)

    def scatter_finish(v):
        def put(j, vals):
            for i in QUARTERS:
                z, y = piece(j, i)
                cols = pl.ds(pl.multiple_of((z * NA + y) * pf, pf), pf)
                gg[v, :, cols] = vals(0)[:, i * pf:(i + 1) * pf]
                gi[v, :, cols] = vals(1)[:, i * pf:(i + 1) * pf]

        put(ja, lambda w: fin[v, ja, w])
        for delta in RING:
            wait_recv(r3.at[v, delta - 1], r3_r.at[v, delta - 1])
            put(rot(ja, -delta), lambda w, delta=delta: r3[v, delta - 1, w])

    def step(fn, *args):
        with jax.named_scope(fn.__name__):
            fn(*args)

    def on(core):
        return pl.when(p == core)

    def take_turn():
        pl.semaphore_wait(turn, 1)

    def give_turn():
        pl.semaphore_signal(turn, inc=1, device_id=(d, 1 - p), device_id_type=MESH)

    h_mid, h_late, e_first, e_last = ((xo.at[i], mc_s.at[1 + i]) for i in QUARTERS)

    def pass_on(part, item, buf, which, vd):
        step(part, item[0], buf, which, vd, item[1])

    AFTER = (MINUS, OPP), (0, PLUS)
    step(direct_send, 0)
    step(small_send, 1, 0)

    @on(0)
    def _():
        step(spread_same, hb, 0, 0, mc_s.at[0])

    step(direct_wait, 0)
    step(small_send, 0, 1)
    step(small_relay, 1, 0)
    step(large_send, 0, (0,), (0,))
    step(small_rest, 1, 0)
    step(small_last, 1, 0)
    step(small_send, 1, 1)
    step(small_relay, 0, 1)
    step(small_relay, 1, 1)
    step(small_rest, 0, 1)
    step(large_send, 0, (PLUS, MINUS), (MINUS, PLUS))
    step(small_last, 0, 1)
    step(large_send, 0, (OPP,), (OPP,))
    step(small_rest, 1, 1)
    step(small_last, 1, 1)
    step(large_relay, 0)

    @on(0)
    def _():
        step(large_send, 1, UP, DOWN)

    step(large_finish, 0, UP_MATS)

    @on(0)
    def _():
        step(large_send, 1, *AFTER)

    @on(1)
    def _():
        step(take_turn)
        step(large_send, 1, UP, DOWN)
        step(spread_own, hb, 0, 0)

    step(block_gates, 0)

    @on(1)
    def _():
        step(large_send, 1, *AFTER)

    step(large_finish, 0, OUT_MAT)
    step(block_out, 0, h_mid[0])
    pass_on(spread_near, h_mid, hb, 0, p)
    step(large_relay, 1)

    @on(0)
    def _():
        step(give_turn)
        step(spread_relay, hb, 0, 0)

    step(spread_own, hb, 0, 1)
    step(large_finish, 1, UP_MATS)
    step(block_gates, 1)
    step(large_finish, 1, OUT_MAT)

    @on(0)
    def _():
        step(block_out, 1, h_late[0])
        pass_on(spread_near, h_late, hb, 0, 1)
        pass_on(spread_far, h_late, hb, 0, 1)
        step(spread_finish, hb, 0, 0)
        step(grad_first, 0, EARLY)
        step(grad_first, 0, LATE)
        step(spread_own, eb, 1, 1)
        pass_on(spread_far, h_mid, hb, 0, p)
        step(block_backward, 1, e_first[0])
        pass_on(spread_near, e_first, eb, 1, 0)
        pass_on(spread_far, e_first, eb, 1, 0)
        step(spread_relay, hb, 0, 1)

    @on(1)
    def _():
        pass_on(spread_far, h_mid, hb, 0, p)
        step(spread_same, eb, 1, 1, mc_s.at[0])
        step(block_backward, 1, e_first[0])
        pass_on(spread_near, e_first, eb, 1, 1)
        pass_on(spread_far, e_first, eb, 1, 1)
        step(spread_relay, hb, 0, 1)

    step(grad_first, 1, EARLY)
    step(spread_relay, eb, 1, 1)

    step(grad_hidden, 1, EARLY)
    step(grad_out, 1, EARLY)

    @on(0)
    def _():
        step(grad_in, 1, EARLY)

    @on(1)
    def _():
        step(spread_own, eb, 1, 0)
        step(block_backward, 0, e_last[0])
        pass_on(spread_near, e_last, eb, 1, 0)
        pass_on(spread_far, e_last, eb, 1, 0)
        step(grad_in, 1, EARLY)

    step(spread_finish, hb, 0, 1)
    step(grad_first, 1, LATE)

    step(spread_finish, eb, 1, 1)
    step(grad_hidden, 1, LATE)
    step(grad_out, 1, LATE)
    step(scatter_send, 1, OUT, 0, MERGED)
    step(grad_in, 1, LATE)
    step(scatter_send, 1, IN, 0, MERGED)
    step(scatter_send, 1, OUT, 0, DIRECT)
    step(scatter_send, 1, IN, 0, DIRECT)

    @on(0)
    def _():
        step(spread_relay, eb, 1, 0)
        step(spread_own, eb, 1, 0)

    @on(1)
    def _():
        step(spread_relay, hb, 0, 0)
        step(grad_first, 0, EARLY)
        step(spread_relay, eb, 1, 0)
        step(spread_finish, hb, 0, 0)
        step(grad_first, 0, LATE)

    step(grad_hidden, 0, EARLY)
    step(grad_in, 0, EARLY)
    step(grad_out, 0, EARLY)
    step(scatter_relay, 1, OUT, 0)
    step(spread_finish, eb, 1, 0)
    step(grad_hidden, 0, LATE)
    step(grad_in, 0, LATE)
    step(scatter_send, 0, IN, 0, MERGED)
    step(grad_out, 0, LATE)
    step(scatter_relay, 1, IN, 0)
    step(scatter_send, 0, OUT, 0, MERGED)
    step(scatter_send, 0, IN, 0, DIRECT)

    @on(0)
    def _():
        step(block_backward, 0, ga)
        send(ga, ga, ga_s, ga_r, d, 1)

    step(scatter_turn, 1, OUT)
    step(scatter_relay, 0, IN, 0)
    step(scatter_send, 0, OUT, 0, DIRECT)
    step(scatter_turn, 1, IN)
    step(scatter_relay, 0, OUT, 0)
    step(scatter_relay, 1, OUT, 1)

    @on(1)
    def _():
        wait_recv(ga, ga_r)

    gact[...] = ga[...]
    step(scatter_turn, 0, IN)
    step(scatter_relay, 1, IN, 1)
    step(scatter_turn, 0, OUT)
    step(scatter_relay, 0, IN, 1)
    step(scatter_out, 1)
    step(scatter_last, 1)
    step(scatter_relay, 0, OUT, 1)
    step(scatter_last, 0)
    step(scatter_finish, 1)
    step(scatter_out, 0)
    step(scatter_finish, 0)

    for v in BLOCKS:
        for k in MATS:
            three = pl.ds(0, len(RING))
            wait_send(part_at(v, k, three, 0, 0), ag_s.at[v, k, 0])
            wait_send(part_at(v, k, whole, three, 0), ag_s.at[v, k, 1])
            wait_send(part_at(v, k, whole, whole, three), ag_s.at[v, k, LARGE])
        for colour in COLOURS:
            for which in HALVES:
                for st in HALVES:
                    wait_send(landing(v, st, which, colour), rs_s.at[st, v, colour, which])
        wait_send(r3.at[v], r3_s.at[v])
        wait_send(hb.at[v, 0], rl_s.at[0, v])
        wait_send(hb.at[v, 0], rl_s.at[1, v])
    wait_send(hb.at[0, pl.ds(0, 2)], mc_s.at[0])
    wait_send(hb.at[0, pl.ds(0, 3)], mc_s.at[1])
    wait_send(hb.at[0, pl.ds(0, 3)], mc_s.at[3])

    @pl.when(p == 0)
    def _():
        wait_send(hb.at[0, pl.ds(0, 3)], mc_s.at[2])
        wait_send(ga, ga_s)

    @pl.when(p == 1)
    def _():
        wait_send(hb.at[0, pl.ds(0, 3)], mc_s.at[4])


def hand_on(*refs):
    copies = [pltpu.make_async_copy(refs[i], refs[NA + i], refs[-1].at[i]) for i in QUARTERS]
    for copy in copies:
        copy.start()
    for copy in copies:
        copy.wait()


def solution(mesh):
    act_spec = P(None, "data", None, None)
    w_spec = P(None, "stage", "data", None)

    def body(act_in, cot_out, w_gate, w_in, w_out):
        shape = act_in.shape
        dm, fd = shape[3], w_gate.shape[3]
        rows = shape[0] * shape[1] * shape[2]
        dr, fr, fs = dm // NL, fd // NL, fd // NA
        pf = fs // NA
        vmem = pltpu.VMEM
        dma = pltpu.SemaphoreType.DMA
        n2, n3, na = NB, len(RING), NA
        ring = (na, na)
        in_widths = (fs // n2, fs // n2, fs - pf, pf)
        scratch = [
            vmem((n2, na, *ring, dr, fd), BF), vmem((n2, na, *ring, dr, fd), BF), vmem((n2, na, *ring, fr, dm), BF),
            vmem((n2, na, rows, dm), BF), vmem((n2, na, rows, dm), BF), vmem((na, rows, dm), BF), vmem((rows, dm), BF),
            vmem((n2, na, rows, dm), BF),
            vmem((n2, rows, fd), F32), vmem((n2, rows, fd), F32),
            vmem((n2, na, rows, fs), F32), vmem((n2, na, rows, fs), F32),
            vmem((n2, na, rows, fs), BF),
            vmem((rows, fd), BF), vmem((rows, fd), BF), vmem((rows, fd), BF),
            vmem((na, rows, fs), BF), vmem((na, rows, fs), BF),
            vmem((rows, dm), F32),
            vmem((n2, dm, fs), BF), vmem((n2, dm, fs), BF), vmem((fs, dm), BF),
            *(vmem((n2, *ring, fr, width), F32) for width in (dm // n2, dm // n2)),
            vmem((n2, na, n2, dr, fs), F32), vmem((n2, n3, n2, dr, fs), F32),
            dma((n2, na)), dma((n2, n3, n3)), dma((n2, n3, n2, 6)), dma((n2, n3, n3 * na)), dma((5,)), dma((n2, n2, 7)), dma((n2, n2)), dma, dma,
            dma((n2, n2, n2, n2)), dma((n2, n2, n2, n2, 6)), dma((n2,)), dma((n2, n3)), pltpu.SemaphoreType.REGULAR,
            *(vmem((n2, *ring, na, dr, width), F32) for width in in_widths),
            *(vmem((6, *lead, width), F32)
              for pair in (in_widths[:2], in_widths[2:]) for lead in ((*ring, dr), (na, dr)) for width in pair),
            *(vmem((n2, 6, *lead, dm // n2), F32) for lead in ((n2, fr), (fr // n2,)) for _ in range(n2)),
        ]
        hbm = pl.BlockSpec(memory_space=pl.ANY)
        whole = pl.BlockSpec(memory_space=pltpu.VMEM)
        out = pl.pallas_call(
            kernel,
            out_shape=(
                vmem((rows, dm), BF), vmem((n2, dr, fd), F32), vmem((n2, dr, fd), F32), vmem((n2, fr, dm), F32),
            ),
            in_specs=[hbm] * 5,
            out_specs=(whole,) * NA,
            scratch_shapes=scratch,
            compiler_params=pltpu.CompilerParams(collective_id=0, has_side_effects=True, vmem_limit_bytes=66300000),
            name="train_step",
        )(act_in.reshape(rows, dm), cot_out.reshape(rows, dm), w_gate[:, 0], w_in[:, 0], w_out[:, 0])
        grad_act, grad_gate, grad_lin, grad_proj = pl.pallas_call(
            hand_on, out_shape=tuple(jax.ShapeDtypeStruct(a.shape, a.dtype) for a in out), in_specs=[whole] * NA, out_specs=(hbm,) * NA,
            scratch_shapes=[dma((NA,))], compiler_params=pltpu.CompilerParams(vmem_limit_bytes=2 ** 20), name="hand_on",
        )(*(pltpu.with_memory_space_constraint(a, vmem) for a in out))
        return grad_act.reshape(shape), grad_gate[:, None], grad_lin[:, None], grad_proj[:, None]

    return jax.shard_map(body, mesh=mesh, in_specs=(act_spec, act_spec, w_spec, w_spec, w_spec),
                         out_specs=(act_spec, w_spec, w_spec, w_spec), check_vma=False)
```

```python
import functools

import jax
import jax.numpy as jnp
from jax import lax
from jax.experimental import pallas as pl
from jax.experimental.pallas import tpu as pltpu
from jax.sharding import PartitionSpec as P

NORM_EPS = 1e-6
BF = jnp.bfloat16
F32 = jnp.float32
MESH = pl.DeviceIdType.MESH
X, Y, Z = 0, 1, 2
BLOCKS = COLOURS = HALVES = (0, 1)
NB, NA, NL = len(BLOCKS), 4, 64
RING = (1, 3, 2)
OPP = RING[-1]
PLUS, MINUS = RING[:-1]
QUARTERS = range(NA)
OWN = 0
AXES = ((Z, X, Y), (Y, Z, X), (X, Y, Z))
UP_MATS, OUT_MAT = (0, 1), (2,)
MATS = UP_MATS + OUT_MAT


def mm(left, right):
    return jnp.dot(left, right, preferred_element_type=F32)


def mm_nt(left, right):
    return lax.dot_general(left, right, (((1,), (1,)), ((), ())), preferred_element_type=F32)


def mm_tn(left, right):
    return lax.dot_general(left, right, (((0,), (0,)), ((), ())), preferred_element_type=F32)


def inv_rms(h):
    return lax.rsqrt(jnp.mean(h * h, axis=-1, keepdims=True) + NORM_EPS)


def kernel(act, cot, wg_in, wi_in, wo_in, gact, gg, gi, go,
           wg, wi, wo, hb, eb, xo, ga, ng, f1, f2, f1s, f2s, us, ub, da, db, das, dbs, qs, gs, is_, os_,
           gin0, gin1, gout0, gout1, fin, r3,
           lsem, ag_s, ag_r, lg_r, mc_s, mc_r, rl_s, ga_s, ga_r, rs_s, rs_r, r3_s, r3_r, turn, *rg):
    dm, fd = wo.shape[-1], wg.shape[-1]
    dr, fr = dm // NL, fd // NL
    fs = fd // NA
    pf = fs // NA
    rows = act.shape[0]
    wts = (wg, wi, wo)
    gin, gout = (gin0, gin1), (gout0, gout1)

    p = lax.axis_index("stage")
    d = lax.axis_index("data")
    zc, yc, xc = lax.div(d, 16), lax.rem(lax.div(d, 4), 4), lax.rem(d, 4)
    coord = (xc, yc, zc)
    stride = (1, 4, 16)
    ja = yc + p * (zc - yc)
    jb = zc + p * (yc - zc)
    sa, sb = 4 + 12 * p, 16 - 12 * p

    def rot(c, delta):
        return lax.rem(c + (delta % 4), 4)

    def peer(ax, delta):
        return d + (rot(coord[ax], delta) - coord[ax]) * stride[ax]

    def peer_a(delta):
        return d + (rot(ja, delta) - ja) * sa

    def peer_b(delta):
        return d + (rot(jb, delta) - jb) * sb

    def remote(src, dst, ssem, rsem, dev, core):
        return pltpu.make_async_remote_copy(src_ref=src, dst_ref=dst, send_sem=ssem, recv_sem=rsem,
                                            device_id=(dev, core), device_id_type=MESH)

    def send(src, dst, ssem, rsem, dev, core):
        remote(src, dst, ssem, rsem, dev, core).start()

    def wait_recv(ref, sem):
        remote(ref, ref, sem, sem, d, p).wait_recv()

    def wait_send(ref, sem):
        remote(ref, ref, sem, sem, d, p).wait_send()

    for v in BLOCKS:
        for k, shard in enumerate((wg_in, wi_in, wo_in)):
            pltpu.make_async_copy(shard.at[v], wts[k].at[v, zc, yc, xc], lsem.at[v, k]).start()

    @pl.when(p == 0)
    def _():
        pltpu.make_async_copy(act, hb.at[0, OWN], lsem.at[0, 3]).start()

    @pl.when(p == 1)
    def _():
        pltpu.make_async_copy(cot, eb.at[1, OWN], lsem.at[0, 3]).start()

    barrier = pltpu.get_barrier_semaphore()
    senders = [(peer(ax, delta), p) for ax in (X, Y, Z) for delta in RING]
    senders += [(d, 1 - p), (peer_a(1), 1 - p), (peer_a(-1), 1 - p)]
    for dev, core in senders:
        pl.semaphore_signal(barrier, inc=1, device_id=(dev, core), device_id_type=MESH)
    for v in BLOCKS:
        for k, shard in enumerate((wg_in, wi_in, wo_in)):
            pltpu.make_async_copy(shard.at[v], wts[k].at[v, zc, yc, xc], lsem.at[v, k]).wait()

    @pl.when(p == 0)
    def _():
        pltpu.make_async_copy(act, hb.at[0, OWN], lsem.at[0, 3]).wait()

    @pl.when(p == 1)
    def _():
        pltpu.make_async_copy(cot, eb.at[1, OWN], lsem.at[0, 3]).wait()

    pl.semaphore_wait(barrier, len(senders))

    FIRST, REST = ((0, PLUS, 0), (1, MINUS, 2)), ((1, PLUS, 1), (0, MINUS, 3))
    LARGE = 2
    whole = slice(None)

    def part_at(v, k, small, middle, large, half=None):
        place = dict(zip(AXES[k], (small, middle, large)))
        width = wts[k].shape[-1] // 2
        cols = whole if half is None else pl.ds(half * width, width)
        return wts[k].at[v, place[Z], place[Y], place[X], :, cols]

    def own(k):
        return [coord[ax] for ax in AXES[k]]

    def chunk(v, k, ph, q, half):
        small, middle, large = own(k)
        return part_at(v, k, q, middle, large, half) if ph == 0 else part_at(v, k, pl.ds(2 * half, 2), q, large)

    def small_copy(v, k, ph, q, half, delta, slot):
        ref = chunk(v, k, ph, q, half)
        send(ref, ref, ag_s.at[v, k, ph], ag_r.at[v, k, ph, slot], peer(AXES[k][ph], delta), p)

    def small_wait(v, k, ph, back, half, slot):
        wait_recv(chunk(v, k, ph, rot(coord[AXES[k][ph]], back), half), ag_r.at[v, k, ph, slot])

    def small_send(v, ph):
        for half, delta, slot in FIRST + REST:
            for k in MATS:
                small_copy(v, k, ph, coord[AXES[k][ph]], half, delta, slot)

    def small_relay(v, ph):
        for half, delta, slot in FIRST:
            for k in MATS:
                small_wait(v, k, ph, -delta, half, slot)
                small_copy(v, k, ph, rot(coord[AXES[k][ph]], -delta), half, delta, 4 + half)

    def small_rest(v, ph):
        for half, delta, slot in REST:
            for k in MATS:
                small_wait(v, k, ph, -delta, half, slot)

    def small_last(v, ph):
        for half in HALVES:
            for k in MATS:
                small_wait(v, k, ph, OPP, half, 4 + half)

    def direct_send(v):
        for delta in (OPP, PLUS, MINUS):
            for k in MATS:
                ref = part_at(v, k, *own(k))
                send(ref, ref, ag_s.at[v, k, 0], ag_r.at[v, k, 0, delta], peer(AXES[k][0], delta), p)

    def direct_wait(v):
        for delta in RING:
            for k in MATS:
                small, middle, large = own(k)
                wait_recv(part_at(v, k, rot(small, -delta), middle, large), ag_r.at[v, k, 0, delta])

    UP, DOWN = (0, PLUS), (MINUS, OPP)
    RELAYS = ((UP[0], PLUS), (DOWN[0], MINUS), (UP[1], PLUS), (DOWN[1], MINUS))

    def row(v, k, q, r):
        return part_at(v, k, whole, rot(coord[AXES[k][1]], r), q)

    def large_slot(r, delta):
        return r if delta == PLUS else NA + r

    def large_send(v, up, down):
        for pair in zip(up, down):
            for r, delta in zip(pair, (PLUS, MINUS)):
                for k in MATS:
                    ax = AXES[k][LARGE]
                    ref = row(v, k, coord[ax], r)
                    send(ref, ref, ag_s.at[v, k, LARGE], lg_r.at[v, k, large_slot(r, delta)], peer(ax, delta), p)

    def large_relay(v):
        for r, delta in RELAYS:
            for k in MATS:
                ax = AXES[k][LARGE]
                ref = row(v, k, rot(coord[ax], -delta), r)
                wait_recv(ref, lg_r.at[v, k, large_slot(r, delta)])
                send(ref, ref, ag_s.at[v, k, LARGE], lg_r.at[v, k, 2 * NA + r], peer(ax, delta), p)

    def large_finish(v, mats):
        for pieces, delta in ((DOWN, PLUS), (UP, MINUS)):
            for r in pieces:
                for k in mats:
                    wait_recv(row(v, k, rot(coord[AXES[k][LARGE]], -delta), r), lg_r.at[v, k, large_slot(r, delta)])
        for r in QUARTERS:
            for k in mats:
                wait_recv(row(v, k, rot(coord[AXES[k][LARGE]], OPP), r), lg_r.at[v, k, 2 * NA + r])

    half_rows = rows // 2
    BACK, AHEAD, FAR = 1, 2, 3

    def spread_near(src, buf, which, vd, ssem):
        send(src, buf.at[vd, OWN], ssem, mc_r.at[which, vd, OWN], d, 1 - p)

    def rows_half(half):
        return pl.ds(half * half_rows, half_rows)

    HALF_ORDER = [(half if first else 1 - half, slot, delta, slot if first else FAR + 1 + slot)
                  for first in (True, False) for half, slot, delta in ((0, BACK, PLUS), (1, AHEAD, MINUS))]

    def spread_far(src, buf, which, vd, ssem):
        for half, slot, delta, sem in HALF_ORDER:
            send(src.at[rows_half(half)], buf.at[vd, slot, rows_half(half)], ssem, mc_r.at[which, vd, sem], peer_b(delta), 1 - p)

    def spread_same(buf, which, v, ssem):
        for half, slot, delta, sem in HALF_ORDER:
            send(buf.at[v, OWN, rows_half(half)], buf.at[v, slot, rows_half(half)], ssem, mc_r.at[which, v, sem], peer_a(delta), p)

    def spread_relay(buf, which, v):
        for half, slot, delta, sem in HALF_ORDER:
            ref = buf.at[v, slot, rows_half(half)]
            wait_recv(ref, mc_r.at[which, v, sem])
            if sem == slot:
                send(ref, buf.at[v, FAR, rows_half(half)], rl_s.at[which, v], mc_r.at[which, v, FAR + half], peer_a(delta), p)

    def spread_finish(buf, which, v):
        for half in HALVES:
            wait_recv(buf.at[v, FAR, rows_half(half)], mc_r.at[which, v, FAR + half])

    def spread_own(buf, which, v):
        wait_recv(buf.at[v, OWN], mc_r.at[which, v, OWN])

    def gates(n, wgt, wlin):
        a, b = mm(n, wgt), mm(n, wlin)
        s = jax.nn.sigmoid(a)
        act_a = a * s
        return (act_a * b).astype(BF), b * s * (1.0 + a * (1.0 - s)), act_a

    def block_gates(v):
        h = hb[v, OWN].astype(F32)
        n = (h * inv_rms(h)).astype(BF)

        def tile(i, carry):
            wide = fs // 2
            cols = pl.ds(pl.multiple_of(i * wide, wide), wide)
            u, t1, t2 = gates(n, wg[v, :, :, :, :, cols].reshape(dm, wide), wi[v, :, :, :, :, cols].reshape(dm, wide))
            ub[:, cols] = u
            f1[v, :, cols] = t1
            f2[v, :, cols] = t2
            return carry

        lax.fori_loop(0, 2 * NA, tile, 0, unroll=True)

    def block_out(v, dst):
        half_dm = dm // 2
        for i in HALVES:
            cols = pl.ds(i * half_dm, half_dm)
            out = mm(ub[...], wo[v, :, :, :, :, cols].reshape(fd, half_dm))
            dst[:, cols] = (hb[v, OWN, :, cols].astype(F32) + out).astype(BF)

    def block_backward(v, dst):
        e = eb[v, OWN]

        def tile(i, carry):
            cols = pl.ds(pl.multiple_of(i * fs, fs), fs)
            t = mm_nt(e, wo[v, i].reshape(fs, dm))
            da[:, cols] = (t * f1[v, :, cols]).astype(BF)
            db[:, cols] = (t * f2[v, :, cols]).astype(BF)
            return carry

        lax.fori_loop(0, NA, tile, 0, unroll=True)
        half_dm = dm // 2
        for i in HALVES:
            q = mm_nt(da[...], wg[v, pl.ds(2 * i, 2)].reshape(half_dm, fd))
            q += mm_nt(db[...], wi[v, pl.ds(2 * i, 2)].reshape(half_dm, fd))
            qs[:, pl.ds(i * half_dm, half_dm)] = q
        h = hb[v, OWN].astype(F32)
        r = inv_rms(h)
        hr = h * r
        q = qs[...]
        dst[...] = (e.astype(F32) + r * (q - hr * jnp.mean(q * hr, axis=-1, keepdims=True))).astype(BF)

    def piece(j, i):
        z = i + p * (j - i)
        y = j + p * (i - j)
        return z, y

    EARLY, LATE = range(FAR), range(FAR, NA)

    def grad_first(v, slots):
        for i in QUARTERS if OWN in slots else ():
            z, y = piece(ja, i)
            cols = pl.ds(pl.multiple_of((z * NA + y) * pf, pf), pf)
            gs[v, :, pl.ds(i * pf, pf)] = wg[v, :, :, :, :, cols].reshape(dm, pf)
            is_[v, :, pl.ds(i * pf, pf)] = wi[v, :, :, :, :, cols].reshape(dm, pf)
        for s in slots:
            h = hb[v, s].astype(F32)
            n = (h * inv_rms(h)).astype(BF)
            ng[v, s] = n
            u, t1, t2 = gates(n, gs[v], is_[v])
            us[v, s] = u
            f1s[v, s] = t1
            f2s[v, s] = t2

    def grad_hidden(v, slots):
        for i in QUARTERS if OWN in slots else ():
            z, y = piece(ja, i)
            os_[pl.ds(i * pf, pf), :] = wo[v, z, y].reshape(pf, dm)
        for s in slots:
            t = mm_nt(eb[v, s], os_[...])
            das[s] = (t * f1s[v, s]).astype(BF)
            dbs[s] = (t * f2s[v, s]).astype(BF)

    def split(width, second):
        return pl.ds(0, width - second), pl.ds(width - second, second)

    IN_COLS, OUT_COLS = split(fs, pf), split(dm, pf)

    def keep(refs, v, place, tile, cols, first):
        b, rest = place[0], place[1:]
        lead = () if v is None else (v,)
        for colour in COLOURS:
            part = tile[..., cols[colour].start:cols[colour].start + cols[colour].size]
            at = lead + ((b, slice(None)) if colour == 0 else (slice(None), b)) + rest
            refs[colour][at] = part if first else refs[colour][at] + part

    def rows_of(slots):
        return pl.ds(slots[0], len(slots)), len(slots) * rows

    def grad_out(v, slots):
        some, count = rows_of(slots)
        for i in HALVES:
            cols = pl.ds(i * 2 * pf, 2 * pf)
            g = mm_tn(us[v, some, :, cols].reshape(count, 2 * pf), eb[v, some].reshape(count, dm)).reshape(2, NA, fr, dm)
            for b in HALVES:
                keep(gout, v, (2 * i + b,), g[b], OUT_COLS, OWN in slots)

    def grad_in(v, slots):
        some, count = rows_of(slots)
        for which, dref in enumerate((das, dbs)):
            for i in QUARTERS:
                cols = pl.ds(i * (dm // NA), dm // NA)
                g = mm_tn(ng[v, some, :, cols].reshape(count, dm // NA), dref[some].reshape(count, fs)).reshape(NA, NA, dr, fs)
                for y in QUARTERS:
                    keep([ref.at[v, which] for ref in gin], None, (i + p * (y - i), y + p * (i - y)), g[y], IN_COLS, OWN in slots)

    IN, OUT = 0, 1

    def view(which, st, v, colour, t, half):
        own = jb if colour == 0 else xc
        if which == IN:
            ref = gin[colour].at[v, half]
            return ref.at[t] if st == 0 else ref.at[own, t]
        ref = gout[colour].at[v]
        return ref.at[t, pl.ds(2 * half, 2)] if st == 0 else ref.at[own, t, pl.ds(half * (fr // 2), fr // 2)]

    RECV = (((rg[0], rg[1]), (rg[2], rg[3])), ((rg[4], rg[5]), (rg[6], rg[7])))
    MERGED, DIRECT = ((0, OPP, PLUS, 0), (1, OPP, MINUS, 1)), ((1, PLUS, PLUS, 2), (0, MINUS, MINUS, 3))
    RELAYED = ((0, PLUS, PLUS, 4), (1, MINUS, MINUS, 5))

    def axis_of(colour, st):
        return (jb, peer_b) if colour == st else (xc, functools.partial(peer, X))

    def scatter_send(v, which, st, copies):
        for colour in COLOURS:
            q, to = axis_of(colour, st)
            for half, c, delta, slot in copies:
                send(view(which, st, v, colour, rot(q, c), half), RECV[st][which][colour].at[v, slot],
                     rs_s.at[st, v, colour, which], rs_r.at[st, v, colour, which, slot], to(delta), p)

    def scatter_relay(v, which, st):
        for colour in COLOURS:
            q, _ = axis_of(colour, st)
            recv = RECV[st][which][colour]
            for half, c, _, slot in RELAYED:
                wait_recv(recv.at[v, slot - 4], rs_r.at[st, v, colour, which, slot - 4])
                ref = view(which, st, v, colour, rot(q, c), half)
                ref[...] = ref[...] + recv[v, slot - 4]
        scatter_send(v, which, st, RELAYED)

    def scatter_sum(v, which, st):
        for colour in COLOURS:
            q, _ = axis_of(colour, st)
            recv = RECV[st][which][colour]
            for half in HALVES:
                direct, merged = 3 - half, 4 + half
                for slot in (direct, merged):
                    wait_recv(recv.at[v, slot], rs_r.at[st, v, colour, which, slot])
                ref = view(which, st, v, colour, q, half)
                ref[...] = ref[...] + recv[v, direct] + recv[v, merged]

    def scatter_turn(v, which):
        scatter_sum(v, which, 0)
        scatter_send(v, which, 1, MERGED + DIRECT)

    def scatter_out(v):
        scatter_sum(v, OUT, 1)
        for colour in COLOURS:
            go[v, :, OUT_COLS[colour]] = gout[colour][(v, jb, xc) if colour == 0 else (v, xc, jb)]

    def scatter_last(v):
        scatter_sum(v, IN, 1)
        for which in HALVES:
            for colour in COLOURS:
                fin[v, :, which, :, IN_COLS[colour]] = gin[colour][(v, which, jb, xc) if colour == 0 else (v, which, xc, jb)]
        for delta in (OPP, PLUS, MINUS):
            send(fin.at[v, rot(ja, delta)], r3.at[v, delta - 1], r3_s.at[v], r3_r.at[v, delta - 1], peer_a(delta), p)

    def scatter_finish(v):
        def put(j, vals):
            for i in QUARTERS:
                z, y = piece(j, i)
                cols = pl.ds(pl.multiple_of((z * NA + y) * pf, pf), pf)
                gg[v, :, cols] = vals(0)[:, i * pf:(i + 1) * pf]
                gi[v, :, cols] = vals(1)[:, i * pf:(i + 1) * pf]

        put(ja, lambda w: fin[v, ja, w])
        for delta in RING:
            wait_recv(r3.at[v, delta - 1], r3_r.at[v, delta - 1])
            put(rot(ja, -delta), lambda w, delta=delta: r3[v, delta - 1, w])

    def step(fn, *args):
        with jax.named_scope(fn.__name__):
            fn(*args)

    def on(core):
        return pl.when(p == core)

    def take_turn():
        pl.semaphore_wait(turn, 1)

    def give_turn():
        pl.semaphore_signal(turn, inc=1, device_id=(d, 1 - p), device_id_type=MESH)

    h_mid, h_late, e_first, e_last = ((xo.at[i], mc_s.at[1 + i]) for i in QUARTERS)

    def pass_on(part, item, buf, which, vd):
        step(part, item[0], buf, which, vd, item[1])

    AFTER = (MINUS, OPP), (0, PLUS)
    step(direct_send, 0)
    step(small_send, 1, 0)

    @on(0)
    def _():
        step(spread_same, hb, 0, 0, mc_s.at[0])

    step(direct_wait, 0)
    step(small_send, 0, 1)
    step(small_relay, 1, 0)
    step(large_send, 0, (0,), (0,))
    step(small_rest, 1, 0)
    step(small_last, 1, 0)
    step(small_send, 1, 1)
    step(small_relay, 0, 1)
    step(small_relay, 1, 1)
    step(small_rest, 0, 1)
    step(large_send, 0, (PLUS, MINUS), (MINUS, PLUS))
    step(small_last, 0, 1)
    step(large_send, 0, (OPP,), (OPP,))
    step(small_rest, 1, 1)
    step(small_last, 1, 1)
    step(large_relay, 0)

    @on(0)
    def _():
        step(large_send, 1, UP, DOWN)

    step(large_finish, 0, UP_MATS)

    @on(0)
    def _():
        step(large_send, 1, *AFTER)

    @on(1)
    def _():
        step(take_turn)
        step(large_send, 1, UP, DOWN)
        step(spread_own, hb, 0, 0)

    step(block_gates, 0)

    @on(1)
    def _():
        step(large_send, 1, *AFTER)

    step(large_finish, 0, OUT_MAT)
    step(block_out, 0, h_mid[0])
    pass_on(spread_near, h_mid, hb, 0, p)
    step(large_relay, 1)

    @on(0)
    def _():
        step(give_turn)
        step(spread_relay, hb, 0, 0)

    @on(1)
    def _():
        pass_on(spread_far, h_mid, hb, 0, p)
        step(spread_same, eb, 1, 1, mc_s.at[0])

    step(spread_own, hb, 0, 1)
    step(large_finish, 1, UP_MATS)
    step(block_gates, 1)
    step(large_finish, 1, OUT_MAT)

    @on(0)
    def _():
        step(block_out, 1, h_late[0])
        pass_on(spread_near, h_late, hb, 0, 1)
        pass_on(spread_far, h_late, hb, 0, 1)
        step(spread_finish, hb, 0, 0)
        step(grad_first, 0, EARLY)
        step(grad_first, 0, LATE)
        step(spread_relay, hb, 0, 1)
        step(grad_first, 1, EARLY)
        step(spread_own, eb, 1, 1)
        pass_on(spread_far, h_mid, hb, 0, p)
        step(block_backward, 1, e_first[0])
        pass_on(spread_near, e_first, eb, 1, 0)
        pass_on(spread_far, e_first, eb, 1, 0)
        step(spread_finish, hb, 0, 1)
        step(grad_first, 1, LATE)

    @on(1)
    def _():
        step(block_backward, 1, e_first[0])
        pass_on(spread_near, e_first, eb, 1, 1)
        pass_on(spread_far, e_first, eb, 1, 1)
        step(spread_relay, hb, 0, 1)
        step(grad_first, 1, EARLY)

    step(spread_relay, eb, 1, 1)

    step(grad_hidden, 1, EARLY)
    step(grad_out, 1, EARLY)

    @on(0)
    def _():
        step(grad_in, 1, EARLY)

    @on(1)
    def _():
        step(spread_own, eb, 1, 0)
        step(block_backward, 0, e_last[0])
        pass_on(spread_near, e_last, eb, 1, 0)
        pass_on(spread_far, e_last, eb, 1, 0)
        step(grad_in, 1, EARLY)
        step(spread_finish, hb, 0, 1)
        step(grad_first, 1, LATE)

    step(spread_finish, eb, 1, 1)
    step(grad_hidden, 1, LATE)
    step(grad_out, 1, LATE)
    step(scatter_send, 1, OUT, 0, MERGED)
    step(grad_in, 1, LATE)
    step(scatter_send, 1, IN, 0, MERGED)
    step(scatter_send, 1, OUT, 0, DIRECT)
    step(scatter_send, 1, IN, 0, DIRECT)

    @on(0)
    def _():
        step(spread_relay, eb, 1, 0)
        step(spread_own, eb, 1, 0)

    @on(1)
    def _():
        step(spread_relay, hb, 0, 0)
        step(grad_first, 0, EARLY)
        step(spread_relay, eb, 1, 0)
        step(spread_finish, hb, 0, 0)
        step(grad_first, 0, LATE)

    step(grad_hidden, 0, EARLY)
    step(grad_in, 0, EARLY)
    step(grad_out, 0, EARLY)
    step(scatter_relay, 1, OUT, 0)
    step(spread_finish, eb, 1, 0)
    step(grad_hidden, 0, LATE)
    step(grad_in, 0, LATE)
    step(scatter_send, 0, IN, 0, MERGED)
    step(grad_out, 0, LATE)
    step(scatter_relay, 1, IN, 0)
    step(scatter_send, 0, OUT, 0, MERGED)
    step(scatter_send, 0, IN, 0, DIRECT)

    @on(0)
    def _():
        step(block_backward, 0, ga)
        send(ga, ga, ga_s, ga_r, d, 1)

    step(scatter_turn, 1, OUT)
    step(scatter_relay, 0, IN, 0)
    step(scatter_send, 0, OUT, 0, DIRECT)
    step(scatter_turn, 1, IN)
    step(scatter_relay, 0, OUT, 0)
    step(scatter_relay, 1, OUT, 1)

    @on(1)
    def _():
        wait_recv(ga, ga_r)

    gact[...] = ga[...]
    step(scatter_turn, 0, IN)
    step(scatter_relay, 1, IN, 1)
    step(scatter_turn, 0, OUT)
    step(scatter_relay, 0, IN, 1)
    step(scatter_out, 1)
    step(scatter_last, 1)
    step(scatter_relay, 0, OUT, 1)
    step(scatter_last, 0)
    step(scatter_finish, 1)
    step(scatter_out, 0)
    step(scatter_finish, 0)

    for v in BLOCKS:
        for k in MATS:
            three = pl.ds(0, len(RING))
            wait_send(part_at(v, k, three, 0, 0), ag_s.at[v, k, 0])
            wait_send(part_at(v, k, whole, three, 0), ag_s.at[v, k, 1])
            wait_send(part_at(v, k, whole, whole, three), ag_s.at[v, k, LARGE])
        for colour in COLOURS:
            for which in HALVES:
                for st in HALVES:
                    wait_send(RECV[st][which][colour].at[v], rs_s.at[st, v, colour, which])
        wait_send(r3.at[v], r3_s.at[v])
        wait_send(hb.at[v, 0], rl_s.at[0, v])
        wait_send(hb.at[v, 0], rl_s.at[1, v])
    wait_send(hb.at[0, pl.ds(0, 2)], mc_s.at[0])
    wait_send(hb.at[0, pl.ds(0, 3)], mc_s.at[1])
    wait_send(hb.at[0, pl.ds(0, 3)], mc_s.at[3])

    @pl.when(p == 0)
    def _():
        wait_send(hb.at[0, pl.ds(0, 3)], mc_s.at[2])
        wait_send(ga, ga_s)

    @pl.when(p == 1)
    def _():
        wait_send(hb.at[0, pl.ds(0, 3)], mc_s.at[4])


def hand_on(*refs):
    copies = [pltpu.make_async_copy(refs[i], refs[NA + i], refs[-1].at[i]) for i in QUARTERS]
    for copy in copies:
        copy.start()
    for copy in copies:
        copy.wait()


def solution(mesh):
    act_spec = P(None, "data", None, None)
    w_spec = P(None, "stage", "data", None)

    def body(act_in, cot_out, w_gate, w_in, w_out):
        shape = act_in.shape
        dm, fd = shape[3], w_gate.shape[3]
        rows = shape[0] * shape[1] * shape[2]
        dr, fr, fs = dm // NL, fd // NL, fd // NA
        pf = fs // NA
        vmem = pltpu.VMEM
        dma = pltpu.SemaphoreType.DMA
        n2, n3, na = NB, len(RING), NA
        ring = (na, na)
        scratch = [
            vmem((n2, na, *ring, dr, fd), BF), vmem((n2, na, *ring, dr, fd), BF), vmem((n2, na, *ring, fr, dm), BF),
            vmem((n2, na, rows, dm), BF), vmem((n2, na, rows, dm), BF), vmem((na, rows, dm), BF), vmem((rows, dm), BF),
            vmem((n2, na, rows, dm), BF),
            vmem((n2, rows, fd), F32), vmem((n2, rows, fd), F32),
            vmem((n2, na, rows, fs), F32), vmem((n2, na, rows, fs), F32),
            vmem((n2, na, rows, fs), BF),
            vmem((rows, fd), BF), vmem((rows, fd), BF), vmem((rows, fd), BF),
            vmem((na, rows, fs), BF), vmem((na, rows, fs), BF),
            vmem((rows, dm), F32),
            vmem((n2, dm, fs), BF), vmem((n2, dm, fs), BF), vmem((fs, dm), BF),
            *(vmem((n2, n2, *ring, na, dr, width), F32) for width in (fs - pf, pf)),
            *(vmem((n2, *ring, fr, width), F32) for width in (dm - pf, pf)),
            vmem((n2, na, n2, dr, fs), F32), vmem((n2, n3, n2, dr, fs), F32),
            dma((n2, na)), dma((n2, n3, n3)), dma((n2, n3, n2, 6)), dma((n2, n3, n3 * na)), dma((5,)), dma((n2, n2, 7)), dma((n2, n2)), dma, dma,
            dma((n2, n2, n2, n2)), dma((n2, n2, n2, n2, 6)), dma((n2,)), dma((n2, n3)), pltpu.SemaphoreType.REGULAR,
            *(vmem((n2, 6, *lead, width), F32)
              for lead_in, lead_out in (((*ring, dr), (n2, fr)), ((na, dr), (fr // n2,)))
              for lead, width in ((lead_in, fs - pf), (lead_in, pf), (lead_out, dm - pf), (lead_out, pf))),
        ]
        hbm = pl.BlockSpec(memory_space=pl.ANY)
        whole = pl.BlockSpec(memory_space=pltpu.VMEM)
        out = pl.pallas_call(
            kernel,
            out_shape=(
                vmem((rows, dm), BF), vmem((n2, dr, fd), F32), vmem((n2, dr, fd), F32), vmem((n2, fr, dm), F32),
            ),
            in_specs=[hbm] * 5,
            out_specs=(whole,) * NA,
            scratch_shapes=scratch,
            compiler_params=pltpu.CompilerParams(collective_id=0, has_side_effects=True, vmem_limit_bytes=66300000),
            name="train_step",
        )(act_in.reshape(rows, dm), cot_out.reshape(rows, dm), w_gate[:, 0], w_in[:, 0], w_out[:, 0])
        grad_act, grad_gate, grad_lin, grad_proj = pl.pallas_call(
            hand_on, out_shape=tuple(jax.ShapeDtypeStruct(a.shape, a.dtype) for a in out), in_specs=[whole] * NA, out_specs=(hbm,) * NA,
            scratch_shapes=[dma((NA,))], compiler_params=pltpu.CompilerParams(vmem_limit_bytes=2 ** 20), name="hand_on",
        )(*(pltpu.with_memory_space_constraint(a, vmem) for a in out))
        return grad_act.reshape(shape), grad_gate[:, None], grad_lin[:, None], grad_proj[:, None]

    return jax.shard_map(body, mesh=mesh, in_specs=(act_spec, act_spec, w_spec, w_spec, w_spec),
                         out_specs=(act_spec, w_spec, w_spec, w_spec), check_vma=False)
```

```python
import functools

import jax
import jax.numpy as jnp
from jax import lax
from jax.experimental import pallas as pl
from jax.experimental.pallas import tpu as pltpu
from jax.sharding import PartitionSpec as P

NORM_EPS = 1e-6
BF = jnp.bfloat16
F32 = jnp.float32
MESH = pl.DeviceIdType.MESH
X, Y, Z = 0, 1, 2
BLOCKS = COLOURS = HALVES = (0, 1)
NB, NA, NL = len(BLOCKS), 4, 64
RING = (1, 3, 2)
OPP = RING[-1]
PLUS, MINUS = RING[:-1]
QUARTERS = range(NA)
OWN = 0
AXES = ((Z, X, Y), (Y, Z, X), (X, Y, Z))
UP_MATS, OUT_MAT = (0, 1), (2,)
MATS = UP_MATS + OUT_MAT


def mm(left, right):
    return jnp.dot(left, right, preferred_element_type=F32)


def mm_nt(left, right):
    return lax.dot_general(left, right, (((1,), (1,)), ((), ())), preferred_element_type=F32)


def mm_tn(left, right):
    return lax.dot_general(left, right, (((0,), (0,)), ((), ())), preferred_element_type=F32)


def inv_rms(h):
    return lax.rsqrt(jnp.mean(h * h, axis=-1, keepdims=True) + NORM_EPS)


def kernel(act, cot, wg_in, wi_in, wo_in, gact, gg, gi, go,
           wg, wi, wo, hb, eb, xo, ga, ng, f1, f2, f1s, f2s, us, ub, da, db, das, dbs, qs, gs, is_, os_,
           gin0, gin1, gout0, gout1, fin, r3,
           lsem, ag_s, ag_r, lg_r, mc_s, mc_r, rl_s, ga_s, ga_r, rs_s, rs_r, r3_s, r3_r, turn, *rg):
    dm, fd = wo.shape[-1], wg.shape[-1]
    dr, fr = dm // NL, fd // NL
    fs = fd // NA
    pf = fs // NA
    rows = act.shape[0]
    wts = (wg, wi, wo)
    gin, gout = (gin0, gin1), (gout0, gout1)

    p = lax.axis_index("stage")
    d = lax.axis_index("data")
    zc, yc, xc = lax.div(d, 16), lax.rem(lax.div(d, 4), 4), lax.rem(d, 4)
    coord = (xc, yc, zc)
    stride = (1, 4, 16)
    ja = yc + p * (zc - yc)
    jb = zc + p * (yc - zc)
    sa, sb = 4 + 12 * p, 16 - 12 * p

    def rot(c, delta):
        return lax.rem(c + (delta % 4), 4)

    def peer(ax, delta):
        return d + (rot(coord[ax], delta) - coord[ax]) * stride[ax]

    def peer_a(delta):
        return d + (rot(ja, delta) - ja) * sa

    def peer_b(delta):
        return d + (rot(jb, delta) - jb) * sb

    def remote(src, dst, ssem, rsem, dev, core):
        return pltpu.make_async_remote_copy(src_ref=src, dst_ref=dst, send_sem=ssem, recv_sem=rsem,
                                            device_id=(dev, core), device_id_type=MESH)

    def send(src, dst, ssem, rsem, dev, core):
        remote(src, dst, ssem, rsem, dev, core).start()

    def wait_recv(ref, sem):
        remote(ref, ref, sem, sem, d, p).wait_recv()

    def wait_send(ref, sem):
        remote(ref, ref, sem, sem, d, p).wait_send()

    for v in BLOCKS:
        for k, shard in enumerate((wg_in, wi_in, wo_in)):
            pltpu.make_async_copy(shard.at[v], wts[k].at[v, zc, yc, xc], lsem.at[v, k]).start()

    @pl.when(p == 0)
    def _():
        pltpu.make_async_copy(act, hb.at[0, OWN], lsem.at[0, 3]).start()

    @pl.when(p == 1)
    def _():
        pltpu.make_async_copy(cot, eb.at[1, OWN], lsem.at[0, 3]).start()

    barrier = pltpu.get_barrier_semaphore()
    senders = [(peer(ax, delta), p) for ax in (X, Y, Z) for delta in RING]
    senders += [(d, 1 - p), (peer_a(1), 1 - p), (peer_a(-1), 1 - p)]
    for dev, core in senders:
        pl.semaphore_signal(barrier, inc=1, device_id=(dev, core), device_id_type=MESH)
    for v in BLOCKS:
        for k, shard in enumerate((wg_in, wi_in, wo_in)):
            pltpu.make_async_copy(shard.at[v], wts[k].at[v, zc, yc, xc], lsem.at[v, k]).wait()

    @pl.when(p == 0)
    def _():
        pltpu.make_async_copy(act, hb.at[0, OWN], lsem.at[0, 3]).wait()

    @pl.when(p == 1)
    def _():
        pltpu.make_async_copy(cot, eb.at[1, OWN], lsem.at[0, 3]).wait()

    pl.semaphore_wait(barrier, len(senders))

    FIRST, REST = ((0, PLUS, 0), (1, MINUS, 2)), ((1, PLUS, 1), (0, MINUS, 3))
    LARGE = 2
    whole = slice(None)

    def part_at(v, k, small, middle, large, half=None):
        place = dict(zip(AXES[k], (small, middle, large)))
        width = wts[k].shape[-1] // 2
        cols = whole if half is None else pl.ds(half * width, width)
        return wts[k].at[v, place[Z], place[Y], place[X], :, cols]

    def own(k):
        return [coord[ax] for ax in AXES[k]]

    def chunk(v, k, ph, q, half):
        small, middle, large = own(k)
        return part_at(v, k, q, middle, large, half) if ph == 0 else part_at(v, k, pl.ds(2 * half, 2), q, large)

    def small_copy(v, k, ph, q, half, delta, slot):
        ref = chunk(v, k, ph, q, half)
        send(ref, ref, ag_s.at[v, k, ph], ag_r.at[v, k, ph, slot], peer(AXES[k][ph], delta), p)

    def small_wait(v, k, ph, back, half, slot):
        wait_recv(chunk(v, k, ph, rot(coord[AXES[k][ph]], back), half), ag_r.at[v, k, ph, slot])

    def small_send(v, ph):
        for half, delta, slot in FIRST + REST:
            for k in MATS:
                small_copy(v, k, ph, coord[AXES[k][ph]], half, delta, slot)

    def small_relay(v, ph):
        for half, delta, slot in FIRST:
            for k in MATS:
                small_wait(v, k, ph, -delta, half, slot)
                small_copy(v, k, ph, rot(coord[AXES[k][ph]], -delta), half, delta, 4 + half)

    def small_rest(v, ph):
        for half, delta, slot in REST:
            for k in MATS:
                small_wait(v, k, ph, -delta, half, slot)

    def small_last(v, ph):
        for half in HALVES:
            for k in MATS:
                small_wait(v, k, ph, OPP, half, 4 + half)

    def direct_send(v):
        for delta in (OPP, PLUS, MINUS):
            for k in MATS:
                ref = part_at(v, k, *own(k))
                send(ref, ref, ag_s.at[v, k, 0], ag_r.at[v, k, 0, delta], peer(AXES[k][0], delta), p)

    def direct_wait(v):
        for delta in RING:
            for k in MATS:
                small, middle, large = own(k)
                wait_recv(part_at(v, k, rot(small, -delta), middle, large), ag_r.at[v, k, 0, delta])

    UP, DOWN = (0, PLUS), (MINUS, OPP)
    RELAYS = ((UP[0], PLUS), (DOWN[0], MINUS), (UP[1], PLUS), (DOWN[1], MINUS))

    def row(v, k, q, r):
        return part_at(v, k, whole, rot(coord[AXES[k][1]], r), q)

    def large_slot(r, delta):
        return r if delta == PLUS else NA + r

    def large_send(v, up, down):
        for pair in zip(up, down):
            for r, delta in zip(pair, (PLUS, MINUS)):
                for k in MATS:
                    ax = AXES[k][LARGE]
                    ref = row(v, k, coord[ax], r)
                    send(ref, ref, ag_s.at[v, k, LARGE], lg_r.at[v, k, large_slot(r, delta)], peer(ax, delta), p)

    def large_relay(v):
        for r, delta in RELAYS:
            for k in MATS:
                ax = AXES[k][LARGE]
                ref = row(v, k, rot(coord[ax], -delta), r)
                wait_recv(ref, lg_r.at[v, k, large_slot(r, delta)])
                send(ref, ref, ag_s.at[v, k, LARGE], lg_r.at[v, k, 2 * NA + r], peer(ax, delta), p)

    def large_finish(v, mats):
        for pieces, delta in ((DOWN, PLUS), (UP, MINUS)):
            for r in pieces:
                for k in mats:
                    wait_recv(row(v, k, rot(coord[AXES[k][LARGE]], -delta), r), lg_r.at[v, k, large_slot(r, delta)])
        for r in QUARTERS:
            for k in mats:
                wait_recv(row(v, k, rot(coord[AXES[k][LARGE]], OPP), r), lg_r.at[v, k, 2 * NA + r])

    half_rows = rows // 2
    BACK, AHEAD, FAR = 1, 2, 3

    def spread_near(src, buf, which, vd, ssem):
        send(src, buf.at[vd, OWN], ssem, mc_r.at[which, vd, OWN], d, 1 - p)

    def rows_half(half):
        return pl.ds(half * half_rows, half_rows)

    HALF_ORDER = [(half if first else 1 - half, slot, delta, slot if first else FAR + 1 + slot)
                  for first in (True, False) for half, slot, delta in ((0, BACK, PLUS), (1, AHEAD, MINUS))]

    def spread_far(src, buf, which, vd, ssem):
        for half, slot, delta, sem in HALF_ORDER:
            send(src.at[rows_half(half)], buf.at[vd, slot, rows_half(half)], ssem, mc_r.at[which, vd, sem], peer_b(delta), 1 - p)

    def spread_same(buf, which, v, ssem):
        for half, slot, delta, sem in HALF_ORDER:
            send(buf.at[v, OWN, rows_half(half)], buf.at[v, slot, rows_half(half)], ssem, mc_r.at[which, v, sem], peer_a(delta), p)

    def spread_relay(buf, which, v):
        for half, slot, delta, sem in HALF_ORDER:
            ref = buf.at[v, slot, rows_half(half)]
            wait_recv(ref, mc_r.at[which, v, sem])
            if sem == slot:
                send(ref, buf.at[v, FAR, rows_half(half)], rl_s.at[which, v], mc_r.at[which, v, FAR + half], peer_a(delta), p)

    def spread_finish(buf, which, v):
        for half in HALVES:
            wait_recv(buf.at[v, FAR, rows_half(half)], mc_r.at[which, v, FAR + half])

    def spread_own(buf, which, v):
        wait_recv(buf.at[v, OWN], mc_r.at[which, v, OWN])

    def gates(n, wgt, wlin):
        a, b = mm(n, wgt), mm(n, wlin)
        s = jax.nn.sigmoid(a)
        act_a = a * s
        return (act_a * b).astype(BF), b * s * (1.0 + a * (1.0 - s)), act_a

    def block_gates(v):
        h = hb[v, OWN].astype(F32)
        n = (h * inv_rms(h)).astype(BF)

        def tile(i, carry):
            wide = fs // 2
            cols = pl.ds(pl.multiple_of(i * wide, wide), wide)
            u, t1, t2 = gates(n, wg[v, :, :, :, :, cols].reshape(dm, wide), wi[v, :, :, :, :, cols].reshape(dm, wide))
            ub[:, cols] = u
            f1[v, :, cols] = t1
            f2[v, :, cols] = t2
            return carry

        lax.fori_loop(0, 2 * NA, tile, 0, unroll=True)

    def block_out(v, dst):
        half_dm = dm // 2
        for i in HALVES:
            cols = pl.ds(i * half_dm, half_dm)
            out = mm(ub[...], wo[v, :, :, :, :, cols].reshape(fd, half_dm))
            dst[:, cols] = (hb[v, OWN, :, cols].astype(F32) + out).astype(BF)

    def block_backward(v, dst):
        e = eb[v, OWN]

        def tile(i, carry):
            cols = pl.ds(pl.multiple_of(i * fs, fs), fs)
            t = mm_nt(e, wo[v, i].reshape(fs, dm))
            da[:, cols] = (t * f1[v, :, cols]).astype(BF)
            db[:, cols] = (t * f2[v, :, cols]).astype(BF)
            return carry

        lax.fori_loop(0, NA, tile, 0, unroll=True)
        half_dm = dm // 2
        for i in HALVES:
            q = mm_nt(da[...], wg[v, pl.ds(2 * i, 2)].reshape(half_dm, fd))
            q += mm_nt(db[...], wi[v, pl.ds(2 * i, 2)].reshape(half_dm, fd))
            qs[:, pl.ds(i * half_dm, half_dm)] = q
        h = hb[v, OWN].astype(F32)
        r = inv_rms(h)
        hr = h * r
        q = qs[...]
        dst[...] = (e.astype(F32) + r * (q - hr * jnp.mean(q * hr, axis=-1, keepdims=True))).astype(BF)

    def piece(j, i):
        z = i + p * (j - i)
        y = j + p * (i - j)
        return z, y

    EARLY, LATE = range(FAR), range(FAR, NA)

    def grad_first(v, slots):
        for i in QUARTERS if OWN in slots else ():
            z, y = piece(ja, i)
            cols = pl.ds(pl.multiple_of((z * NA + y) * pf, pf), pf)
            gs[v, :, pl.ds(i * pf, pf)] = wg[v, :, :, :, :, cols].reshape(dm, pf)
            is_[v, :, pl.ds(i * pf, pf)] = wi[v, :, :, :, :, cols].reshape(dm, pf)
        for s in slots:
            h = hb[v, s].astype(F32)
            n = (h * inv_rms(h)).astype(BF)
            ng[v, s] = n
            u, t1, t2 = gates(n, gs[v], is_[v])
            us[v, s] = u
            f1s[v, s] = t1
            f2s[v, s] = t2

    def grad_hidden(v, slots):
        for i in QUARTERS if OWN in slots else ():
            z, y = piece(ja, i)
            os_[pl.ds(i * pf, pf), :] = wo[v, z, y].reshape(pf, dm)
        for s in slots:
            t = mm_nt(eb[v, s], os_[...])
            das[s] = (t * f1s[v, s]).astype(BF)
            dbs[s] = (t * f2s[v, s]).astype(BF)

    def split(width, second):
        return pl.ds(0, width - second), pl.ds(width - second, second)

    IN_COLS, OUT_COLS = split(fs, pf), split(dm, pf)

    def keep(refs, v, place, tile, cols, first):
        b, rest = place[0], place[1:]
        lead = () if v is None else (v,)
        for colour in COLOURS:
            part = tile[..., cols[colour].start:cols[colour].start + cols[colour].size]
            at = lead + ((b, slice(None)) if colour == 0 else (slice(None), b)) + rest
            refs[colour][at] = part if first else refs[colour][at] + part

    def rows_of(slots):
        return pl.ds(slots[0], len(slots)), len(slots) * rows

    def grad_out(v, slots):
        some, count = rows_of(slots)
        for i in HALVES:
            cols = pl.ds(i * 2 * pf, 2 * pf)
            g = mm_tn(us[v, some, :, cols].reshape(count, 2 * pf), eb[v, some].reshape(count, dm)).reshape(2, NA, fr, dm)
            for b in HALVES:
                keep(gout, v, (2 * i + b,), g[b], OUT_COLS, OWN in slots)

    def grad_in(v, slots):
        some, count = rows_of(slots)
        for which, dref in enumerate((das, dbs)):
            for i in QUARTERS:
                cols = pl.ds(i * (dm // NA), dm // NA)
                g = mm_tn(ng[v, some, :, cols].reshape(count, dm // NA), dref[some].reshape(count, fs)).reshape(NA, NA, dr, fs)
                for y in QUARTERS:
                    keep([ref.at[v, which] for ref in gin], None, (i + p * (y - i), y + p * (i - y)), g[y], IN_COLS, OWN in slots)

    IN, OUT = 0, 1

    def view(which, st, v, colour, t, half):
        own = jb if colour == 0 else xc
        if which == IN:
            ref = gin[colour].at[v, half]
            return ref.at[t] if st == 0 else ref.at[own, t]
        ref = gout[colour].at[v]
        return ref.at[t, pl.ds(2 * half, 2)] if st == 0 else ref.at[own, t, pl.ds(half * (fr // 2), fr // 2)]

    RECV = (((rg[0], rg[1]), (rg[2], rg[3])), ((rg[4], rg[5]), (rg[6], rg[7])))
    MERGED, DIRECT = ((0, OPP, PLUS, 0), (1, OPP, MINUS, 1)), ((1, PLUS, PLUS, 2), (0, MINUS, MINUS, 3))
    RELAYED = ((0, PLUS, PLUS, 4), (1, MINUS, MINUS, 5))

    def axis_of(colour, st):
        return (jb, peer_b) if colour == st else (xc, functools.partial(peer, X))

    def scatter_send(v, which, st, copies):
        for colour in COLOURS:
            q, to = axis_of(colour, st)
            for half, c, delta, slot in copies:
                send(view(which, st, v, colour, rot(q, c), half), RECV[st][which][colour].at[v, slot],
                     rs_s.at[st, v, colour, which], rs_r.at[st, v, colour, which, slot], to(delta), p)

    def scatter_relay(v, which, st):
        for colour in COLOURS:
            q, _ = axis_of(colour, st)
            recv = RECV[st][which][colour]
            for half, c, _, slot in RELAYED:
                wait_recv(recv.at[v, slot - 4], rs_r.at[st, v, colour, which, slot - 4])
                ref = view(which, st, v, colour, rot(q, c), half)
                ref[...] = ref[...] + recv[v, slot - 4]
        scatter_send(v, which, st, RELAYED)

    def scatter_sum(v, which, st):
        for colour in COLOURS:
            q, _ = axis_of(colour, st)
            recv = RECV[st][which][colour]
            for half in HALVES:
                direct, merged = 3 - half, 4 + half
                for slot in (direct, merged):
                    wait_recv(recv.at[v, slot], rs_r.at[st, v, colour, which, slot])
                ref = view(which, st, v, colour, q, half)
                ref[...] = ref[...] + recv[v, direct] + recv[v, merged]

    def scatter_turn(v, which):
        scatter_sum(v, which, 0)
        scatter_send(v, which, 1, MERGED + DIRECT)

    def scatter_out(v):
        scatter_sum(v, OUT, 1)
        for colour in COLOURS:
            go[v, :, OUT_COLS[colour]] = gout[colour][(v, jb, xc) if colour == 0 else (v, xc, jb)]

    def scatter_last(v):
        scatter_sum(v, IN, 1)
        for which in HALVES:
            for colour in COLOURS:
                fin[v, :, which, :, IN_COLS[colour]] = gin[colour][(v, which, jb, xc) if colour == 0 else (v, which, xc, jb)]
        for delta in (OPP, PLUS, MINUS):
            send(fin.at[v, rot(ja, delta)], r3.at[v, delta - 1], r3_s.at[v], r3_r.at[v, delta - 1], peer_a(delta), p)

    def scatter_finish(v):
        def put(j, vals):
            for i in QUARTERS:
                z, y = piece(j, i)
                cols = pl.ds(pl.multiple_of((z * NA + y) * pf, pf), pf)
                gg[v, :, cols] = vals(0)[:, i * pf:(i + 1) * pf]
                gi[v, :, cols] = vals(1)[:, i * pf:(i + 1) * pf]

        put(ja, lambda w: fin[v, ja, w])
        for delta in RING:
            wait_recv(r3.at[v, delta - 1], r3_r.at[v, delta - 1])
            put(rot(ja, -delta), lambda w, delta=delta: r3[v, delta - 1, w])

    def step(fn, *args):
        with jax.named_scope(fn.__name__):
            fn(*args)

    def on(core):
        return pl.when(p == core)

    def take_turn():
        pl.semaphore_wait(turn, 1)

    def give_turn():
        pl.semaphore_signal(turn, inc=1, device_id=(d, 1 - p), device_id_type=MESH)

    h_mid, h_late, e_first, e_last = ((xo.at[i], mc_s.at[1 + i]) for i in QUARTERS)

    def pass_on(part, item, buf, which, vd):
        step(part, item[0], buf, which, vd, item[1])

    AFTER = (MINUS, OPP), (0, PLUS)
    step(direct_send, 0)
    step(small_send, 1, 0)

    @on(0)
    def _():
        step(spread_same, hb, 0, 0, mc_s.at[0])

    step(direct_wait, 0)
    step(small_send, 0, 1)
    step(small_relay, 1, 0)
    step(large_send, 0, (0,), (0,))
    step(small_rest, 1, 0)
    step(small_last, 1, 0)
    step(small_send, 1, 1)
    step(small_relay, 0, 1)
    step(small_relay, 1, 1)
    step(small_rest, 0, 1)
    step(large_send, 0, (PLUS, MINUS), (MINUS, PLUS))
    step(small_last, 0, 1)
    step(large_send, 0, (OPP,), (OPP,))
    step(small_rest, 1, 1)
    step(small_last, 1, 1)
    step(large_relay, 0)

    @on(0)
    def _():
        step(large_send, 1, UP, DOWN)

    step(large_finish, 0, UP_MATS)

    @on(0)
    def _():
        step(large_send, 1, *AFTER)

    @on(1)
    def _():
        step(take_turn)
        step(large_send, 1, UP, DOWN)
        step(spread_own, hb, 0, 0)

    step(block_gates, 0)

    @on(1)
    def _():
        step(large_send, 1, *AFTER)

    step(large_finish, 0, OUT_MAT)
    step(block_out, 0, h_mid[0])
    pass_on(spread_near, h_mid, hb, 0, p)
    step(large_relay, 1)

    @on(0)
    def _():
        step(give_turn)
        step(spread_relay, hb, 0, 0)

    @on(1)
    def _():
        pass_on(spread_far, h_mid, hb, 0, p)
        step(spread_same, eb, 1, 1, mc_s.at[0])

    step(spread_own, hb, 0, 1)
    step(large_finish, 1, UP_MATS)
    step(block_gates, 1)
    step(large_finish, 1, OUT_MAT)

    @on(0)
    def _():
        step(block_out, 1, h_late[0])
        pass_on(spread_near, h_late, hb, 0, 1)
        pass_on(spread_far, h_late, hb, 0, 1)
        pass_on(spread_far, h_mid, hb, 0, p)
        step(spread_finish, hb, 0, 0)
        step(grad_first, 0, EARLY)
        step(grad_first, 0, LATE)
        step(spread_relay, hb, 0, 1)
        step(grad_first, 1, EARLY)
        step(spread_own, eb, 1, 1)
        step(block_backward, 1, e_first[0])
        pass_on(spread_near, e_first, eb, 1, 0)
        pass_on(spread_far, e_first, eb, 1, 0)
        step(spread_finish, hb, 0, 1)
        step(grad_first, 1, LATE)

    @on(1)
    def _():
        step(block_backward, 1, e_first[0])
        pass_on(spread_near, e_first, eb, 1, 1)
        pass_on(spread_far, e_first, eb, 1, 1)
        step(spread_relay, hb, 0, 1)
        step(grad_first, 1, EARLY)
        step(spread_relay, hb, 0, 0)

    step(spread_relay, eb, 1, 1)

    step(grad_hidden, 1, EARLY)
    step(grad_out, 1, EARLY)
    step(grad_in, 1, EARLY)

    @on(1)
    def _():
        step(spread_own, eb, 1, 0)
        step(block_backward, 0, e_last[0])
        pass_on(spread_near, e_last, eb, 1, 0)
        pass_on(spread_far, e_last, eb, 1, 0)
        step(spread_finish, hb, 0, 1)
        step(grad_first, 1, LATE)

    step(spread_finish, eb, 1, 1)
    step(grad_hidden, 1, LATE)
    step(grad_out, 1, LATE)
    step(scatter_send, 1, OUT, 0, MERGED)
    step(grad_in, 1, LATE)
    step(scatter_send, 1, IN, 0, MERGED)
    step(scatter_send, 1, OUT, 0, DIRECT)
    step(scatter_send, 1, IN, 0, DIRECT)

    @on(0)
    def _():
        step(spread_relay, eb, 1, 0)
        step(spread_own, eb, 1, 0)

    @on(1)
    def _():
        step(grad_first, 0, EARLY)
        step(spread_relay, eb, 1, 0)
        step(spread_finish, hb, 0, 0)
        step(grad_first, 0, LATE)

    step(grad_hidden, 0, EARLY)
    step(grad_in, 0, EARLY)
    step(grad_out, 0, EARLY)
    step(scatter_relay, 1, OUT, 0)
    step(spread_finish, eb, 1, 0)
    step(grad_hidden, 0, LATE)
    step(grad_in, 0, LATE)
    step(scatter_send, 0, IN, 0, MERGED)
    step(grad_out, 0, LATE)
    step(scatter_relay, 1, IN, 0)
    step(scatter_send, 0, OUT, 0, MERGED)
    step(scatter_send, 0, IN, 0, DIRECT)

    @on(0)
    def _():
        step(block_backward, 0, ga)
        send(ga, ga, ga_s, ga_r, d, 1)

    step(scatter_turn, 1, OUT)
    step(scatter_relay, 0, IN, 0)
    step(scatter_send, 0, OUT, 0, DIRECT)
    step(scatter_turn, 1, IN)
    step(scatter_relay, 0, OUT, 0)
    step(scatter_relay, 1, OUT, 1)

    @on(1)
    def _():
        wait_recv(ga, ga_r)

    gact[...] = ga[...]
    step(scatter_turn, 0, IN)
    step(scatter_relay, 1, IN, 1)
    step(scatter_turn, 0, OUT)
    step(scatter_relay, 0, IN, 1)
    step(scatter_out, 1)
    step(scatter_last, 1)
    step(scatter_relay, 0, OUT, 1)
    step(scatter_last, 0)
    step(scatter_finish, 1)
    step(scatter_out, 0)
    step(scatter_finish, 0)

    for v in BLOCKS:
        for k in MATS:
            three = pl.ds(0, len(RING))
            wait_send(part_at(v, k, three, 0, 0), ag_s.at[v, k, 0])
            wait_send(part_at(v, k, whole, three, 0), ag_s.at[v, k, 1])
            wait_send(part_at(v, k, whole, whole, three), ag_s.at[v, k, LARGE])
        for colour in COLOURS:
            for which in HALVES:
                for st in HALVES:
                    wait_send(RECV[st][which][colour].at[v], rs_s.at[st, v, colour, which])
        wait_send(r3.at[v], r3_s.at[v])
        wait_send(hb.at[v, 0], rl_s.at[0, v])
        wait_send(hb.at[v, 0], rl_s.at[1, v])
    wait_send(hb.at[0, pl.ds(0, 2)], mc_s.at[0])
    wait_send(hb.at[0, pl.ds(0, 3)], mc_s.at[1])
    wait_send(hb.at[0, pl.ds(0, 3)], mc_s.at[3])

    @pl.when(p == 0)
    def _():
        wait_send(hb.at[0, pl.ds(0, 3)], mc_s.at[2])
        wait_send(ga, ga_s)

    @pl.when(p == 1)
    def _():
        wait_send(hb.at[0, pl.ds(0, 3)], mc_s.at[4])


def hand_on(*refs):
    copies = [pltpu.make_async_copy(refs[i], refs[NA + i], refs[-1].at[i]) for i in QUARTERS]
    for copy in copies:
        copy.start()
    for copy in copies:
        copy.wait()


def solution(mesh):
    act_spec = P(None, "data", None, None)
    w_spec = P(None, "stage", "data", None)

    def body(act_in, cot_out, w_gate, w_in, w_out):
        shape = act_in.shape
        dm, fd = shape[3], w_gate.shape[3]
        rows = shape[0] * shape[1] * shape[2]
        dr, fr, fs = dm // NL, fd // NL, fd // NA
        pf = fs // NA
        vmem = pltpu.VMEM
        dma = pltpu.SemaphoreType.DMA
        n2, n3, na = NB, len(RING), NA
        ring = (na, na)
        scratch = [
            vmem((n2, na, *ring, dr, fd), BF), vmem((n2, na, *ring, dr, fd), BF), vmem((n2, na, *ring, fr, dm), BF),
            vmem((n2, na, rows, dm), BF), vmem((n2, na, rows, dm), BF), vmem((na, rows, dm), BF), vmem((rows, dm), BF),
            vmem((n2, na, rows, dm), BF),
            vmem((n2, rows, fd), F32), vmem((n2, rows, fd), F32),
            vmem((n2, na, rows, fs), F32), vmem((n2, na, rows, fs), F32),
            vmem((n2, na, rows, fs), BF),
            vmem((rows, fd), BF), vmem((rows, fd), BF), vmem((rows, fd), BF),
            vmem((na, rows, fs), BF), vmem((na, rows, fs), BF),
            vmem((rows, dm), F32),
            vmem((n2, dm, fs), BF), vmem((n2, dm, fs), BF), vmem((fs, dm), BF),
            *(vmem((n2, n2, *ring, na, dr, width), F32) for width in (fs - pf, pf)),
            *(vmem((n2, *ring, fr, width), F32) for width in (dm - pf, pf)),
            vmem((n2, na, n2, dr, fs), F32), vmem((n2, n3, n2, dr, fs), F32),
            dma((n2, na)), dma((n2, n3, n3)), dma((n2, n3, n2, 6)), dma((n2, n3, n3 * na)), dma((5,)), dma((n2, n2, 7)), dma((n2, n2)), dma, dma,
            dma((n2, n2, n2, n2)), dma((n2, n2, n2, n2, 6)), dma((n2,)), dma((n2, n3)), pltpu.SemaphoreType.REGULAR,
            *(vmem((n2, 6, *lead, width), F32)
              for lead_in, lead_out in (((*ring, dr), (n2, fr)), ((na, dr), (fr // n2,)))
              for lead, width in ((lead_in, fs - pf), (lead_in, pf), (lead_out, dm - pf), (lead_out, pf))),
        ]
        hbm = pl.BlockSpec(memory_space=pl.ANY)
        whole = pl.BlockSpec(memory_space=pltpu.VMEM)
        out = pl.pallas_call(
            kernel,
            out_shape=(
                vmem((rows, dm), BF), vmem((n2, dr, fd), F32), vmem((n2, dr, fd), F32), vmem((n2, fr, dm), F32),
            ),
            in_specs=[hbm] * 5,
            out_specs=(whole,) * NA,
            scratch_shapes=scratch,
            compiler_params=pltpu.CompilerParams(collective_id=0, has_side_effects=True, vmem_limit_bytes=66300000),
            name="train_step",
        )(act_in.reshape(rows, dm), cot_out.reshape(rows, dm), w_gate[:, 0], w_in[:, 0], w_out[:, 0])
        grad_act, grad_gate, grad_lin, grad_proj = pl.pallas_call(
            hand_on, out_shape=tuple(jax.ShapeDtypeStruct(a.shape, a.dtype) for a in out), in_specs=[whole] * NA, out_specs=(hbm,) * NA,
            scratch_shapes=[dma((NA,))], compiler_params=pltpu.CompilerParams(vmem_limit_bytes=2 ** 20), name="hand_on",
        )(*(pltpu.with_memory_space_constraint(a, vmem) for a in out))
        return grad_act.reshape(shape), grad_gate[:, None], grad_lin[:, None], grad_proj[:, None]

    return jax.shard_map(body, mesh=mesh, in_specs=(act_spec, act_spec, w_spec, w_spec, w_spec),
                         out_specs=(act_spec, w_spec, w_spec, w_spec), check_vma=False)
```

```python
import functools

import jax
import jax.numpy as jnp
from jax import lax
from jax.experimental import pallas as pl
from jax.experimental.pallas import tpu as pltpu
from jax.sharding import PartitionSpec as P

NORM_EPS = 1e-6
BF = jnp.bfloat16
F32 = jnp.float32
MESH = pl.DeviceIdType.MESH
X, Y, Z = 0, 1, 2
BLOCKS = COLOURS = HALVES = (0, 1)
NB, NA, NL = len(BLOCKS), 4, 64
RING = (1, 3, 2)
OPP = RING[-1]
PLUS, MINUS = RING[:-1]
QUARTERS = range(NA)
OWN = 0
AXES = ((Z, X, Y), (Y, Z, X), (X, Y, Z))
UP_MATS, OUT_MAT = (0, 1), (2,)
MATS = UP_MATS + OUT_MAT


def mm(left, right):
    return jnp.dot(left, right, preferred_element_type=F32)


def mm_nt(left, right):
    return lax.dot_general(left, right, (((1,), (1,)), ((), ())), preferred_element_type=F32)


def mm_tn(left, right):
    return lax.dot_general(left, right, (((0,), (0,)), ((), ())), preferred_element_type=F32)


def inv_rms(h):
    return lax.rsqrt(jnp.mean(h * h, axis=-1, keepdims=True) + NORM_EPS)


def kernel(act, cot, wg_in, wi_in, wo_in, gact, gg, gi, go,
           wg, wi, wo, hb, eb, xo, ga, ng, f1, f2, f1s, f2s, us, ub, da, db, das, dbs, qs, gs, is_, os_,
           gin0, gin1, gout0, gout1, fin, r3,
           lsem, ag_s, ag_r, lg_r, mc_s, mc_r, rl_s, ga_s, ga_r, rs_s, rs_r, r3_s, r3_r, turn, *rg):
    dm, fd = wo.shape[-1], wg.shape[-1]
    dr, fr = dm // NL, fd // NL
    fs = fd // NA
    pf = fs // NA
    rows = act.shape[0]
    wts = (wg, wi, wo)
    gin, gout = (gin0, gin1), (gout0, gout1)

    p = lax.axis_index("stage")
    d = lax.axis_index("data")
    zc, yc, xc = lax.div(d, 16), lax.rem(lax.div(d, 4), 4), lax.rem(d, 4)
    coord = (xc, yc, zc)
    stride = (1, 4, 16)
    ja = yc + p * (zc - yc)
    jb = zc + p * (yc - zc)
    sa, sb = 4 + 12 * p, 16 - 12 * p

    def rot(c, delta):
        return lax.rem(c + (delta % 4), 4)

    def peer(ax, delta):
        return d + (rot(coord[ax], delta) - coord[ax]) * stride[ax]

    def peer_a(delta):
        return d + (rot(ja, delta) - ja) * sa

    def peer_b(delta):
        return d + (rot(jb, delta) - jb) * sb

    def remote(src, dst, ssem, rsem, dev, core):
        return pltpu.make_async_remote_copy(src_ref=src, dst_ref=dst, send_sem=ssem, recv_sem=rsem,
                                            device_id=(dev, core), device_id_type=MESH)

    def send(src, dst, ssem, rsem, dev, core):
        remote(src, dst, ssem, rsem, dev, core).start()

    def wait_recv(ref, sem):
        remote(ref, ref, sem, sem, d, p).wait_recv()

    def wait_send(ref, sem):
        remote(ref, ref, sem, sem, d, p).wait_send()

    for v in BLOCKS:
        for k, shard in enumerate((wg_in, wi_in, wo_in)):
            pltpu.make_async_copy(shard.at[v], wts[k].at[v, zc, yc, xc], lsem.at[v, k]).start()

    @pl.when(p == 0)
    def _():
        pltpu.make_async_copy(act, hb.at[0, OWN], lsem.at[0, 3]).start()

    @pl.when(p == 1)
    def _():
        pltpu.make_async_copy(cot, eb.at[1, OWN], lsem.at[0, 3]).start()

    barrier = pltpu.get_barrier_semaphore()
    senders = [(peer(ax, delta), p) for ax in (X, Y, Z) for delta in RING]
    senders += [(d, 1 - p), (peer_a(1), 1 - p), (peer_a(-1), 1 - p)]
    for dev, core in senders:
        pl.semaphore_signal(barrier, inc=1, device_id=(dev, core), device_id_type=MESH)
    for v in BLOCKS:
        for k, shard in enumerate((wg_in, wi_in, wo_in)):
            pltpu.make_async_copy(shard.at[v], wts[k].at[v, zc, yc, xc], lsem.at[v, k]).wait()

    @pl.when(p == 0)
    def _():
        pltpu.make_async_copy(act, hb.at[0, OWN], lsem.at[0, 3]).wait()

    @pl.when(p == 1)
    def _():
        pltpu.make_async_copy(cot, eb.at[1, OWN], lsem.at[0, 3]).wait()

    pl.semaphore_wait(barrier, len(senders))

    FIRST, REST = ((0, PLUS, 0), (1, MINUS, 2)), ((1, PLUS, 1), (0, MINUS, 3))
    LARGE = 2
    whole = slice(None)

    def part_at(v, k, small, middle, large, half=None):
        place = dict(zip(AXES[k], (small, middle, large)))
        width = wts[k].shape[-1] // 2
        cols = whole if half is None else pl.ds(half * width, width)
        return wts[k].at[v, place[Z], place[Y], place[X], :, cols]

    def own(k):
        return [coord[ax] for ax in AXES[k]]

    def chunk(v, k, ph, q, half):
        small, middle, large = own(k)
        return part_at(v, k, q, middle, large, half) if ph == 0 else part_at(v, k, pl.ds(2 * half, 2), q, large)

    def small_copy(v, k, ph, q, half, delta, slot):
        ref = chunk(v, k, ph, q, half)
        send(ref, ref, ag_s.at[v, k, ph], ag_r.at[v, k, ph, slot], peer(AXES[k][ph], delta), p)

    def small_wait(v, k, ph, back, half, slot):
        wait_recv(chunk(v, k, ph, rot(coord[AXES[k][ph]], back), half), ag_r.at[v, k, ph, slot])

    def small_send(v, ph):
        for half, delta, slot in FIRST + REST:
            for k in MATS:
                small_copy(v, k, ph, coord[AXES[k][ph]], half, delta, slot)

    def small_relay(v, ph):
        for half, delta, slot in FIRST:
            for k in MATS:
                small_wait(v, k, ph, -delta, half, slot)
                small_copy(v, k, ph, rot(coord[AXES[k][ph]], -delta), half, delta, 4 + half)

    def small_rest(v, ph):
        for half, delta, slot in REST:
            for k in MATS:
                small_wait(v, k, ph, -delta, half, slot)

    def small_last(v, ph):
        for half in HALVES:
            for k in MATS:
                small_wait(v, k, ph, OPP, half, 4 + half)

    def direct_send(v):
        for delta in (OPP, PLUS, MINUS):
            for k in MATS:
                ref = part_at(v, k, *own(k))
                send(ref, ref, ag_s.at[v, k, 0], ag_r.at[v, k, 0, delta], peer(AXES[k][0], delta), p)

    def direct_wait(v):
        for delta in RING:
            for k in MATS:
                small, middle, large = own(k)
                wait_recv(part_at(v, k, rot(small, -delta), middle, large), ag_r.at[v, k, 0, delta])

    UP, DOWN = (0, PLUS), (MINUS, OPP)
    RELAYS = ((UP[0], PLUS), (DOWN[0], MINUS), (UP[1], PLUS), (DOWN[1], MINUS))

    def row(v, k, q, r):
        return part_at(v, k, whole, rot(coord[AXES[k][1]], r), q)

    def large_slot(r, delta):
        return r if delta == PLUS else NA + r

    def large_send(v, up, down):
        for pair in zip(up, down):
            for r, delta in zip(pair, (PLUS, MINUS)):
                for k in MATS:
                    ax = AXES[k][LARGE]
                    ref = row(v, k, coord[ax], r)
                    send(ref, ref, ag_s.at[v, k, LARGE], lg_r.at[v, k, large_slot(r, delta)], peer(ax, delta), p)

    def large_relay(v):
        for r, delta in RELAYS:
            for k in MATS:
                ax = AXES[k][LARGE]
                ref = row(v, k, rot(coord[ax], -delta), r)
                wait_recv(ref, lg_r.at[v, k, large_slot(r, delta)])
                send(ref, ref, ag_s.at[v, k, LARGE], lg_r.at[v, k, 2 * NA + r], peer(ax, delta), p)

    def large_finish(v, mats):
        for pieces, delta in ((DOWN, PLUS), (UP, MINUS)):
            for r in pieces:
                for k in mats:
                    wait_recv(row(v, k, rot(coord[AXES[k][LARGE]], -delta), r), lg_r.at[v, k, large_slot(r, delta)])
        for r in QUARTERS:
            for k in mats:
                wait_recv(row(v, k, rot(coord[AXES[k][LARGE]], OPP), r), lg_r.at[v, k, 2 * NA + r])

    half_rows = rows // 2
    BACK, AHEAD, FAR = 1, 2, 3

    def spread_near(src, buf, which, vd, ssem):
        send(src, buf.at[vd, OWN], ssem, mc_r.at[which, vd, OWN], d, 1 - p)

    def rows_half(half):
        return pl.ds(half * half_rows, half_rows)

    HALF_ORDER = [(half if first else 1 - half, slot, delta, slot if first else FAR + 1 + slot)
                  for first in (True, False) for half, slot, delta in ((0, BACK, PLUS), (1, AHEAD, MINUS))]

    def spread_far(src, buf, which, vd, ssem):
        for half, slot, delta, sem in HALF_ORDER:
            send(src.at[rows_half(half)], buf.at[vd, slot, rows_half(half)], ssem, mc_r.at[which, vd, sem], peer_b(delta), 1 - p)

    def spread_same(buf, which, v, ssem):
        for half, slot, delta, sem in HALF_ORDER:
            send(buf.at[v, OWN, rows_half(half)], buf.at[v, slot, rows_half(half)], ssem, mc_r.at[which, v, sem], peer_a(delta), p)

    def spread_relay(buf, which, v):
        for half, slot, delta, sem in HALF_ORDER:
            ref = buf.at[v, slot, rows_half(half)]
            wait_recv(ref, mc_r.at[which, v, sem])
            if sem == slot:
                send(ref, buf.at[v, FAR, rows_half(half)], rl_s.at[which, v], mc_r.at[which, v, FAR + half], peer_a(delta), p)

    def spread_finish(buf, which, v):
        for half in HALVES:
            wait_recv(buf.at[v, FAR, rows_half(half)], mc_r.at[which, v, FAR + half])

    def spread_own(buf, which, v):
        wait_recv(buf.at[v, OWN], mc_r.at[which, v, OWN])

    def gates(n, wgt, wlin):
        a, b = mm(n, wgt), mm(n, wlin)
        s = jax.nn.sigmoid(a)
        act_a = a * s
        return (act_a * b).astype(BF), b * s * (1.0 + a * (1.0 - s)), act_a

    def block_gates(v):
        h = hb[v, OWN].astype(F32)
        n = (h * inv_rms(h)).astype(BF)

        def tile(i, carry):
            wide = fs // 2
            cols = pl.ds(pl.multiple_of(i * wide, wide), wide)
            u, t1, t2 = gates(n, wg[v, :, :, :, :, cols].reshape(dm, wide), wi[v, :, :, :, :, cols].reshape(dm, wide))
            ub[:, cols] = u
            f1[v, :, cols] = t1
            f2[v, :, cols] = t2
            return carry

        lax.fori_loop(0, 2 * NA, tile, 0, unroll=True)

    def block_out(v, dst):
        half_dm = dm // 2
        for i in HALVES:
            cols = pl.ds(i * half_dm, half_dm)
            out = mm(ub[...], wo[v, :, :, :, :, cols].reshape(fd, half_dm))
            dst[:, cols] = (hb[v, OWN, :, cols].astype(F32) + out).astype(BF)

    def block_backward(v, dst):
        e = eb[v, OWN]

        def tile(i, carry):
            cols = pl.ds(pl.multiple_of(i * fs, fs), fs)
            t = mm_nt(e, wo[v, i].reshape(fs, dm))
            da[:, cols] = (t * f1[v, :, cols]).astype(BF)
            db[:, cols] = (t * f2[v, :, cols]).astype(BF)
            return carry

        lax.fori_loop(0, NA, tile, 0, unroll=True)
        half_dm = dm // 2
        for i in HALVES:
            q = mm_nt(da[...], wg[v, pl.ds(2 * i, 2)].reshape(half_dm, fd))
            q += mm_nt(db[...], wi[v, pl.ds(2 * i, 2)].reshape(half_dm, fd))
            qs[:, pl.ds(i * half_dm, half_dm)] = q
        h = hb[v, OWN].astype(F32)
        r = inv_rms(h)
        hr = h * r
        q = qs[...]
        dst[...] = (e.astype(F32) + r * (q - hr * jnp.mean(q * hr, axis=-1, keepdims=True))).astype(BF)

    def piece(j, i):
        z = i + p * (j - i)
        y = j + p * (i - j)
        return z, y

    EARLY, LATE = range(FAR), range(FAR, NA)

    def grad_first(v, slots):
        for i in QUARTERS if OWN in slots else ():
            z, y = piece(ja, i)
            cols = pl.ds(pl.multiple_of((z * NA + y) * pf, pf), pf)
            gs[v, :, pl.ds(i * pf, pf)] = wg[v, :, :, :, :, cols].reshape(dm, pf)
            is_[v, :, pl.ds(i * pf, pf)] = wi[v, :, :, :, :, cols].reshape(dm, pf)
        for s in slots:
            h = hb[v, s].astype(F32)
            n = (h * inv_rms(h)).astype(BF)
            ng[v, s] = n
            u, t1, t2 = gates(n, gs[v], is_[v])
            us[v, s] = u
            f1s[v, s] = t1
            f2s[v, s] = t2

    def grad_hidden(v, slots):
        for i in QUARTERS if OWN in slots else ():
            z, y = piece(ja, i)
            os_[pl.ds(i * pf, pf), :] = wo[v, z, y].reshape(pf, dm)
        for s in slots:
            t = mm_nt(eb[v, s], os_[...])
            das[s] = (t * f1s[v, s]).astype(BF)
            dbs[s] = (t * f2s[v, s]).astype(BF)

    def split(width, second):
        return pl.ds(0, width - second), pl.ds(width - second, second)

    IN_COLS, OUT_COLS = split(fs, pf), split(dm, pf)

    def keep(refs, v, place, tile, cols, first):
        b, rest = place[0], place[1:]
        lead = () if v is None else (v,)
        for colour in COLOURS:
            part = tile[..., cols[colour].start:cols[colour].start + cols[colour].size]
            at = lead + ((b, slice(None)) if colour == 0 else (slice(None), b)) + rest
            refs[colour][at] = part if first else refs[colour][at] + part

    def rows_of(slots):
        return pl.ds(slots[0], len(slots)), len(slots) * rows

    def grad_out(v, slots):
        some, count = rows_of(slots)
        for i in HALVES:
            cols = pl.ds(i * 2 * pf, 2 * pf)
            g = mm_tn(us[v, some, :, cols].reshape(count, 2 * pf), eb[v, some].reshape(count, dm)).reshape(2, NA, fr, dm)
            for b in HALVES:
                keep(gout, v, (2 * i + b,), g[b], OUT_COLS, OWN in slots)

    def grad_in(v, slots):
        some, count = rows_of(slots)
        for which, dref in enumerate((das, dbs)):
            for i in QUARTERS:
                cols = pl.ds(i * (dm // NA), dm // NA)
                g = mm_tn(ng[v, some, :, cols].reshape(count, dm // NA), dref[some].reshape(count, fs)).reshape(NA, NA, dr, fs)
                for y in QUARTERS:
                    keep([ref.at[v, which] for ref in gin], None, (i + p * (y - i), y + p * (i - y)), g[y], IN_COLS, OWN in slots)

    IN, OUT = 0, 1

    def view(which, st, v, colour, t, half):
        own = jb if colour == 0 else xc
        if which == IN:
            ref = gin[colour].at[v, half]
            return ref.at[t] if st == 0 else ref.at[own, t]
        ref = gout[colour].at[v]
        return ref.at[t, pl.ds(2 * half, 2)] if st == 0 else ref.at[own, t, pl.ds(half * (fr // 2), fr // 2)]

    RECV = (((rg[0], rg[1]), (rg[2], rg[3])), ((rg[4], rg[5]), (rg[6], rg[7])))
    MERGED, DIRECT = ((0, OPP, PLUS, 0), (1, OPP, MINUS, 1)), ((1, PLUS, PLUS, 2), (0, MINUS, MINUS, 3))
    RELAYED = ((0, PLUS, PLUS, 4), (1, MINUS, MINUS, 5))

    def axis_of(colour, st):
        return (jb, peer_b) if colour == st else (xc, functools.partial(peer, X))

    def scatter_send(v, which, st, copies):
        for colour in COLOURS:
            q, to = axis_of(colour, st)
            for half, c, delta, slot in copies:
                send(view(which, st, v, colour, rot(q, c), half), RECV[st][which][colour].at[v, slot],
                     rs_s.at[st, v, colour, which], rs_r.at[st, v, colour, which, slot], to(delta), p)

    def scatter_relay(v, which, st):
        for colour in COLOURS:
            q, _ = axis_of(colour, st)
            recv = RECV[st][which][colour]
            for half, c, _, slot in RELAYED:
                wait_recv(recv.at[v, slot - 4], rs_r.at[st, v, colour, which, slot - 4])
                ref = view(which, st, v, colour, rot(q, c), half)
                ref[...] = ref[...] + recv[v, slot - 4]
        scatter_send(v, which, st, RELAYED)

    def scatter_sum(v, which, st):
        for colour in COLOURS:
            q, _ = axis_of(colour, st)
            recv = RECV[st][which][colour]
            for half in HALVES:
                direct, merged = 3 - half, 4 + half
                for slot in (direct, merged):
                    wait_recv(recv.at[v, slot], rs_r.at[st, v, colour, which, slot])
                ref = view(which, st, v, colour, q, half)
                ref[...] = ref[...] + recv[v, direct] + recv[v, merged]

    def scatter_turn(v, which):
        scatter_sum(v, which, 0)
        scatter_send(v, which, 1, MERGED + DIRECT)

    def scatter_out(v):
        scatter_sum(v, OUT, 1)
        for colour in COLOURS:
            go[v, :, OUT_COLS[colour]] = gout[colour][(v, jb, xc) if colour == 0 else (v, xc, jb)]

    def scatter_last(v):
        scatter_sum(v, IN, 1)
        for which in HALVES:
            for colour in COLOURS:
                fin[v, :, which, :, IN_COLS[colour]] = gin[colour][(v, which, jb, xc) if colour == 0 else (v, which, xc, jb)]
        for delta in (OPP, PLUS, MINUS):
            send(fin.at[v, rot(ja, delta)], r3.at[v, delta - 1], r3_s.at[v], r3_r.at[v, delta - 1], peer_a(delta), p)

    def scatter_finish(v):
        def put(j, vals):
            for i in QUARTERS:
                z, y = piece(j, i)
                cols = pl.ds(pl.multiple_of((z * NA + y) * pf, pf), pf)
                gg[v, :, cols] = vals(0)[:, i * pf:(i + 1) * pf]
                gi[v, :, cols] = vals(1)[:, i * pf:(i + 1) * pf]

        put(ja, lambda w: fin[v, ja, w])
        for delta in RING:
            wait_recv(r3.at[v, delta - 1], r3_r.at[v, delta - 1])
            put(rot(ja, -delta), lambda w, delta=delta: r3[v, delta - 1, w])

    def step(fn, *args):
        with jax.named_scope(fn.__name__):
            fn(*args)

    def on(core):
        return pl.when(p == core)

    def take_turn():
        pl.semaphore_wait(turn, 1)

    def give_turn():
        pl.semaphore_signal(turn, inc=1, device_id=(d, 1 - p), device_id_type=MESH)

    h_mid, h_late, e_first, e_last = ((xo.at[i], mc_s.at[1 + i]) for i in QUARTERS)

    def pass_on(part, item, buf, which, vd):
        step(part, item[0], buf, which, vd, item[1])

    AFTER = (MINUS, OPP), (0, PLUS)
    step(direct_send, 0)
    step(small_send, 1, 0)

    @on(0)
    def _():
        step(spread_same, hb, 0, 0, mc_s.at[0])

    step(direct_wait, 0)
    step(small_send, 0, 1)
    step(small_relay, 1, 0)
    step(large_send, 0, (0,), (0,))
    step(small_rest, 1, 0)
    step(small_last, 1, 0)
    step(small_send, 1, 1)
    step(small_relay, 0, 1)
    step(small_relay, 1, 1)
    step(small_rest, 0, 1)
    step(large_send, 0, (PLUS, MINUS), (MINUS, PLUS))
    step(small_last, 0, 1)
    step(large_send, 0, (OPP,), (OPP,))
    step(small_rest, 1, 1)
    step(small_last, 1, 1)
    step(large_relay, 0)

    @on(0)
    def _():
        step(large_send, 1, UP, DOWN)

    step(large_finish, 0, UP_MATS)

    @on(0)
    def _():
        step(large_send, 1, *AFTER)

    @on(1)
    def _():
        step(take_turn)
        step(large_send, 1, UP, DOWN)
        step(spread_own, hb, 0, 0)

    step(block_gates, 0)

    @on(1)
    def _():
        step(large_send, 1, *AFTER)

    step(large_finish, 0, OUT_MAT)
    step(block_out, 0, h_mid[0])
    pass_on(spread_near, h_mid, hb, 0, p)
    step(large_relay, 1)

    @on(0)
    def _():
        step(give_turn)
        step(spread_relay, hb, 0, 0)

    @on(1)
    def _():
        pass_on(spread_far, h_mid, hb, 0, p)
        step(spread_same, eb, 1, 1, mc_s.at[0])

    step(spread_own, hb, 0, 1)
    step(large_finish, 1, UP_MATS)
    step(block_gates, 1)
    step(large_finish, 1, OUT_MAT)

    @on(0)
    def _():
        step(block_out, 1, h_late[0])
        pass_on(spread_near, h_late, hb, 0, 1)
        pass_on(spread_far, h_late, hb, 0, 1)
        pass_on(spread_far, h_mid, hb, 0, p)
        step(spread_finish, hb, 0, 0)
        step(grad_first, 0, EARLY)
        step(grad_first, 0, LATE)
        step(spread_relay, hb, 0, 1)
        step(grad_first, 1, EARLY)
        step(spread_own, eb, 1, 1)
        step(block_backward, 1, e_first[0])
        pass_on(spread_near, e_first, eb, 1, 0)
        pass_on(spread_far, e_first, eb, 1, 0)
        step(spread_finish, hb, 0, 1)
        step(grad_first, 1, LATE)

    @on(1)
    def _():
        step(block_backward, 1, e_first[0])
        pass_on(spread_near, e_first, eb, 1, 1)
        pass_on(spread_far, e_first, eb, 1, 1)
        step(spread_relay, hb, 0, 1)
        step(grad_first, 1, EARLY)

    step(spread_relay, eb, 1, 1)

    step(grad_hidden, 1, EARLY)
    step(grad_out, 1, EARLY)
    step(grad_in, 1, EARLY)

    @on(1)
    def _():
        step(spread_own, eb, 1, 0)
        step(block_backward, 0, e_last[0])
        pass_on(spread_near, e_last, eb, 1, 0)
        pass_on(spread_far, e_last, eb, 1, 0)
        step(spread_relay, hb, 0, 0)
        step(spread_finish, hb, 0, 1)
        step(grad_first, 1, LATE)

    step(spread_finish, eb, 1, 1)
    step(grad_hidden, 1, LATE)
    step(grad_out, 1, LATE)
    step(scatter_send, 1, OUT, 0, MERGED)
    step(grad_in, 1, LATE)
    step(scatter_send, 1, IN, 0, MERGED)
    step(scatter_send, 1, OUT, 0, DIRECT)
    step(scatter_send, 1, IN, 0, DIRECT)

    @on(0)
    def _():
        step(spread_relay, eb, 1, 0)
        step(spread_own, eb, 1, 0)

    @on(1)
    def _():
        step(grad_first, 0, EARLY)
        step(spread_relay, eb, 1, 0)
        step(spread_finish, hb, 0, 0)
        step(grad_first, 0, LATE)

    step(grad_hidden, 0, EARLY)
    step(grad_in, 0, EARLY)
    step(grad_out, 0, EARLY)
    step(scatter_relay, 1, OUT, 0)
    step(spread_finish, eb, 1, 0)
    step(grad_hidden, 0, LATE)
    step(grad_in, 0, LATE)
    step(scatter_send, 0, IN, 0, MERGED)
    step(grad_out, 0, LATE)
    step(scatter_relay, 1, IN, 0)
    step(scatter_send, 0, OUT, 0, MERGED)
    step(scatter_send, 0, IN, 0, DIRECT)

    @on(0)
    def _():
        step(block_backward, 0, ga)
        send(ga, ga, ga_s, ga_r, d, 1)

    step(scatter_turn, 1, OUT)
    step(scatter_relay, 0, IN, 0)
    step(scatter_send, 0, OUT, 0, DIRECT)
    step(scatter_turn, 1, IN)
    step(scatter_relay, 0, OUT, 0)
    step(scatter_relay, 1, OUT, 1)

    @on(1)
    def _():
        wait_recv(ga, ga_r)

    gact[...] = ga[...]
    step(scatter_turn, 0, IN)
    step(scatter_relay, 1, IN, 1)
    step(scatter_turn, 0, OUT)
    step(scatter_relay, 0, IN, 1)
    step(scatter_out, 1)
    step(scatter_last, 1)
    step(scatter_relay, 0, OUT, 1)
    step(scatter_last, 0)
    step(scatter_finish, 1)
    step(scatter_out, 0)
    step(scatter_finish, 0)

    for v in BLOCKS:
        for k in MATS:
            three = pl.ds(0, len(RING))
            wait_send(part_at(v, k, three, 0, 0), ag_s.at[v, k, 0])
            wait_send(part_at(v, k, whole, three, 0), ag_s.at[v, k, 1])
            wait_send(part_at(v, k, whole, whole, three), ag_s.at[v, k, LARGE])
        for colour in COLOURS:
            for which in HALVES:
                for st in HALVES:
                    wait_send(RECV[st][which][colour].at[v], rs_s.at[st, v, colour, which])
        wait_send(r3.at[v], r3_s.at[v])
        wait_send(hb.at[v, 0], rl_s.at[0, v])
        wait_send(hb.at[v, 0], rl_s.at[1, v])
    wait_send(hb.at[0, pl.ds(0, 2)], mc_s.at[0])
    wait_send(hb.at[0, pl.ds(0, 3)], mc_s.at[1])
    wait_send(hb.at[0, pl.ds(0, 3)], mc_s.at[3])

    @pl.when(p == 0)
    def _():
        wait_send(hb.at[0, pl.ds(0, 3)], mc_s.at[2])
        wait_send(ga, ga_s)

    @pl.when(p == 1)
    def _():
        wait_send(hb.at[0, pl.ds(0, 3)], mc_s.at[4])


def hand_on(*refs):
    copies = [pltpu.make_async_copy(refs[i], refs[NA + i], refs[-1].at[i]) for i in QUARTERS]
    for copy in copies:
        copy.start()
    for copy in copies:
        copy.wait()


def solution(mesh):
    act_spec = P(None, "data", None, None)
    w_spec = P(None, "stage", "data", None)

    def body(act_in, cot_out, w_gate, w_in, w_out):
        shape = act_in.shape
        dm, fd = shape[3], w_gate.shape[3]
        rows = shape[0] * shape[1] * shape[2]
        dr, fr, fs = dm // NL, fd // NL, fd // NA
        pf = fs // NA
        vmem = pltpu.VMEM
        dma = pltpu.SemaphoreType.DMA
        n2, n3, na = NB, len(RING), NA
        ring = (na, na)
        scratch = [
            vmem((n2, na, *ring, dr, fd), BF), vmem((n2, na, *ring, dr, fd), BF), vmem((n2, na, *ring, fr, dm), BF),
            vmem((n2, na, rows, dm), BF), vmem((n2, na, rows, dm), BF), vmem((na, rows, dm), BF), vmem((rows, dm), BF),
            vmem((n2, na, rows, dm), BF),
            vmem((n2, rows, fd), F32), vmem((n2, rows, fd), F32),
            vmem((n2, na, rows, fs), F32), vmem((n2, na, rows, fs), F32),
            vmem((n2, na, rows, fs), BF),
            vmem((rows, fd), BF), vmem((rows, fd), BF), vmem((rows, fd), BF),
            vmem((na, rows, fs), BF), vmem((na, rows, fs), BF),
            vmem((rows, dm), F32),
            vmem((n2, dm, fs), BF), vmem((n2, dm, fs), BF), vmem((fs, dm), BF),
            *(vmem((n2, n2, *ring, na, dr, width), F32) for width in (fs - pf, pf)),
            *(vmem((n2, *ring, fr, width), F32) for width in (dm - pf, pf)),
            vmem((n2, na, n2, dr, fs), F32), vmem((n2, n3, n2, dr, fs), F32),
            dma((n2, na)), dma((n2, n3, n3)), dma((n2, n3, n2, 6)), dma((n2, n3, n3 * na)), dma((5,)), dma((n2, n2, 7)), dma((n2, n2)), dma, dma,
            dma((n2, n2, n2, n2)), dma((n2, n2, n2, n2, 6)), dma((n2,)), dma((n2, n3)), pltpu.SemaphoreType.REGULAR,
            *(vmem((n2, 6, *lead, width), F32)
              for lead_in, lead_out in (((*ring, dr), (n2, fr)), ((na, dr), (fr // n2,)))
              for lead, width in ((lead_in, fs - pf), (lead_in, pf), (lead_out, dm - pf), (lead_out, pf))),
        ]
        hbm = pl.BlockSpec(memory_space=pl.ANY)
        whole = pl.BlockSpec(memory_space=pltpu.VMEM)
        out = pl.pallas_call(
            kernel,
            out_shape=(
                vmem((rows, dm), BF), vmem((n2, dr, fd), F32), vmem((n2, dr, fd), F32), vmem((n2, fr, dm), F32),
            ),
            in_specs=[hbm] * 5,
            out_specs=(whole,) * NA,
            scratch_shapes=scratch,
            compiler_params=pltpu.CompilerParams(collective_id=0, has_side_effects=True, vmem_limit_bytes=66300000),
            name="train_step",
        )(act_in.reshape(rows, dm), cot_out.reshape(rows, dm), w_gate[:, 0], w_in[:, 0], w_out[:, 0])
        grad_act, grad_gate, grad_lin, grad_proj = pl.pallas_call(
            hand_on, out_shape=tuple(jax.ShapeDtypeStruct(a.shape, a.dtype) for a in out), in_specs=[whole] * NA, out_specs=(hbm,) * NA,
            scratch_shapes=[dma((NA,))], compiler_params=pltpu.CompilerParams(vmem_limit_bytes=2 ** 20), name="hand_on",
        )(*(pltpu.with_memory_space_constraint(a, vmem) for a in out))
        return grad_act.reshape(shape), grad_gate[:, None], grad_lin[:, None], grad_proj[:, None]

    return jax.shard_map(body, mesh=mesh, in_specs=(act_spec, act_spec, w_spec, w_spec, w_spec),
                         out_specs=(act_spec, w_spec, w_spec, w_spec), check_vma=False)
```

```python
import functools

import jax
import jax.numpy as jnp
from jax import lax
from jax.experimental import pallas as pl
from jax.experimental.pallas import tpu as pltpu
from jax.sharding import PartitionSpec as P

NORM_EPS = 1e-6
BF = jnp.bfloat16
F32 = jnp.float32
MESH = pl.DeviceIdType.MESH
X, Y, Z = 0, 1, 2
BLOCKS = COLOURS = HALVES = (0, 1)
NB, NA, NL = len(BLOCKS), 4, 64
RING = (1, 3, 2)
OPP = RING[-1]
PLUS, MINUS = RING[:-1]
QUARTERS = range(NA)
OWN = 0
AXES = ((Z, X, Y), (Y, Z, X), (X, Y, Z))
UP_MATS, OUT_MAT = (0, 1), (2,)
MATS = UP_MATS + OUT_MAT


def mm(left, right):
    return jnp.dot(left, right, preferred_element_type=F32)


def mm_nt(left, right):
    return lax.dot_general(left, right, (((1,), (1,)), ((), ())), preferred_element_type=F32)


def mm_tn(left, right):
    return lax.dot_general(left, right, (((0,), (0,)), ((), ())), preferred_element_type=F32)


def inv_rms(h):
    return lax.rsqrt(jnp.mean(h * h, axis=-1, keepdims=True) + NORM_EPS)


def kernel(act, cot, wg_in, wi_in, wo_in, gact, gg, gi, go,
           wg, wi, wo, hb, eb, xo, ga, ng, f1, f2, f1s, f2s, us, ub, da, db, das, dbs, qs, gs, is_, os_,
           gin0, gin1, gout0, gout1, fin, r3,
           lsem, ag_s, ag_r, lg_r, mc_s, mc_r, rl_s, ga_s, ga_r, rs_s, rs_r, r3_s, r3_r, turn, *rg):
    dm, fd = wo.shape[-1], wg.shape[-1]
    dr, fr = dm // NL, fd // NL
    fs = fd // NA
    pf = fs // NA
    rows = act.shape[0]
    wts = (wg, wi, wo)
    gin, gout = (gin0, gin1), (gout0, gout1)

    p = lax.axis_index("stage")
    d = lax.axis_index("data")
    zc, yc, xc = lax.div(d, 16), lax.rem(lax.div(d, 4), 4), lax.rem(d, 4)
    coord = (xc, yc, zc)
    stride = (1, 4, 16)
    ja = yc + p * (zc - yc)
    jb = zc + p * (yc - zc)
    sa, sb = 4 + 12 * p, 16 - 12 * p

    def rot(c, delta):
        return lax.rem(c + (delta % 4), 4)

    def peer(ax, delta):
        return d + (rot(coord[ax], delta) - coord[ax]) * stride[ax]

    def peer_a(delta):
        return d + (rot(ja, delta) - ja) * sa

    def peer_b(delta):
        return d + (rot(jb, delta) - jb) * sb

    def remote(src, dst, ssem, rsem, dev, core):
        return pltpu.make_async_remote_copy(src_ref=src, dst_ref=dst, send_sem=ssem, recv_sem=rsem,
                                            device_id=(dev, core), device_id_type=MESH)

    def send(src, dst, ssem, rsem, dev, core):
        remote(src, dst, ssem, rsem, dev, core).start()

    def wait_recv(ref, sem):
        remote(ref, ref, sem, sem, d, p).wait_recv()

    def wait_send(ref, sem):
        remote(ref, ref, sem, sem, d, p).wait_send()

    for v in BLOCKS:
        for k, shard in enumerate((wg_in, wi_in, wo_in)):
            pltpu.make_async_copy(shard.at[v], wts[k].at[v, zc, yc, xc], lsem.at[v, k]).start()

    @pl.when(p == 0)
    def _():
        pltpu.make_async_copy(act, hb.at[0, OWN], lsem.at[0, 3]).start()

    @pl.when(p == 1)
    def _():
        pltpu.make_async_copy(cot, eb.at[1, OWN], lsem.at[0, 3]).start()

    barrier = pltpu.get_barrier_semaphore()
    senders = [(peer(ax, delta), p) for ax in (X, Y, Z) for delta in RING]
    senders += [(d, 1 - p), (peer_a(1), 1 - p), (peer_a(-1), 1 - p)]
    for dev, core in senders:
        pl.semaphore_signal(barrier, inc=1, device_id=(dev, core), device_id_type=MESH)
    for v in BLOCKS:
        for k, shard in enumerate((wg_in, wi_in, wo_in)):
            pltpu.make_async_copy(shard.at[v], wts[k].at[v, zc, yc, xc], lsem.at[v, k]).wait()

    @pl.when(p == 0)
    def _():
        pltpu.make_async_copy(act, hb.at[0, OWN], lsem.at[0, 3]).wait()

    @pl.when(p == 1)
    def _():
        pltpu.make_async_copy(cot, eb.at[1, OWN], lsem.at[0, 3]).wait()

    pl.semaphore_wait(barrier, len(senders))

    FIRST, REST = ((0, PLUS, 0), (1, MINUS, 2)), ((1, PLUS, 1), (0, MINUS, 3))
    LARGE = 2
    whole = slice(None)

    def part_at(v, k, small, middle, large, half=None):
        place = dict(zip(AXES[k], (small, middle, large)))
        width = wts[k].shape[-1] // 2
        cols = whole if half is None else pl.ds(half * width, width)
        return wts[k].at[v, place[Z], place[Y], place[X], :, cols]

    def own(k):
        return [coord[ax] for ax in AXES[k]]

    def chunk(v, k, ph, q, half):
        small, middle, large = own(k)
        return part_at(v, k, q, middle, large, half) if ph == 0 else part_at(v, k, pl.ds(2 * half, 2), q, large)

    def small_copy(v, k, ph, q, half, delta, slot):
        ref = chunk(v, k, ph, q, half)
        send(ref, ref, ag_s.at[v, k, ph], ag_r.at[v, k, ph, slot], peer(AXES[k][ph], delta), p)

    def small_wait(v, k, ph, back, half, slot):
        wait_recv(chunk(v, k, ph, rot(coord[AXES[k][ph]], back), half), ag_r.at[v, k, ph, slot])

    def small_send(v, ph):
        for half, delta, slot in FIRST + REST:
            for k in MATS:
                small_copy(v, k, ph, coord[AXES[k][ph]], half, delta, slot)

    def small_relay(v, ph):
        for half, delta, slot in FIRST:
            for k in MATS:
                small_wait(v, k, ph, -delta, half, slot)
                small_copy(v, k, ph, rot(coord[AXES[k][ph]], -delta), half, delta, 4 + half)

    def small_rest(v, ph):
        for half, delta, slot in REST:
            for k in MATS:
                small_wait(v, k, ph, -delta, half, slot)

    def small_last(v, ph):
        for half in HALVES:
            for k in MATS:
                small_wait(v, k, ph, OPP, half, 4 + half)

    def direct_send(v):
        for delta in (OPP, PLUS, MINUS):
            for k in MATS:
                ref = part_at(v, k, *own(k))
                send(ref, ref, ag_s.at[v, k, 0], ag_r.at[v, k, 0, delta], peer(AXES[k][0], delta), p)

    def direct_wait(v):
        for delta in RING:
            for k in MATS:
                small, middle, large = own(k)
                wait_recv(part_at(v, k, rot(small, -delta), middle, large), ag_r.at[v, k, 0, delta])

    UP, DOWN = (0, PLUS), (MINUS, OPP)
    RELAYS = ((UP[0], PLUS), (DOWN[0], MINUS), (UP[1], PLUS), (DOWN[1], MINUS))

    def row(v, k, q, r):
        return part_at(v, k, whole, rot(coord[AXES[k][1]], r), q)

    def large_slot(r, delta):
        return r if delta == PLUS else NA + r

    def large_send(v, up, down):
        for pair in zip(up, down):
            for r, delta in zip(pair, (PLUS, MINUS)):
                for k in MATS:
                    ax = AXES[k][LARGE]
                    ref = row(v, k, coord[ax], r)
                    send(ref, ref, ag_s.at[v, k, LARGE], lg_r.at[v, k, large_slot(r, delta)], peer(ax, delta), p)

    def large_relay(v):
        for r, delta in RELAYS:
            for k in MATS:
                ax = AXES[k][LARGE]
                ref = row(v, k, rot(coord[ax], -delta), r)
                wait_recv(ref, lg_r.at[v, k, large_slot(r, delta)])
                send(ref, ref, ag_s.at[v, k, LARGE], lg_r.at[v, k, 2 * NA + r], peer(ax, delta), p)

    def large_finish(v, mats):
        for pieces, delta in ((DOWN, PLUS), (UP, MINUS)):
            for r in pieces:
                for k in mats:
                    wait_recv(row(v, k, rot(coord[AXES[k][LARGE]], -delta), r), lg_r.at[v, k, large_slot(r, delta)])
        for r in QUARTERS:
            for k in mats:
                wait_recv(row(v, k, rot(coord[AXES[k][LARGE]], OPP), r), lg_r.at[v, k, 2 * NA + r])

    half_rows = rows // 2
    BACK, AHEAD, FAR = 1, 2, 3

    def spread_near(src, buf, which, vd, ssem):
        send(src, buf.at[vd, OWN], ssem, mc_r.at[which, vd, OWN], d, 1 - p)

    def rows_half(half):
        return pl.ds(half * half_rows, half_rows)

    HALF_ORDER = [(half if first else 1 - half, slot, delta, slot if first else FAR + 1 + slot)
                  for first in (True, False) for half, slot, delta in ((0, BACK, PLUS), (1, AHEAD, MINUS))]

    def spread_far(src, buf, which, vd, ssem):
        for half, slot, delta, sem in HALF_ORDER:
            send(src.at[rows_half(half)], buf.at[vd, slot, rows_half(half)], ssem, mc_r.at[which, vd, sem], peer_b(delta), 1 - p)

    def spread_same(buf, which, v, ssem):
        for half, slot, delta, sem in HALF_ORDER:
            send(buf.at[v, OWN, rows_half(half)], buf.at[v, slot, rows_half(half)], ssem, mc_r.at[which, v, sem], peer_a(delta), p)

    def spread_relay(buf, which, v):
        for half, slot, delta, sem in HALF_ORDER:
            ref = buf.at[v, slot, rows_half(half)]
            wait_recv(ref, mc_r.at[which, v, sem])
            if sem == slot:
                send(ref, buf.at[v, FAR, rows_half(half)], rl_s.at[which, v], mc_r.at[which, v, FAR + half], peer_a(delta), p)

    def spread_finish(buf, which, v):
        for half in HALVES:
            wait_recv(buf.at[v, FAR, rows_half(half)], mc_r.at[which, v, FAR + half])

    def spread_own(buf, which, v):
        wait_recv(buf.at[v, OWN], mc_r.at[which, v, OWN])

    def gates(n, wgt, wlin):
        a, b = mm(n, wgt), mm(n, wlin)
        s = jax.nn.sigmoid(a)
        act_a = a * s
        return (act_a * b).astype(BF), b * s * (1.0 + a * (1.0 - s)), act_a

    def block_gates(v):
        h = hb[v, OWN].astype(F32)
        n = (h * inv_rms(h)).astype(BF)

        def tile(i, carry):
            wide = fs // 2
            cols = pl.ds(pl.multiple_of(i * wide, wide), wide)
            u, t1, t2 = gates(n, wg[v, :, :, :, :, cols].reshape(dm, wide), wi[v, :, :, :, :, cols].reshape(dm, wide))
            ub[:, cols] = u
            f1[v, :, cols] = t1
            f2[v, :, cols] = t2
            return carry

        lax.fori_loop(0, 2 * NA, tile, 0, unroll=True)

    def block_out(v, dst):
        half_dm = dm // 2
        for i in HALVES:
            cols = pl.ds(i * half_dm, half_dm)
            out = mm(ub[...], wo[v, :, :, :, :, cols].reshape(fd, half_dm))
            dst[:, cols] = (hb[v, OWN, :, cols].astype(F32) + out).astype(BF)

    def block_backward(v, dst):
        e = eb[v, OWN]

        def tile(i, carry):
            cols = pl.ds(pl.multiple_of(i * fs, fs), fs)
            t = mm_nt(e, wo[v, i].reshape(fs, dm))
            da[:, cols] = (t * f1[v, :, cols]).astype(BF)
            db[:, cols] = (t * f2[v, :, cols]).astype(BF)
            return carry

        lax.fori_loop(0, NA, tile, 0, unroll=True)
        half_dm = dm // 2
        for i in HALVES:
            q = mm_nt(da[...], wg[v, pl.ds(2 * i, 2)].reshape(half_dm, fd))
            q += mm_nt(db[...], wi[v, pl.ds(2 * i, 2)].reshape(half_dm, fd))
            qs[:, pl.ds(i * half_dm, half_dm)] = q
        h = hb[v, OWN].astype(F32)
        r = inv_rms(h)
        hr = h * r
        q = qs[...]
        dst[...] = (e.astype(F32) + r * (q - hr * jnp.mean(q * hr, axis=-1, keepdims=True))).astype(BF)

    def piece(j, i):
        z = i + p * (j - i)
        y = j + p * (i - j)
        return z, y

    EARLY, LATE = range(FAR), range(FAR, NA)

    def grad_first(v, slots):
        for i in QUARTERS if OWN in slots else ():
            z, y = piece(ja, i)
            cols = pl.ds(pl.multiple_of((z * NA + y) * pf, pf), pf)
            gs[v, :, pl.ds(i * pf, pf)] = wg[v, :, :, :, :, cols].reshape(dm, pf)
            is_[v, :, pl.ds(i * pf, pf)] = wi[v, :, :, :, :, cols].reshape(dm, pf)
        for s in slots:
            h = hb[v, s].astype(F32)
            n = (h * inv_rms(h)).astype(BF)
            ng[v, s] = n
            u, t1, t2 = gates(n, gs[v], is_[v])
            us[v, s] = u
            f1s[v, s] = t1
            f2s[v, s] = t2

    def grad_hidden(v, slots):
        for i in QUARTERS if OWN in slots else ():
            z, y = piece(ja, i)
            os_[pl.ds(i * pf, pf), :] = wo[v, z, y].reshape(pf, dm)
        for s in slots:
            t = mm_nt(eb[v, s], os_[...])
            das[s] = (t * f1s[v, s]).astype(BF)
            dbs[s] = (t * f2s[v, s]).astype(BF)

    def split(width, second):
        return pl.ds(0, width - second), pl.ds(width - second, second)

    IN_COLS, OUT_COLS = split(fs, pf), split(dm, pf)

    def keep(refs, v, place, tile, cols, first):
        b, rest = place[0], place[1:]
        lead = () if v is None else (v,)
        for colour in COLOURS:
            part = tile[..., cols[colour].start:cols[colour].start + cols[colour].size]
            at = lead + ((b, slice(None)) if colour == 0 else (slice(None), b)) + rest
            refs[colour][at] = part if first else refs[colour][at] + part

    def rows_of(slots):
        return pl.ds(slots[0], len(slots)), len(slots) * rows

    def grad_out(v, slots):
        some, count = rows_of(slots)
        for i in HALVES:
            cols = pl.ds(i * 2 * pf, 2 * pf)
            g = mm_tn(us[v, some, :, cols].reshape(count, 2 * pf), eb[v, some].reshape(count, dm)).reshape(2, NA, fr, dm)
            for b in HALVES:
                keep(gout, v, (2 * i + b,), g[b], OUT_COLS, OWN in slots)

    def grad_in(v, slots):
        some, count = rows_of(slots)
        for which, dref in enumerate((das, dbs)):
            for i in QUARTERS:
                cols = pl.ds(i * (dm // NA), dm // NA)
                g = mm_tn(ng[v, some, :, cols].reshape(count, dm // NA), dref[some].reshape(count, fs)).reshape(NA, NA, dr, fs)
                for y in QUARTERS:
                    keep([ref.at[v, which] for ref in gin], None, (i + p * (y - i), y + p * (i - y)), g[y], IN_COLS, OWN in slots)

    IN, OUT = 0, 1

    def view(which, st, v, colour, t, half):
        own = jb if colour == 0 else xc
        if which == IN:
            ref = gin[colour].at[v, half]
            return ref.at[t] if st == 0 else ref.at[own, t]
        ref = gout[colour].at[v]
        return ref.at[t, pl.ds(2 * half, 2)] if st == 0 else ref.at[own, t, pl.ds(half * (fr // 2), fr // 2)]

    RECV = (((rg[0], rg[1]), (rg[2], rg[3])), ((rg[4], rg[5]), (rg[6], rg[7])))
    MERGED, DIRECT = ((0, OPP, PLUS, 0), (1, OPP, MINUS, 1)), ((1, PLUS, PLUS, 2), (0, MINUS, MINUS, 3))
    RELAYED = ((0, PLUS, PLUS, 4), (1, MINUS, MINUS, 5))

    def axis_of(colour, st):
        return (jb, peer_b) if colour == st else (xc, functools.partial(peer, X))

    def scatter_send(v, which, st, copies):
        for colour in COLOURS:
            q, to = axis_of(colour, st)
            for half, c, delta, slot in copies:
                send(view(which, st, v, colour, rot(q, c), half), RECV[st][which][colour].at[v, slot],
                     rs_s.at[st, v, colour, which], rs_r.at[st, v, colour, which, slot], to(delta), p)

    def scatter_relay(v, which, st):
        for colour in COLOURS:
            q, _ = axis_of(colour, st)
            recv = RECV[st][which][colour]
            for half, c, _, slot in RELAYED:
                wait_recv(recv.at[v, slot - 4], rs_r.at[st, v, colour, which, slot - 4])
                ref = view(which, st, v, colour, rot(q, c), half)
                ref[...] = ref[...] + recv[v, slot - 4]
        scatter_send(v, which, st, RELAYED)

    def scatter_sum(v, which, st):
        for colour in COLOURS:
            q, _ = axis_of(colour, st)
            recv = RECV[st][which][colour]
            for half in HALVES:
                direct, merged = 3 - half, 4 + half
                for slot in (direct, merged):
                    wait_recv(recv.at[v, slot], rs_r.at[st, v, colour, which, slot])
                ref = view(which, st, v, colour, q, half)
                ref[...] = ref[...] + recv[v, direct] + recv[v, merged]

    def scatter_turn(v, which):
        scatter_sum(v, which, 0)
        scatter_send(v, which, 1, MERGED + DIRECT)

    def scatter_out(v):
        scatter_sum(v, OUT, 1)
        for colour in COLOURS:
            go[v, :, OUT_COLS[colour]] = gout[colour][(v, jb, xc) if colour == 0 else (v, xc, jb)]

    def scatter_last(v):
        scatter_sum(v, IN, 1)
        for which in HALVES:
            for colour in COLOURS:
                fin[v, :, which, :, IN_COLS[colour]] = gin[colour][(v, which, jb, xc) if colour == 0 else (v, which, xc, jb)]
        for delta in (OPP, PLUS, MINUS):
            send(fin.at[v, rot(ja, delta)], r3.at[v, delta - 1], r3_s.at[v], r3_r.at[v, delta - 1], peer_a(delta), p)

    def scatter_finish(v):
        def put(j, vals):
            for i in QUARTERS:
                z, y = piece(j, i)
                cols = pl.ds(pl.multiple_of((z * NA + y) * pf, pf), pf)
                gg[v, :, cols] = vals(0)[:, i * pf:(i + 1) * pf]
                gi[v, :, cols] = vals(1)[:, i * pf:(i + 1) * pf]

        put(ja, lambda w: fin[v, ja, w])
        for delta in RING:
            wait_recv(r3.at[v, delta - 1], r3_r.at[v, delta - 1])
            put(rot(ja, -delta), lambda w, delta=delta: r3[v, delta - 1, w])

    def step(fn, *args):
        with jax.named_scope(fn.__name__):
            fn(*args)

    def on(core):
        return pl.when(p == core)

    def take_turn():
        pl.semaphore_wait(turn, 1)

    def give_turn():
        pl.semaphore_signal(turn, inc=1, device_id=(d, 1 - p), device_id_type=MESH)

    h_mid, h_late, e_first, e_last = ((xo.at[i], mc_s.at[1 + i]) for i in QUARTERS)

    def pass_on(part, item, buf, which, vd):
        step(part, item[0], buf, which, vd, item[1])

    AFTER = (MINUS, OPP), (0, PLUS)
    step(direct_send, 0)
    step(small_send, 1, 0)
    step(direct_wait, 0)
    step(small_send, 0, 1)
    step(small_relay, 1, 0)
    step(large_send, 0, (0,), (0,))
    step(small_rest, 1, 0)
    step(small_last, 1, 0)
    step(small_send, 1, 1)
    step(small_relay, 0, 1)
    step(small_relay, 1, 1)
    step(small_rest, 0, 1)
    step(large_send, 0, (PLUS, MINUS), (MINUS, PLUS))
    step(small_last, 0, 1)
    step(large_send, 0, (OPP,), (OPP,))
    step(small_rest, 1, 1)
    step(small_last, 1, 1)
    step(large_relay, 0)

    @on(0)
    def _():
        step(large_send, 1, UP, DOWN)

    step(large_finish, 0, UP_MATS)

    @on(0)
    def _():
        step(large_send, 1, *AFTER)

    @on(1)
    def _():
        step(take_turn)
        step(large_send, 1, UP, DOWN)
        step(spread_own, hb, 0, 0)

    step(block_gates, 0)

    @on(1)
    def _():
        step(large_send, 1, *AFTER)

    step(large_finish, 0, OUT_MAT)
    step(block_out, 0, h_mid[0])
    pass_on(spread_near, h_mid, hb, 0, p)
    step(large_relay, 1)

    @on(0)
    def _():
        step(give_turn)

    @on(1)
    def _():
        pass_on(spread_far, h_mid, hb, 0, p)
        step(spread_same, eb, 1, 1, mc_s.at[0])

    step(spread_own, hb, 0, 1)
    step(large_finish, 1, UP_MATS)
    step(block_gates, 1)
    step(large_finish, 1, OUT_MAT)

    @on(0)
    def _():
        step(block_out, 1, h_late[0])
        pass_on(spread_near, h_late, hb, 0, 1)
        pass_on(spread_far, h_late, hb, 0, 1)
        pass_on(spread_far, h_mid, hb, 0, p)
        step(spread_same, hb, 0, 0, mc_s.at[0])
        step(spread_own, eb, 1, 1)
        step(block_backward, 1, e_first[0])
        pass_on(spread_near, e_first, eb, 1, 0)
        pass_on(spread_far, e_first, eb, 1, 0)
        step(spread_relay, hb, 0, 1)
        step(grad_first, 1, EARLY)

    @on(1)
    def _():
        step(block_backward, 1, e_first[0])
        pass_on(spread_near, e_first, eb, 1, 1)
        pass_on(spread_far, e_first, eb, 1, 1)
        step(spread_relay, hb, 0, 1)
        step(grad_first, 1, EARLY)

    step(spread_relay, eb, 1, 1)

    step(grad_hidden, 1, EARLY)
    step(grad_out, 1, EARLY)
    step(grad_in, 1, EARLY)

    @on(0)
    def _():
        step(spread_relay, hb, 0, 0)
        step(spread_finish, hb, 0, 1)
        step(grad_first, 1, LATE)

    @on(1)
    def _():
        step(spread_own, eb, 1, 0)
        step(block_backward, 0, e_last[0])
        pass_on(spread_near, e_last, eb, 1, 0)
        pass_on(spread_far, e_last, eb, 1, 0)
        step(spread_relay, hb, 0, 0)
        step(spread_finish, hb, 0, 1)
        step(grad_first, 1, LATE)

    step(spread_finish, eb, 1, 1)
    step(grad_hidden, 1, LATE)
    step(grad_out, 1, LATE)
    step(scatter_send, 1, OUT, 0, MERGED)
    step(grad_in, 1, LATE)
    step(scatter_send, 1, IN, 0, MERGED)
    step(scatter_send, 1, OUT, 0, DIRECT)
    step(scatter_send, 1, IN, 0, DIRECT)

    @on(0)
    def _():
        step(grad_first, 0, EARLY)
        step(spread_relay, eb, 1, 0)
        step(spread_finish, hb, 0, 0)
        step(grad_first, 0, LATE)
        step(spread_own, eb, 1, 0)

    @on(1)
    def _():
        step(grad_first, 0, EARLY)
        step(spread_relay, eb, 1, 0)
        step(spread_finish, hb, 0, 0)
        step(grad_first, 0, LATE)

    step(grad_hidden, 0, EARLY)
    step(grad_in, 0, EARLY)
    step(grad_out, 0, EARLY)
    step(scatter_relay, 1, OUT, 0)
    step(spread_finish, eb, 1, 0)
    step(grad_hidden, 0, LATE)
    step(grad_in, 0, LATE)
    step(scatter_send, 0, IN, 0, MERGED)
    step(grad_out, 0, LATE)
    step(scatter_relay, 1, IN, 0)
    step(scatter_send, 0, OUT, 0, MERGED)
    step(scatter_send, 0, IN, 0, DIRECT)

    @on(0)
    def _():
        step(block_backward, 0, ga)
        send(ga, ga, ga_s, ga_r, d, 1)

    step(scatter_turn, 1, OUT)
    step(scatter_relay, 0, IN, 0)
    step(scatter_send, 0, OUT, 0, DIRECT)
    step(scatter_turn, 1, IN)
    step(scatter_relay, 0, OUT, 0)
    step(scatter_relay, 1, OUT, 1)

    @on(1)
    def _():
        wait_recv(ga, ga_r)

    gact[...] = ga[...]
    step(scatter_turn, 0, IN)
    step(scatter_relay, 1, IN, 1)
    step(scatter_turn, 0, OUT)
    step(scatter_relay, 0, IN, 1)
    step(scatter_out, 1)
    step(scatter_last, 1)
    step(scatter_relay, 0, OUT, 1)
    step(scatter_last, 0)
    step(scatter_finish, 1)
    step(scatter_out, 0)
    step(scatter_finish, 0)

    for v in BLOCKS:
        for k in MATS:
            three = pl.ds(0, len(RING))
            wait_send(part_at(v, k, three, 0, 0), ag_s.at[v, k, 0])
            wait_send(part_at(v, k, whole, three, 0), ag_s.at[v, k, 1])
            wait_send(part_at(v, k, whole, whole, three), ag_s.at[v, k, LARGE])
        for colour in COLOURS:
            for which in HALVES:
                for st in HALVES:
                    wait_send(RECV[st][which][colour].at[v], rs_s.at[st, v, colour, which])
        wait_send(r3.at[v], r3_s.at[v])
        wait_send(hb.at[v, 0], rl_s.at[0, v])
        wait_send(hb.at[v, 0], rl_s.at[1, v])
    wait_send(hb.at[0, pl.ds(0, 2)], mc_s.at[0])
    wait_send(hb.at[0, pl.ds(0, 3)], mc_s.at[1])
    wait_send(hb.at[0, pl.ds(0, 3)], mc_s.at[3])

    @pl.when(p == 0)
    def _():
        wait_send(hb.at[0, pl.ds(0, 3)], mc_s.at[2])
        wait_send(ga, ga_s)

    @pl.when(p == 1)
    def _():
        wait_send(hb.at[0, pl.ds(0, 3)], mc_s.at[4])


def hand_on(*refs):
    copies = [pltpu.make_async_copy(refs[i], refs[NA + i], refs[-1].at[i]) for i in QUARTERS]
    for copy in copies:
        copy.start()
    for copy in copies:
        copy.wait()


def solution(mesh):
    act_spec = P(None, "data", None, None)
    w_spec = P(None, "stage", "data", None)

    def body(act_in, cot_out, w_gate, w_in, w_out):
        shape = act_in.shape
        dm, fd = shape[3], w_gate.shape[3]
        rows = shape[0] * shape[1] * shape[2]
        dr, fr, fs = dm // NL, fd // NL, fd // NA
        pf = fs // NA
        vmem = pltpu.VMEM
        dma = pltpu.SemaphoreType.DMA
        n2, n3, na = NB, len(RING), NA
        ring = (na, na)
        scratch = [
            vmem((n2, na, *ring, dr, fd), BF), vmem((n2, na, *ring, dr, fd), BF), vmem((n2, na, *ring, fr, dm), BF),
            vmem((n2, na, rows, dm), BF), vmem((n2, na, rows, dm), BF), vmem((na, rows, dm), BF), vmem((rows, dm), BF),
            vmem((n2, na, rows, dm), BF),
            vmem((n2, rows, fd), F32), vmem((n2, rows, fd), F32),
            vmem((n2, na, rows, fs), F32), vmem((n2, na, rows, fs), F32),
            vmem((n2, na, rows, fs), BF),
            vmem((rows, fd), BF), vmem((rows, fd), BF), vmem((rows, fd), BF),
            vmem((na, rows, fs), BF), vmem((na, rows, fs), BF),
            vmem((rows, dm), F32),
            vmem((n2, dm, fs), BF), vmem((n2, dm, fs), BF), vmem((fs, dm), BF),
            *(vmem((n2, n2, *ring, na, dr, width), F32) for width in (fs - pf, pf)),
            *(vmem((n2, *ring, fr, width), F32) for width in (dm - pf, pf)),
            vmem((n2, na, n2, dr, fs), F32), vmem((n2, n3, n2, dr, fs), F32),
            dma((n2, na)), dma((n2, n3, n3)), dma((n2, n3, n2, 6)), dma((n2, n3, n3 * na)), dma((5,)), dma((n2, n2, 7)), dma((n2, n2)), dma, dma,
            dma((n2, n2, n2, n2)), dma((n2, n2, n2, n2, 6)), dma((n2,)), dma((n2, n3)), pltpu.SemaphoreType.REGULAR,
            *(vmem((n2, 6, *lead, width), F32)
              for lead_in, lead_out in (((*ring, dr), (n2, fr)), ((na, dr), (fr // n2,)))
              for lead, width in ((lead_in, fs - pf), (lead_in, pf), (lead_out, dm - pf), (lead_out, pf))),
        ]
        hbm = pl.BlockSpec(memory_space=pl.ANY)
        whole = pl.BlockSpec(memory_space=pltpu.VMEM)
        out = pl.pallas_call(
            kernel,
            out_shape=(
                vmem((rows, dm), BF), vmem((n2, dr, fd), F32), vmem((n2, dr, fd), F32), vmem((n2, fr, dm), F32),
            ),
            in_specs=[hbm] * 5,
            out_specs=(whole,) * NA,
            scratch_shapes=scratch,
            compiler_params=pltpu.CompilerParams(collective_id=0, has_side_effects=True, vmem_limit_bytes=66300000),
            name="train_step",
        )(act_in.reshape(rows, dm), cot_out.reshape(rows, dm), w_gate[:, 0], w_in[:, 0], w_out[:, 0])
        grad_act, grad_gate, grad_lin, grad_proj = pl.pallas_call(
            hand_on, out_shape=tuple(jax.ShapeDtypeStruct(a.shape, a.dtype) for a in out), in_specs=[whole] * NA, out_specs=(hbm,) * NA,
            scratch_shapes=[dma((NA,))], compiler_params=pltpu.CompilerParams(vmem_limit_bytes=2 ** 20), name="hand_on",
        )(*(pltpu.with_memory_space_constraint(a, vmem) for a in out))
        return grad_act.reshape(shape), grad_gate[:, None], grad_lin[:, None], grad_proj[:, None]

    return jax.shard_map(body, mesh=mesh, in_specs=(act_spec, act_spec, w_spec, w_spec, w_spec),
                         out_specs=(act_spec, w_spec, w_spec, w_spec), check_vma=False)
```

```python
import functools

import jax
import jax.numpy as jnp
from jax import lax
from jax.experimental import pallas as pl
from jax.experimental.pallas import tpu as pltpu
from jax.sharding import PartitionSpec as P

NORM_EPS = 1e-6
BF = jnp.bfloat16
F32 = jnp.float32
MESH = pl.DeviceIdType.MESH
X, Y, Z = 0, 1, 2
BLOCKS = COLOURS = HALVES = (0, 1)
NB, NA, NL = len(BLOCKS), 4, 64
RING = (1, 3, 2)
OPP = RING[-1]
PLUS, MINUS = RING[:-1]
QUARTERS = range(NA)
OWN = 0
AXES = ((Z, X, Y), (Y, Z, X), (X, Y, Z))
UP_MATS, OUT_MAT = (0, 1), (2,)
MATS = UP_MATS + OUT_MAT


def mm(left, right):
    return jnp.dot(left, right, preferred_element_type=F32)


def mm_nt(left, right):
    return lax.dot_general(left, right, (((1,), (1,)), ((), ())), preferred_element_type=F32)


def mm_tn(left, right):
    return lax.dot_general(left, right, (((0,), (0,)), ((), ())), preferred_element_type=F32)


def inv_rms(h):
    return lax.rsqrt(jnp.mean(h * h, axis=-1, keepdims=True) + NORM_EPS)


def kernel(act, cot, wg_in, wi_in, wo_in, gact, gg, gi, go,
           wg, wi, wo, hb, eb, xo, ga, ng, f1, f2, f1s, f2s, us, ub, da, db, das, dbs, qs, gs, is_, os_,
           gin0, gin1, gout0, gout1, fin, r3,
           lsem, ag_s, ag_r, lg_r, mc_s, mc_r, rl_s, ga_s, ga_r, rs_s, rs_r, r3_s, r3_r, turn, *rg):
    dm, fd = wo.shape[-1], wg.shape[-1]
    dr, fr = dm // NL, fd // NL
    fs = fd // NA
    pf = fs // NA
    rows = act.shape[0]
    wts = (wg, wi, wo)
    gin, gout = (gin0, gin1), (gout0, gout1)

    p = lax.axis_index("stage")
    d = lax.axis_index("data")
    zc, yc, xc = lax.div(d, 16), lax.rem(lax.div(d, 4), 4), lax.rem(d, 4)
    coord = (xc, yc, zc)
    stride = (1, 4, 16)
    ja = yc + p * (zc - yc)
    jb = zc + p * (yc - zc)
    sa, sb = 4 + 12 * p, 16 - 12 * p

    def rot(c, delta):
        return lax.rem(c + (delta % 4), 4)

    def peer(ax, delta):
        return d + (rot(coord[ax], delta) - coord[ax]) * stride[ax]

    def peer_a(delta):
        return d + (rot(ja, delta) - ja) * sa

    def peer_b(delta):
        return d + (rot(jb, delta) - jb) * sb

    def remote(src, dst, ssem, rsem, dev, core):
        return pltpu.make_async_remote_copy(src_ref=src, dst_ref=dst, send_sem=ssem, recv_sem=rsem,
                                            device_id=(dev, core), device_id_type=MESH)

    def send(src, dst, ssem, rsem, dev, core):
        remote(src, dst, ssem, rsem, dev, core).start()

    def wait_recv(ref, sem):
        remote(ref, ref, sem, sem, d, p).wait_recv()

    def wait_send(ref, sem):
        remote(ref, ref, sem, sem, d, p).wait_send()

    for v in BLOCKS:
        for k, shard in enumerate((wg_in, wi_in, wo_in)):
            pltpu.make_async_copy(shard.at[v], wts[k].at[v, zc, yc, xc], lsem.at[v, k]).start()

    @pl.when(p == 0)
    def _():
        pltpu.make_async_copy(act, hb.at[0, OWN], lsem.at[0, 3]).start()

    @pl.when(p == 1)
    def _():
        pltpu.make_async_copy(cot, eb.at[1, OWN], lsem.at[0, 3]).start()

    barrier = pltpu.get_barrier_semaphore()
    senders = [(peer(ax, delta), p) for ax in (X, Y, Z) for delta in RING]
    senders += [(d, 1 - p), (peer_a(1), 1 - p), (peer_a(-1), 1 - p)]
    for dev, core in senders:
        pl.semaphore_signal(barrier, inc=1, device_id=(dev, core), device_id_type=MESH)
    for v in BLOCKS:
        for k, shard in enumerate((wg_in, wi_in, wo_in)):
            pltpu.make_async_copy(shard.at[v], wts[k].at[v, zc, yc, xc], lsem.at[v, k]).wait()

    @pl.when(p == 0)
    def _():
        pltpu.make_async_copy(act, hb.at[0, OWN], lsem.at[0, 3]).wait()

    @pl.when(p == 1)
    def _():
        pltpu.make_async_copy(cot, eb.at[1, OWN], lsem.at[0, 3]).wait()

    pl.semaphore_wait(barrier, len(senders))

    FIRST, REST = ((0, PLUS, 0), (1, MINUS, 2)), ((1, PLUS, 1), (0, MINUS, 3))
    LARGE = 2
    whole = slice(None)

    def part_at(v, k, small, middle, large, half=None):
        place = dict(zip(AXES[k], (small, middle, large)))
        width = wts[k].shape[-1] // 2
        cols = whole if half is None else pl.ds(half * width, width)
        return wts[k].at[v, place[Z], place[Y], place[X], :, cols]

    def own(k):
        return [coord[ax] for ax in AXES[k]]

    def chunk(v, k, ph, q, half):
        small, middle, large = own(k)
        return part_at(v, k, q, middle, large, half) if ph == 0 else part_at(v, k, pl.ds(2 * half, 2), q, large)

    def small_copy(v, k, ph, q, half, delta, slot):
        ref = chunk(v, k, ph, q, half)
        send(ref, ref, ag_s.at[v, k, ph], ag_r.at[v, k, ph, slot], peer(AXES[k][ph], delta), p)

    def small_wait(v, k, ph, back, half, slot):
        wait_recv(chunk(v, k, ph, rot(coord[AXES[k][ph]], back), half), ag_r.at[v, k, ph, slot])

    def small_send(v, ph):
        for half, delta, slot in FIRST + REST:
            for k in MATS:
                small_copy(v, k, ph, coord[AXES[k][ph]], half, delta, slot)

    def small_relay(v, ph):
        for half, delta, slot in FIRST:
            for k in MATS:
                small_wait(v, k, ph, -delta, half, slot)
                small_copy(v, k, ph, rot(coord[AXES[k][ph]], -delta), half, delta, 4 + half)

    def small_rest(v, ph):
        for half, delta, slot in REST:
            for k in MATS:
                small_wait(v, k, ph, -delta, half, slot)

    def small_last(v, ph):
        for half in HALVES:
            for k in MATS:
                small_wait(v, k, ph, OPP, half, 4 + half)

    def direct_send(v):
        for delta in (OPP, PLUS, MINUS):
            for k in MATS:
                ref = part_at(v, k, *own(k))
                send(ref, ref, ag_s.at[v, k, 0], ag_r.at[v, k, 0, delta], peer(AXES[k][0], delta), p)

    def direct_wait(v):
        for delta in RING:
            for k in MATS:
                small, middle, large = own(k)
                wait_recv(part_at(v, k, rot(small, -delta), middle, large), ag_r.at[v, k, 0, delta])

    UP, DOWN = (0, PLUS), (MINUS, OPP)
    RELAYS = ((UP[0], PLUS), (DOWN[0], MINUS), (UP[1], PLUS), (DOWN[1], MINUS))

    def row(v, k, q, r):
        return part_at(v, k, whole, rot(coord[AXES[k][1]], r), q)

    def large_slot(r, delta):
        return r if delta == PLUS else NA + r

    def large_send(v, up, down):
        for pair in zip(up, down):
            for r, delta in zip(pair, (PLUS, MINUS)):
                for k in MATS:
                    ax = AXES[k][LARGE]
                    ref = row(v, k, coord[ax], r)
                    send(ref, ref, ag_s.at[v, k, LARGE], lg_r.at[v, k, large_slot(r, delta)], peer(ax, delta), p)

    def large_relay(v):
        for r, delta in RELAYS:
            for k in MATS:
                ax = AXES[k][LARGE]
                ref = row(v, k, rot(coord[ax], -delta), r)
                wait_recv(ref, lg_r.at[v, k, large_slot(r, delta)])
                send(ref, ref, ag_s.at[v, k, LARGE], lg_r.at[v, k, 2 * NA + r], peer(ax, delta), p)

    def large_finish(v, mats):
        for pieces, delta in ((DOWN, PLUS), (UP, MINUS)):
            for r in pieces:
                for k in mats:
                    wait_recv(row(v, k, rot(coord[AXES[k][LARGE]], -delta), r), lg_r.at[v, k, large_slot(r, delta)])
        for r in QUARTERS:
            for k in mats:
                wait_recv(row(v, k, rot(coord[AXES[k][LARGE]], OPP), r), lg_r.at[v, k, 2 * NA + r])

    half_rows = rows // 2
    BACK, AHEAD, FAR = 1, 2, 3

    def spread_near(src, buf, which, vd, ssem):
        send(src, buf.at[vd, OWN], ssem, mc_r.at[which, vd, OWN], d, 1 - p)

    def rows_half(half):
        return pl.ds(half * half_rows, half_rows)

    HALF_ORDER = [(half if first else 1 - half, slot, delta, slot if first else FAR + 1 + slot)
                  for first in (True, False) for half, slot, delta in ((0, BACK, PLUS), (1, AHEAD, MINUS))]

    def spread_far(src, buf, which, vd, ssem):
        for half, slot, delta, sem in HALF_ORDER:
            send(src.at[rows_half(half)], buf.at[vd, slot, rows_half(half)], ssem, mc_r.at[which, vd, sem], peer_b(delta), 1 - p)

    def spread_same(buf, which, v, ssem):
        for half, slot, delta, sem in HALF_ORDER:
            send(buf.at[v, OWN, rows_half(half)], buf.at[v, slot, rows_half(half)], ssem, mc_r.at[which, v, sem], peer_a(delta), p)

    def spread_relay(buf, which, v):
        for half, slot, delta, sem in HALF_ORDER:
            ref = buf.at[v, slot, rows_half(half)]
            wait_recv(ref, mc_r.at[which, v, sem])
            if sem == slot:
                send(ref, buf.at[v, FAR, rows_half(half)], rl_s.at[which, v], mc_r.at[which, v, FAR + half], peer_a(delta), p)

    def spread_finish(buf, which, v):
        for half in HALVES:
            wait_recv(buf.at[v, FAR, rows_half(half)], mc_r.at[which, v, FAR + half])

    def spread_own(buf, which, v):
        wait_recv(buf.at[v, OWN], mc_r.at[which, v, OWN])

    def gates(n, wgt, wlin):
        a, b = mm(n, wgt), mm(n, wlin)
        s = jax.nn.sigmoid(a)
        act_a = a * s
        return (act_a * b).astype(BF), b * s * (1.0 + a * (1.0 - s)), act_a

    def block_gates(v):
        h = hb[v, OWN].astype(F32)
        n = (h * inv_rms(h)).astype(BF)

        def tile(i, carry):
            wide = fs // 2
            cols = pl.ds(pl.multiple_of(i * wide, wide), wide)
            u, t1, t2 = gates(n, wg[v, :, :, :, :, cols].reshape(dm, wide), wi[v, :, :, :, :, cols].reshape(dm, wide))
            ub[:, cols] = u
            f1[v, :, cols] = t1
            f2[v, :, cols] = t2
            return carry

        lax.fori_loop(0, 2 * NA, tile, 0, unroll=True)

    def block_out(v, dst):
        half_dm = dm // 2
        for i in HALVES:
            cols = pl.ds(i * half_dm, half_dm)
            out = mm(ub[...], wo[v, :, :, :, :, cols].reshape(fd, half_dm))
            dst[:, cols] = (hb[v, OWN, :, cols].astype(F32) + out).astype(BF)

    def block_backward(v, dst):
        e = eb[v, OWN]

        def tile(i, carry):
            cols = pl.ds(pl.multiple_of(i * fs, fs), fs)
            t = mm_nt(e, wo[v, i].reshape(fs, dm))
            da[:, cols] = (t * f1[v, :, cols]).astype(BF)
            db[:, cols] = (t * f2[v, :, cols]).astype(BF)
            return carry

        lax.fori_loop(0, NA, tile, 0, unroll=True)
        half_dm = dm // 2
        for i in HALVES:
            q = mm_nt(da[...], wg[v, pl.ds(2 * i, 2)].reshape(half_dm, fd))
            q += mm_nt(db[...], wi[v, pl.ds(2 * i, 2)].reshape(half_dm, fd))
            qs[:, pl.ds(i * half_dm, half_dm)] = q
        h = hb[v, OWN].astype(F32)
        r = inv_rms(h)
        hr = h * r
        q = qs[...]
        dst[...] = (e.astype(F32) + r * (q - hr * jnp.mean(q * hr, axis=-1, keepdims=True))).astype(BF)

    def piece(j, i):
        z = i + p * (j - i)
        y = j + p * (i - j)
        return z, y

    EARLY, LATE = range(FAR), range(FAR, NA)

    def grad_first(v, slots):
        for i in QUARTERS if OWN in slots else ():
            z, y = piece(ja, i)
            cols = pl.ds(pl.multiple_of((z * NA + y) * pf, pf), pf)
            gs[v, :, pl.ds(i * pf, pf)] = wg[v, :, :, :, :, cols].reshape(dm, pf)
            is_[v, :, pl.ds(i * pf, pf)] = wi[v, :, :, :, :, cols].reshape(dm, pf)
        for s in slots:
            h = hb[v, s].astype(F32)
            n = (h * inv_rms(h)).astype(BF)
            ng[v, s] = n
            u, t1, t2 = gates(n, gs[v], is_[v])
            us[v, s] = u
            f1s[v, s] = t1
            f2s[v, s] = t2

    def grad_hidden(v, slots):
        for i in QUARTERS if OWN in slots else ():
            z, y = piece(ja, i)
            os_[pl.ds(i * pf, pf), :] = wo[v, z, y].reshape(pf, dm)
        for s in slots:
            t = mm_nt(eb[v, s], os_[...])
            das[s] = (t * f1s[v, s]).astype(BF)
            dbs[s] = (t * f2s[v, s]).astype(BF)

    def split(width, second):
        return pl.ds(0, width - second), pl.ds(width - second, second)

    IN_COLS, OUT_COLS = split(fs, pf), split(dm, pf)

    def keep(refs, v, place, tile, cols, first):
        b, rest = place[0], place[1:]
        lead = () if v is None else (v,)
        for colour in COLOURS:
            part = tile[..., cols[colour].start:cols[colour].start + cols[colour].size]
            at = lead + ((b, slice(None)) if colour == 0 else (slice(None), b)) + rest
            refs[colour][at] = part if first else refs[colour][at] + part

    def rows_of(slots):
        return pl.ds(slots[0], len(slots)), len(slots) * rows

    def grad_out(v, slots):
        some, count = rows_of(slots)
        for i in HALVES:
            cols = pl.ds(i * 2 * pf, 2 * pf)
            g = mm_tn(us[v, some, :, cols].reshape(count, 2 * pf), eb[v, some].reshape(count, dm)).reshape(2, NA, fr, dm)
            for b in HALVES:
                keep(gout, v, (2 * i + b,), g[b], OUT_COLS, OWN in slots)

    def grad_in(v, slots):
        some, count = rows_of(slots)
        for which, dref in enumerate((das, dbs)):
            for i in QUARTERS:
                cols = pl.ds(i * (dm // NA), dm // NA)
                g = mm_tn(ng[v, some, :, cols].reshape(count, dm // NA), dref[some].reshape(count, fs)).reshape(NA, NA, dr, fs)
                for y in QUARTERS:
                    keep([ref.at[v, which] for ref in gin], None, (i + p * (y - i), y + p * (i - y)), g[y], IN_COLS, OWN in slots)

    IN, OUT = 0, 1

    def view(which, st, v, colour, t, half):
        own = jb if colour == 0 else xc
        if which == IN:
            ref = gin[colour].at[v, half]
            return ref.at[t] if st == 0 else ref.at[own, t]
        ref = gout[colour].at[v]
        return ref.at[t, pl.ds(2 * half, 2)] if st == 0 else ref.at[own, t, pl.ds(half * (fr // 2), fr // 2)]

    RECV = (((rg[0], rg[1]), (rg[2], rg[3])), ((rg[4], rg[5]), (rg[6], rg[7])))
    MERGED, DIRECT = ((0, OPP, PLUS, 0), (1, OPP, MINUS, 1)), ((1, PLUS, PLUS, 2), (0, MINUS, MINUS, 3))
    RELAYED = ((0, PLUS, PLUS, 4), (1, MINUS, MINUS, 5))

    def axis_of(colour, st):
        return (jb, peer_b) if colour == st else (xc, functools.partial(peer, X))

    def scatter_send(v, which, st, copies):
        for colour in COLOURS:
            q, to = axis_of(colour, st)
            for half, c, delta, slot in copies:
                send(view(which, st, v, colour, rot(q, c), half), RECV[st][which][colour].at[v, slot],
                     rs_s.at[st, v, colour, which], rs_r.at[st, v, colour, which, slot], to(delta), p)

    def scatter_relay(v, which, st):
        for colour in COLOURS:
            q, _ = axis_of(colour, st)
            recv = RECV[st][which][colour]
            for half, c, _, slot in RELAYED:
                wait_recv(recv.at[v, slot - 4], rs_r.at[st, v, colour, which, slot - 4])
                ref = view(which, st, v, colour, rot(q, c), half)
                ref[...] = ref[...] + recv[v, slot - 4]
        scatter_send(v, which, st, RELAYED)

    def scatter_sum(v, which, st):
        for colour in COLOURS:
            q, _ = axis_of(colour, st)
            recv = RECV[st][which][colour]
            for half in HALVES:
                direct, merged = 3 - half, 4 + half
                for slot in (direct, merged):
                    wait_recv(recv.at[v, slot], rs_r.at[st, v, colour, which, slot])
                ref = view(which, st, v, colour, q, half)
                ref[...] = ref[...] + recv[v, direct] + recv[v, merged]

    def scatter_turn(v, which):
        scatter_sum(v, which, 0)
        scatter_send(v, which, 1, MERGED + DIRECT)

    def scatter_out(v):
        scatter_sum(v, OUT, 1)
        for colour in COLOURS:
            go[v, :, OUT_COLS[colour]] = gout[colour][(v, jb, xc) if colour == 0 else (v, xc, jb)]

    def scatter_last(v):
        scatter_sum(v, IN, 1)
        for which in HALVES:
            for colour in COLOURS:
                fin[v, :, which, :, IN_COLS[colour]] = gin[colour][(v, which, jb, xc) if colour == 0 else (v, which, xc, jb)]
        for delta in (OPP, PLUS, MINUS):
            send(fin.at[v, rot(ja, delta)], r3.at[v, delta - 1], r3_s.at[v], r3_r.at[v, delta - 1], peer_a(delta), p)

    def scatter_finish(v):
        def put(j, vals):
            for i in QUARTERS:
                z, y = piece(j, i)
                cols = pl.ds(pl.multiple_of((z * NA + y) * pf, pf), pf)
                gg[v, :, cols] = vals(0)[:, i * pf:(i + 1) * pf]
                gi[v, :, cols] = vals(1)[:, i * pf:(i + 1) * pf]

        put(ja, lambda w: fin[v, ja, w])
        for delta in RING:
            wait_recv(r3.at[v, delta - 1], r3_r.at[v, delta - 1])
            put(rot(ja, -delta), lambda w, delta=delta: r3[v, delta - 1, w])

    def step(fn, *args):
        with jax.named_scope(fn.__name__):
            fn(*args)

    def on(core):
        return pl.when(p == core)

    def take_turn():
        pl.semaphore_wait(turn, 1)

    def give_turn():
        pl.semaphore_signal(turn, inc=1, device_id=(d, 1 - p), device_id_type=MESH)

    h_mid, h_late, e_first, e_last = ((xo.at[i], mc_s.at[1 + i]) for i in QUARTERS)

    def pass_on(part, item, buf, which, vd):
        step(part, item[0], buf, which, vd, item[1])

    AFTER = (MINUS, OPP), (0, PLUS)
    step(direct_send, 0)
    step(small_send, 1, 0)
    step(direct_wait, 0)
    step(small_send, 0, 1)
    step(small_relay, 1, 0)
    step(large_send, 0, (0,), (0,))
    step(small_rest, 1, 0)
    step(small_last, 1, 0)
    step(small_send, 1, 1)
    step(small_relay, 0, 1)
    step(small_relay, 1, 1)
    step(small_rest, 0, 1)
    step(large_send, 0, (PLUS, MINUS), (MINUS, PLUS))
    step(small_last, 0, 1)
    step(large_send, 0, (OPP,), (OPP,))
    step(small_rest, 1, 1)
    step(small_last, 1, 1)
    step(large_relay, 0)

    @on(0)
    def _():
        step(large_send, 1, UP, DOWN)

    step(large_finish, 0, UP_MATS)

    @on(0)
    def _():
        step(large_send, 1, *AFTER)

    @on(1)
    def _():
        step(take_turn)
        step(large_send, 1, UP, DOWN)
        step(spread_own, hb, 0, 0)

    step(block_gates, 0)

    @on(1)
    def _():
        step(large_send, 1, *AFTER)

    step(large_finish, 0, OUT_MAT)
    step(block_out, 0, h_mid[0])
    pass_on(spread_near, h_mid, hb, 0, p)
    step(large_relay, 1)

    @on(0)
    def _():
        step(give_turn)

    @on(1)
    def _():
        pass_on(spread_far, h_mid, hb, 0, p)

    step(spread_own, hb, 0, 1)
    step(large_finish, 1, UP_MATS)

    @on(1)
    def _():
        step(spread_same, eb, 1, 1, mc_s.at[0])

    step(block_gates, 1)
    step(large_finish, 1, OUT_MAT)

    @on(0)
    def _():
        step(block_out, 1, h_late[0])
        pass_on(spread_near, h_late, hb, 0, 1)
        pass_on(spread_far, h_late, hb, 0, 1)
        pass_on(spread_far, h_mid, hb, 0, p)
        step(spread_same, hb, 0, 0, mc_s.at[0])
        step(spread_own, eb, 1, 1)
        step(block_backward, 1, e_first[0])
        pass_on(spread_near, e_first, eb, 1, 0)
        pass_on(spread_far, e_first, eb, 1, 0)
        step(spread_relay, hb, 0, 1)
        step(grad_first, 1, EARLY)

    @on(1)
    def _():
        step(block_backward, 1, e_first[0])
        pass_on(spread_near, e_first, eb, 1, 1)
        pass_on(spread_far, e_first, eb, 1, 1)
        step(spread_relay, hb, 0, 1)
        step(grad_first, 1, EARLY)

    step(spread_relay, eb, 1, 1)

    step(grad_hidden, 1, EARLY)
    step(grad_out, 1, EARLY)
    step(grad_in, 1, EARLY)

    @on(0)
    def _():
        step(spread_relay, hb, 0, 0)
        step(spread_finish, hb, 0, 1)
        step(grad_first, 1, LATE)

    @on(1)
    def _():
        step(spread_own, eb, 1, 0)
        step(block_backward, 0, e_last[0])
        pass_on(spread_near, e_last, eb, 1, 0)
        pass_on(spread_far, e_last, eb, 1, 0)
        step(spread_relay, hb, 0, 0)
        step(spread_finish, hb, 0, 1)
        step(grad_first, 1, LATE)

    step(spread_finish, eb, 1, 1)
    step(grad_hidden, 1, LATE)
    step(grad_out, 1, LATE)
    step(scatter_send, 1, OUT, 0, MERGED)
    step(grad_in, 1, LATE)
    step(scatter_send, 1, IN, 0, MERGED)
    step(scatter_send, 1, OUT, 0, DIRECT)
    step(scatter_send, 1, IN, 0, DIRECT)

    @on(0)
    def _():
        step(grad_first, 0, EARLY)
        step(spread_relay, eb, 1, 0)
        step(spread_finish, hb, 0, 0)
        step(grad_first, 0, LATE)
        step(spread_own, eb, 1, 0)

    @on(1)
    def _():
        step(grad_first, 0, EARLY)
        step(spread_relay, eb, 1, 0)
        step(spread_finish, hb, 0, 0)
        step(grad_first, 0, LATE)

    step(grad_hidden, 0, EARLY)
    step(grad_in, 0, EARLY)
    step(grad_out, 0, EARLY)
    step(scatter_relay, 1, OUT, 0)
    step(spread_finish, eb, 1, 0)
    step(grad_hidden, 0, LATE)
    step(grad_in, 0, LATE)
    step(scatter_send, 0, IN, 0, MERGED)
    step(grad_out, 0, LATE)
    step(scatter_relay, 1, IN, 0)
    step(scatter_send, 0, OUT, 0, MERGED)
    step(scatter_send, 0, IN, 0, DIRECT)

    @on(0)
    def _():
        step(block_backward, 0, ga)
        send(ga, ga, ga_s, ga_r, d, 1)

    step(scatter_turn, 1, OUT)
    step(scatter_relay, 0, IN, 0)
    step(scatter_send, 0, OUT, 0, DIRECT)
    step(scatter_turn, 1, IN)
    step(scatter_relay, 0, OUT, 0)
    step(scatter_relay, 1, OUT, 1)

    @on(1)
    def _():
        wait_recv(ga, ga_r)

    gact[...] = ga[...]
    step(scatter_turn, 0, IN)
    step(scatter_relay, 1, IN, 1)
    step(scatter_turn, 0, OUT)
    step(scatter_relay, 0, IN, 1)
    step(scatter_out, 1)
    step(scatter_last, 1)
    step(scatter_relay, 0, OUT, 1)
    step(scatter_last, 0)
    step(scatter_finish, 1)
    step(scatter_out, 0)
    step(scatter_finish, 0)

    for v in BLOCKS:
        for k in MATS:
            three = pl.ds(0, len(RING))
            wait_send(part_at(v, k, three, 0, 0), ag_s.at[v, k, 0])
            wait_send(part_at(v, k, whole, three, 0), ag_s.at[v, k, 1])
            wait_send(part_at(v, k, whole, whole, three), ag_s.at[v, k, LARGE])
        for colour in COLOURS:
            for which in HALVES:
                for st in HALVES:
                    wait_send(RECV[st][which][colour].at[v], rs_s.at[st, v, colour, which])
        wait_send(r3.at[v], r3_s.at[v])
        wait_send(hb.at[v, 0], rl_s.at[0, v])
        wait_send(hb.at[v, 0], rl_s.at[1, v])
    wait_send(hb.at[0, pl.ds(0, 2)], mc_s.at[0])
    wait_send(hb.at[0, pl.ds(0, 3)], mc_s.at[1])
    wait_send(hb.at[0, pl.ds(0, 3)], mc_s.at[3])

    @pl.when(p == 0)
    def _():
        wait_send(hb.at[0, pl.ds(0, 3)], mc_s.at[2])
        wait_send(ga, ga_s)

    @pl.when(p == 1)
    def _():
        wait_send(hb.at[0, pl.ds(0, 3)], mc_s.at[4])


def hand_on(*refs):
    copies = [pltpu.make_async_copy(refs[i], refs[NA + i], refs[-1].at[i]) for i in QUARTERS]
    for copy in copies:
        copy.start()
    for copy in copies:
        copy.wait()


def solution(mesh):
    act_spec = P(None, "data", None, None)
    w_spec = P(None, "stage", "data", None)

    def body(act_in, cot_out, w_gate, w_in, w_out):
        shape = act_in.shape
        dm, fd = shape[3], w_gate.shape[3]
        rows = shape[0] * shape[1] * shape[2]
        dr, fr, fs = dm // NL, fd // NL, fd // NA
        pf = fs // NA
        vmem = pltpu.VMEM
        dma = pltpu.SemaphoreType.DMA
        n2, n3, na = NB, len(RING), NA
        ring = (na, na)
        scratch = [
            vmem((n2, na, *ring, dr, fd), BF), vmem((n2, na, *ring, dr, fd), BF), vmem((n2, na, *ring, fr, dm), BF),
            vmem((n2, na, rows, dm), BF), vmem((n2, na, rows, dm), BF), vmem((na, rows, dm), BF), vmem((rows, dm), BF),
            vmem((n2, na, rows, dm), BF),
            vmem((n2, rows, fd), F32), vmem((n2, rows, fd), F32),
            vmem((n2, na, rows, fs), F32), vmem((n2, na, rows, fs), F32),
            vmem((n2, na, rows, fs), BF),
            vmem((rows, fd), BF), vmem((rows, fd), BF), vmem((rows, fd), BF),
            vmem((na, rows, fs), BF), vmem((na, rows, fs), BF),
            vmem((rows, dm), F32),
            vmem((n2, dm, fs), BF), vmem((n2, dm, fs), BF), vmem((fs, dm), BF),
            *(vmem((n2, n2, *ring, na, dr, width), F32) for width in (fs - pf, pf)),
            *(vmem((n2, *ring, fr, width), F32) for width in (dm - pf, pf)),
            vmem((n2, na, n2, dr, fs), F32), vmem((n2, n3, n2, dr, fs), F32),
            dma((n2, na)), dma((n2, n3, n3)), dma((n2, n3, n2, 6)), dma((n2, n3, n3 * na)), dma((5,)), dma((n2, n2, 7)), dma((n2, n2)), dma, dma,
            dma((n2, n2, n2, n2)), dma((n2, n2, n2, n2, 6)), dma((n2,)), dma((n2, n3)), pltpu.SemaphoreType.REGULAR,
            *(vmem((n2, 6, *lead, width), F32)
              for lead_in, lead_out in (((*ring, dr), (n2, fr)), ((na, dr), (fr // n2,)))
              for lead, width in ((lead_in, fs - pf), (lead_in, pf), (lead_out, dm - pf), (lead_out, pf))),
        ]
        hbm = pl.BlockSpec(memory_space=pl.ANY)
        whole = pl.BlockSpec(memory_space=pltpu.VMEM)
        out = pl.pallas_call(
            kernel,
            out_shape=(
                vmem((rows, dm), BF), vmem((n2, dr, fd), F32), vmem((n2, dr, fd), F32), vmem((n2, fr, dm), F32),
            ),
            in_specs=[hbm] * 5,
            out_specs=(whole,) * NA,
            scratch_shapes=scratch,
            compiler_params=pltpu.CompilerParams(collective_id=0, has_side_effects=True, vmem_limit_bytes=66300000),
            name="train_step",
        )(act_in.reshape(rows, dm), cot_out.reshape(rows, dm), w_gate[:, 0], w_in[:, 0], w_out[:, 0])
        grad_act, grad_gate, grad_lin, grad_proj = pl.pallas_call(
            hand_on, out_shape=tuple(jax.ShapeDtypeStruct(a.shape, a.dtype) for a in out), in_specs=[whole] * NA, out_specs=(hbm,) * NA,
            scratch_shapes=[dma((NA,))], compiler_params=pltpu.CompilerParams(vmem_limit_bytes=2 ** 20), name="hand_on",
        )(*(pltpu.with_memory_space_constraint(a, vmem) for a in out))
        return grad_act.reshape(shape), grad_gate[:, None], grad_lin[:, None], grad_proj[:, None]

    return jax.shard_map(body, mesh=mesh, in_specs=(act_spec, act_spec, w_spec, w_spec, w_spec),
                         out_specs=(act_spec, w_spec, w_spec, w_spec), check_vma=False)
```

```python
import functools

import jax
import jax.numpy as jnp
from jax import lax
from jax.experimental import pallas as pl
from jax.experimental.pallas import tpu as pltpu
from jax.sharding import PartitionSpec as P

NORM_EPS = 1e-6
BF = jnp.bfloat16
F32 = jnp.float32
MESH = pl.DeviceIdType.MESH
X, Y, Z = 0, 1, 2
BLOCKS = COLOURS = HALVES = (0, 1)
NB, NA, NL = len(BLOCKS), 4, 64
RING = (1, 3, 2)
OPP = RING[-1]
PLUS, MINUS = RING[:-1]
QUARTERS = range(NA)
OWN = 0
AXES = ((Z, X, Y), (Y, Z, X), (X, Y, Z))
UP_MATS, OUT_MAT = (0, 1), (2,)
MATS = UP_MATS + OUT_MAT


def mm(left, right):
    return jnp.dot(left, right, preferred_element_type=F32)


def mm_nt(left, right):
    return lax.dot_general(left, right, (((1,), (1,)), ((), ())), preferred_element_type=F32)


def mm_tn(left, right):
    return lax.dot_general(left, right, (((0,), (0,)), ((), ())), preferred_element_type=F32)


def inv_rms(h):
    return lax.rsqrt(jnp.mean(h * h, axis=-1, keepdims=True) + NORM_EPS)


def kernel(act, cot, wg_in, wi_in, wo_in, gact, gg, gi, go,
           wg, wi, wo, hb, eb, xo, ga, ng, f1, f2, f1s, f2s, us, ub, da, db, das, dbs, qs, gs, is_, os_,
           gin0, gin1, gout0, gout1, fin, r3,
           lsem, ag_s, ag_r, lg_r, mc_s, mc_r, rl_s, ga_s, ga_r, rs_s, rs_r, r3_s, r3_r, turn, *rg):
    dm, fd = wo.shape[-1], wg.shape[-1]
    dr, fr = dm // NL, fd // NL
    fs = fd // NA
    pf = fs // NA
    rows = act.shape[0]
    wts = (wg, wi, wo)
    gin, gout = (gin0, gin1), (gout0, gout1)

    p = lax.axis_index("stage")
    d = lax.axis_index("data")
    zc, yc, xc = lax.div(d, 16), lax.rem(lax.div(d, 4), 4), lax.rem(d, 4)
    coord = (xc, yc, zc)
    stride = (1, 4, 16)
    ja = yc + p * (zc - yc)
    jb = zc + p * (yc - zc)
    sa, sb = 4 + 12 * p, 16 - 12 * p

    def rot(c, delta):
        return lax.rem(c + (delta % 4), 4)

    def peer(ax, delta):
        return d + (rot(coord[ax], delta) - coord[ax]) * stride[ax]

    def peer_a(delta):
        return d + (rot(ja, delta) - ja) * sa

    def peer_b(delta):
        return d + (rot(jb, delta) - jb) * sb

    def remote(src, dst, ssem, rsem, dev, core):
        return pltpu.make_async_remote_copy(src_ref=src, dst_ref=dst, send_sem=ssem, recv_sem=rsem,
                                            device_id=(dev, core), device_id_type=MESH)

    def send(src, dst, ssem, rsem, dev, core):
        remote(src, dst, ssem, rsem, dev, core).start()

    def wait_recv(ref, sem):
        remote(ref, ref, sem, sem, d, p).wait_recv()

    def wait_send(ref, sem):
        remote(ref, ref, sem, sem, d, p).wait_send()

    for v in BLOCKS:
        for k, shard in enumerate((wg_in, wi_in, wo_in)):
            pltpu.make_async_copy(shard.at[v], wts[k].at[v, zc, yc, xc], lsem.at[v, k]).start()

    @pl.when(p == 0)
    def _():
        pltpu.make_async_copy(act, hb.at[0, OWN], lsem.at[0, 3]).start()

    @pl.when(p == 1)
    def _():
        pltpu.make_async_copy(cot, eb.at[1, OWN], lsem.at[0, 3]).start()

    barrier = pltpu.get_barrier_semaphore()
    senders = [(peer(ax, delta), p) for ax in (X, Y, Z) for delta in RING]
    senders += [(d, 1 - p), (peer_a(1), 1 - p), (peer_a(-1), 1 - p)]
    for dev, core in senders:
        pl.semaphore_signal(barrier, inc=1, device_id=(dev, core), device_id_type=MESH)
    for v in BLOCKS:
        for k, shard in enumerate((wg_in, wi_in, wo_in)):
            pltpu.make_async_copy(shard.at[v], wts[k].at[v, zc, yc, xc], lsem.at[v, k]).wait()

    @pl.when(p == 0)
    def _():
        pltpu.make_async_copy(act, hb.at[0, OWN], lsem.at[0, 3]).wait()

    @pl.when(p == 1)
    def _():
        pltpu.make_async_copy(cot, eb.at[1, OWN], lsem.at[0, 3]).wait()

    pl.semaphore_wait(barrier, len(senders))

    FIRST, REST = ((0, PLUS, 0), (1, MINUS, 2)), ((1, PLUS, 1), (0, MINUS, 3))
    LARGE = 2
    whole = slice(None)

    def part_at(v, k, small, middle, large, half=None):
        place = dict(zip(AXES[k], (small, middle, large)))
        width = wts[k].shape[-1] // 2
        cols = whole if half is None else pl.ds(half * width, width)
        return wts[k].at[v, place[Z], place[Y], place[X], :, cols]

    def own(k):
        return [coord[ax] for ax in AXES[k]]

    def chunk(v, k, ph, q, half):
        small, middle, large = own(k)
        return part_at(v, k, q, middle, large, half) if ph == 0 else part_at(v, k, pl.ds(2 * half, 2), q, large)

    def small_copy(v, k, ph, q, half, delta, slot):
        ref = chunk(v, k, ph, q, half)
        send(ref, ref, ag_s.at[v, k, ph], ag_r.at[v, k, ph, slot], peer(AXES[k][ph], delta), p)

    def small_wait(v, k, ph, back, half, slot):
        wait_recv(chunk(v, k, ph, rot(coord[AXES[k][ph]], back), half), ag_r.at[v, k, ph, slot])

    def small_send(v, ph):
        for half, delta, slot in FIRST + REST:
            for k in MATS:
                small_copy(v, k, ph, coord[AXES[k][ph]], half, delta, slot)

    def small_relay(v, ph):
        for half, delta, slot in FIRST:
            for k in MATS:
                small_wait(v, k, ph, -delta, half, slot)
                small_copy(v, k, ph, rot(coord[AXES[k][ph]], -delta), half, delta, 4 + half)

    def small_rest(v, ph):
        for half, delta, slot in REST:
            for k in MATS:
                small_wait(v, k, ph, -delta, half, slot)

    def small_last(v, ph):
        for half in HALVES:
            for k in MATS:
                small_wait(v, k, ph, OPP, half, 4 + half)

    def direct_send(v):
        for delta in (OPP, PLUS, MINUS):
            for k in MATS:
                ref = part_at(v, k, *own(k))
                send(ref, ref, ag_s.at[v, k, 0], ag_r.at[v, k, 0, delta], peer(AXES[k][0], delta), p)

    def direct_wait(v):
        for delta in RING:
            for k in MATS:
                small, middle, large = own(k)
                wait_recv(part_at(v, k, rot(small, -delta), middle, large), ag_r.at[v, k, 0, delta])

    UP, DOWN = (0, PLUS), (MINUS, OPP)
    RELAYS = ((UP[0], PLUS), (DOWN[0], MINUS), (UP[1], PLUS), (DOWN[1], MINUS))

    def row(v, k, q, r):
        return part_at(v, k, whole, rot(coord[AXES[k][1]], r), q)

    def large_slot(r, delta):
        return r if delta == PLUS else NA + r

    def large_send(v, up, down):
        for pair in zip(up, down):
            for r, delta in zip(pair, (PLUS, MINUS)):
                for k in MATS:
                    ax = AXES[k][LARGE]
                    ref = row(v, k, coord[ax], r)
                    send(ref, ref, ag_s.at[v, k, LARGE], lg_r.at[v, k, large_slot(r, delta)], peer(ax, delta), p)

    def large_relay(v):
        for r, delta in RELAYS:
            for k in MATS:
                ax = AXES[k][LARGE]
                ref = row(v, k, rot(coord[ax], -delta), r)
                wait_recv(ref, lg_r.at[v, k, large_slot(r, delta)])
                send(ref, ref, ag_s.at[v, k, LARGE], lg_r.at[v, k, 2 * NA + r], peer(ax, delta), p)

    def large_finish(v, mats):
        for pieces, delta in ((DOWN, PLUS), (UP, MINUS)):
            for r in pieces:
                for k in mats:
                    wait_recv(row(v, k, rot(coord[AXES[k][LARGE]], -delta), r), lg_r.at[v, k, large_slot(r, delta)])
        for r in QUARTERS:
            for k in mats:
                wait_recv(row(v, k, rot(coord[AXES[k][LARGE]], OPP), r), lg_r.at[v, k, 2 * NA + r])

    half_rows = rows // 2
    BACK, AHEAD, FAR = 1, 2, 3

    def spread_near(src, buf, which, vd, ssem):
        send(src, buf.at[vd, OWN], ssem, mc_r.at[which, vd, OWN], d, 1 - p)

    def rows_half(half):
        return pl.ds(half * half_rows, half_rows)

    HALF_ORDER = [(half if first else 1 - half, slot, delta, slot if first else FAR + 1 + slot)
                  for first in (True, False) for half, slot, delta in ((0, BACK, PLUS), (1, AHEAD, MINUS))]

    def spread_far(src, buf, which, vd, ssem):
        for half, slot, delta, sem in HALF_ORDER:
            send(src.at[rows_half(half)], buf.at[vd, slot, rows_half(half)], ssem, mc_r.at[which, vd, sem], peer_b(delta), 1 - p)

    def spread_same(buf, which, v, ssem):
        for half, slot, delta, sem in HALF_ORDER:
            send(buf.at[v, OWN, rows_half(half)], buf.at[v, slot, rows_half(half)], ssem, mc_r.at[which, v, sem], peer_a(delta), p)

    def spread_relay(buf, which, v):
        for half, slot, delta, sem in HALF_ORDER:
            ref = buf.at[v, slot, rows_half(half)]
            wait_recv(ref, mc_r.at[which, v, sem])
            if sem == slot:
                send(ref, buf.at[v, FAR, rows_half(half)], rl_s.at[which, v], mc_r.at[which, v, FAR + half], peer_a(delta), p)

    def spread_finish(buf, which, v):
        for half in HALVES:
            wait_recv(buf.at[v, FAR, rows_half(half)], mc_r.at[which, v, FAR + half])

    def spread_own(buf, which, v):
        wait_recv(buf.at[v, OWN], mc_r.at[which, v, OWN])

    def gates(n, wgt, wlin):
        a, b = mm(n, wgt), mm(n, wlin)
        s = jax.nn.sigmoid(a)
        act_a = a * s
        return (act_a * b).astype(BF), b * s * (1.0 + a * (1.0 - s)), act_a

    def block_gates(v):
        h = hb[v, OWN].astype(F32)
        n = (h * inv_rms(h)).astype(BF)

        def tile(i, carry):
            wide = fs // 2
            cols = pl.ds(pl.multiple_of(i * wide, wide), wide)
            u, t1, t2 = gates(n, wg[v, :, :, :, :, cols].reshape(dm, wide), wi[v, :, :, :, :, cols].reshape(dm, wide))
            ub[:, cols] = u
            f1[v, :, cols] = t1
            f2[v, :, cols] = t2
            return carry

        lax.fori_loop(0, 2 * NA, tile, 0, unroll=True)

    def block_out(v, dst):
        half_dm = dm // 2
        for i in HALVES:
            cols = pl.ds(i * half_dm, half_dm)
            out = mm(ub[...], wo[v, :, :, :, :, cols].reshape(fd, half_dm))
            dst[:, cols] = (hb[v, OWN, :, cols].astype(F32) + out).astype(BF)

    def block_backward(v, dst):
        e = eb[v, OWN]

        def tile(i, carry):
            cols = pl.ds(pl.multiple_of(i * fs, fs), fs)
            t = mm_nt(e, wo[v, i].reshape(fs, dm))
            da[:, cols] = (t * f1[v, :, cols]).astype(BF)
            db[:, cols] = (t * f2[v, :, cols]).astype(BF)
            return carry

        lax.fori_loop(0, NA, tile, 0, unroll=True)
        half_dm = dm // 2
        for i in HALVES:
            q = mm_nt(da[...], wg[v, pl.ds(2 * i, 2)].reshape(half_dm, fd))
            q += mm_nt(db[...], wi[v, pl.ds(2 * i, 2)].reshape(half_dm, fd))
            qs[:, pl.ds(i * half_dm, half_dm)] = q
        h = hb[v, OWN].astype(F32)
        r = inv_rms(h)
        hr = h * r
        q = qs[...]
        dst[...] = (e.astype(F32) + r * (q - hr * jnp.mean(q * hr, axis=-1, keepdims=True))).astype(BF)

    def piece(j, i):
        z = i + p * (j - i)
        y = j + p * (i - j)
        return z, y

    EARLY, LATE = range(FAR), range(FAR, NA)

    def grad_first(v, slots):
        for i in QUARTERS if OWN in slots else ():
            z, y = piece(ja, i)
            cols = pl.ds(pl.multiple_of((z * NA + y) * pf, pf), pf)
            gs[v, :, pl.ds(i * pf, pf)] = wg[v, :, :, :, :, cols].reshape(dm, pf)
            is_[v, :, pl.ds(i * pf, pf)] = wi[v, :, :, :, :, cols].reshape(dm, pf)
        for s in slots:
            h = hb[v, s].astype(F32)
            n = (h * inv_rms(h)).astype(BF)
            ng[v, s] = n
            u, t1, t2 = gates(n, gs[v], is_[v])
            us[v, s] = u
            f1s[v, s] = t1
            f2s[v, s] = t2

    def grad_hidden(v, slots):
        for i in QUARTERS if OWN in slots else ():
            z, y = piece(ja, i)
            os_[pl.ds(i * pf, pf), :] = wo[v, z, y].reshape(pf, dm)
        for s in slots:
            t = mm_nt(eb[v, s], os_[...])
            das[s] = (t * f1s[v, s]).astype(BF)
            dbs[s] = (t * f2s[v, s]).astype(BF)

    def split(width, second):
        return pl.ds(0, width - second), pl.ds(width - second, second)

    IN_COLS, OUT_COLS = split(fs, pf), split(dm, pf)

    def keep(refs, v, place, tile, cols, first):
        b, rest = place[0], place[1:]
        lead = () if v is None else (v,)
        for colour in COLOURS:
            part = tile[..., cols[colour].start:cols[colour].start + cols[colour].size]
            at = lead + ((b, slice(None)) if colour == 0 else (slice(None), b)) + rest
            refs[colour][at] = part if first else refs[colour][at] + part

    def rows_of(slots):
        return pl.ds(slots[0], len(slots)), len(slots) * rows

    def grad_out(v, slots):
        some, count = rows_of(slots)
        for i in HALVES:
            cols = pl.ds(i * 2 * pf, 2 * pf)
            g = mm_tn(us[v, some, :, cols].reshape(count, 2 * pf), eb[v, some].reshape(count, dm)).reshape(2, NA, fr, dm)
            for b in HALVES:
                keep(gout, v, (2 * i + b,), g[b], OUT_COLS, OWN in slots)

    def grad_in(v, slots):
        some, count = rows_of(slots)
        for which, dref in enumerate((das, dbs)):
            for i in QUARTERS:
                cols = pl.ds(i * (dm // NA), dm // NA)
                g = mm_tn(ng[v, some, :, cols].reshape(count, dm // NA), dref[some].reshape(count, fs)).reshape(NA, NA, dr, fs)
                for y in QUARTERS:
                    keep([ref.at[v, which] for ref in gin], None, (i + p * (y - i), y + p * (i - y)), g[y], IN_COLS, OWN in slots)

    IN, OUT = 0, 1

    def view(which, st, v, colour, t, half):
        own = jb if colour == 0 else xc
        if which == IN:
            ref = gin[colour].at[v, half]
            return ref.at[t] if st == 0 else ref.at[own, t]
        ref = gout[colour].at[v]
        return ref.at[t, pl.ds(2 * half, 2)] if st == 0 else ref.at[own, t, pl.ds(half * (fr // 2), fr // 2)]

    RECV = (((rg[0], rg[1]), (rg[2], rg[3])), ((rg[4], rg[5]), (rg[6], rg[7])))
    MERGED, DIRECT = ((0, OPP, PLUS, 0), (1, OPP, MINUS, 1)), ((1, PLUS, PLUS, 2), (0, MINUS, MINUS, 3))
    RELAYED = ((0, PLUS, PLUS, 4), (1, MINUS, MINUS, 5))

    def axis_of(colour, st):
        return (jb, peer_b) if colour == st else (xc, functools.partial(peer, X))

    def scatter_send(v, which, st, copies):
        for colour in COLOURS:
            q, to = axis_of(colour, st)
            for half, c, delta, slot in copies:
                send(view(which, st, v, colour, rot(q, c), half), RECV[st][which][colour].at[v, slot],
                     rs_s.at[st, v, colour, which], rs_r.at[st, v, colour, which, slot], to(delta), p)

    def scatter_relay(v, which, st):
        for colour in COLOURS:
            q, _ = axis_of(colour, st)
            recv = RECV[st][which][colour]
            for half, c, _, slot in RELAYED:
                wait_recv(recv.at[v, slot - 4], rs_r.at[st, v, colour, which, slot - 4])
                ref = view(which, st, v, colour, rot(q, c), half)
                ref[...] = ref[...] + recv[v, slot - 4]
        scatter_send(v, which, st, RELAYED)

    def scatter_sum(v, which, st):
        for colour in COLOURS:
            q, _ = axis_of(colour, st)
            recv = RECV[st][which][colour]
            for half in HALVES:
                direct, merged = 3 - half, 4 + half
                for slot in (direct, merged):
                    wait_recv(recv.at[v, slot], rs_r.at[st, v, colour, which, slot])
                ref = view(which, st, v, colour, q, half)
                ref[...] = ref[...] + recv[v, direct] + recv[v, merged]

    def scatter_turn(v, which):
        scatter_sum(v, which, 0)
        scatter_send(v, which, 1, MERGED + DIRECT)

    def scatter_out(v):
        scatter_sum(v, OUT, 1)
        for colour in COLOURS:
            go[v, :, OUT_COLS[colour]] = gout[colour][(v, jb, xc) if colour == 0 else (v, xc, jb)]

    def scatter_last(v):
        scatter_sum(v, IN, 1)
        for which in HALVES:
            for colour in COLOURS:
                fin[v, :, which, :, IN_COLS[colour]] = gin[colour][(v, which, jb, xc) if colour == 0 else (v, which, xc, jb)]
        for delta in (OPP, PLUS, MINUS):
            send(fin.at[v, rot(ja, delta)], r3.at[v, delta - 1], r3_s.at[v], r3_r.at[v, delta - 1], peer_a(delta), p)

    def scatter_finish(v):
        def put(j, vals):
            for i in QUARTERS:
                z, y = piece(j, i)
                cols = pl.ds(pl.multiple_of((z * NA + y) * pf, pf), pf)
                gg[v, :, cols] = vals(0)[:, i * pf:(i + 1) * pf]
                gi[v, :, cols] = vals(1)[:, i * pf:(i + 1) * pf]

        put(ja, lambda w: fin[v, ja, w])
        for delta in RING:
            wait_recv(r3.at[v, delta - 1], r3_r.at[v, delta - 1])
            put(rot(ja, -delta), lambda w, delta=delta: r3[v, delta - 1, w])

    def step(fn, *args):
        with jax.named_scope(fn.__name__):
            fn(*args)

    def on(core):
        return pl.when(p == core)

    def take_turn():
        pl.semaphore_wait(turn, 1)

    def give_turn():
        pl.semaphore_signal(turn, inc=1, device_id=(d, 1 - p), device_id_type=MESH)

    h_mid, h_late, e_first, e_last = ((xo.at[i], mc_s.at[1 + i]) for i in QUARTERS)

    def pass_on(part, item, buf, which, vd):
        step(part, item[0], buf, which, vd, item[1])

    AFTER = (MINUS, OPP), (0, PLUS)
    step(direct_send, 0)
    step(small_send, 1, 0)
    step(direct_wait, 0)
    step(small_send, 0, 1)
    step(small_relay, 1, 0)
    step(large_send, 0, (0,), (0,))
    step(small_rest, 1, 0)
    step(small_last, 1, 0)
    step(small_send, 1, 1)
    step(small_relay, 0, 1)
    step(small_relay, 1, 1)
    step(small_rest, 0, 1)
    step(large_send, 0, (PLUS, MINUS), (MINUS, PLUS))
    step(small_last, 0, 1)
    step(large_send, 0, (OPP,), (OPP,))
    step(small_rest, 1, 1)
    step(small_last, 1, 1)
    step(large_relay, 0)

    @on(0)
    def _():
        step(large_send, 1, UP, DOWN)

    step(large_finish, 0, UP_MATS)

    @on(0)
    def _():
        step(large_send, 1, *AFTER)

    @on(1)
    def _():
        step(take_turn)
        step(large_send, 1, UP, DOWN)
        step(spread_own, hb, 0, 0)

    step(block_gates, 0)

    @on(1)
    def _():
        step(large_send, 1, *AFTER)

    step(large_finish, 0, OUT_MAT)
    step(block_out, 0, h_mid[0])
    pass_on(spread_near, h_mid, hb, 0, p)
    step(large_relay, 1)

    @on(0)
    def _():
        step(give_turn)

    @on(1)
    def _():
        pass_on(spread_far, h_mid, hb, 0, p)
        step(spread_same, eb, 1, 1, mc_s.at[0])

    step(spread_own, hb, 0, 1)
    step(large_finish, 1, UP_MATS)
    step(block_gates, 1)
    step(large_finish, 1, OUT_MAT)

    @on(0)
    def _():
        step(block_out, 1, h_late[0])
        pass_on(spread_near, h_late, hb, 0, 1)
        pass_on(spread_far, h_late, hb, 0, 1)
        pass_on(spread_far, h_mid, hb, 0, p)
        step(spread_same, hb, 0, 0, mc_s.at[0])
        step(spread_own, eb, 1, 1)
        step(block_backward, 1, e_first[0])
        pass_on(spread_near, e_first, eb, 1, 0)
        pass_on(spread_far, e_first, eb, 1, 0)
        step(spread_relay, hb, 0, 1)
        step(grad_first, 1, EARLY)

    @on(1)
    def _():
        step(block_backward, 1, e_first[0])
        pass_on(spread_near, e_first, eb, 1, 1)
        pass_on(spread_far, e_first, eb, 1, 1)
        step(spread_relay, hb, 0, 1)
        step(grad_first, 1, EARLY)

    step(spread_relay, eb, 1, 1)

    step(grad_hidden, 1, EARLY)
    step(grad_out, 1, EARLY)
    step(grad_in, 1, EARLY)

    @on(0)
    def _():
        step(spread_relay, hb, 0, 0)
        step(spread_finish, hb, 0, 1)
        step(grad_first, 1, LATE)

    @on(1)
    def _():
        step(spread_own, eb, 1, 0)
        step(block_backward, 0, e_last[0])
        pass_on(spread_near, e_last, eb, 1, 0)
        pass_on(spread_far, e_last, eb, 1, 0)
        step(spread_relay, hb, 0, 0)
        step(spread_finish, hb, 0, 1)
        step(grad_first, 1, LATE)

    step(spread_finish, eb, 1, 1)
    step(grad_hidden, 1, LATE)
    step(grad_out, 1, LATE)
    step(scatter_send, 1, OUT, 0, MERGED)
    step(grad_in, 1, LATE)
    step(scatter_send, 1, IN, 0, MERGED)
    step(scatter_send, 1, OUT, 0, DIRECT)
    step(scatter_send, 1, IN, 0, DIRECT)

    @on(0)
    def _():
        step(grad_first, 0, EARLY)
        step(spread_relay, eb, 1, 0)
        step(spread_finish, hb, 0, 0)
        step(grad_first, 0, LATE)
        step(spread_own, eb, 1, 0)

    @on(1)
    def _():
        step(grad_first, 0, EARLY)
        step(spread_relay, eb, 1, 0)
        step(spread_finish, hb, 0, 0)
        step(grad_first, 0, LATE)

    step(grad_hidden, 0, EARLY)
    step(grad_in, 0, EARLY)

    @on(0)
    def _():
        step(scatter_relay, 1, OUT, 0)

    step(grad_out, 0, EARLY)

    @on(0)
    def _():
        step(scatter_relay, 1, IN, 0)

    @on(1)
    def _():
        step(scatter_relay, 1, OUT, 0)

    step(spread_finish, eb, 1, 0)
    step(grad_hidden, 0, LATE)
    step(grad_in, 0, LATE)
    step(scatter_send, 0, IN, 0, MERGED)
    step(grad_out, 0, LATE)

    @on(1)
    def _():
        step(scatter_relay, 1, IN, 0)

    step(scatter_send, 0, OUT, 0, MERGED)
    step(scatter_send, 0, IN, 0, DIRECT)

    @on(0)
    def _():
        step(block_backward, 0, ga)
        send(ga, ga, ga_s, ga_r, d, 1)

    step(scatter_turn, 1, OUT)
    step(scatter_relay, 0, IN, 0)
    step(scatter_send, 0, OUT, 0, DIRECT)
    step(scatter_turn, 1, IN)
    step(scatter_relay, 0, OUT, 0)
    step(scatter_relay, 1, OUT, 1)

    @on(1)
    def _():
        wait_recv(ga, ga_r)

    gact[...] = ga[...]
    step(scatter_turn, 0, IN)
    step(scatter_relay, 1, IN, 1)
    step(scatter_turn, 0, OUT)
    step(scatter_relay, 0, IN, 1)
    step(scatter_out, 1)
    step(scatter_last, 1)
    step(scatter_relay, 0, OUT, 1)
    step(scatter_last, 0)
    step(scatter_finish, 1)
    step(scatter_out, 0)
    step(scatter_finish, 0)

    for v in BLOCKS:
        for k in MATS:
            three = pl.ds(0, len(RING))
            wait_send(part_at(v, k, three, 0, 0), ag_s.at[v, k, 0])
            wait_send(part_at(v, k, whole, three, 0), ag_s.at[v, k, 1])
            wait_send(part_at(v, k, whole, whole, three), ag_s.at[v, k, LARGE])
        for colour in COLOURS:
            for which in HALVES:
                for st in HALVES:
                    wait_send(RECV[st][which][colour].at[v], rs_s.at[st, v, colour, which])
        wait_send(r3.at[v], r3_s.at[v])
        wait_send(hb.at[v, 0], rl_s.at[0, v])
        wait_send(hb.at[v, 0], rl_s.at[1, v])
    wait_send(hb.at[0, pl.ds(0, 2)], mc_s.at[0])
    wait_send(hb.at[0, pl.ds(0, 3)], mc_s.at[1])
    wait_send(hb.at[0, pl.ds(0, 3)], mc_s.at[3])

    @pl.when(p == 0)
    def _():
        wait_send(hb.at[0, pl.ds(0, 3)], mc_s.at[2])
        wait_send(ga, ga_s)

    @pl.when(p == 1)
    def _():
        wait_send(hb.at[0, pl.ds(0, 3)], mc_s.at[4])


def hand_on(*refs):
    copies = [pltpu.make_async_copy(refs[i], refs[NA + i], refs[-1].at[i]) for i in QUARTERS]
    for copy in copies:
        copy.start()
    for copy in copies:
        copy.wait()


def solution(mesh):
    act_spec = P(None, "data", None, None)
    w_spec = P(None, "stage", "data", None)

    def body(act_in, cot_out, w_gate, w_in, w_out):
        shape = act_in.shape
        dm, fd = shape[3], w_gate.shape[3]
        rows = shape[0] * shape[1] * shape[2]
        dr, fr, fs = dm // NL, fd // NL, fd // NA
        pf = fs // NA
        vmem = pltpu.VMEM
        dma = pltpu.SemaphoreType.DMA
        n2, n3, na = NB, len(RING), NA
        ring = (na, na)
        scratch = [
            vmem((n2, na, *ring, dr, fd), BF), vmem((n2, na, *ring, dr, fd), BF), vmem((n2, na, *ring, fr, dm), BF),
            vmem((n2, na, rows, dm), BF), vmem((n2, na, rows, dm), BF), vmem((na, rows, dm), BF), vmem((rows, dm), BF),
            vmem((n2, na, rows, dm), BF),
            vmem((n2, rows, fd), F32), vmem((n2, rows, fd), F32),
            vmem((n2, na, rows, fs), F32), vmem((n2, na, rows, fs), F32),
            vmem((n2, na, rows, fs), BF),
            vmem((rows, fd), BF), vmem((rows, fd), BF), vmem((rows, fd), BF),
            vmem((na, rows, fs), BF), vmem((na, rows, fs), BF),
            vmem((rows, dm), F32),
            vmem((n2, dm, fs), BF), vmem((n2, dm, fs), BF), vmem((fs, dm), BF),
            *(vmem((n2, n2, *ring, na, dr, width), F32) for width in (fs - pf, pf)),
            *(vmem((n2, *ring, fr, width), F32) for width in (dm - pf, pf)),
            vmem((n2, na, n2, dr, fs), F32), vmem((n2, n3, n2, dr, fs), F32),
            dma((n2, na)), dma((n2, n3, n3)), dma((n2, n3, n2, 6)), dma((n2, n3, n3 * na)), dma((5,)), dma((n2, n2, 7)), dma((n2, n2)), dma, dma,
            dma((n2, n2, n2, n2)), dma((n2, n2, n2, n2, 6)), dma((n2,)), dma((n2, n3)), pltpu.SemaphoreType.REGULAR,
            *(vmem((n2, 6, *lead, width), F32)
              for lead_in, lead_out in (((*ring, dr), (n2, fr)), ((na, dr), (fr // n2,)))
              for lead, width in ((lead_in, fs - pf), (lead_in, pf), (lead_out, dm - pf), (lead_out, pf))),
        ]
        hbm = pl.BlockSpec(memory_space=pl.ANY)
        whole = pl.BlockSpec(memory_space=pltpu.VMEM)
        out = pl.pallas_call(
            kernel,
            out_shape=(
                vmem((rows, dm), BF), vmem((n2, dr, fd), F32), vmem((n2, dr, fd), F32), vmem((n2, fr, dm), F32),
            ),
            in_specs=[hbm] * 5,
            out_specs=(whole,) * NA,
            scratch_shapes=scratch,
            compiler_params=pltpu.CompilerParams(collective_id=0, has_side_effects=True, vmem_limit_bytes=66300000),
            name="train_step",
        )(act_in.reshape(rows, dm), cot_out.reshape(rows, dm), w_gate[:, 0], w_in[:, 0], w_out[:, 0])
        grad_act, grad_gate, grad_lin, grad_proj = pl.pallas_call(
            hand_on, out_shape=tuple(jax.ShapeDtypeStruct(a.shape, a.dtype) for a in out), in_specs=[whole] * NA, out_specs=(hbm,) * NA,
            scratch_shapes=[dma((NA,))], compiler_params=pltpu.CompilerParams(vmem_limit_bytes=2 ** 20), name="hand_on",
        )(*(pltpu.with_memory_space_constraint(a, vmem) for a in out))
        return grad_act.reshape(shape), grad_gate[:, None], grad_lin[:, None], grad_proj[:, None]

    return jax.shard_map(body, mesh=mesh, in_specs=(act_spec, act_spec, w_spec, w_spec, w_spec),
                         out_specs=(act_spec, w_spec, w_spec, w_spec), check_vma=False)
```
